32 devices in a mesh: data: 1 (over z), model: 4 (over y), stage: 8 (over x, core).
Axes of the slice: x: 4, y: 4, z: 1, core: 2. Of those that a mesh axis runs over, the one named last changes fastest.
The devices are a block of a 4x4x8 slice.
Arguments:
- tokens_in: bfloat16 [4, 1024, 512], P(None, 'data')
- targets: bfloat16 [4, 1024, 512], P(None, 'data')
- w_qkv: bfloat16 [8, 1, 512, 8, 3, 64], P('stage', None, None, 'model')
- w_out: bfloat16 [8, 1, 8, 64, 512], P('stage', None, 'model')
- w_up: bfloat16 [8, 1, 512, 2048], P('stage', None, None, 'model')
- w_down: bfloat16 [8, 1, 2048, 512], P('stage', None, 'model')
Outputs:
- output 1: float32 [8, 1, 512, 8, 3, 64], P(('data', 'stage'), None, None, 'model')
- output 2: float32 [8, 1, 8, 64, 512], P(('data', 'stage'), None, 'model')
- output 3: float32 [8, 1, 512, 2048], P(('data', 'stage'), None, None, 'model')
- output 4: float32 [8, 1, 2048, 512], P(('data', 'stage'), None, 'model')
- output 5: float32 [1], P('data')
All inputs are finite; a program needn't handle non-finite values.
Results may differ from the reference program's by a relative error of at most 0.0164868.
Values are sent between devices in bfloat16 or wider.
A program may use at most 768 MiB of HBM per device.

```python
import jax
import jax.numpy as jnp
from jax import lax

STAGES = 8
LAYERS_STAGE = 1
MICRO = 4
TOKENS = 1024
DMODEL = 512
FF = 2048
HEADS = 8
HEAD_DIM = 64

NUM_LAYERS = STAGES * LAYERS_STAGE
SM_SCALE = HEAD_DIM ** -0.5
INV_COUNT = 1.0 / (MICRO * TOKENS * DMODEL)


def setup_inputs(seed: int = 0, part: int = 0) -> dict:
    data_key = jax.random.fold_in(jax.random.key(seed), part)
    key_x, key_t = jax.random.split(data_key)
    w_keys = jax.random.split(jax.random.key(seed + 1), 4)
    branch_gain = NUM_LAYERS ** -0.5
    tokens_in = jax.random.normal(key_x, (MICRO, TOKENS, DMODEL), jnp.float32).astype(jnp.bfloat16)
    targets = jax.random.normal(key_t, (MICRO, TOKENS, DMODEL), jnp.float32).astype(jnp.bfloat16)
    w_qkv = (jax.random.normal(w_keys[0], (STAGES, LAYERS_STAGE, DMODEL, HEADS, 3, HEAD_DIM), jnp.float32) * (1.5 * DMODEL ** -0.5)).astype(jnp.bfloat16)
    w_out = (jax.random.normal(w_keys[1], (STAGES, LAYERS_STAGE, HEADS, HEAD_DIM, DMODEL), jnp.float32) * (branch_gain * (HEADS * HEAD_DIM) ** -0.5)).astype(jnp.bfloat16)
    w_up = (jax.random.normal(w_keys[2], (STAGES, LAYERS_STAGE, DMODEL, FF), jnp.float32) * DMODEL ** -0.5).astype(jnp.bfloat16)
    w_down = (jax.random.normal(w_keys[3], (STAGES, LAYERS_STAGE, FF, DMODEL), jnp.float32) * (1.5 * branch_gain * FF ** -0.5)).astype(jnp.bfloat16)
    return {"tokens_in": tokens_in, "targets": targets, "w_qkv": w_qkv, "w_out": w_out, "w_up": w_up, "w_down": w_down}


def rms_norm(hidden):
    hid32 = hidden.astype(jnp.float32)
    inv_rms = lax.rsqrt(jnp.mean(hid32 * hid32, axis=-1, keepdims=True) + 1e-6)
    return (hid32 * inv_rms).astype(jnp.bfloat16)


def attn_core(queries, keys_in, values):
    scores = jnp.einsum("qhe,khe->hqk", queries.astype(jnp.float32), keys_in.astype(jnp.float32)) * SM_SCALE
    causal = jnp.arange(TOKENS)[:, None] >= jnp.arange(TOKENS)[None, :]
    scores = jnp.where(causal[None], scores, -1e30)
    prob_bf = jax.nn.softmax(scores, axis=-1).astype(jnp.bfloat16)
    return jnp.einsum("hqk,khe->qhe", prob_bf.astype(jnp.float32), values.astype(jnp.float32)).astype(jnp.bfloat16)


def layer_fn(hidden, w_qkv, w_out, w_up, w_down):
    normed = rms_norm(hidden)
    qkv_all = jnp.einsum("bd,dhse->bhse", normed.astype(jnp.float32), w_qkv).astype(jnp.bfloat16)
    attn_out = attn_core(qkv_all[:, :, 0], qkv_all[:, :, 1], qkv_all[:, :, 2])
    branch_a = jnp.einsum("bhe,hed->bd", attn_out.astype(jnp.float32), w_out).astype(jnp.bfloat16)
    h_mid = (hidden.astype(jnp.float32) + branch_a.astype(jnp.float32)).astype(jnp.bfloat16)
    pre_act = jnp.dot(rms_norm(h_mid).astype(jnp.float32), w_up, preferred_element_type=jnp.float32).astype(jnp.bfloat16)
    act_bf = jax.nn.gelu(pre_act.astype(jnp.float32), approximate=True).astype(jnp.bfloat16)
    branch_m = jnp.dot(act_bf.astype(jnp.float32), w_down, preferred_element_type=jnp.float32).astype(jnp.bfloat16)
    return (h_mid.astype(jnp.float32) + branch_m.astype(jnp.float32)).astype(jnp.bfloat16)


def reference(tokens_in, targets, w_qkv, w_out, w_up, w_down):
    w_stack = tuple(weight.astype(jnp.float32).reshape((NUM_LAYERS,) + weight.shape[2:]) for weight in (w_qkv, w_out, w_up, w_down))
    layer_ck = jax.checkpoint(layer_fn)

    def micro_loss(weights, x_mb, t_mb):
        def layer_body(hidden, layer_w):
            return layer_ck(hidden, *layer_w), None
        h_final, _ = lax.scan(layer_body, x_mb, weights)
        err_vec = h_final.astype(jnp.float32) - t_mb.astype(jnp.float32)
        return 0.5 * jnp.sum(err_vec * err_vec) * INV_COUNT

    def micro_step(loop_carry, xs_pair):
        loss_acc, grad_acc = loop_carry
        loss_mb, pull_back = jax.vjp(lambda weights: micro_loss(weights, xs_pair[0], xs_pair[1]), w_stack)
        grad_mb = pull_back(jnp.ones((), jnp.float32))[0]
        grad_acc = tuple(acc_g + new_g for acc_g, new_g in zip(grad_acc, grad_mb))
        return (loss_acc + loss_mb, grad_acc), None

    init_carry = (jnp.zeros((), jnp.float32), tuple(jnp.zeros_like(weight) for weight in w_stack))
    (loss_sum, grad_sum), _ = lax.scan(micro_step, init_carry, (tokens_in, targets))
    grad_list = tuple(grad_arr.reshape((STAGES, LAYERS_STAGE) + grad_arr.shape[1:]) for grad_arr in grad_sum)
    return (grad_list[0], grad_list[1], grad_list[2], grad_list[3], loss_sum.reshape(1))
```

```python
import functools
import math

import jax
import jax.numpy as jnp
from jax import lax
from jax.experimental import pallas as pl
from jax.experimental.pallas import tpu as pltpu
from jax.sharding import PartitionSpec as P

F32 = jnp.float32
BF16 = jnp.bfloat16
MESH = pl.DeviceIdType.MESH
CHUNK = 256
NEG = -1e30
GELU_C = math.sqrt(2.0 / math.pi)
GELU_A = 0.044715

W_QT, W_OT, W_UT, W_DT, W_D, W_U, W_O, W_Q = range(8)


def dot(lhs, rhs):
    return jnp.dot(lhs, rhs, preferred_element_type=F32)


def dot_t(lhs, rhs):
    return lax.dot_general(lhs, rhs, (((1,), (1,)), ((), ())), preferred_element_type=F32)


def inv_rms(x32):
    return lax.rsqrt(jnp.mean(x32 * x32, axis=0, keepdims=True) + 1e-6)


def norm_pull(x32, inv, g32):
    mean_gx = jnp.mean(g32 * x32, axis=0, keepdims=True)
    return g32 * inv - x32 * (inv * inv * inv * mean_gx)


def gelu(u):
    inner = jnp.tanh(GELU_C * (u + GELU_A * (u * u * u)))
    return u * (0.5 * (1.0 + inner))


def gelu_grad(u):
    u2 = u * u
    inner = jnp.tanh(GELU_C * (u + GELU_A * (u2 * u)))
    cdf = 0.5 * (1.0 + inner)
    return cdf + u * (0.5 * GELU_C) * (1.0 - inner * inner) * (1.0 + (3.0 * GELU_A) * u2)


def step_kernel(cfg, x_hbm, t_hbm, wqT_in, woT_in, wuT_in, wdT_in, wd_in, wu_in, wo_in, wq_in,
                gq_out, go_out, gu_out, gd_out, loss_out, rq, ro, ru, rd,
                wqT, woT, wuT, wdT, wd, wu, wo, wq,
                xin, hbuf, n1buf, qkv, qkvn, obuf, mbuf, n2buf, ubuf, zbuf, pbuf, dybuf, dvacc, dkacc, sscr,
                ybuf, dobuf, losst, lossv, stage_buf, go_buf, radd,
                ag_send, ag_recv, ag_loc, xsem, fsend, frecv, bsend, brecv, lsend, lrecv, lfsend, lfrecv,
                rs_send, rs_recv, ld_sem, out_sem):
    ns, nm, nc, tc, dm_, hl, hd, fl = cfg
    heads = nm * hl
    qrows = hl * 3 * hd
    orows = hl * hd
    inv_d = 1.0 / (nm * nc * tc * dm_)
    scale = hd ** -0.5
    exp_c = scale * math.log2(math.e)
    me = lax.axis_index("model")
    st = lax.axis_index("stage")
    nxt = lax.rem(st + 1, ns)
    prv = lax.rem(st + ns - 1, ns)
    first = st == 0
    last = st == ns - 1

    def peer(k):
        return lax.rem(me + k, nm)

    bar = pltpu.get_barrier_semaphore()
    pl.semaphore_signal(bar, inc=1, device_id={"stage": nxt}, device_id_type=MESH)
    pl.semaphore_signal(bar, inc=1, device_id={"stage": prv}, device_id_type=MESH)
    for k in range(1, nm):
        pl.semaphore_signal(bar, inc=1, device_id={"model": peer(k)}, device_id_type=MESH)
    pl.semaphore_wait(bar, 2 + nm - 1)

    def rowsl(start, size, mult):
        return pl.ds(pl.multiple_of(start, mult), size)

    w_src = (wqT_in, woT_in, wuT_in, wdT_in, wd_in, wu_in, wo_in, wq_in)

    def w_dst(idx, who):
        if idx == W_QT:
            return wqT.at[rowsl(who * qrows, qrows, qrows), :]
        if idx == W_OT:
            return woT.at[:, rowsl(who * orows, orows, orows)]
        if idx == W_UT:
            return wuT.at[rowsl(who * fl, fl, fl), :]
        if idx == W_DT:
            return wdT.at[who]
        if idx == W_D:
            return wd.at[rowsl(who * fl, fl, fl), :]
        if idx == W_U:
            return wu.at[who]
        if idx == W_O:
            return wo.at[rowsl(who * orows, orows, orows), :]
        return wq.at[:, rowsl(who * qrows, qrows, qrows)]

    def w_send(idx, k):
        return pltpu.make_async_remote_copy(
            src_ref=w_src[idx], dst_ref=w_dst(idx, me), send_sem=ag_send.at[idx, k - 1],
            recv_sem=ag_recv.at[idx, k - 1], device_id={"model": peer(k)}, device_id_type=MESH)

    def w_recv(idx, k):
        return pltpu.make_async_remote_copy(
            src_ref=w_src[idx], dst_ref=w_dst(idx, peer(nm - k)), send_sem=ag_send.at[idx, k - 1],
            recv_sem=ag_recv.at[idx, k - 1], device_id={"model": peer(k)}, device_id_type=MESH)

    def w_local(idx):
        return pltpu.make_async_copy(w_src[idx], w_dst(idx, me), ag_loc.at[idx])

    def x_copy(c):
        return pltpu.make_async_copy(x_hbm.at[me, pl.ds(c * tc, tc), :], xin.at[c], xsem.at[c])

    def t_copy(c):
        return pltpu.make_async_copy(t_hbm.at[me, pl.ds(c * tc, tc), :], xin.at[c], xsem.at[c])

    @pl.when(first)
    def _():
        for c in range(nc):
            x_copy(c).start()

    @pl.when(last)
    def _():
        for c in range(nc):
            t_copy(c).start()

    for idx in range(8):
        w_local(idx).start()
        for k in range(1, nm):
            w_send(idx, k).start()

    def w_wait(idx):
        w_local(idx).wait()
        for k in range(1, nm):
            w_recv(idx, k).wait_recv()

    def f_copy(c):
        return pltpu.make_async_remote_copy(
            src_ref=ybuf.at[c], dst_ref=hbuf.at[c], send_sem=fsend.at[c], recv_sem=frecv.at[c],
            device_id={"stage": nxt}, device_id_type=MESH)

    def b_copy(c):
        return pltpu.make_async_remote_copy(
            src_ref=ybuf.at[c], dst_ref=dybuf.at[c], send_sem=bsend.at[c], recv_sem=brecv.at[c],
            device_id={"stage": prv}, device_id_type=MESH)

    lossv[...] = jnp.zeros_like(lossv)

    def head_rows(p, h, part):
        return pl.ds(pl.multiple_of(p * (2 * 3 * hd) + (h * 3 + part) * hd, hd), hd)

    k_lane = (0, 2 * 2 * hd)
    v_lane = (2 * hd, 2 * 2 * hd)
    two = 2 * hd

    def pad_k(val, h):
        zero = jnp.zeros_like(val)
        return jnp.concatenate([zero, val] if h == 0 else [val, zero], axis=0)

    def pad_v(val, h):
        zero = jnp.zeros_like(val)
        return jnp.concatenate([val, zero] if h == 0 else [zero, val], axis=0)

    def causal(shape):
        return lax.broadcasted_iota(jnp.int32, shape, 0) <= lax.broadcasted_iota(jnp.int32, shape, 1)

    @pl.loop(0, nc)
    def _(c):
        @pl.when(first)
        def _():
            x_copy(c).wait()
            hbuf[c] = jnp.transpose(xin[c])

        @pl.when(jnp.logical_not(first))
        def _():
            f_copy(c).wait_recv()

        @pl.when(c == 0)
        def _():
            w_wait(W_QT)

        h32 = hbuf[c].astype(F32)
        n1 = (h32 * inv_rms(h32)).astype(BF16)
        n1buf[c] = n1
        for r in range(nm):
            rows = pl.ds(r * qrows, qrows)
            blk = dot(wqT[rows, :], n1).astype(BF16)
            qkv[c, rows, :] = blk
            qkvn[r, pl.ds(pl.multiple_of(c * tc, tc), tc), :] = jnp.transpose(blk)

        for cc in range(nc):
            @pl.when(c == cc)
            def _():
                @pl.loop(0, heads // 2)
                def _(p):
                    for h in range(2):
                        q_t = qkv[cc, head_rows(p, h, 0), :]
                        qz = pad_k(q_t, h)
                        mx = None
                        for j in range(cc + 1):
                            s = dot(qkvn[p, pl.ds(j * tc, tc), pl.ds(k_lane[h], two)], qz)
                            if j == cc:
                                s = jnp.where(causal(s.shape), s, NEG)
                            sscr[pl.ds(j * tc, tc), :] = s
                            bm = jnp.max(s, axis=0, keepdims=True)
                            mx = bm if mx is None else jnp.maximum(mx, bm)
                        den = None
                        for j in range(cc + 1):
                            e = jnp.exp2((sscr[pl.ds(j * tc, tc), :] - mx) * exp_c)
                            sscr[pl.ds(j * tc, tc), :] = e
                            es = jnp.sum(e, axis=0, keepdims=True)
                            den = es if den is None else den + es
                        inv = 1.0 / den
                        o_t = None
                        for j in range(cc + 1):
                            pr = (sscr[pl.ds(j * tc, tc), :] * inv).astype(BF16)
                            pbuf[cc * (cc + 1) // 2 + j, p * 2 + h] = pr
                            part = dot(qkv[j, head_rows(p, h, 2), :], pr)
                            o_t = part if o_t is None else o_t + part
                        obuf[cc, pl.ds(pl.multiple_of((p * 2 + h) * hd, hd), hd), :] = o_t.astype(BF16)

        @pl.when(c == 0)
        def _():
            w_wait(W_OT)

        a = dot(woT[...], obuf[c]).astype(BF16)
        m32 = (hbuf[c].astype(F32) + a.astype(F32)).astype(BF16).astype(F32)
        mbuf[c] = m32.astype(BF16)
        n2 = (m32 * inv_rms(m32)).astype(BF16)
        n2buf[c] = n2

        @pl.when(c == 0)
        def _():
            w_wait(W_UT)
            w_wait(W_DT)

        acc = None
        for f in range(nm):
            rows = pl.ds(f * fl, fl)
            u = dot(wuT[rows, :], n2buf[c]).astype(BF16)
            ubuf[c, rows, :] = u
            z = gelu(u.astype(F32)).astype(BF16)
            zbuf[c, rows, :] = z
            part = dot(wdT[f], z)
            acc = part if acc is None else acc + part
        y32 = (mbuf[c].astype(F32) + acc.astype(BF16).astype(F32)).astype(BF16)
        ybuf[c] = y32

        @pl.when(jnp.logical_not(last))
        def _():
            f_copy(c).start()

        @pl.when(last)
        def _():
            t_copy(c).wait()
            err = ybuf[c].astype(F32) - jnp.transpose(xin[c]).astype(F32)
            lossv[...] += jnp.sum((err * err).reshape(dm_ // 8, 8, tc), axis=0)
            dybuf[c] = (err * inv_d).astype(BF16)

    def l_copy(k):
        return pltpu.make_async_remote_copy(
            src_ref=losst.at[nm], dst_ref=losst.at[3 - k if nm == 4 else nm - 1 - k], send_sem=lsend.at[k - 1],
            recv_sem=lrecv.at[k - 1], device_id={"model": peer(k)}, device_id_type=MESH)

    def lf_copy():
        return pltpu.make_async_remote_copy(
            src_ref=losst.at[nm + 1], dst_ref=losst.at[nm + 1], send_sem=lfsend, recv_sem=lfrecv,
            device_id={"stage": prv}, device_id_type=MESH)

    @pl.when(last)
    def _():
        tot = jnp.sum(lossv[...]) * (0.5 * inv_d)
        losst[nm] = jnp.full(losst.shape[1:], tot, F32)
        for k in range(1, nm):
            l_copy(k).start()

    @pl.loop(0, nc)
    def _(i):
        c = nc - 1 - i

        @pl.when(jnp.logical_not(last))
        def _():
            b_copy(c).wait_recv()

        @pl.when(i == 0)
        def _():
            w_wait(W_D)
            w_wait(W_U)
            w_wait(W_O)
            w_wait(W_Q)

        acc = None
        for f in range(nm):
            rows = pl.ds(f * fl, fl)
            dz = dot(wd[rows, :], dybuf[c]).astype(BF16).astype(F32)
            du = (dz * gelu_grad(ubuf[c, rows, :].astype(F32))).astype(BF16)
            ubuf[c, rows, :] = du
            part = dot(wu[f], du)
            acc = part if acc is None else acc + part
        dn2 = acc.astype(BF16).astype(F32)
        m32 = mbuf[c].astype(F32)
        pull = norm_pull(m32, inv_rms(m32), dn2).astype(BF16)
        dmid = (dybuf[c].astype(F32) + pull.astype(F32)).astype(BF16)
        mbuf[c] = dmid
        dobuf[...] = dot(wo[...], dmid).astype(BF16)

        for cc in range(nc):
            @pl.when(c == cc)
            def _():
                @pl.loop(0, heads // 2)
                def _(p):
                    dq = [None, None]
                    qz = []
                    dz_v = []
                    dsum = []
                    for h in range(2):
                        orow = pl.ds(pl.multiple_of((p * 2 + h) * hd, hd), hd)
                        do_t = dobuf[orow, :]
                        dsum.append(jnp.sum(do_t.astype(F32) * obuf[cc, orow, :].astype(F32), axis=0, keepdims=True))
                        dz_v.append(pad_v(do_t, h))
                        qz.append(pad_v(qkv[cc, head_rows(p, h, 0), :], h))
                    for j in range(cc + 1):
                        dv_new = None
                        dk_new = None
                        for h in range(2):
                            pr = pbuf[cc * (cc + 1) // 2 + j, p * 2 + h]
                            dp = dot(qkvn[p, pl.ds(j * tc, tc), pl.ds(v_lane[h], two)], dz_v[h]).astype(BF16).astype(F32)
                            ds = (pr.astype(F32) * (dp - dsum[h])).astype(BF16)
                            dv_h = dot_t(pr, dz_v[h])
                            dk_h = dot_t(ds, qz[h])
                            dv_new = dv_h if dv_new is None else dv_new + dv_h
                            dk_new = dk_h if dk_new is None else dk_new + dk_h
                            dq_h = dot(qkv[j, head_rows(p, h, 1), :], ds)
                            dq[h] = dq_h if dq[h] is None else dq[h] + dq_h
                        rows = pl.ds(j * tc, tc)
                        if cc < nc - 1:
                            dv_new = dv_new + dvacc[p, rows, :]
                            dk_new = dk_new + dkacc[p, rows, :]
                        if j < cc:
                            dvacc[p, rows, :] = dv_new
                            dkacc[p, rows, :] = dk_new
                        else:
                            dv_t = jnp.transpose(dv_new).astype(BF16)
                            dk_t = (jnp.transpose(dk_new) * scale).astype(BF16)
                            for h in range(2):
                                qkv[cc, head_rows(p, h, 0), :] = (dq[h] * scale).astype(BF16)
                                qkv[cc, head_rows(p, h, 1), :] = dk_t[h * hd:(h + 1) * hd, :]
                                qkv[cc, head_rows(p, h, 2), :] = dv_t[h * hd:(h + 1) * hd, :]

        dn1 = dot(wq[...], qkv[c]).astype(BF16).astype(F32)
        h32 = hbuf[c].astype(F32)
        pull1 = norm_pull(h32, inv_rms(h32), dn1).astype(BF16)

        @pl.when(jnp.logical_not(last))
        def _():
            f_copy(c).wait_send()

        ybuf[c] = (mbuf[c].astype(F32) + pull1.astype(F32)).astype(BF16)

        @pl.when(jnp.logical_not(first))
        def _():
            b_copy(c).start()

    @pl.when(last)
    def _():
        for k in range(1, nm):
            l_copy(k).wait_recv()
        vals = [losst[nm]] + [losst[k - 1] for k in range(1, nm)]
        tot = jnp.zeros_like(vals[0])
        for who in range(nm):
            pick = vals[0]
            for k in range(1, nm):
                pick = jnp.where(peer(k) == who, vals[k], pick)
            tot = tot + pick
        losst[nm + 1] = tot

    @pl.when(jnp.logical_not(last))
    def _():
        lf_copy().wait_recv()

    @pl.when(jnp.logical_not(first))
    def _():
        lf_copy().start()

    loss_out[...] = losst[nm + 1]

    def wgrad(mat, d):
        acc = None
        for c in range(nc):
            if mat == 0:
                part = dot_t(qkv[c, rowsl(d * qrows, qrows, qrows), :], n1buf[c])
            elif mat == 1:
                part = dot_t(obuf[c, rowsl(d * orows, orows, orows), :], mbuf[c])
            elif mat == 2:
                part = dot_t(n2buf[c], ubuf[c, rowsl(d * fl, fl, fl), :])
            else:
                part = dot_t(zbuf[c, rowsl(d * fl, fl, fl), :], dybuf[c])
            acc = part if acc is None else acc + part
        return acc

    sizes = (qrows, orows, dm_, fl)
    offs = (0, qrows, qrows + orows, qrows + orows + dm_)

    def rows_of(mat):
        return pl.ds(offs[mat], sizes[mat])

    recv_bufs = (rq, ro, ru, rd)
    outs = (gq_out, go_out, gu_out, gd_out)
    order = [2, 1, 3][: nm - 1] if nm == 4 else list(range(1, nm))

    def rs_copy(mat, k):
        return pltpu.make_async_remote_copy(
            src_ref=stage_buf.at[order.index(k), rows_of(mat)],
            dst_ref=recv_bufs[mat].at[nm - 1 - k], send_sem=rs_send.at[mat, k - 1],
            recv_sem=rs_recv.at[mat, nm - 1 - k], device_id={"model": peer(k)}, device_id_type=MESH)

    def rs_recv_copy(mat, slot):
        return pltpu.make_async_remote_copy(
            src_ref=stage_buf.at[0, rows_of(mat)],
            dst_ref=recv_bufs[mat].at[slot], send_sem=rs_send.at[mat, 0],
            recv_sem=rs_recv.at[mat, slot], device_id={"model": peer(1)}, device_id_type=MESH)

    mats = (3, 2, 0, 1)
    for k in order:
        for mat in mats:
            stage_buf[order.index(k), rows_of(mat)] = wgrad(mat, peer(k))
            rs_copy(mat, k).start()

    for mat in mats:
        go_buf[rows_of(mat)] = wgrad(mat, me)

    def load(mat, slot, r0, nr):
        return pltpu.make_async_copy(recv_bufs[mat].at[slot, pl.ds(r0, nr)], radd.at[pl.ds(0, nr)], ld_sem.at[0])

    def out_copy(mat):
        return pltpu.make_async_copy(go_buf.at[rows_of(mat)], outs[mat], out_sem.at[mat])

    slot_order = [nm - 1 - k for k in order]
    for pos, slot in enumerate(slot_order):
        for mat in mats:
            rs_recv_copy(mat, slot).wait_recv()
            for r0 in range(0, sizes[mat], 256):
                nr = min(256, sizes[mat] - r0)
                load(mat, slot, r0, nr).start()
                load(mat, slot, r0, nr).wait()
                go_buf[pl.ds(offs[mat] + r0, nr)] += radd[pl.ds(0, nr)]
            if pos == nm - 2:
                out_copy(mat).start()

    for mat in mats:
        out_copy(mat).wait()
    for idx in range(8):
        for k in range(1, nm):
            w_send(idx, k).wait_send()
    for k in order:
        for mat in mats:
            rs_copy(mat, k).wait_send()

    @pl.when(jnp.logical_not(first))
    def _():
        for c in range(nc):
            b_copy(c).wait_send()
        lf_copy().wait_send()

    @pl.when(last)
    def _():
        for k in range(1, nm):
            l_copy(k).wait_send()


def solution(mesh):
    ns = mesh.shape["stage"]
    nm = mesh.shape["model"]

    def per_device(tokens_in, targets, w_qkv, w_out, w_up, w_down):
        n_micro, seq_len, d_model = tokens_in.shape
        hl, hd, fl = w_qkv.shape[3], w_qkv.shape[5], w_up.shape[3]
        tc = min(CHUNK, seq_len // 2)
        nc = seq_len // tc
        assert n_micro == nm and w_qkv.shape[1] == 1 and hl == 2
        qrows, orows = hl * 3 * hd, hl * hd
        wqT = jnp.transpose(w_qkv[0, 0], (1, 2, 3, 0)).reshape(qrows, d_model)
        wq = jnp.transpose(wqT)
        wo = w_out[0, 0].reshape(orows, d_model)
        wu, wd = w_up[0, 0], w_down[0, 0]
        cfg = (ns, nm, nc, tc, d_model, hl, hd, fl)
        heads = nm * hl
        any_spec = pl.BlockSpec(memory_space=pl.ANY)
        rsum = qrows + orows + d_model + fl
        f32 = lambda *shape: jax.ShapeDtypeStruct(shape, F32)
        out_shape = (f32(qrows, d_model), f32(orows, d_model), f32(d_model, fl), f32(fl, d_model), f32(8, 128),
                     f32(nm - 1, qrows, d_model), f32(nm - 1, orows, d_model), f32(nm - 1, d_model, fl), f32(nm - 1, fl, d_model))
        vb = lambda *shape: pltpu.VMEM(shape, BF16)
        vf = lambda *shape: pltpu.VMEM(shape, F32)
        dma = lambda *shape: pltpu.SemaphoreType.DMA(shape)
        seqb = nc * tc
        scratch = [
            vb(nm * qrows, d_model), vb(d_model, nm * orows), vb(nm * fl, d_model), vb(nm, d_model, fl),
            vb(nm * fl, d_model), vb(nm, d_model, fl), vb(nm * orows, d_model), vb(d_model, nm * qrows),
            vb(nc, tc, d_model), vb(nc, d_model, tc), vb(nc, d_model, tc), vb(nc, nm * qrows, tc), vb(nm, seqb, qrows),
            vb(nc, nm * orows, tc), vb(nc, d_model, tc), vb(nc, d_model, tc), vb(nc, nm * fl, tc), vb(nc, nm * fl, tc),
            vb(nc * (nc + 1) // 2, heads, tc, tc), vb(nc, d_model, tc), vf(heads // 2, seqb, 2 * hd), vf(heads // 2, seqb, 2 * hd),
            vf(seqb, tc), vb(nc, d_model, tc), vb(nm * orows, tc), vf(nm + 2, 8, 128), vf(8, tc),
            vf(nm - 1, rsum, d_model), vf(rsum, d_model), vf(256, d_model),
            dma(8, nm - 1), dma(8, nm - 1), dma(8), dma(nc), dma(nc), dma(nc), dma(nc), dma(nc),
            dma(nm - 1), dma(nm - 1), pltpu.SemaphoreType.DMA, pltpu.SemaphoreType.DMA,
            dma(4, nm - 1), dma(4, nm - 1), dma(1), dma(4),
        ]
        res = pl.pallas_call(
            functools.partial(step_kernel, cfg),
            out_shape=out_shape,
            in_specs=[any_spec] * 10,
            out_specs=[any_spec] * 4 + [pl.BlockSpec(memory_space=pltpu.VMEM)] + [any_spec] * 4,
            scratch_shapes=scratch,
            compiler_params=pltpu.CompilerParams(collective_id=0, has_side_effects=True, vmem_limit_bytes=67043328),
            name="train_step",
        )(tokens_in, targets, wqT, jnp.transpose(wo), jnp.transpose(wu), jnp.transpose(wd), wd, wu, wo, wq)
        g_qkv = jnp.transpose(res[0].reshape(hl, 3, hd, d_model), (3, 0, 1, 2))[None, None]
        g_out = res[1].reshape(1, 1, hl, hd, d_model)
        return g_qkv, g_out, res[2][None, None], res[3][None, None], res[4][0, :1]

    tok_spec = P(None, "data", None)
    qkv_spec = P("stage", None, None, "model", None, None)
    out_spec = P("stage", None, "model", None, None)
    up_spec = P("stage", None, None, "model")
    down_spec = P("stage", None, "model", None)
    g_qkv_spec = P(("data", "stage"), None, None, "model", None, None)
    g_out_spec = P(("data", "stage"), None, "model", None, None)
    g_up_spec = P(("data", "stage"), None, None, "model")
    g_down_spec = P(("data", "stage"), None, "model", None)
    return jax.shard_map(per_device, mesh=mesh, in_specs=(tok_spec, tok_spec, qkv_spec, out_spec, up_spec, down_spec), out_specs=(g_qkv_spec, g_out_spec, g_up_spec, g_down_spec, P("data")), check_vma=False)
```

```python
import functools
import math

import jax
import jax.numpy as jnp
from jax import lax
from jax.experimental import pallas as pl
from jax.experimental.pallas import tpu as pltpu
from jax.sharding import PartitionSpec as P

F32 = jnp.float32
BF16 = jnp.bfloat16
MESH = pl.DeviceIdType.MESH
CHUNK = 256
NEG = -1e30
GELU_C = math.sqrt(2.0 / math.pi)
GELU_A = 0.044715

W_Q, W_O, W_U, W_D = range(4)


def dot(lhs, rhs):
    return jnp.dot(lhs, rhs, preferred_element_type=F32)


def dot_t(lhs, rhs):
    return lax.dot_general(lhs, rhs, (((1,), (1,)), ((), ())), preferred_element_type=F32)


def inv_rms(x32):
    return lax.rsqrt(jnp.mean(x32 * x32, axis=0, keepdims=True) + 1e-6)


def norm_pull(x32, inv, g32):
    mean_gx = jnp.mean(g32 * x32, axis=0, keepdims=True)
    return g32 * inv - x32 * (inv * inv * inv * mean_gx)


def gelu(u):
    inner = jnp.tanh(GELU_C * (u + GELU_A * (u * u * u)))
    return u * (0.5 * (1.0 + inner))


def gelu_grad(u):
    u2 = u * u
    inner = jnp.tanh(GELU_C * (u + GELU_A * (u2 * u)))
    cdf = 0.5 * (1.0 + inner)
    return cdf + u * (0.5 * GELU_C) * (1.0 - inner * inner) * (1.0 + (3.0 * GELU_A) * u2)


def step_kernel(cfg, x_hbm, t_hbm, wqT_in, wo_in, wu_in, wd_in,
                gq_out, go_out, gu_out, gd_out, loss_out, far_p, far_m, near_p, near_m,
                wqT, woT, wuT, wdT, wd, wu, wo, wq,
                xin, hbuf, n1buf, qkv, qkvn, obuf, mbuf, n2buf, ubuf, zbuf, pbuf, dybuf, dvacc, dkacc, sscr,
                ybuf, dobuf, losst, lossv, stage_buf, radd,
                ag_send, ag_recv, ag_loc, go_sem, xsem, fsend, frecv, bsend, brecv, lsend, lrecv, lfsend, lfrecv,
                rs_send, rs_recv, ld_sem, out_sem):
    ns, nm, nc, tc, dm_, hl, hd, fl = cfg
    heads = nm * hl
    qrows = hl * 3 * hd
    orows = hl * hd
    inv_d = 1.0 / (nm * nc * tc * dm_)
    scale = hd ** -0.5
    exp_c = scale * math.log2(math.e)
    me = lax.axis_index("model")
    st = lax.axis_index("stage")
    nxt = lax.rem(st + 1, ns)
    prv = lax.rem(st + ns - 1, ns)
    first = st == 0
    last = st == ns - 1

    def peer(k):
        return lax.rem(me + k, nm)

    bar = pltpu.get_barrier_semaphore()
    pl.semaphore_signal(bar, inc=1, device_id={"stage": nxt}, device_id_type=MESH)
    pl.semaphore_signal(bar, inc=1, device_id={"stage": prv}, device_id_type=MESH)
    for k in range(1, nm):
        pl.semaphore_signal(bar, inc=1, device_id={"model": peer(k)}, device_id_type=MESH)
    pl.semaphore_wait(bar, 2 + nm - 1)

    def rowsl(start, size, mult):
        return pl.ds(pl.multiple_of(start, mult), size)

    plus, minus, far = 1, nm - 1, 2

    def w_rows(idx, who, half=None):
        size = (qrows, orows, fl, fl)[idx]
        if idx in (W_Q, W_U):
            buf = wqT if idx == W_Q else wuT
            if half is None:
                return buf.at[rowsl(who * size, size, size), :]
            return buf.at[rowsl(who * size + half * (size // 2), size // 2, size // 2), :]
        view = woT.at[:, rowsl(who * size, size, size)] if idx == W_O else wdT.at[who]
        return view if half is None else view.at[pl.ds(half * (dm_ // 2), dm_ // 2), :]

    def w_copy(idx, way):
        to = plus if way in (0, 2) else minus
        if way < 2:
            src = wqT_in if idx == W_Q else w_rows(idx, me)
            dst = w_rows(idx, me)
        else:
            src = dst = w_rows(idx, peer(minus if way == 2 else plus), way - 2)
        return pltpu.make_async_remote_copy(
            src_ref=src, dst_ref=dst, send_sem=ag_send.at[idx, way], recv_sem=ag_recv.at[idx, way],
            device_id={"model": peer(to)}, device_id_type=MESH)

    def w_arrival(idx, way):
        who = peer((minus, plus, far, far)[way])
        ref = w_rows(idx, who) if way < 2 else w_rows(idx, who, way - 2)
        return pltpu.make_async_remote_copy(
            src_ref=ref, dst_ref=ref, send_sem=ag_send.at[idx, way], recv_sem=ag_recv.at[idx, way],
            device_id={"model": peer(plus)}, device_id_type=MESH)

    def w_local(idx):
        src = (wqT_in, wo_in, wu_in, wd_in)[idx]
        dst = (w_rows(W_Q, me), wo.at[rowsl(me * orows, orows, orows), :], wu.at[me], wd.at[rowsl(me * fl, fl, fl), :])[idx]
        return pltpu.make_async_copy(src, dst, ag_loc.at[idx])

    def w_own(idx):
        for way in range(2):
            w_copy(idx, way).start()

    def w_forward(idx):
        for way in range(2):
            w_arrival(idx, way).wait_recv()
        for way in range(2, 4):
            w_copy(idx, way).start()

    def w_wait(idx):
        for way in range(2, 4):
            w_arrival(idx, way).wait_recv()

    def x_copy(c):
        return pltpu.make_async_copy(x_hbm.at[me, pl.ds(c * tc, tc), :], xin.at[c], xsem.at[c])

    def t_copy(c):
        return pltpu.make_async_copy(t_hbm.at[me, pl.ds(c * tc, tc), :], xin.at[c], xsem.at[c])

    @pl.when(first)
    def _():
        for c in range(nc):
            x_copy(c).start()

    @pl.when(last)
    def _():
        for c in range(nc):
            t_copy(c).start()

    for idx in range(4):
        w_local(idx).start()

    odd = lax.rem(st, 2) == 1
    early = st < 2

    @pl.when(odd)
    def _():
        pl.semaphore_wait(go_sem, 1)

    w_own(W_Q)
    w_local(W_O).wait()
    woT[:, rowsl(me * orows, orows, orows)] = jnp.transpose(wo[rowsl(me * orows, orows, orows), :])
    w_own(W_O)
    w_local(W_U).wait()
    wuT[rowsl(me * fl, fl, fl), :] = jnp.transpose(wu[me])
    w_local(W_Q).wait()
    w_forward(W_Q)
    w_own(W_U)
    w_local(W_D).wait()
    wdT[me] = jnp.transpose(wd[rowsl(me * fl, fl, fl), :])
    w_forward(W_O)
    w_own(W_D)

    def pass_go():
        @pl.when(jnp.logical_not(odd))
        def _():
            pl.semaphore_signal(go_sem, inc=1, device_id={"stage": nxt}, device_id_type=MESH)

    def natural_weights():
        @pl.loop(0, nm)
        def _(f):
            wu[f] = jnp.transpose(wuT[rowsl(f * fl, fl, fl), :])
            wd[rowsl(f * fl, fl, fl), :] = jnp.transpose(wdT[f])
            wo[rowsl(f * orows, orows, orows), :] = jnp.transpose(woT[:, rowsl(f * orows, orows, orows)])
            wq[:, rowsl(f * qrows, qrows, qrows)] = jnp.transpose(wqT[rowsl(f * qrows, qrows, qrows), :])

    late = st >= max(2, ns // 2)

    @pl.when(jnp.logical_not(early))
    def _():
        w_forward(W_U)
        w_forward(W_D)
        pass_go()
        for idx in range(4):
            w_wait(idx)

    @pl.when(late)
    def _():
        natural_weights()

    def f_copy(c):
        return pltpu.make_async_remote_copy(
            src_ref=ybuf.at[c], dst_ref=hbuf.at[c], send_sem=fsend.at[c], recv_sem=frecv.at[c],
            device_id={"stage": nxt}, device_id_type=MESH)

    def b_copy(c):
        return pltpu.make_async_remote_copy(
            src_ref=ybuf.at[c], dst_ref=dybuf.at[c], send_sem=bsend.at[c], recv_sem=brecv.at[c],
            device_id={"stage": prv}, device_id_type=MESH)

    lossv[...] = jnp.zeros_like(lossv)

    def head_rows(p, h, part):
        return pl.ds(pl.multiple_of(p * (2 * 3 * hd) + (h * 3 + part) * hd, hd), hd)

    k_lane = (0, 2 * 2 * hd)
    v_lane = (2 * hd, 2 * 2 * hd)
    two = 2 * hd

    def pad_k(val, h):
        zero = jnp.zeros_like(val)
        return jnp.concatenate([zero, val] if h == 0 else [val, zero], axis=0)

    def pad_v(val, h):
        zero = jnp.zeros_like(val)
        return jnp.concatenate([val, zero] if h == 0 else [zero, val], axis=0)

    def causal(shape):
        return lax.broadcasted_iota(jnp.int32, shape, 0) <= lax.broadcasted_iota(jnp.int32, shape, 1)

    def attention_step(c):
        @pl.when(first)
        def _():
            x_copy(c).wait()
            hbuf[c] = jnp.transpose(xin[c])

        @pl.when(jnp.logical_not(first))
        def _():
            f_copy(c).wait_recv()

        @pl.when(early & (c == 0))
        def _():
            w_wait(W_Q)

        h32 = hbuf[c].astype(F32)
        n1 = (h32 * inv_rms(h32)).astype(BF16)
        n1buf[c] = n1
        for r in range(nm):
            rows = pl.ds(r * qrows, qrows)
            blk = dot(wqT[rows, :], n1).astype(BF16)
            qkv[c, rows, :] = blk
            qkvn[r, pl.ds(pl.multiple_of(c * tc, tc), tc), :] = jnp.transpose(blk)

        for cc in range(nc):
            @pl.when(c == cc)
            def _():
                @pl.loop(0, heads // 2)
                def _(p):
                    for h in range(2):
                        q_t = qkv[cc, head_rows(p, h, 0), :]
                        qz = pad_k(q_t, h)
                        mx = None
                        for j in range(cc + 1):
                            s = dot(qkvn[p, pl.ds(j * tc, tc), pl.ds(k_lane[h], two)], qz)
                            if j == cc:
                                s = jnp.where(causal(s.shape), s, NEG)
                            sscr[pl.ds(j * tc, tc), :] = s
                            bm = jnp.max(s, axis=0, keepdims=True)
                            mx = bm if mx is None else jnp.maximum(mx, bm)
                        den = None
                        for j in range(cc + 1):
                            e = jnp.exp2((sscr[pl.ds(j * tc, tc), :] - mx) * exp_c)
                            sscr[pl.ds(j * tc, tc), :] = e
                            es = jnp.sum(e, axis=0, keepdims=True)
                            den = es if den is None else den + es
                        inv = 1.0 / den
                        o_t = None
                        for j in range(cc + 1):
                            pr = (sscr[pl.ds(j * tc, tc), :] * inv).astype(BF16)
                            pbuf[cc * (cc + 1) // 2 + j, p * 2 + h] = pr
                            part = dot(qkv[j, head_rows(p, h, 2), :], pr)
                            o_t = part if o_t is None else o_t + part
                        obuf[cc, pl.ds(pl.multiple_of((p * 2 + h) * hd, hd), hd), :] = o_t.astype(BF16)

    def mlp_step(c):
        a = dot(woT[...], obuf[c]).astype(BF16)
        m32 = (hbuf[c].astype(F32) + a.astype(F32)).astype(BF16).astype(F32)
        mbuf[c] = m32.astype(BF16)
        n2 = (m32 * inv_rms(m32)).astype(BF16)
        n2buf[c] = n2

        acc = None
        for f in range(nm):
            rows = pl.ds(f * fl, fl)
            u = dot(wuT[rows, :], n2buf[c]).astype(BF16)
            ubuf[c, rows, :] = u
            z = gelu(u.astype(F32)).astype(BF16)
            zbuf[c, rows, :] = z
            part = dot(wdT[f], z)
            acc = part if acc is None else acc + part
        y32 = (mbuf[c].astype(F32) + acc.astype(BF16).astype(F32)).astype(BF16)
        ybuf[c] = y32

        @pl.when(jnp.logical_not(last))
        def _():
            f_copy(c).start()

        @pl.when(last)
        def _():
            t_copy(c).wait()
            err = ybuf[c].astype(F32) - jnp.transpose(xin[c]).astype(F32)
            lossv[...] += jnp.sum((err * err).reshape(dm_ // 8, 8, tc), axis=0)
            dybuf[c] = (err * inv_d).astype(BF16)

    @pl.loop(0, 2 * nc)
    def _(n):
        attn_turn = jnp.where(early, jnp.where(n < nc, 1, 0), 1 - lax.rem(n, 2))
        c = jnp.where(early, lax.rem(n, nc), n // 2)

        @pl.when(early & (n == 2))
        def _():
            w_forward(W_U)

        @pl.when(early & (n == min(3, nc)))
        def _():
            w_forward(W_D)
            pass_go()

        @pl.when(attn_turn == 1)
        def _():
            attention_step(c)

        @pl.when(early & (n == nc))
        def _():
            w_wait(W_O)
            w_wait(W_U)
            w_wait(W_D)

        @pl.when(attn_turn == 0)
        def _():
            mlp_step(c)

    @pl.when(jnp.logical_not(late))
    def _():
        natural_weights()

    def l_copy(k):
        return pltpu.make_async_remote_copy(
            src_ref=losst.at[nm], dst_ref=losst.at[3 - k if nm == 4 else nm - 1 - k], send_sem=lsend.at[k - 1],
            recv_sem=lrecv.at[k - 1], device_id={"model": peer(k)}, device_id_type=MESH)

    def lf_copy():
        return pltpu.make_async_remote_copy(
            src_ref=losst.at[nm + 1], dst_ref=losst.at[nm + 1], send_sem=lfsend, recv_sem=lfrecv,
            device_id={"stage": prv}, device_id_type=MESH)

    @pl.when(last)
    def _():
        tot = jnp.sum(lossv[...]) * (0.5 * inv_d)
        losst[nm] = jnp.full(losst.shape[1:], tot, F32)
        for k in range(1, nm):
            l_copy(k).start()

    @pl.loop(0, nc)
    def _(i):
        c = nc - 1 - i

        @pl.when(jnp.logical_not(last))
        def _():
            b_copy(c).wait_recv()

        acc = None
        for f in range(nm):
            rows = pl.ds(f * fl, fl)
            dz = dot(wd[rows, :], dybuf[c]).astype(BF16).astype(F32)
            du = (dz * gelu_grad(ubuf[c, rows, :].astype(F32))).astype(BF16)
            ubuf[c, rows, :] = du
            part = dot(wu[f], du)
            acc = part if acc is None else acc + part
        dn2 = acc.astype(BF16).astype(F32)
        m32 = mbuf[c].astype(F32)
        pull = norm_pull(m32, inv_rms(m32), dn2).astype(BF16)
        dmid = (dybuf[c].astype(F32) + pull.astype(F32)).astype(BF16)
        mbuf[c] = dmid
        dobuf[...] = dot(wo[...], dmid).astype(BF16)

        for cc in range(nc):
            @pl.when(c == cc)
            def _():
                @pl.loop(0, heads // 2)
                def _(p):
                    dq = [None, None]
                    qz = []
                    dz_v = []
                    dsum = []
                    for h in range(2):
                        orow = pl.ds(pl.multiple_of((p * 2 + h) * hd, hd), hd)
                        do_t = dobuf[orow, :]
                        dsum.append(jnp.sum(do_t.astype(F32) * obuf[cc, orow, :].astype(F32), axis=0, keepdims=True))
                        dz_v.append(pad_v(do_t, h))
                        qz.append(pad_v(qkv[cc, head_rows(p, h, 0), :], h))
                    for j in range(cc + 1):
                        dv_new = None
                        dk_new = None
                        for h in range(2):
                            pr = pbuf[cc * (cc + 1) // 2 + j, p * 2 + h]
                            dp = dot(qkvn[p, pl.ds(j * tc, tc), pl.ds(v_lane[h], two)], dz_v[h]).astype(BF16).astype(F32)
                            ds = (pr.astype(F32) * (dp - dsum[h])).astype(BF16)
                            dv_h = dot_t(pr, dz_v[h])
                            dk_h = dot_t(ds, qz[h])
                            dv_new = dv_h if dv_new is None else dv_new + dv_h
                            dk_new = dk_h if dk_new is None else dk_new + dk_h
                            dq_h = dot(qkv[j, head_rows(p, h, 1), :], ds)
                            dq[h] = dq_h if dq[h] is None else dq[h] + dq_h
                        rows = pl.ds(j * tc, tc)
                        if cc < nc - 1:
                            dv_new = dv_new + dvacc[p, rows, :]
                            dk_new = dk_new + dkacc[p, rows, :]
                        if j < cc:
                            dvacc[p, rows, :] = dv_new
                            dkacc[p, rows, :] = dk_new
                        else:
                            dv_t = jnp.transpose(dv_new).astype(BF16)
                            dk_t = (jnp.transpose(dk_new) * scale).astype(BF16)
                            for h in range(2):
                                qkv[cc, head_rows(p, h, 0), :] = (dq[h] * scale).astype(BF16)
                                qkv[cc, head_rows(p, h, 1), :] = dk_t[h * hd:(h + 1) * hd, :]
                                qkv[cc, head_rows(p, h, 2), :] = dv_t[h * hd:(h + 1) * hd, :]

        dn1 = dot(wq[...], qkv[c]).astype(BF16).astype(F32)
        h32 = hbuf[c].astype(F32)
        pull1 = norm_pull(h32, inv_rms(h32), dn1).astype(BF16)

        @pl.when(jnp.logical_not(last))
        def _():
            f_copy(c).wait_send()

        ybuf[c] = (mbuf[c].astype(F32) + pull1.astype(F32)).astype(BF16)

        @pl.when(jnp.logical_not(first))
        def _():
            b_copy(c).start()

    @pl.when(last)
    def _():
        for k in range(1, nm):
            l_copy(k).wait_recv()
        vals = [losst[nm]] + [losst[k - 1] for k in range(1, nm)]
        tot = jnp.zeros_like(vals[0])
        for who in range(nm):
            pick = vals[0]
            for k in range(1, nm):
                pick = jnp.where(peer(k) == who, vals[k], pick)
            tot = tot + pick
        losst[nm + 1] = tot

    @pl.when(jnp.logical_not(last))
    def _():
        lf_copy().wait_recv()

    @pl.when(jnp.logical_not(first))
    def _():
        lf_copy().start()

    loss_out[...] = losst[nm + 1]

    def wgrad(mat, d):
        acc = None
        for c in range(nc):
            if mat == 0:
                part = dot_t(qkv[c, rowsl(d * qrows, qrows, qrows), :], n1buf[c])
            elif mat == 1:
                part = dot_t(obuf[c, rowsl(d * orows, orows, orows), :], mbuf[c])
            elif mat == 2:
                part = dot_t(n2buf[c], ubuf[c, rowsl(d * fl, fl, fl), :])
            else:
                part = dot_t(zbuf[c, rowsl(d * fl, fl, fl), :], dybuf[c])
            acc = part if acc is None else acc + part
        return acc

    sizes = (qrows, orows, dm_, fl)
    offs = (0, qrows, qrows + orows, qrows + orows + dm_)

    def rows_of(mat):
        return pl.ds(offs[mat], sizes[mat])

    outs = (gq_out, go_out, gu_out, gd_out)

    def half_of(mat, half):
        return pl.ds(offs[mat] + half * (sizes[mat] // 2), sizes[mat] // 2)

    def far_copy(mat, half):
        buf = (far_p, far_m)[half]
        rows = pl.ds(offs[mat] // 2, sizes[mat] // 2)
        return pltpu.make_async_remote_copy(
            src_ref=stage_buf.at[0, half_of(mat, half)], dst_ref=buf.at[rows], send_sem=rs_send.at[mat, half],
            recv_sem=rs_recv.at[mat, half], device_id={"model": peer((plus, minus)[half])}, device_id_type=MESH)

    def near_copy(mat, side, half):
        buf = (near_p, near_m)[side]
        return pltpu.make_async_remote_copy(
            src_ref=stage_buf.at[1 + side, half_of(mat, half)], dst_ref=buf.at[half_of(mat, half)],
            send_sem=rs_send.at[mat, 2 + 2 * side + half], recv_sem=rs_recv.at[mat, 2 + 2 * side + half],
            device_id={"model": peer((plus, minus)[side])}, device_id_type=MESH)

    mats = (3, 2, 0, 1)
    for mat in mats:
        stage_buf[0, rows_of(mat)] = wgrad(mat, peer(far))
        for half in range(2):
            far_copy(mat, half).start()
    for mat in mats:
        for side in range(2):
            stage_buf[1 + side, rows_of(mat)] = wgrad(mat, peer((plus, minus)[side]))
            near_copy(mat, side, 1 - side).start()

    def load(src, nr):
        return pltpu.make_async_copy(src, radd.at[pl.ds(0, nr)], ld_sem.at[0])

    for mat in mats:
        nr = sizes[mat] // 2
        for half in range(2):
            far_copy(mat, half).wait_recv()
            src = (far_p, far_m)[half].at[pl.ds(offs[mat] // 2, nr)]
            load(src, nr).start()
            load(src, nr).wait()
            stage_buf[1 + half, half_of(mat, half)] += radd[pl.ds(0, nr)]
            near_copy(mat, half, half).start()

    for mat in mats:
        for half in range(2):
            far_copy(mat, half).wait_send()
        stage_buf[0, rows_of(mat)] = wgrad(mat, me)

    def out_copy(mat):
        return pltpu.make_async_copy(stage_buf.at[0, rows_of(mat)], outs[mat], out_sem.at[mat])

    def add_near(mat, side, half):
        nr = sizes[mat] // 2
        near_copy(mat, side, half).wait_recv()
        src = (near_p, near_m)[side].at[half_of(mat, half)]
        load(src, nr).start()
        load(src, nr).wait()
        stage_buf[0, half_of(mat, half)] += radd[pl.ds(0, nr)]

    for mat in mats:
        for side in range(2):
            add_near(mat, side, 1 - side)
    for mat in mats:
        for side in range(2):
            add_near(mat, side, side)
        out_copy(mat).start()

    for mat in mats:
        out_copy(mat).wait()
    for idx in range(4):
        for way in range(4):
            w_copy(idx, way).wait_send()
    for mat in mats:
        for half in range(2):
            for side in range(2):
                near_copy(mat, side, half).wait_send()

    @pl.when(jnp.logical_not(first))
    def _():
        for c in range(nc):
            b_copy(c).wait_send()
        lf_copy().wait_send()

    @pl.when(last)
    def _():
        for k in range(1, nm):
            l_copy(k).wait_send()


def solution(mesh):
    ns = mesh.shape["stage"]
    nm = mesh.shape["model"]

    def per_device(tokens_in, targets, w_qkv, w_out, w_up, w_down):
        n_micro, seq_len, d_model = tokens_in.shape
        hl, hd, fl = w_qkv.shape[3], w_qkv.shape[5], w_up.shape[3]
        tc = min(CHUNK, seq_len // 2)
        nc = seq_len // tc
        assert n_micro == nm == 4 and w_qkv.shape[1] == 1 and hl == 2
        qrows, orows = hl * 3 * hd, hl * hd
        wqT = jnp.transpose(w_qkv[0, 0], (1, 2, 3, 0)).reshape(qrows, d_model)
        wo = w_out[0, 0].reshape(orows, d_model)
        wu, wd = w_up[0, 0], w_down[0, 0]
        cfg = (ns, nm, nc, tc, d_model, hl, hd, fl)
        heads = nm * hl
        any_spec = pl.BlockSpec(memory_space=pl.ANY)
        rsum = qrows + orows + d_model + fl
        f32 = lambda *shape: jax.ShapeDtypeStruct(shape, F32)
        out_shape = (f32(qrows, d_model), f32(orows, d_model), f32(d_model, fl), f32(fl, d_model), f32(8, 128),
                     f32(rsum // 2, d_model), f32(rsum // 2, d_model), f32(rsum, d_model), f32(rsum, d_model))
        vb = lambda *shape: pltpu.VMEM(shape, BF16)
        vf = lambda *shape: pltpu.VMEM(shape, F32)
        dma = lambda *shape: pltpu.SemaphoreType.DMA(shape)
        seqb = nc * tc
        scratch = [
            vb(nm * qrows, d_model), vb(d_model, nm * orows), vb(nm * fl, d_model), vb(nm, d_model, fl),
            vb(nm * fl, d_model), vb(nm, d_model, fl), vb(nm * orows, d_model), vb(d_model, nm * qrows),
            vb(nc, tc, d_model), vb(nc, d_model, tc), vb(nc, d_model, tc), vb(nc, nm * qrows, tc), vb(nm, seqb, qrows),
            vb(nc, nm * orows, tc), vb(nc, d_model, tc), vb(nc, d_model, tc), vb(nc, nm * fl, tc), vb(nc, nm * fl, tc),
            vb(nc * (nc + 1) // 2, heads, tc, tc), vb(nc, d_model, tc), vf(heads // 2, seqb, 2 * hd), vf(heads // 2, seqb, 2 * hd),
            vf(seqb, tc), vb(nc, d_model, tc), vb(nm * orows, tc), vf(nm + 2, 8, 128), vf(8, tc),
            vf(3, rsum, d_model), vf(256, d_model),
            dma(4, 4), dma(4, 4), dma(4), pltpu.SemaphoreType.REGULAR, dma(nc), dma(nc), dma(nc), dma(nc), dma(nc),
            dma(nm - 1), dma(nm - 1), pltpu.SemaphoreType.DMA, pltpu.SemaphoreType.DMA,
            dma(4, 6), dma(4, 6), dma(1), dma(4),
        ]
        res = pl.pallas_call(
            functools.partial(step_kernel, cfg),
            out_shape=out_shape,
            in_specs=[any_spec] * 6,
            out_specs=[any_spec] * 4 + [pl.BlockSpec(memory_space=pltpu.VMEM)] + [any_spec] * 4,
            scratch_shapes=scratch,
            compiler_params=pltpu.CompilerParams(collective_id=0, has_side_effects=True, vmem_limit_bytes=67043328),
            name="train_step",
        )(tokens_in, targets, wqT, wo, wu, wd)
        g_qkv = jnp.transpose(res[0].reshape(hl, 3, hd, d_model), (3, 0, 1, 2))[None, None]
        g_out = res[1].reshape(1, 1, hl, hd, d_model)
        return g_qkv, g_out, res[2][None, None], res[3][None, None], res[4][0, :1]

    tok_spec = P(None, "data", None)
    qkv_spec = P("stage", None, None, "model", None, None)
    out_spec = P("stage", None, "model", None, None)
    up_spec = P("stage", None, None, "model")
    down_spec = P("stage", None, "model", None)
    g_qkv_spec = P(("data", "stage"), None, None, "model", None, None)
    g_out_spec = P(("data", "stage"), None, "model", None, None)
    g_up_spec = P(("data", "stage"), None, None, "model")
    g_down_spec = P(("data", "stage"), None, "model", None)
    return jax.shard_map(per_device, mesh=mesh, in_specs=(tok_spec, tok_spec, qkv_spec, out_spec, up_spec, down_spec), out_specs=(g_qkv_spec, g_out_spec, g_up_spec, g_down_spec, P("data")), check_vma=False)
```

```python
import functools
import math

import jax
import jax.numpy as jnp
from jax import lax
from jax.experimental import pallas as pl
from jax.experimental.pallas import tpu as pltpu
from jax.sharding import PartitionSpec as P

F32 = jnp.float32
BF16 = jnp.bfloat16
MESH = pl.DeviceIdType.MESH
CHUNK = 256
NEG = -1e30
GELU_C = math.sqrt(2.0 / math.pi)
GELU_A = 0.044715

W_Q, W_O, W_U, W_D = range(4)


def dot(lhs, rhs):
    return jnp.dot(lhs, rhs, preferred_element_type=F32)


def dot_t(lhs, rhs):
    return lax.dot_general(lhs, rhs, (((1,), (1,)), ((), ())), preferred_element_type=F32)


def inv_rms(x32):
    return lax.rsqrt(jnp.mean(x32 * x32, axis=0, keepdims=True) + 1e-6)


def norm_pull(x32, inv, g32):
    mean_gx = jnp.mean(g32 * x32, axis=0, keepdims=True)
    return g32 * inv - x32 * (inv * inv * inv * mean_gx)


def gelu(u):
    tanh = jnp.tanh(u * (GELU_C + (GELU_C * GELU_A) * (u * u)))
    half = 0.5 * u
    return half + half * tanh


def gelu_grad(u):
    u2 = u * u
    sig = 0.5 + 0.5 * jnp.tanh(u * (GELU_C + (GELU_C * GELU_A) * u2))
    slope = u * (2.0 * GELU_C + (6.0 * GELU_C * GELU_A) * u2)
    return sig * (1.0 + slope * (1.0 - sig))


def step_kernel(cfg, x_hbm, t_hbm, wqT_in, wo_in, wu_in, wd_in,
                gq_out, go_out, gu_out, gd_out, loss_out, far_p, far_m, near_p, near_m,
                wqT, woT, wuT, wdT, wd, wu, wo, wq,
                xin, hbuf, n1buf, qkv, qkvn, obuf, mbuf, n2buf, ubuf, zbuf, pbuf, dybuf, dvacc, dkacc, sscr,
                ybuf, dobuf, losst, lossv, stage_buf, radd,
                ag_send, ag_recv, ag_loc, go_sem, xsem, fsend, frecv, bsend, brecv, lsend, lrecv, lfsend, lfrecv,
                rs_send, rs_recv, ld_sem, out_sem):
    ns, nm, nc, tc, dm_, hl, hd, fl = cfg
    heads = nm * hl
    qrows = hl * 3 * hd
    orows = hl * hd
    inv_d = 1.0 / (nm * nc * tc * dm_)
    scale = hd ** -0.5
    exp_c = scale * math.log2(math.e)
    me = lax.axis_index("model")
    st = lax.axis_index("stage")
    nxt = lax.rem(st + 1, ns)
    prv = lax.rem(st + ns - 1, ns)
    first = st == 0
    last = st == ns - 1

    def peer(k):
        return lax.rem(me + k, nm)

    bar = pltpu.get_barrier_semaphore()
    pl.semaphore_signal(bar, inc=1, device_id={"stage": nxt}, device_id_type=MESH)
    pl.semaphore_signal(bar, inc=1, device_id={"stage": prv}, device_id_type=MESH)
    for k in range(1, nm):
        pl.semaphore_signal(bar, inc=1, device_id={"model": peer(k)}, device_id_type=MESH)
    pl.semaphore_wait(bar, 2 + nm - 1)

    def rowsl(start, size, mult):
        return pl.ds(pl.multiple_of(start, mult), size)

    plus, minus, far = 1, nm - 1, 2

    def w_rows(idx, who, half=None):
        size = (qrows, orows, fl, fl)[idx]
        if idx in (W_Q, W_U):
            buf = wqT if idx == W_Q else wuT
            if half is None:
                return buf.at[rowsl(who * size, size, size), :]
            return buf.at[rowsl(who * size + half * (size // 2), size // 2, size // 2), :]
        view = (woT if idx == W_O else wdT).at[:, rowsl(who * size, size, size)]
        return view if half is None else view.at[pl.ds(half * (dm_ // 2), dm_ // 2), :]

    def w_copy(idx, way):
        to = plus if way in (0, 2) else minus
        if way < 2:
            src = wqT_in if idx == W_Q else w_rows(idx, me)
            dst = w_rows(idx, me)
        else:
            src = dst = w_rows(idx, peer(minus if way == 2 else plus), way - 2)
        return pltpu.make_async_remote_copy(
            src_ref=src, dst_ref=dst, send_sem=ag_send.at[idx, way], recv_sem=ag_recv.at[idx, way],
            device_id={"model": peer(to)}, device_id_type=MESH)

    def w_arrival(idx, way):
        who = peer((minus, plus, far, far)[way])
        ref = w_rows(idx, who) if way < 2 else w_rows(idx, who, way - 2)
        return pltpu.make_async_remote_copy(
            src_ref=ref, dst_ref=ref, send_sem=ag_send.at[idx, way], recv_sem=ag_recv.at[idx, way],
            device_id={"model": peer(plus)}, device_id_type=MESH)

    def w_local(idx):
        src = (wqT_in, wo_in, wu_in, wd_in)[idx]
        dst = (w_rows(W_Q, me), wo.at[rowsl(me * orows, orows, orows), :], wu.at[:, rowsl(me * fl, fl, fl)], wd.at[rowsl(me * fl, fl, fl), :])[idx]
        return pltpu.make_async_copy(src, dst, ag_loc.at[idx])

    def w_own(idx):
        for way in range(2):
            w_copy(idx, way).start()

    def w_forward(idx):
        for way in range(2):
            w_arrival(idx, way).wait_recv()
        for way in range(2, 4):
            w_copy(idx, way).start()

    def w_wait(idx):
        for way in range(2, 4):
            w_arrival(idx, way).wait_recv()

    def x_copy(c):
        return pltpu.make_async_copy(x_hbm.at[me, pl.ds(c * tc, tc), :], xin.at[c], xsem.at[c])

    def t_copy(c):
        return pltpu.make_async_copy(t_hbm.at[me, pl.ds(c * tc, tc), :], xin.at[c], xsem.at[c])

    @pl.when(first)
    def _():
        for c in range(nc):
            x_copy(c).start()

    @pl.when(last)
    def _():
        for c in range(nc):
            t_copy(c).start()

    for idx in range(4):
        w_local(idx).start()

    odd = lax.rem(st, 2) == 1
    early = st < 2

    @pl.when(odd)
    def _():
        pl.semaphore_wait(go_sem, 1)

    w_own(W_Q)
    w_local(W_O).wait()
    woT[:, rowsl(me * orows, orows, orows)] = jnp.transpose(wo[rowsl(me * orows, orows, orows), :])
    w_own(W_O)
    w_local(W_U).wait()
    wuT[rowsl(me * fl, fl, fl), :] = jnp.transpose(wu[:, rowsl(me * fl, fl, fl)])
    w_local(W_Q).wait()
    w_forward(W_Q)
    w_own(W_U)
    w_local(W_D).wait()
    wdT[:, rowsl(me * fl, fl, fl)] = jnp.transpose(wd[rowsl(me * fl, fl, fl), :])
    w_forward(W_O)
    w_own(W_D)

    def pass_go():
        @pl.when(jnp.logical_not(odd))
        def _():
            pl.semaphore_signal(go_sem, inc=1, device_id={"stage": nxt}, device_id_type=MESH)

    def natural_weights():
        @pl.loop(0, nm)
        def _(f):
            wu[:, rowsl(f * fl, fl, fl)] = jnp.transpose(wuT[rowsl(f * fl, fl, fl), :])
            wd[rowsl(f * fl, fl, fl), :] = jnp.transpose(wdT[:, rowsl(f * fl, fl, fl)])
            wo[rowsl(f * orows, orows, orows), :] = jnp.transpose(woT[:, rowsl(f * orows, orows, orows)])
            wq[:, rowsl(f * qrows, qrows, qrows)] = jnp.transpose(wqT[rowsl(f * qrows, qrows, qrows), :])

    late = st >= max(2, ns // 2)

    @pl.when(jnp.logical_not(early))
    def _():
        w_forward(W_U)
        w_forward(W_D)
        pass_go()
        for idx in range(4):
            w_wait(idx)

    @pl.when(late)
    def _():
        natural_weights()

    def f_copy(c):
        return pltpu.make_async_remote_copy(
            src_ref=ybuf.at[c], dst_ref=hbuf.at[c], send_sem=fsend.at[c], recv_sem=frecv.at[c],
            device_id={"stage": nxt}, device_id_type=MESH)

    def b_copy(c):
        return pltpu.make_async_remote_copy(
            src_ref=ybuf.at[c], dst_ref=dybuf.at[c], send_sem=bsend.at[c], recv_sem=brecv.at[c],
            device_id={"stage": prv}, device_id_type=MESH)

    lossv[...] = jnp.zeros_like(lossv)

    def head_rows(p, h, part):
        return pl.ds(p * (2 * 3 * hd) + (h * 3 + part) * hd, hd)

    k_lane = (0, 2 * 2 * hd)
    v_lane = (2 * hd, 2 * 2 * hd)
    two = 2 * hd

    def pad_k(val, h):
        zero = jnp.zeros_like(val)
        return jnp.concatenate([zero, val] if h == 0 else [val, zero], axis=0)

    def pad_v(val, h):
        zero = jnp.zeros_like(val)
        return jnp.concatenate([val, zero] if h == 0 else [zero, val], axis=0)

    def causal(shape, row0):
        return lax.broadcasted_iota(jnp.int32, shape, 0) + row0 <= lax.broadcasted_iota(jnp.int32, shape, 1)

    def attention(cc):
        nk = (cc + 1) * tc
        slots = min(heads, sscr.shape[0] // nk)
        ahead = min(4, slots - 1)
        sub = tc // 2

        def front(head):
            p, h = head // 2, head % 2
            base = (head % slots) * nk
            qz = pad_k(qkv[cc, head_rows(p, h, 0), :], h)
            tops, sums = [], []
            for j in range(cc + 1):
                s = dot(qkvn[p, pl.ds(j * tc, tc), pl.ds(k_lane[h], two)], qz)
                for r in range(0, tc, sub):
                    part = s[r:r + sub]
                    if j == cc:
                        part = jnp.where(causal(part.shape, r), part, NEG)
                    top = jnp.max(part, axis=0, keepdims=True)
                    e = jnp.exp2((part - top) * exp_c)
                    sscr[pl.ds(base + j * tc + r, sub), :] = e
                    tops.append(top)
                    sums.append(jnp.sum(e, axis=0, keepdims=True))
            mx = functools.reduce(jnp.maximum, tops)
            scales = [jnp.exp2((top - mx) * exp_c) for top in tops]
            inv = 1.0 / functools.reduce(jnp.add, [a * b for a, b in zip(scales, sums)])
            return [a * inv for a in scales]

        def back(head, factors):
            p, h = head // 2, head % 2
            base = (head % slots) * nk
            o_t = None
            for j in range(cc + 1):
                parts = []
                for i in range(2):
                    pr = (sscr[pl.ds(base + j * tc + i * sub, sub), :] * factors[2 * j + i]).astype(BF16)
                    pbuf[cc * (cc + 1) // 2 + j, head, pl.ds(i * sub, sub), :] = pr
                    parts.append(pr)
                part = dot(qkv[j, head_rows(p, h, 2), :], jnp.concatenate(parts, axis=0))
                o_t = part if o_t is None else o_t + part
            obuf[cc, pl.ds(head * hd, hd), :] = o_t.astype(BF16)

        factors = {}
        for head in range(ahead):
            factors[head] = front(head)
        for head in range(heads):
            if head + ahead < heads:
                factors[head + ahead] = front(head + ahead)
            back(head, factors.pop(head))

    def attention_grad(cc):
        units = [(p, j) for p in range(heads // 2) for j in range(cc + 1)]
        dqs = {}
        held = {}

        def of_head(p, h):
            if (p, h) not in held:
                rows = pl.ds((p * 2 + h) * hd, hd)
                do_t = dobuf[rows, :]
                dsum = jnp.sum(do_t.astype(F32) * obuf[cc, rows, :].astype(F32), axis=0, keepdims=True)
                held[p, h] = (pad_v(do_t, h), dsum)
            return held[p, h]

        def front(p, j):
            out = []
            for h in range(2):
                do_z, dsum = of_head(p, h)
                pr = pbuf[cc * (cc + 1) // 2 + j, p * 2 + h]
                dp = dot(qkvn[p, pl.ds(j * tc, tc), pl.ds(v_lane[h], two)], do_z).astype(BF16).astype(F32)
                out.append((pr.astype(F32) * (dp - dsum)).astype(BF16))
            return out

        def back(p, j, ds):
            dv_new = dk_new = None
            for h in range(2):
                do_z, _ = of_head(p, h)
                dv_h = dot_t(pbuf[cc * (cc + 1) // 2 + j, p * 2 + h], do_z)
                dk_h = dot_t(ds[h], pad_v(qkv[cc, head_rows(p, h, 0), :], h))
                dv_new = dv_h if dv_new is None else dv_new + dv_h
                dk_new = dk_h if dk_new is None else dk_new + dk_h
                dq_h = dot(qkv[j, head_rows(p, h, 1), :], ds[h])
                dqs[p, h] = dq_h if j == 0 else dqs[p, h] + dq_h
            rows = pl.ds(j * tc, tc)
            if cc < nc - 1:
                dv_new = dv_new + dvacc[p, rows, :]
                dk_new = dk_new + dkacc[p, rows, :]
            if j < cc:
                dvacc[p, rows, :] = dv_new
                dkacc[p, rows, :] = dk_new
                return
            dv_t = jnp.transpose(dv_new).astype(BF16)
            dk_t = (jnp.transpose(dk_new) * scale).astype(BF16)
            for h in range(2):
                qkv[cc, head_rows(p, h, 0), :] = (dqs[p, h] * scale).astype(BF16)
                qkv[cc, head_rows(p, h, 1), :] = dk_t[h * hd:(h + 1) * hd, :]
                qkv[cc, head_rows(p, h, 2), :] = dv_t[h * hd:(h + 1) * hd, :]

        ds = front(*units[0])
        for n, unit in enumerate(units):
            later = front(*units[n + 1]) if n + 1 < len(units) else None
            back(*unit, ds)
            ds = later

    def attention_step(c):
        @pl.when(first)
        def _():
            x_copy(c).wait()
            hbuf[c] = jnp.transpose(xin[c])

        @pl.when(jnp.logical_not(first))
        def _():
            f_copy(c).wait_recv()

        @pl.when(early & (c == 0))
        def _():
            w_wait(W_Q)

        h32 = hbuf[c].astype(F32)
        n1 = (h32 * inv_rms(h32)).astype(BF16)
        n1buf[c] = n1
        for r in range(nm):
            rows = pl.ds(r * qrows, qrows)
            blk = dot(wqT[rows, :], n1).astype(BF16)
            qkv[c, rows, :] = blk
            qkvn[r, pl.ds(pl.multiple_of(c * tc, tc), tc), :] = jnp.transpose(blk)

        for cc in range(nc):
            pl.when(c == cc)(functools.partial(attention, cc))

    def mlp_step(c):
        a = dot(woT[...], obuf[c]).astype(BF16)
        m32 = (hbuf[c].astype(F32) + a.astype(F32)).astype(BF16).astype(F32)
        mbuf[c] = m32.astype(BF16)
        n2 = (m32 * inv_rms(m32)).astype(BF16)
        n2buf[c] = n2

        blk = fl // 2
        for f in range(2 * nm):
            rows = pl.ds(f * blk, blk)
            u = dot(wuT[rows, :], n2buf[c]).astype(BF16)
            ubuf[c, rows, :] = u
            zbuf[c, rows, :] = gelu(u.astype(F32)).astype(BF16)
        acc = dot(wdT[...], zbuf[c])
        y32 = (mbuf[c].astype(F32) + acc.astype(BF16).astype(F32)).astype(BF16)
        ybuf[c] = y32

        @pl.when(jnp.logical_not(last))
        def _():
            f_copy(c).start()

        @pl.when(last)
        def _():
            t_copy(c).wait()
            err = ybuf[c].astype(F32) - jnp.transpose(xin[c]).astype(F32)
            lossv[...] += jnp.sum((err * err).reshape(dm_ // 8, 8, tc), axis=0)
            dybuf[c] = (err * inv_d).astype(BF16)

    @pl.loop(0, 2 * nc)
    def _(n):
        attn_turn = jnp.where(early, jnp.where(n < nc, 1, 0), 1 - lax.rem(n, 2))
        c = jnp.where(early, lax.rem(n, nc), n // 2)

        @pl.when(early & (n == 2))
        def _():
            w_forward(W_U)

        @pl.when(early & (n == min(3, nc)))
        def _():
            w_forward(W_D)
            pass_go()

        @pl.when(attn_turn == 1)
        def _():
            attention_step(c)

        @pl.when(early & (n == nc))
        def _():
            w_wait(W_O)
            w_wait(W_U)
            w_wait(W_D)

        @pl.when(attn_turn == 0)
        def _():
            mlp_step(c)

    @pl.when(jnp.logical_not(late))
    def _():
        natural_weights()

    def l_copy(k):
        return pltpu.make_async_remote_copy(
            src_ref=losst.at[nm], dst_ref=losst.at[3 - k if nm == 4 else nm - 1 - k], send_sem=lsend.at[k - 1],
            recv_sem=lrecv.at[k - 1], device_id={"model": peer(k)}, device_id_type=MESH)

    def lf_copy():
        return pltpu.make_async_remote_copy(
            src_ref=losst.at[nm + 1], dst_ref=losst.at[nm + 1], send_sem=lfsend, recv_sem=lfrecv,
            device_id={"stage": prv}, device_id_type=MESH)

    @pl.when(last)
    def _():
        tot = jnp.sum(lossv[...]) * (0.5 * inv_d)
        losst[nm] = jnp.full(losst.shape[1:], tot, F32)
        for k in range(1, nm):
            l_copy(k).start()

    @pl.loop(0, nc)
    def _(i):
        c = nc - 1 - i

        @pl.when(jnp.logical_not(last))
        def _():
            b_copy(c).wait_recv()

        blk = fl // 4
        for f in range(4 * nm):
            rows = pl.ds(f * blk, blk)
            dz = dot(wd[rows, :], dybuf[c]).astype(BF16).astype(F32)
            ubuf[c, rows, :] = (dz * gelu_grad(ubuf[c, rows, :].astype(F32))).astype(BF16)
        acc = dot(wu[...], ubuf[c])
        dn2 = acc.astype(BF16).astype(F32)
        m32 = mbuf[c].astype(F32)
        pull = norm_pull(m32, inv_rms(m32), dn2).astype(BF16)
        dmid = (dybuf[c].astype(F32) + pull.astype(F32)).astype(BF16)
        mbuf[c] = dmid
        dobuf[...] = dot(wo[...], dmid).astype(BF16)

        for cc in range(nc):
            pl.when(c == cc)(functools.partial(attention_grad, cc))

        dn1 = dot(wq[...], qkv[c]).astype(BF16).astype(F32)
        h32 = hbuf[c].astype(F32)
        pull1 = norm_pull(h32, inv_rms(h32), dn1).astype(BF16)

        @pl.when(jnp.logical_not(last))
        def _():
            f_copy(c).wait_send()

        ybuf[c] = (mbuf[c].astype(F32) + pull1.astype(F32)).astype(BF16)

        @pl.when(jnp.logical_not(first))
        def _():
            b_copy(c).start()

    @pl.when(last)
    def _():
        for k in range(1, nm):
            l_copy(k).wait_recv()
        vals = [losst[nm]] + [losst[k - 1] for k in range(1, nm)]
        tot = jnp.zeros_like(vals[0])
        for who in range(nm):
            pick = vals[0]
            for k in range(1, nm):
                pick = jnp.where(peer(k) == who, vals[k], pick)
            tot = tot + pick
        losst[nm + 1] = tot

    @pl.when(jnp.logical_not(last))
    def _():
        lf_copy().wait_recv()

    @pl.when(jnp.logical_not(first))
    def _():
        lf_copy().start()

    loss_out[...] = losst[nm + 1]

    def wgrad(mat, d):
        acc = None
        for c in range(nc):
            if mat == 0:
                part = dot_t(qkv[c, rowsl(d * qrows, qrows, qrows), :], n1buf[c])
            elif mat == 1:
                part = dot_t(obuf[c, rowsl(d * orows, orows, orows), :], mbuf[c])
            elif mat == 2:
                part = dot_t(n2buf[c], ubuf[c, rowsl(d * fl, fl, fl), :])
            else:
                part = dot_t(zbuf[c, rowsl(d * fl, fl, fl), :], dybuf[c])
            acc = part if acc is None else acc + part
        return acc

    sizes = (qrows, orows, dm_, fl)
    offs = (0, qrows, qrows + orows, qrows + orows + dm_)

    def rows_of(mat):
        return pl.ds(offs[mat], sizes[mat])

    outs = (gq_out, go_out, gu_out, gd_out)

    def half_of(mat, half):
        return pl.ds(offs[mat] + half * (sizes[mat] // 2), sizes[mat] // 2)

    def far_copy(mat, half):
        buf = (far_p, far_m)[half]
        rows = pl.ds(offs[mat] // 2, sizes[mat] // 2)
        return pltpu.make_async_remote_copy(
            src_ref=stage_buf.at[0, half_of(mat, half)], dst_ref=buf.at[rows], send_sem=rs_send.at[mat, half],
            recv_sem=rs_recv.at[mat, half], device_id={"model": peer((plus, minus)[half])}, device_id_type=MESH)

    def near_copy(mat, side, half):
        buf = (near_p, near_m)[side]
        return pltpu.make_async_remote_copy(
            src_ref=stage_buf.at[1 + side, half_of(mat, half)], dst_ref=buf.at[half_of(mat, half)],
            send_sem=rs_send.at[mat, 2 + 2 * side + half], recv_sem=rs_recv.at[mat, 2 + 2 * side + half],
            device_id={"model": peer((plus, minus)[side])}, device_id_type=MESH)

    mats = (3, 2, 0, 1)
    for mat in mats:
        stage_buf[0, rows_of(mat)] = wgrad(mat, peer(far))
        for half in range(2):
            far_copy(mat, half).start()
    for mat in mats:
        for side in range(2):
            stage_buf[1 + side, rows_of(mat)] = wgrad(mat, peer((plus, minus)[side]))
            near_copy(mat, side, 1 - side).start()

    def load(src, nr):
        return pltpu.make_async_copy(src, radd.at[pl.ds(0, nr)], ld_sem.at[0])

    for mat in mats:
        nr = sizes[mat] // 2
        for half in range(2):
            far_copy(mat, half).wait_recv()
            src = (far_p, far_m)[half].at[pl.ds(offs[mat] // 2, nr)]
            load(src, nr).start()
            load(src, nr).wait()
            stage_buf[1 + half, half_of(mat, half)] += radd[pl.ds(0, nr)]
            near_copy(mat, half, half).start()

    for mat in mats:
        for half in range(2):
            far_copy(mat, half).wait_send()
        stage_buf[0, rows_of(mat)] = wgrad(mat, me)

    def out_copy(mat):
        return pltpu.make_async_copy(stage_buf.at[0, rows_of(mat)], outs[mat], out_sem.at[mat])

    def add_near(mat, side, half):
        nr = sizes[mat] // 2
        near_copy(mat, side, half).wait_recv()
        src = (near_p, near_m)[side].at[half_of(mat, half)]
        load(src, nr).start()
        load(src, nr).wait()
        stage_buf[0, half_of(mat, half)] += radd[pl.ds(0, nr)]

    for mat in mats:
        for side in range(2):
            add_near(mat, side, 1 - side)
    for mat in mats:
        for side in range(2):
            add_near(mat, side, side)
        out_copy(mat).start()

    for mat in mats:
        out_copy(mat).wait()
    for idx in range(4):
        for way in range(4):
            w_copy(idx, way).wait_send()
    for mat in mats:
        for half in range(2):
            for side in range(2):
                near_copy(mat, side, half).wait_send()

    @pl.when(jnp.logical_not(first))
    def _():
        for c in range(nc):
            b_copy(c).wait_send()
        lf_copy().wait_send()

    @pl.when(last)
    def _():
        for k in range(1, nm):
            l_copy(k).wait_send()


def solution(mesh):
    ns = mesh.shape["stage"]
    nm = mesh.shape["model"]

    def per_device(tokens_in, targets, w_qkv, w_out, w_up, w_down):
        n_micro, seq_len, d_model = tokens_in.shape
        hl, hd, fl = w_qkv.shape[3], w_qkv.shape[5], w_up.shape[3]
        tc = min(CHUNK, seq_len // 2)
        nc = seq_len // tc
        assert n_micro == nm == 4 and w_qkv.shape[1] == 1 and hl == 2
        qrows, orows = hl * 3 * hd, hl * hd
        wqT = jnp.transpose(w_qkv[0, 0], (1, 2, 3, 0)).reshape(qrows, d_model)
        wo = w_out[0, 0].reshape(orows, d_model)
        wu, wd = w_up[0, 0], w_down[0, 0]
        cfg = (ns, nm, nc, tc, d_model, hl, hd, fl)
        heads = nm * hl
        any_spec = pl.BlockSpec(memory_space=pl.ANY)
        rsum = qrows + orows + d_model + fl
        f32 = lambda *shape: jax.ShapeDtypeStruct(shape, F32)
        out_shape = (f32(qrows, d_model), f32(orows, d_model), f32(d_model, fl), f32(fl, d_model), f32(8, 128),
                     f32(rsum // 2, d_model), f32(rsum // 2, d_model), f32(rsum, d_model), f32(rsum, d_model))
        vb = lambda *shape: pltpu.VMEM(shape, BF16)
        vf = lambda *shape: pltpu.VMEM(shape, F32)
        dma = lambda *shape: pltpu.SemaphoreType.DMA(shape)
        seqb = nc * tc
        scratch = [
            vb(nm * qrows, d_model), vb(d_model, nm * orows), vb(nm * fl, d_model), vb(d_model, nm * fl),
            vb(nm * fl, d_model), vb(d_model, nm * fl), vb(nm * orows, d_model), vb(d_model, nm * qrows),
            vb(nc, tc, d_model), vb(nc, d_model, tc), vb(nc, d_model, tc), vb(nc, nm * qrows, tc), vb(nm, seqb, qrows),
            vb(nc, nm * orows, tc), vb(nc, d_model, tc), vb(nc, d_model, tc), vb(nc, nm * fl, tc), vb(nc, nm * fl, tc),
            vb(nc * (nc + 1) // 2, heads, tc, tc), vb(nc, d_model, tc), vf(heads // 2, seqb, 2 * hd), vf(heads // 2, seqb, 2 * hd),
            vf(2 * seqb, tc), vb(nc, d_model, tc), vb(nm * orows, tc), vf(nm + 2, 8, 128), vf(8, tc),
            vf(3, rsum, d_model), vf(256, d_model),
            dma(4, 4), dma(4, 4), dma(4), pltpu.SemaphoreType.REGULAR, dma(nc), dma(nc), dma(nc), dma(nc), dma(nc),
            dma(nm - 1), dma(nm - 1), pltpu.SemaphoreType.DMA, pltpu.SemaphoreType.DMA,
            dma(4, 6), dma(4, 6), dma(1), dma(4),
        ]
        res = pl.pallas_call(
            functools.partial(step_kernel, cfg),
            out_shape=out_shape,
            in_specs=[any_spec] * 6,
            out_specs=[any_spec] * 4 + [pl.BlockSpec(memory_space=pltpu.VMEM)] + [any_spec] * 4,
            scratch_shapes=scratch,
            compiler_params=pltpu.CompilerParams(collective_id=0, has_side_effects=True, vmem_limit_bytes=67043328),
            name="train_step",
        )(tokens_in, targets, wqT, wo, wu, wd)
        g_qkv = jnp.transpose(res[0].reshape(hl, 3, hd, d_model), (3, 0, 1, 2))[None, None]
        g_out = res[1].reshape(1, 1, hl, hd, d_model)
        return g_qkv, g_out, res[2][None, None], res[3][None, None], res[4][0, :1]

    tok_spec = P(None, "data", None)
    qkv_spec = P("stage", None, None, "model", None, None)
    out_spec = P("stage", None, "model", None, None)
    up_spec = P("stage", None, None, "model")
    down_spec = P("stage", None, "model", None)
    g_qkv_spec = P(("data", "stage"), None, None, "model", None, None)
    g_out_spec = P(("data", "stage"), None, "model", None, None)
    g_up_spec = P(("data", "stage"), None, None, "model")
    g_down_spec = P(("data", "stage"), None, "model", None)
    return jax.shard_map(per_device, mesh=mesh, in_specs=(tok_spec, tok_spec, qkv_spec, out_spec, up_spec, down_spec), out_specs=(g_qkv_spec, g_out_spec, g_up_spec, g_down_spec, P("data")), check_vma=False)
```

```python
import functools
import math

import jax
import jax.numpy as jnp
from jax import lax
from jax.experimental import pallas as pl
from jax.experimental.pallas import tpu as pltpu
from jax.sharding import PartitionSpec as P

F32 = jnp.float32
BF16 = jnp.bfloat16
MESH = pl.DeviceIdType.MESH
CHUNK = 256
NEG = -1e30
GELU_C = math.sqrt(2.0 / math.pi)
GELU_A = 0.044715

W_Q, W_O, W_U, W_D = range(4)


def dot(lhs, rhs):
    return jnp.dot(lhs, rhs, preferred_element_type=F32)


def dot_t(lhs, rhs):
    return lax.dot_general(lhs, rhs, (((1,), (1,)), ((), ())), preferred_element_type=F32)


def inv_rms(x32):
    return lax.rsqrt(jnp.mean(x32 * x32, axis=0, keepdims=True) + 1e-6)


def norm_pull(x32, inv, g32):
    mean_gx = jnp.mean(g32 * x32, axis=0, keepdims=True)
    return g32 * inv - x32 * (inv * inv * inv * mean_gx)


def gelu(u):
    tanh = jnp.tanh(u * (GELU_C + (GELU_C * GELU_A) * (u * u)))
    half = 0.5 * u
    return half + half * tanh


def gelu_grad(u):
    u2 = u * u
    sig = 0.5 + 0.5 * jnp.tanh(u * (GELU_C + (GELU_C * GELU_A) * u2))
    slope = u * (2.0 * GELU_C + (6.0 * GELU_C * GELU_A) * u2)
    return sig * (1.0 + slope * (1.0 - sig))


def step_kernel(cfg, x_hbm, t_hbm, wqT_in, wo_in, wu_in, wd_in,
                sum_out, loss_out, far_p, far_m, near_e, near_l, z_recv, z_fwd, dy_recv,
                wqT, woT, wuT, wdT, wd, wu, wo, wq,
                xin, hbuf, n1buf, qkv, qkvn, obuf, mbuf, n2buf, ubuf, zbuf, pbuf, dybuf, dvacc, dkacc, sscr,
                ybuf, dobuf, losst, lossv, stage_buf, radd, gdacc, zdy,
                ag_send, ag_recv, ag_loc, go_sem, xsem, fsend, frecv, bsend, brecv, lsend, lrecv, lfsend, lfrecv,
                rs_send, rs_recv, ld_sem, out_sem, z_send, z_arr, dy_send, dy_arr):
    ns, nm, nc, tc, dm_, hl, hd, fl = cfg
    heads = nm * hl
    qrows = hl * 3 * hd
    orows = hl * hd
    inv_d = 1.0 / (nm * nc * tc * dm_)
    scale = hd ** -0.5
    exp_c = scale * math.log2(math.e)
    me = lax.axis_index("model")
    st = lax.axis_index("stage")
    nxt = lax.rem(st + 1, ns)
    prv = lax.rem(st + ns - 1, ns)
    first = st == 0
    last = st == ns - 1

    def peer(k):
        return lax.rem(me + k, nm)

    bar = pltpu.get_barrier_semaphore()
    pl.semaphore_signal(bar, inc=1, device_id={"stage": nxt}, device_id_type=MESH)
    pl.semaphore_signal(bar, inc=1, device_id={"stage": prv}, device_id_type=MESH)
    for k in range(1, nm):
        pl.semaphore_signal(bar, inc=1, device_id={"model": peer(k)}, device_id_type=MESH)
    pl.semaphore_wait(bar, 2 + nm - 1)

    def rowsl(start, size, mult):
        return pl.ds(pl.multiple_of(start, mult), size)

    plus, minus, far = 1, nm - 1, 2

    def w_rows(idx, who, half=None):
        size = (qrows, orows, fl, fl)[idx]
        if idx in (W_Q, W_U):
            buf = wqT if idx == W_Q else wuT
            if half is None:
                return buf.at[rowsl(who * size, size, size), :]
            return buf.at[rowsl(who * size + half * (size // 2), size // 2, size // 2), :]
        view = (woT if idx == W_O else wdT).at[:, rowsl(who * size, size, size)]
        return view if half is None else view.at[pl.ds(half * (dm_ // 2), dm_ // 2), :]

    def w_copy(idx, way):
        to = plus if way in (0, 2) else minus
        if way < 2:
            src = wqT_in if idx == W_Q else w_rows(idx, me)
            dst = w_rows(idx, me)
        else:
            src = dst = w_rows(idx, peer(minus if way == 2 else plus), way - 2)
        return pltpu.make_async_remote_copy(
            src_ref=src, dst_ref=dst, send_sem=ag_send.at[idx, way], recv_sem=ag_recv.at[idx, way],
            device_id={"model": peer(to)}, device_id_type=MESH)

    def w_arrival(idx, way):
        who = peer((minus, plus, far, far)[way])
        ref = w_rows(idx, who) if way < 2 else w_rows(idx, who, way - 2)
        return pltpu.make_async_remote_copy(
            src_ref=ref, dst_ref=ref, send_sem=ag_send.at[idx, way], recv_sem=ag_recv.at[idx, way],
            device_id={"model": peer(plus)}, device_id_type=MESH)

    def w_local(idx):
        src = (wqT_in, wo_in, wu_in, wd_in)[idx]
        dst = (w_rows(W_Q, me), wo.at[rowsl(me * orows, orows, orows), :], wu.at[:, rowsl(me * fl, fl, fl)], wd.at[rowsl(me * fl, fl, fl), :])[idx]
        return pltpu.make_async_copy(src, dst, ag_loc.at[idx])

    def w_own(idx):
        for way in range(2):
            w_copy(idx, way).start()

    def w_forward(idx):
        for way in range(2):
            w_arrival(idx, way).wait_recv()
        for way in range(2, 4):
            w_copy(idx, way).start()

    def w_wait(idx):
        for way in range(2, 4):
            w_arrival(idx, way).wait_recv()

    def x_copy(c):
        return pltpu.make_async_copy(x_hbm.at[me, pl.ds(c * tc, tc), :], xin.at[c], xsem.at[c])

    def t_copy(c):
        return pltpu.make_async_copy(t_hbm.at[me, pl.ds(c * tc, tc), :], xin.at[c], xsem.at[c])

    @pl.when(first)
    def _():
        for c in range(nc):
            x_copy(c).start()

    @pl.when(last)
    def _():
        for c in range(nc):
            t_copy(c).start()

    for idx in range(4):
        w_local(idx).start()

    odd = lax.rem(st, 2) == 1
    early = st < 2

    @pl.when(odd)
    def _():
        pl.semaphore_wait(go_sem, 1)

    w_own(W_Q)
    w_local(W_O).wait()
    woT[:, rowsl(me * orows, orows, orows)] = jnp.transpose(wo[rowsl(me * orows, orows, orows), :])
    w_own(W_O)
    w_local(W_U).wait()
    wuT[rowsl(me * fl, fl, fl), :] = jnp.transpose(wu[:, rowsl(me * fl, fl, fl)])
    w_local(W_Q).wait()
    w_forward(W_Q)
    w_own(W_U)
    w_local(W_D).wait()
    wdT[:, rowsl(me * fl, fl, fl)] = jnp.transpose(wd[rowsl(me * fl, fl, fl), :])
    w_forward(W_O)
    w_own(W_D)

    def pass_go():
        @pl.when(jnp.logical_not(odd))
        def _():
            pl.semaphore_signal(go_sem, inc=1, device_id={"stage": nxt}, device_id_type=MESH)

    def natural_weights():
        @pl.loop(0, nm)
        def _(f):
            wu[:, rowsl(f * fl, fl, fl)] = jnp.transpose(wuT[rowsl(f * fl, fl, fl), :])
            wd[rowsl(f * fl, fl, fl), :] = jnp.transpose(wdT[:, rowsl(f * fl, fl, fl)])
            wo[rowsl(f * orows, orows, orows), :] = jnp.transpose(woT[:, rowsl(f * orows, orows, orows)])
            wq[:, rowsl(f * qrows, qrows, qrows)] = jnp.transpose(wqT[rowsl(f * qrows, qrows, qrows), :])

    late = st >= max(2, ns // 2)

    @pl.when(jnp.logical_not(early))
    def _():
        w_forward(W_U)
        w_forward(W_D)
        pass_go()
        for idx in range(4):
            w_wait(idx)

    @pl.when(late)
    def _():
        natural_weights()

    def f_copy(c):
        return pltpu.make_async_remote_copy(
            src_ref=ybuf.at[c], dst_ref=hbuf.at[c], send_sem=fsend.at[c], recv_sem=frecv.at[c],
            device_id={"stage": nxt}, device_id_type=MESH)

    def b_copy(c):
        return pltpu.make_async_remote_copy(
            src_ref=ybuf.at[c], dst_ref=dybuf.at[c], send_sem=bsend.at[c], recv_sem=brecv.at[c],
            device_id={"stage": prv}, device_id_type=MESH)

    def ring_copy(src, dst, send, recv, way):
        return pltpu.make_async_remote_copy(
            src_ref=src, dst_ref=dst, send_sem=send, recv_sem=recv,
            device_id={"model": peer((plus, minus)[way % 2])}, device_id_type=MESH)

    hf = fl // 2

    def z_copy(c, way):
        if way < 2:
            src, dst = zbuf.at[c, rowsl(peer((plus, minus)[way]) * fl, fl, fl), :], z_recv.at[way, c]
        elif way < 4:
            src, dst = zbuf.at[c, rowsl(peer(far) * fl + (way - 2) * hf, hf, hf), :], z_fwd.at[way - 2, c]
        else:
            src, dst = z_fwd.at[way - 4, c], z_recv.at[2, c, pl.ds((way - 4) * hf, hf)]
        return ring_copy(src, dst, z_send.at[way, c], z_arr.at[way, c], way)

    def z_forward(c):
        for way in (2, 3):
            z_copy(c, way).wait_recv()
        for way in (4, 5):
            z_copy(c, way).start()

    def dy_copy(c, way):
        if way < 2:
            src, dst = dybuf.at[c], dy_recv.at[way, c]
        else:
            rows = pl.ds((way - 2) * (dm_ // 2), dm_ // 2)
            src, dst = dy_recv.at[way - 2, c, rows], dy_recv.at[2, c, rows]
        return ring_copy(src, dst, dy_send.at[way, c], dy_arr.at[way, c], way)

    def dy_forward(c):
        for way in (0, 1):
            dy_copy(c, way).wait_recv()
        for way in (2, 3):
            dy_copy(c, way).start()

    lossv[...] = jnp.zeros_like(lossv)

    def head_rows(p, h, part):
        return pl.ds(p * (2 * 3 * hd) + (h * 3 + part) * hd, hd)

    k_lane = (0, 2 * 2 * hd)
    v_lane = (2 * hd, 2 * 2 * hd)
    two = 2 * hd

    def pad_k(val, h):
        zero = jnp.zeros_like(val)
        return jnp.concatenate([zero, val] if h == 0 else [val, zero], axis=0)

    def pad_v(val, h):
        zero = jnp.zeros_like(val)
        return jnp.concatenate([val, zero] if h == 0 else [zero, val], axis=0)

    def causal(shape, row0):
        return lax.broadcasted_iota(jnp.int32, shape, 0) + row0 <= lax.broadcasted_iota(jnp.int32, shape, 1)

    def attention(cc):
        nk = (cc + 1) * tc
        slots = min(heads, sscr.shape[0] // nk)
        ahead = min(4, slots - 1)
        sub = tc // 2

        def front(head):
            p, h = head // 2, head % 2
            base = (head % slots) * nk
            qz = pad_k(qkv[cc, head_rows(p, h, 0), :], h)
            tops, sums = [], []
            for j in range(cc + 1):
                s = dot(qkvn[p, pl.ds(j * tc, tc), pl.ds(k_lane[h], two)], qz)
                for r in range(0, tc, sub):
                    part = s[r:r + sub]
                    if j == cc:
                        part = jnp.where(causal(part.shape, r), part, NEG)
                    top = jnp.max(part, axis=0, keepdims=True)
                    e = jnp.exp2((part - top) * exp_c)
                    sscr[pl.ds(base + j * tc + r, sub), :] = e
                    tops.append(top)
                    sums.append(jnp.sum(e, axis=0, keepdims=True))
            mx = functools.reduce(jnp.maximum, tops)
            scales = [jnp.exp2((top - mx) * exp_c) for top in tops]
            inv = 1.0 / functools.reduce(jnp.add, [a * b for a, b in zip(scales, sums)])
            return [a * inv for a in scales]

        def back(head, factors):
            p, h = head // 2, head % 2
            base = (head % slots) * nk
            o_t = None
            for j in range(cc + 1):
                parts = []
                for i in range(2):
                    pr = (sscr[pl.ds(base + j * tc + i * sub, sub), :] * factors[2 * j + i]).astype(BF16)
                    pbuf[cc * (cc + 1) // 2 + j, head, pl.ds(i * sub, sub), :] = pr
                    parts.append(pr)
                part = dot(qkv[j, head_rows(p, h, 2), :], jnp.concatenate(parts, axis=0))
                o_t = part if o_t is None else o_t + part
            obuf[cc, pl.ds(head * hd, hd), :] = o_t.astype(BF16)

        factors = {}
        for head in range(ahead):
            factors[head] = front(head)
        for head in range(heads):
            if head + ahead < heads:
                factors[head + ahead] = front(head + ahead)
            back(head, factors.pop(head))

    def attention_grad(cc):
        units = [(p, j) for p in range(heads // 2) for j in range(cc + 1)]
        dqs = {}
        held = {}

        def of_head(p, h):
            if (p, h) not in held:
                rows = pl.ds((p * 2 + h) * hd, hd)
                do_t = dobuf[rows, :]
                dsum = jnp.sum(do_t.astype(F32) * obuf[cc, rows, :].astype(F32), axis=0, keepdims=True)
                held[p, h] = (pad_v(do_t, h), dsum)
            return held[p, h]

        def front(p, j):
            out = []
            for h in range(2):
                do_z, dsum = of_head(p, h)
                pr = pbuf[cc * (cc + 1) // 2 + j, p * 2 + h]
                dp = dot(qkvn[p, pl.ds(j * tc, tc), pl.ds(v_lane[h], two)], do_z).astype(BF16).astype(F32)
                out.append((pr.astype(F32) * (dp - dsum)).astype(BF16))
            return out

        def back(p, j, ds):
            dv_new = dk_new = None
            for h in range(2):
                do_z, _ = of_head(p, h)
                dv_h = dot_t(pbuf[cc * (cc + 1) // 2 + j, p * 2 + h], do_z)
                dk_h = dot_t(ds[h], pad_v(qkv[cc, head_rows(p, h, 0), :], h))
                dv_new = dv_h if dv_new is None else dv_new + dv_h
                dk_new = dk_h if dk_new is None else dk_new + dk_h
                dq_h = dot(qkv[j, head_rows(p, h, 1), :], ds[h])
                dqs[p, h] = dq_h if j == 0 else dqs[p, h] + dq_h
            rows = pl.ds(j * tc, tc)
            if cc < nc - 1:
                dv_new = dv_new + dvacc[p, rows, :]
                dk_new = dk_new + dkacc[p, rows, :]
            if j < cc:
                dvacc[p, rows, :] = dv_new
                dkacc[p, rows, :] = dk_new
                return
            dv_t = jnp.transpose(dv_new).astype(BF16)
            dk_t = (jnp.transpose(dk_new) * scale).astype(BF16)
            for h in range(2):
                qkv[cc, head_rows(p, h, 0), :] = (dqs[p, h] * scale).astype(BF16)
                qkv[cc, head_rows(p, h, 1), :] = dk_t[h * hd:(h + 1) * hd, :]
                qkv[cc, head_rows(p, h, 2), :] = dv_t[h * hd:(h + 1) * hd, :]

        ds = front(*units[0])
        for n, unit in enumerate(units):
            later = front(*units[n + 1]) if n + 1 < len(units) else None
            back(*unit, ds)
            ds = later

    def attention_step(c):
        @pl.when(first)
        def _():
            x_copy(c).wait()
            hbuf[c] = jnp.transpose(xin[c])

        @pl.when(jnp.logical_not(first))
        def _():
            f_copy(c).wait_recv()

        @pl.when(early & (c == 0))
        def _():
            w_wait(W_Q)

        h32 = hbuf[c].astype(F32)
        n1 = (h32 * inv_rms(h32)).astype(BF16)
        n1buf[c] = n1
        for r in range(nm):
            rows = pl.ds(r * qrows, qrows)
            blk = dot(wqT[rows, :], n1).astype(BF16)
            qkv[c, rows, :] = blk
            qkvn[r, pl.ds(pl.multiple_of(c * tc, tc), tc), :] = jnp.transpose(blk)

        for cc in range(nc):
            pl.when(c == cc)(functools.partial(attention, cc))

    def mlp_step(c):
        a = dot(woT[...], obuf[c]).astype(BF16)
        m32 = (hbuf[c].astype(F32) + a.astype(F32)).astype(BF16).astype(F32)
        mbuf[c] = m32.astype(BF16)
        n2 = (m32 * inv_rms(m32)).astype(BF16)
        n2buf[c] = n2

        blk = fl // 2
        for f in range(2 * nm):
            rows = pl.ds(f * blk, blk)
            u = dot(wuT[rows, :], n2buf[c]).astype(BF16)
            ubuf[c, rows, :] = u
            zbuf[c, rows, :] = gelu(u.astype(F32)).astype(BF16)
        for way in range(4):
            z_copy(c, way).start()
        acc = dot(wdT[...], zbuf[c])
        y32 = (mbuf[c].astype(F32) + acc.astype(BF16).astype(F32)).astype(BF16)
        ybuf[c] = y32

        @pl.when(jnp.logical_not(last))
        def _():
            f_copy(c).start()

        @pl.when(last)
        def _():
            t_copy(c).wait()
            err = ybuf[c].astype(F32) - jnp.transpose(xin[c]).astype(F32)
            lossv[...] += jnp.sum((err * err).reshape(dm_ // 8, 8, tc), axis=0)
            dybuf[c] = (err * inv_d).astype(BF16)

    @pl.loop(0, 2 * nc)
    def _(n):
        attn_turn = jnp.where(early, jnp.where(n < nc, 1, 0), 1 - lax.rem(n, 2))
        c = jnp.where(early, lax.rem(n, nc), n // 2)

        @pl.when(early & (n == 2))
        def _():
            w_forward(W_U)

        @pl.when(early & (n == min(3, nc)))
        def _():
            w_forward(W_D)
            pass_go()

        @pl.when(attn_turn == 1)
        def _():
            attention_step(c)

        @pl.when(early & (n == nc))
        def _():
            w_wait(W_O)
            w_wait(W_U)
            w_wait(W_D)

        @pl.when(attn_turn == 0)
        def _():
            mlp_step(c)

    @pl.when(jnp.logical_not(late))
    def _():
        natural_weights()
        for c in range(nc):
            z_forward(c)

    def l_copy(k):
        return pltpu.make_async_remote_copy(
            src_ref=losst.at[nm], dst_ref=losst.at[3 - k if nm == 4 else nm - 1 - k], send_sem=lsend.at[k - 1],
            recv_sem=lrecv.at[k - 1], device_id={"model": peer(k)}, device_id_type=MESH)

    def lf_copy():
        return pltpu.make_async_remote_copy(
            src_ref=losst.at[nm + 1], dst_ref=losst.at[nm + 1], send_sem=lfsend, recv_sem=lfrecv,
            device_id={"stage": prv}, device_id_type=MESH)

    @pl.when(last)
    def _():
        tot = jnp.sum(lossv[...]) * (0.5 * inv_d)
        losst[nm] = jnp.full(losst.shape[1:], tot, F32)
        for k in range(1, nm):
            l_copy(k).start()

    delay = jnp.where(late, 2, 1)

    @pl.loop(0, nc)
    def _(i):
        c = nc - 1 - i

        @pl.when(jnp.logical_not(last))
        def _():
            b_copy(c).wait_recv()

        for way in range(2):
            dy_copy(c, way).start()

        blk = fl // 4
        for f in range(4 * nm):
            rows = pl.ds(f * blk, blk)
            dz = dot(wd[rows, :], dybuf[c]).astype(BF16).astype(F32)
            ubuf[c, rows, :] = (dz * gelu_grad(ubuf[c, rows, :].astype(F32))).astype(BF16)
        acc = dot(wu[...], ubuf[c])
        dn2 = acc.astype(BF16).astype(F32)
        m32 = mbuf[c].astype(F32)
        pull = norm_pull(m32, inv_rms(m32), dn2).astype(BF16)
        dmid = (dybuf[c].astype(F32) + pull.astype(F32)).astype(BF16)
        mbuf[c] = dmid
        dobuf[...] = dot(wo[...], dmid).astype(BF16)

        for cc in range(nc):
            pl.when(c == cc)(functools.partial(attention_grad, cc))

        dn1 = dot(wq[...], qkv[c]).astype(BF16).astype(F32)
        h32 = hbuf[c].astype(F32)
        pull1 = norm_pull(h32, inv_rms(h32), dn1).astype(BF16)

        @pl.when(jnp.logical_not(last))
        def _():
            f_copy(c).wait_send()

        ybuf[c] = (mbuf[c].astype(F32) + pull1.astype(F32)).astype(BF16)

        @pl.when(jnp.logical_not(first))
        def _():
            b_copy(c).start()

        @pl.when(late)
        def _():
            z_forward(i)

        @pl.when(c + delay < nc)
        def _():
            dy_forward(c + delay)

    for c in range(2):
        @pl.when(c < delay)
        def _():
            dy_forward(c)

    @pl.when(last)
    def _():
        for k in range(1, nm):
            l_copy(k).wait_recv()
        vals = [losst[nm]] + [losst[k - 1] for k in range(1, nm)]
        tot = jnp.zeros_like(vals[0])
        for who in range(nm):
            pick = vals[0]
            for k in range(1, nm):
                pick = jnp.where(peer(k) == who, vals[k], pick)
            tot = tot + pick
        losst[nm + 1] = tot

    @pl.when(jnp.logical_not(last))
    def _():
        lf_copy().wait_recv()

    @pl.when(jnp.logical_not(first))
    def _():
        lf_copy().start()

    loss_out[...] = losst[nm + 1]

    def wgrad(mat, d):
        acc = None
        for c in range(nc):
            if mat == 0:
                part = dot_t(qkv[c, rowsl(d * qrows, qrows, qrows), :], n1buf[c])
            elif mat == 1:
                part = dot_t(obuf[c, rowsl(d * orows, orows, orows), :], mbuf[c])
            elif mat == 2:
                part = dot_t(n2buf[c], ubuf[c, rowsl(d * fl, fl, fl), :])
            else:
                part = dot_t(zbuf[c, rowsl(d * fl, fl, fl), :], dybuf[c])
            acc = part if acc is None else acc + part
        return acc

    sizes = (qrows, orows, dm_)
    offs = (0, qrows, qrows + orows)

    def rows_of(mat):
        return pl.ds(offs[mat], sizes[mat])

    def half_of(mat, half):
        return pl.ds(offs[mat] + half * (sizes[mat] // 2), sizes[mat] // 2)

    def far_copy(mat, half):
        rows = pl.ds(offs[mat] // 2, sizes[mat] // 2)
        return ring_copy(stage_buf.at[0, half_of(mat, half)], (far_p, far_m)[half].at[rows],
                         rs_send.at[mat, half], rs_recv.at[mat, half], half)

    def near_copy(mat, side, half):
        way = 2 + 2 * side + half
        return ring_copy(stage_buf.at[1 + side, half_of(mat, half)], (near_l if side == half else near_e).at[half_of(mat, half)],
                         rs_send.at[mat, way], rs_recv.at[mat, way], side)

    mats = (2, 0, 1)
    for mat in mats:
        stage_buf[0, rows_of(mat)] = wgrad(mat, peer(far))
        for half in range(2):
            far_copy(mat, half).start()
    for mat in mats:
        for side in range(2):
            stage_buf[1 + side, rows_of(mat)] = wgrad(mat, peer((plus, minus)[side]))
            near_copy(mat, side, 1 - side).start()

    def load(src, nr):
        return pltpu.make_async_copy(src, radd.at[pl.ds(0, nr)], ld_sem.at[0])

    for mat in mats:
        nr = sizes[mat] // 2
        for half in range(2):
            far_copy(mat, half).wait_recv()
            src = (far_p, far_m)[half].at[pl.ds(offs[mat] // 2, nr)]
            load(src, nr).start()
            load(src, nr).wait()
            stage_buf[1 + half, half_of(mat, half)] += radd[pl.ds(0, nr)]
            near_copy(mat, half, half).start()

    for mat in mats:
        for half in range(2):
            far_copy(mat, half).wait_send()
        stage_buf[0, rows_of(mat)] = wgrad(mat, me)

    def zdy_load(n, buf):
        slot, c = n // nc, lax.rem(n, nc)
        return (pltpu.make_async_copy(z_recv.at[slot, c], zdy.at[buf, pl.ds(0, fl)], ld_sem.at[1 + buf]),
                pltpu.make_async_copy(dy_recv.at[slot, c], zdy.at[buf, pl.ds(fl, dm_)], ld_sem.at[3 + buf]))

    gdacc[...] = wgrad(3, me)
    for c in range(nc):
        for way in (0, 1, 4, 5):
            z_copy(c, way).wait_recv()
        for way in (2, 3):
            dy_copy(c, way).wait_recv()
    for cp in zdy_load(0, 0):
        cp.start()

    @pl.loop(0, 3 * nc)
    def _(n):
        buf = lax.rem(n, 2)

        @pl.when(n + 1 < 3 * nc)
        def _():
            for cp in zdy_load(n + 1, 1 - buf):
                cp.start()

        for cp in zdy_load(n, buf):
            cp.wait()
        gdacc[...] += dot_t(zdy[buf, pl.ds(0, fl), :], zdy[buf, pl.ds(fl, dm_), :])

    def out_copy(mat):
        if mat == 3:
            return pltpu.make_async_copy(gdacc, sum_out.at[pl.ds(qrows + orows + dm_, fl)], out_sem.at[3])
        return pltpu.make_async_copy(stage_buf.at[0, rows_of(mat)], sum_out.at[rows_of(mat)], out_sem.at[mat])

    out_copy(3).start()
    for mat in mats:
        nr = sizes[mat] // 2
        for side in range(2):
            near_copy(mat, side, 1 - side).wait_recv()
            load(near_e.at[half_of(mat, 1 - side)], nr).start()
            load(near_e.at[half_of(mat, 1 - side)], nr).wait()
            stage_buf[0, half_of(mat, 1 - side)] += radd[pl.ds(0, nr)]
        out_copy(mat).start()
    for mat in mats:
        for side in range(2):
            near_copy(mat, side, side).wait_recv()

    for mat in range(4):
        out_copy(mat).wait()
    for c in range(nc):
        for way in range(6):
            z_copy(c, way).wait_send()
        for way in range(4):
            dy_copy(c, way).wait_send()
    for idx in range(4):
        for way in range(4):
            w_copy(idx, way).wait_send()
    for mat in mats:
        for half in range(2):
            for side in range(2):
                near_copy(mat, side, half).wait_send()

    @pl.when(jnp.logical_not(first))
    def _():
        for c in range(nc):
            b_copy(c).wait_send()
        lf_copy().wait_send()

    @pl.when(last)
    def _():
        for k in range(1, nm):
            l_copy(k).wait_send()


def finish_kernel(sq, so, su, sd, lq, lo, lu, loss, gq, go, gu, gd, loss_out):
    gq[...] = sq[...] + lq[...]
    go[...] = so[...] + lo[...]
    gu[...] = su[...] + lu[...]
    gd[...] = sd[...]
    loss_out[0] = loss[0, 0]


def solution(mesh):
    ns = mesh.shape["stage"]
    nm = mesh.shape["model"]

    def per_device(tokens_in, targets, w_qkv, w_out, w_up, w_down):
        n_micro, seq_len, d_model = tokens_in.shape
        hl, hd, fl = w_qkv.shape[3], w_qkv.shape[5], w_up.shape[3]
        tc = min(CHUNK, seq_len // 2)
        nc = seq_len // tc
        assert n_micro == nm == 4 and w_qkv.shape[1] == 1 and hl == 2
        qrows, orows = hl * 3 * hd, hl * hd
        wqT = jnp.transpose(w_qkv[0, 0], (1, 2, 3, 0)).reshape(qrows, d_model)
        wo = w_out[0, 0].reshape(orows, d_model)
        wu, wd = w_up[0, 0], w_down[0, 0]
        cfg = (ns, nm, nc, tc, d_model, hl, hd, fl)
        heads = nm * hl
        any_spec = pl.BlockSpec(memory_space=pl.ANY)
        f32 = lambda *shape: jax.ShapeDtypeStruct(shape, F32)
        rsum = qrows + orows + d_model
        seqb = nc * tc
        b16 = lambda *shape: jax.ShapeDtypeStruct(shape, BF16)
        out_shape = (f32(rsum + fl, d_model), f32(8, 128), f32(rsum // 2, d_model), f32(rsum // 2, d_model), f32(rsum, d_model),
                     f32(rsum, d_model), b16(3, nc, fl, tc), b16(2, nc, fl // 2, tc), b16(3, nc, d_model, tc))
        vb = lambda *shape: pltpu.VMEM(shape, BF16)
        vf = lambda *shape: pltpu.VMEM(shape, F32)
        dma = lambda *shape: pltpu.SemaphoreType.DMA(shape)
        scratch = [
            vb(nm * qrows, d_model), vb(d_model, nm * orows), vb(nm * fl, d_model), vb(d_model, nm * fl),
            vb(nm * fl, d_model), vb(d_model, nm * fl), vb(nm * orows, d_model), vb(d_model, nm * qrows),
            vb(nc, tc, d_model), vb(nc, d_model, tc), vb(nc, d_model, tc), vb(nc, nm * qrows, tc), vb(nm, seqb, qrows),
            vb(nc, nm * orows, tc), vb(nc, d_model, tc), vb(nc, d_model, tc), vb(nc, nm * fl, tc), vb(nc, nm * fl, tc),
            vb(nc * (nc + 1) // 2, heads, tc, tc), vb(nc, d_model, tc), vf(heads // 2, seqb, 2 * hd), vf(heads // 2, seqb, 2 * hd),
            vf(2 * seqb, tc), vb(nc, d_model, tc), vb(nm * orows, tc), vf(nm + 2, 8, 128), vf(8, tc),
            vf(3, rsum, d_model), vf(256, d_model), vf(fl, d_model), vb(2, fl + d_model, tc),
            dma(4, 4), dma(4, 4), dma(4), pltpu.SemaphoreType.REGULAR, dma(nc), dma(nc), dma(nc), dma(nc), dma(nc),
            dma(nm - 1), dma(nm - 1), pltpu.SemaphoreType.DMA, pltpu.SemaphoreType.DMA,
            dma(3, 6), dma(3, 6), dma(5), dma(4), dma(6, nc), dma(6, nc), dma(4, nc), dma(4, nc),
        ]
        res = pl.pallas_call(
            functools.partial(step_kernel, cfg),
            out_shape=out_shape,
            in_specs=[any_spec] * 6,
            out_specs=[any_spec, pl.BlockSpec(memory_space=pltpu.VMEM)] + [any_spec] * 7,
            scratch_shapes=scratch,
            compiler_params=pltpu.CompilerParams(collective_id=0, has_side_effects=True, vmem_limit_bytes=67043328),
            name="train_step",
        )(tokens_in, targets, wqT, wo, wu, wd)
        part, loss, late = res[0], res[1], res[5]
        steps = 4

        def spec(size, start):
            rows = size // steps
            return pl.BlockSpec((rows, d_model), lambda i: (start // rows + i, 0))

        q_s, o_s, u_s = spec(qrows, 0), spec(orows, qrows), spec(d_model, qrows + orows)
        g_qkv, g_out, g_up, g_down, loss = pl.pallas_call(
            finish_kernel,
            grid=(steps,),
            out_shape=(f32(qrows, d_model), f32(orows, d_model), f32(d_model, fl), f32(fl, d_model), f32(1)),
            in_specs=[q_s, o_s, u_s, spec(fl, rsum), q_s, o_s, u_s, pl.BlockSpec(memory_space=pltpu.SMEM)],
            out_specs=[spec(qrows, 0), spec(orows, 0), spec(d_model, 0), spec(fl, 0), pl.BlockSpec(memory_space=pltpu.SMEM)],
            name="finish",
        )(part, part, part, part, late, late, late, loss)
        g_qkv = jnp.transpose(g_qkv.reshape(hl, 3, hd, d_model), (3, 0, 1, 2))[None, None]
        return g_qkv, g_out.reshape(1, 1, hl, hd, d_model), g_up[None, None], g_down[None, None], loss

    tok_spec = P(None, "data", None)
    qkv_spec = P("stage", None, None, "model", None, None)
    out_spec = P("stage", None, "model", None, None)
    up_spec = P("stage", None, None, "model")
    down_spec = P("stage", None, "model", None)
    g_qkv_spec = P(("data", "stage"), None, None, "model", None, None)
    g_out_spec = P(("data", "stage"), None, "model", None, None)
    g_up_spec = P(("data", "stage"), None, None, "model")
    g_down_spec = P(("data", "stage"), None, "model", None)
    return jax.shard_map(per_device, mesh=mesh, in_specs=(tok_spec, tok_spec, qkv_spec, out_spec, up_spec, down_spec), out_specs=(g_qkv_spec, g_out_spec, g_up_spec, g_down_spec, P("data")), check_vma=False)
```

```python
import functools
import math

import jax
import jax.numpy as jnp
from jax import lax
from jax.experimental import pallas as pl
from jax.experimental.pallas import tpu as pltpu
from jax.sharding import PartitionSpec as P

F32 = jnp.float32
BF16 = jnp.bfloat16
MESH = pl.DeviceIdType.MESH
CHUNK = 256
NEG = -1e30
GELU_C = math.sqrt(2.0 / math.pi)
GELU_A = 0.044715

W_Q, W_O, W_U, W_D = range(4)


def dot(lhs, rhs):
    return jnp.dot(lhs, rhs, preferred_element_type=F32)


def dot_t(lhs, rhs):
    return lax.dot_general(lhs, rhs, (((1,), (1,)), ((), ())), preferred_element_type=F32)


def inv_rms(x32):
    return lax.rsqrt(jnp.mean(x32 * x32, axis=0, keepdims=True) + 1e-6)


def norm_pull(x32, inv, g32):
    mean_gx = jnp.mean(g32 * x32, axis=0, keepdims=True)
    return g32 * inv - x32 * (inv * inv * inv * mean_gx)


def gelu(u):
    tanh = jnp.tanh(u * (GELU_C + (GELU_C * GELU_A) * (u * u)))
    half = 0.5 * u
    return half + half * tanh


def gelu_grad(u):
    u2 = u * u
    sig = 0.5 + 0.5 * jnp.tanh(u * (GELU_C + (GELU_C * GELU_A) * u2))
    slope = u * (2.0 * GELU_C + (6.0 * GELU_C * GELU_A) * u2)
    return sig * (1.0 + slope * (1.0 - sig))


def step_kernel(cfg, x_hbm, t_hbm, wqT_in, wo_in, wu_in, wd_in,
                sum_out, loss_out, far_p, far_m, near_e, near_l, z_recv, z_fwd, dy_recv,
                wqT, woT, wuT, wdT, wd, wu, wo, wq,
                xin, hbuf, n1buf, qkv, qkvn, obuf, mbuf, n2buf, ubuf, zbuf, pbuf, dybuf, dvacc, dkacc, sscr,
                ybuf, dobuf, losst, lossv, stage_buf, radd, gdacc, zdy,
                ag_send, ag_recv, ag_loc, go_sem, xsem, fsend, frecv, bsend, brecv, lsend, lrecv, lfsend, lfrecv,
                rs_send, rs_recv, ld_sem, out_sem, z_send, z_arr, dy_send, dy_arr):
    ns, nm, nc, tc, dm_, hl, hd, fl = cfg
    heads = nm * hl
    qrows = hl * 3 * hd
    orows = hl * hd
    inv_d = 1.0 / (nm * nc * tc * dm_)
    scale = hd ** -0.5
    exp_c = scale * math.log2(math.e)
    me = lax.axis_index("model")
    st = lax.axis_index("stage")
    nxt = lax.rem(st + 1, ns)
    prv = lax.rem(st + ns - 1, ns)
    first = st == 0
    last = st == ns - 1

    def peer(k):
        return lax.rem(me + k, nm)

    bar = pltpu.get_barrier_semaphore()
    pl.semaphore_signal(bar, inc=1, device_id={"stage": nxt}, device_id_type=MESH)
    pl.semaphore_signal(bar, inc=1, device_id={"stage": prv}, device_id_type=MESH)
    for k in range(1, nm):
        pl.semaphore_signal(bar, inc=1, device_id={"model": peer(k)}, device_id_type=MESH)
    pl.semaphore_wait(bar, 2 + nm - 1)

    def rowsl(start, size, mult):
        return pl.ds(pl.multiple_of(start, mult), size)

    plus, minus, far = 1, nm - 1, 2

    def w_rows(idx, who, half=None):
        size = (qrows, orows, fl, fl)[idx]
        if idx in (W_Q, W_U):
            buf = wqT if idx == W_Q else wuT
            if half is None:
                return buf.at[rowsl(who * size, size, size), :]
            return buf.at[rowsl(who * size + half * (size // 2), size // 2, size // 2), :]
        view = (woT if idx == W_O else wdT).at[:, rowsl(who * size, size, size)]
        return view if half is None else view.at[pl.ds(half * (dm_ // 2), dm_ // 2), :]

    def w_copy(idx, way):
        to = plus if way in (0, 2) else minus
        if way < 2:
            src = wqT_in if idx == W_Q else w_rows(idx, me)
            dst = w_rows(idx, me)
        else:
            src = dst = w_rows(idx, peer(minus if way == 2 else plus), way - 2)
        return pltpu.make_async_remote_copy(
            src_ref=src, dst_ref=dst, send_sem=ag_send.at[idx, way], recv_sem=ag_recv.at[idx, way],
            device_id={"model": peer(to)}, device_id_type=MESH)

    def w_arrival(idx, way):
        who = peer((minus, plus, far, far)[way])
        ref = w_rows(idx, who) if way < 2 else w_rows(idx, who, way - 2)
        return pltpu.make_async_remote_copy(
            src_ref=ref, dst_ref=ref, send_sem=ag_send.at[idx, way], recv_sem=ag_recv.at[idx, way],
            device_id={"model": peer(plus)}, device_id_type=MESH)

    def w_local(idx):
        src = (wqT_in, wo_in, wu_in, wd_in)[idx]
        dst = (w_rows(W_Q, me), wo.at[rowsl(me * orows, orows, orows), :], wu.at[:, rowsl(me * fl, fl, fl)], wd.at[rowsl(me * fl, fl, fl), :])[idx]
        return pltpu.make_async_copy(src, dst, ag_loc.at[idx])

    def w_own(idx):
        for way in range(2):
            w_copy(idx, way).start()

    def w_forward(idx):
        for way in range(2):
            w_arrival(idx, way).wait_recv()
        for way in range(2, 4):
            w_copy(idx, way).start()

    def w_wait(idx):
        for way in range(2, 4):
            w_arrival(idx, way).wait_recv()

    def x_copy(c):
        return pltpu.make_async_copy(x_hbm.at[me, pl.ds(c * tc, tc), :], xin.at[c], xsem.at[c])

    def t_copy(c):
        return pltpu.make_async_copy(t_hbm.at[me, pl.ds(c * tc, tc), :], xin.at[c], xsem.at[c])

    @pl.when(first)
    def _():
        for c in range(nc):
            x_copy(c).start()

    @pl.when(last)
    def _():
        for c in range(nc):
            t_copy(c).start()

    for idx in range(4):
        w_local(idx).start()

    odd = lax.rem(st, 2) == 1
    early = st < 2

    @pl.when(odd)
    def _():
        pl.semaphore_wait(go_sem, 1)

    w_own(W_Q)
    w_local(W_O).wait()
    woT[:, rowsl(me * orows, orows, orows)] = jnp.transpose(wo[rowsl(me * orows, orows, orows), :])
    w_own(W_O)
    w_local(W_U).wait()
    wuT[rowsl(me * fl, fl, fl), :] = jnp.transpose(wu[:, rowsl(me * fl, fl, fl)])
    w_local(W_Q).wait()
    w_forward(W_Q)
    w_own(W_U)
    w_local(W_D).wait()
    wdT[:, rowsl(me * fl, fl, fl)] = jnp.transpose(wd[rowsl(me * fl, fl, fl), :])
    w_forward(W_O)
    w_own(W_D)

    def pass_go():
        @pl.when(jnp.logical_not(odd))
        def _():
            pl.semaphore_signal(go_sem, inc=1, device_id={"stage": nxt}, device_id_type=MESH)

    def natural_weights():
        @pl.loop(0, nm)
        def _(f):
            wu[:, rowsl(f * fl, fl, fl)] = jnp.transpose(wuT[rowsl(f * fl, fl, fl), :])
            wd[rowsl(f * fl, fl, fl), :] = jnp.transpose(wdT[:, rowsl(f * fl, fl, fl)])
            wo[rowsl(f * orows, orows, orows), :] = jnp.transpose(woT[:, rowsl(f * orows, orows, orows)])
            wq[:, rowsl(f * qrows, qrows, qrows)] = jnp.transpose(wqT[rowsl(f * qrows, qrows, qrows), :])

    late = st >= max(2, ns // 2)

    @pl.when(jnp.logical_not(early))
    def _():
        w_forward(W_U)
        w_forward(W_D)
        pass_go()
        for idx in range(4):
            w_wait(idx)

    @pl.when(late)
    def _():
        natural_weights()

    def f_copy(c):
        return pltpu.make_async_remote_copy(
            src_ref=ybuf.at[c], dst_ref=hbuf.at[c], send_sem=fsend.at[c], recv_sem=frecv.at[c],
            device_id={"stage": nxt}, device_id_type=MESH)

    def b_copy(c):
        return pltpu.make_async_remote_copy(
            src_ref=ybuf.at[c], dst_ref=dybuf.at[c], send_sem=bsend.at[c], recv_sem=brecv.at[c],
            device_id={"stage": prv}, device_id_type=MESH)

    def ring_copy(src, dst, send, recv, way):
        return pltpu.make_async_remote_copy(
            src_ref=src, dst_ref=dst, send_sem=send, recv_sem=recv,
            device_id={"model": peer((plus, minus)[way % 2])}, device_id_type=MESH)

    hf = fl // 2

    def z_copy(c, way):
        if way < 2:
            src, dst = zbuf.at[c, rowsl(peer((plus, minus)[way]) * fl, fl, fl), :], z_recv.at[way, c]
        elif way < 4:
            src, dst = zbuf.at[c, rowsl(peer(far) * fl + (way - 2) * hf, hf, hf), :], z_fwd.at[way - 2, c]
        else:
            src, dst = z_fwd.at[way - 4, c], z_recv.at[2, c, pl.ds((way - 4) * hf, hf)]
        return ring_copy(src, dst, z_send.at[way, c], z_arr.at[way, c], way)

    def z_forward(c):
        for way in (2, 3):
            z_copy(c, way).wait_recv()
        for way in (4, 5):
            z_copy(c, way).start()

    def dy_copy(c, way):
        if way < 2:
            src, dst = dybuf.at[c], dy_recv.at[way, c]
        else:
            rows = pl.ds((way - 2) * (dm_ // 2), dm_ // 2)
            src, dst = dy_recv.at[way - 2, c, rows], dy_recv.at[2, c, rows]
        return ring_copy(src, dst, dy_send.at[way, c], dy_arr.at[way, c], way)

    def dy_forward(c):
        for way in (0, 1):
            dy_copy(c, way).wait_recv()
        for way in (2, 3):
            dy_copy(c, way).start()

    lossv[...] = jnp.zeros_like(lossv)

    def head_rows(p, h, part):
        return pl.ds(p * (2 * 3 * hd) + (h * 3 + part) * hd, hd)

    k_lane = (0, 2 * 2 * hd)
    v_lane = (2 * hd, 2 * 2 * hd)
    two = 2 * hd

    def pad_k(val, h):
        zero = jnp.zeros_like(val)
        return jnp.concatenate([zero, val] if h == 0 else [val, zero], axis=0)

    def pad_v(val, h):
        zero = jnp.zeros_like(val)
        return jnp.concatenate([val, zero] if h == 0 else [zero, val], axis=0)

    def causal(shape, row0):
        return lax.broadcasted_iota(jnp.int32, shape, 0) + row0 <= lax.broadcasted_iota(jnp.int32, shape, 1)

    def attention(cc):
        nk = (cc + 1) * tc
        slots = min(heads, sscr.shape[0] // nk)
        ahead = min(4, slots - 1)
        sub = tc // 2

        def front(head):
            p, h = head // 2, head % 2
            base = (head % slots) * nk
            qz = pad_k(qkv[cc, head_rows(p, h, 0), :], h)
            tops, sums = [], []
            for j in range(cc + 1):
                s = dot(qkvn[p, pl.ds(j * tc, tc), pl.ds(k_lane[h], two)], qz)
                for r in range(0, tc, sub):
                    part = s[r:r + sub]
                    if j == cc:
                        part = jnp.where(causal(part.shape, r), part, NEG)
                    top = jnp.max(part, axis=0, keepdims=True)
                    e = jnp.exp2((part - top) * exp_c)
                    sscr[pl.ds(base + j * tc + r, sub), :] = e
                    tops.append(top)
                    sums.append(jnp.sum(e, axis=0, keepdims=True))
            mx = functools.reduce(jnp.maximum, tops)
            scales = [jnp.exp2((top - mx) * exp_c) for top in tops]
            inv = 1.0 / functools.reduce(jnp.add, [a * b for a, b in zip(scales, sums)])
            return [a * inv for a in scales]

        def back(head, factors):
            p, h = head // 2, head % 2
            base = (head % slots) * nk
            o_t = None
            for j in range(cc + 1):
                parts = []
                for i in range(2):
                    pr = (sscr[pl.ds(base + j * tc + i * sub, sub), :] * factors[2 * j + i]).astype(BF16)
                    pbuf[cc * (cc + 1) // 2 + j, head, pl.ds(i * sub, sub), :] = pr
                    parts.append(pr)
                part = dot(qkv[j, head_rows(p, h, 2), :], jnp.concatenate(parts, axis=0))
                o_t = part if o_t is None else o_t + part
            obuf[cc, pl.ds(head * hd, hd), :] = o_t.astype(BF16)

        factors = {}
        for head in range(ahead):
            factors[head] = front(head)
        for head in range(heads):
            if head + ahead < heads:
                factors[head + ahead] = front(head + ahead)
            back(head, factors.pop(head))

    def attention_grad(cc):
        units = [(p, j) for p in range(heads // 2) for j in range(cc + 1)]
        dqs = {}
        held = {}

        def of_head(p, h):
            if (p, h) not in held:
                rows = pl.ds((p * 2 + h) * hd, hd)
                do_t = dobuf[rows, :]
                dsum = jnp.sum(do_t.astype(F32) * obuf[cc, rows, :].astype(F32), axis=0, keepdims=True)
                held[p, h] = (pad_v(do_t, h), dsum)
            return held[p, h]

        def front(p, j):
            out = []
            for h in range(2):
                do_z, dsum = of_head(p, h)
                pr = pbuf[cc * (cc + 1) // 2 + j, p * 2 + h]
                dp = dot(qkvn[p, pl.ds(j * tc, tc), pl.ds(v_lane[h], two)], do_z).astype(BF16).astype(F32)
                out.append((pr.astype(F32) * (dp - dsum)).astype(BF16))
            return out

        def back(p, j, ds):
            dv_new = dk_new = None
            for h in range(2):
                do_z, _ = of_head(p, h)
                dv_h = dot_t(pbuf[cc * (cc + 1) // 2 + j, p * 2 + h], do_z)
                dk_h = dot_t(ds[h], pad_v(qkv[cc, head_rows(p, h, 0), :], h))
                dv_new = dv_h if dv_new is None else dv_new + dv_h
                dk_new = dk_h if dk_new is None else dk_new + dk_h
                dq_h = dot(qkv[j, head_rows(p, h, 1), :], ds[h])
                dqs[p, h] = dq_h if j == 0 else dqs[p, h] + dq_h
            rows = pl.ds(j * tc, tc)
            if cc < nc - 1:
                dv_new = dv_new + dvacc[p, rows, :]
                dk_new = dk_new + dkacc[p, rows, :]
            if j < cc:
                dvacc[p, rows, :] = dv_new
                dkacc[p, rows, :] = dk_new
                return
            dv_t = jnp.transpose(dv_new).astype(BF16)
            dk_t = (jnp.transpose(dk_new) * scale).astype(BF16)
            for h in range(2):
                qkv[cc, head_rows(p, h, 0), :] = (dqs[p, h] * scale).astype(BF16)
                qkv[cc, head_rows(p, h, 1), :] = dk_t[h * hd:(h + 1) * hd, :]
                qkv[cc, head_rows(p, h, 2), :] = dv_t[h * hd:(h + 1) * hd, :]

        ds = front(*units[0])
        for n, unit in enumerate(units):
            later = front(*units[n + 1]) if n + 1 < len(units) else None
            back(*unit, ds)
            ds = later

    def attention_step(c):
        @pl.when(first)
        def _():
            x_copy(c).wait()
            hbuf[c] = jnp.transpose(xin[c])

        @pl.when(jnp.logical_not(first))
        def _():
            f_copy(c).wait_recv()

        @pl.when(early & (c == 0))
        def _():
            w_wait(W_Q)

        h32 = hbuf[c].astype(F32)
        n1 = (h32 * inv_rms(h32)).astype(BF16)
        n1buf[c] = n1
        for r in range(nm):
            rows = pl.ds(r * qrows, qrows)
            blk = dot(wqT[rows, :], n1).astype(BF16)
            qkv[c, rows, :] = blk
            qkvn[r, pl.ds(pl.multiple_of(c * tc, tc), tc), :] = jnp.transpose(blk)

        for cc in range(nc):
            pl.when(c == cc)(functools.partial(attention, cc))

    def mlp_step(c):
        a = dot(woT[...], obuf[c]).astype(BF16)
        m32 = (hbuf[c].astype(F32) + a.astype(F32)).astype(BF16).astype(F32)
        mbuf[c] = m32.astype(BF16)
        n2 = (m32 * inv_rms(m32)).astype(BF16)
        n2buf[c] = n2

        blk = fl // 2
        for f in range(2 * nm):
            rows = pl.ds(f * blk, blk)
            u = dot(wuT[rows, :], n2buf[c]).astype(BF16)
            ubuf[c, rows, :] = u
            zbuf[c, rows, :] = gelu(u.astype(F32)).astype(BF16)
        acc = dot(wdT[...], zbuf[c])
        y32 = (mbuf[c].astype(F32) + acc.astype(BF16).astype(F32)).astype(BF16)
        ybuf[c] = y32

        @pl.when(jnp.logical_not(last))
        def _():
            f_copy(c).start()

        @pl.when(last)
        def _():
            t_copy(c).wait()
            err = ybuf[c].astype(F32) - jnp.transpose(xin[c]).astype(F32)
            lossv[...] += jnp.sum((err * err).reshape(dm_ // 8, 8, tc), axis=0)
            dybuf[c] = (err * inv_d).astype(BF16)

    @pl.loop(0, 2 * nc)
    def _(n):
        attn_turn = jnp.where(early, jnp.where(n < nc, 1, 0), 1 - lax.rem(n, 2))
        c = jnp.where(early, lax.rem(n, nc), n // 2)

        @pl.when(early & (n == 2))
        def _():
            w_forward(W_U)

        @pl.when(early & (n == min(3, nc)))
        def _():
            w_forward(W_D)
            pass_go()

        @pl.when(attn_turn == 1)
        def _():
            attention_step(c)

        @pl.when(early & (n == nc))
        def _():
            w_wait(W_O)
            w_wait(W_U)
            w_wait(W_D)

        @pl.when(attn_turn == 0)
        def _():
            mlp_step(c)

    def z_start():
        for c in range(nc):
            for way in range(4):
                z_copy(c, way).start()

    z_last = st >= ns - 2

    @pl.when(jnp.logical_not(z_last))
    def _():
        z_start()

    @pl.when(jnp.logical_not(late))
    def _():
        natural_weights()

    @pl.when(jnp.logical_not(z_last))
    def _():
        for c in range(nc):
            z_forward(c)

    def l_copy(k):
        return pltpu.make_async_remote_copy(
            src_ref=losst.at[nm], dst_ref=losst.at[3 - k if nm == 4 else nm - 1 - k], send_sem=lsend.at[k - 1],
            recv_sem=lrecv.at[k - 1], device_id={"model": peer(k)}, device_id_type=MESH)

    def lf_copy():
        return pltpu.make_async_remote_copy(
            src_ref=losst.at[nm + 1], dst_ref=losst.at[nm + 1], send_sem=lfsend, recv_sem=lfrecv,
            device_id={"stage": prv}, device_id_type=MESH)

    @pl.when(last)
    def _():
        tot = jnp.sum(lossv[...]) * (0.5 * inv_d)
        losst[nm] = jnp.full(losst.shape[1:], tot, F32)
        for k in range(1, nm):
            l_copy(k).start()

    @pl.loop(0, nc)
    def _(i):
        c = nc - 1 - i

        @pl.when(jnp.logical_not(last))
        def _():
            b_copy(c).wait_recv()

        for way in range(2):
            dy_copy(c, way).start()

        blk = fl // 4
        for f in range(4 * nm):
            rows = pl.ds(f * blk, blk)
            dz = dot(wd[rows, :], dybuf[c]).astype(BF16).astype(F32)
            ubuf[c, rows, :] = (dz * gelu_grad(ubuf[c, rows, :].astype(F32))).astype(BF16)
        acc = dot(wu[...], ubuf[c])
        dn2 = acc.astype(BF16).astype(F32)
        m32 = mbuf[c].astype(F32)
        pull = norm_pull(m32, inv_rms(m32), dn2).astype(BF16)
        dmid = (dybuf[c].astype(F32) + pull.astype(F32)).astype(BF16)
        mbuf[c] = dmid
        dobuf[...] = dot(wo[...], dmid).astype(BF16)

        for cc in range(nc):
            pl.when(c == cc)(functools.partial(attention_grad, cc))

        dn1 = dot(wq[...], qkv[c]).astype(BF16).astype(F32)
        h32 = hbuf[c].astype(F32)
        pull1 = norm_pull(h32, inv_rms(h32), dn1).astype(BF16)

        @pl.when(jnp.logical_not(last))
        def _():
            f_copy(c).wait_send()

        ybuf[c] = (mbuf[c].astype(F32) + pull1.astype(F32)).astype(BF16)

        @pl.when(jnp.logical_not(first))
        def _():
            b_copy(c).start()

        @pl.when(i > 0)
        def _():
            dy_forward(c + 1)

    dy_forward(0)

    @pl.when(z_last)
    def _():
        z_start()

    @pl.when(last)
    def _():
        for k in range(1, nm):
            l_copy(k).wait_recv()
        vals = [losst[nm]] + [losst[k - 1] for k in range(1, nm)]
        tot = jnp.zeros_like(vals[0])
        for who in range(nm):
            pick = vals[0]
            for k in range(1, nm):
                pick = jnp.where(peer(k) == who, vals[k], pick)
            tot = tot + pick
        losst[nm + 1] = tot

    @pl.when(jnp.logical_not(last))
    def _():
        lf_copy().wait_recv()

    @pl.when(jnp.logical_not(first))
    def _():
        lf_copy().start()

    loss_out[...] = losst[nm + 1]

    def wgrad(mat, d):
        acc = None
        for c in range(nc):
            if mat == 0:
                part = dot_t(qkv[c, rowsl(d * qrows, qrows, qrows), :], n1buf[c])
            elif mat == 1:
                part = dot_t(obuf[c, rowsl(d * orows, orows, orows), :], mbuf[c])
            elif mat == 2:
                part = dot_t(n2buf[c], ubuf[c, rowsl(d * fl, fl, fl), :])
            else:
                part = dot_t(zbuf[c, rowsl(d * fl, fl, fl), :], dybuf[c])
            acc = part if acc is None else acc + part
        return acc

    sizes = (qrows, orows, dm_)
    offs = (0, qrows, qrows + orows)

    def rows_of(mat):
        return pl.ds(offs[mat], sizes[mat])

    def half_of(mat, half):
        return pl.ds(offs[mat] + half * (sizes[mat] // 2), sizes[mat] // 2)

    def far_copy(mat, half):
        rows = pl.ds(offs[mat] // 2, sizes[mat] // 2)
        return ring_copy(stage_buf.at[0, half_of(mat, half)], (far_p, far_m)[half].at[rows],
                         rs_send.at[mat, half], rs_recv.at[mat, half], half)

    def near_copy(mat, side, half):
        way = 2 + 2 * side + half
        return ring_copy(stage_buf.at[1 + side, half_of(mat, half)], (near_l if side == half else near_e).at[half_of(mat, half)],
                         rs_send.at[mat, way], rs_recv.at[mat, way], side)

    mats = (2, 0, 1)
    for mat in mats:
        stage_buf[0, rows_of(mat)] = wgrad(mat, peer(far))
        for half in range(2):
            far_copy(mat, half).start()
    for mat in mats:
        for side in range(2):
            stage_buf[1 + side, rows_of(mat)] = wgrad(mat, peer((plus, minus)[side]))
            near_copy(mat, side, 1 - side).start()

    def load(src, nr):
        return pltpu.make_async_copy(src, radd.at[pl.ds(0, nr)], ld_sem.at[0])

    for mat in mats:
        nr = sizes[mat] // 2
        for half in range(2):
            far_copy(mat, half).wait_recv()
            src = (far_p, far_m)[half].at[pl.ds(offs[mat] // 2, nr)]
            load(src, nr).start()
            load(src, nr).wait()
            stage_buf[1 + half, half_of(mat, half)] += radd[pl.ds(0, nr)]
            near_copy(mat, half, half).start()

    for mat in mats:
        for half in range(2):
            far_copy(mat, half).wait_send()
        stage_buf[0, rows_of(mat)] = wgrad(mat, me)

    def zdy_load(n, buf):
        slot, c = n // nc, lax.rem(n, nc)
        return (pltpu.make_async_copy(z_recv.at[slot, c], zdy.at[buf, pl.ds(0, fl)], ld_sem.at[1 + buf]),
                pltpu.make_async_copy(dy_recv.at[slot, c], zdy.at[buf, pl.ds(fl, dm_)], ld_sem.at[3 + buf]))

    @pl.when(z_last)
    def _():
        for c in range(nc):
            z_forward(c)

    gdacc[...] = wgrad(3, me)
    for c in range(nc):
        for way in (0, 1, 4, 5):
            z_copy(c, way).wait_recv()
        for way in (2, 3):
            dy_copy(c, way).wait_recv()
    for cp in zdy_load(0, 0):
        cp.start()

    @pl.loop(0, 3 * nc)
    def _(n):
        buf = lax.rem(n, 2)

        @pl.when(n + 1 < 3 * nc)
        def _():
            for cp in zdy_load(n + 1, 1 - buf):
                cp.start()

        for cp in zdy_load(n, buf):
            cp.wait()
        gdacc[...] += dot_t(zdy[buf, pl.ds(0, fl), :], zdy[buf, pl.ds(fl, dm_), :])

    def out_copy(mat):
        if mat == 3:
            return pltpu.make_async_copy(gdacc, sum_out.at[pl.ds(qrows + orows + dm_, fl)], out_sem.at[3])
        return pltpu.make_async_copy(stage_buf.at[0, rows_of(mat)], sum_out.at[rows_of(mat)], out_sem.at[mat])

    out_copy(3).start()
    for mat in mats:
        nr = sizes[mat] // 2
        for side in range(2):
            near_copy(mat, side, 1 - side).wait_recv()
            load(near_e.at[half_of(mat, 1 - side)], nr).start()
            load(near_e.at[half_of(mat, 1 - side)], nr).wait()
            stage_buf[0, half_of(mat, 1 - side)] += radd[pl.ds(0, nr)]
        out_copy(mat).start()
    for mat in mats:
        for side in range(2):
            near_copy(mat, side, side).wait_recv()

    for mat in range(4):
        out_copy(mat).wait()
    for c in range(nc):
        for way in range(6):
            z_copy(c, way).wait_send()
        for way in range(4):
            dy_copy(c, way).wait_send()
    for idx in range(4):
        for way in range(4):
            w_copy(idx, way).wait_send()
    for mat in mats:
        for half in range(2):
            for side in range(2):
                near_copy(mat, side, half).wait_send()

    @pl.when(jnp.logical_not(first))
    def _():
        for c in range(nc):
            b_copy(c).wait_send()
        lf_copy().wait_send()

    @pl.when(last)
    def _():
        for k in range(1, nm):
            l_copy(k).wait_send()


def finish_kernel(sq, so, su, sd, lq, lo, lu, loss, gq, go, gu, gd, loss_out):
    gq[...] = sq[...] + lq[...]
    go[...] = so[...] + lo[...]
    gu[...] = su[...] + lu[...]
    gd[...] = sd[...]
    loss_out[0] = loss[0, 0]


def solution(mesh):
    ns = mesh.shape["stage"]
    nm = mesh.shape["model"]

    def per_device(tokens_in, targets, w_qkv, w_out, w_up, w_down):
        n_micro, seq_len, d_model = tokens_in.shape
        hl, hd, fl = w_qkv.shape[3], w_qkv.shape[5], w_up.shape[3]
        tc = min(CHUNK, seq_len // 2)
        nc = seq_len // tc
        assert n_micro == nm == 4 and w_qkv.shape[1] == 1 and hl == 2
        qrows, orows = hl * 3 * hd, hl * hd
        wqT = jnp.transpose(w_qkv[0, 0], (1, 2, 3, 0)).reshape(qrows, d_model)
        wo = w_out[0, 0].reshape(orows, d_model)
        wu, wd = w_up[0, 0], w_down[0, 0]
        cfg = (ns, nm, nc, tc, d_model, hl, hd, fl)
        heads = nm * hl
        any_spec = pl.BlockSpec(memory_space=pl.ANY)
        f32 = lambda *shape: jax.ShapeDtypeStruct(shape, F32)
        rsum = qrows + orows + d_model
        seqb = nc * tc
        b16 = lambda *shape: jax.ShapeDtypeStruct(shape, BF16)
        out_shape = (f32(rsum + fl, d_model), f32(8, 128), f32(rsum // 2, d_model), f32(rsum // 2, d_model), f32(rsum, d_model),
                     f32(rsum, d_model), b16(3, nc, fl, tc), b16(2, nc, fl // 2, tc), b16(3, nc, d_model, tc))
        vb = lambda *shape: pltpu.VMEM(shape, BF16)
        vf = lambda *shape: pltpu.VMEM(shape, F32)
        dma = lambda *shape: pltpu.SemaphoreType.DMA(shape)
        scratch = [
            vb(nm * qrows, d_model), vb(d_model, nm * orows), vb(nm * fl, d_model), vb(d_model, nm * fl),
            vb(nm * fl, d_model), vb(d_model, nm * fl), vb(nm * orows, d_model), vb(d_model, nm * qrows),
            vb(nc, tc, d_model), vb(nc, d_model, tc), vb(nc, d_model, tc), vb(nc, nm * qrows, tc), vb(nm, seqb, qrows),
            vb(nc, nm * orows, tc), vb(nc, d_model, tc), vb(nc, d_model, tc), vb(nc, nm * fl, tc), vb(nc, nm * fl, tc),
            vb(nc * (nc + 1) // 2, heads, tc, tc), vb(nc, d_model, tc), vf(heads // 2, seqb, 2 * hd), vf(heads // 2, seqb, 2 * hd),
            vf(2 * seqb, tc), vb(nc, d_model, tc), vb(nm * orows, tc), vf(nm + 2, 8, 128), vf(8, tc),
            vf(3, rsum, d_model), vf(256, d_model), vf(fl, d_model), vb(2, fl + d_model, tc),
            dma(4, 4), dma(4, 4), dma(4), pltpu.SemaphoreType.REGULAR, dma(nc), dma(nc), dma(nc), dma(nc), dma(nc),
            dma(nm - 1), dma(nm - 1), pltpu.SemaphoreType.DMA, pltpu.SemaphoreType.DMA,
            dma(3, 6), dma(3, 6), dma(5), dma(4), dma(6, nc), dma(6, nc), dma(4, nc), dma(4, nc),
        ]
        res = pl.pallas_call(
            functools.partial(step_kernel, cfg),
            out_shape=out_shape,
            in_specs=[any_spec] * 6,
            out_specs=[any_spec, pl.BlockSpec(memory_space=pltpu.VMEM)] + [any_spec] * 7,
            scratch_shapes=scratch,
            compiler_params=pltpu.CompilerParams(collective_id=0, has_side_effects=True, vmem_limit_bytes=67043328),
            name="train_step",
        )(tokens_in, targets, wqT, wo, wu, wd)
        part, loss, late = res[0], res[1], res[5]
        steps = 4

        def spec(size, start):
            rows = size // steps
            return pl.BlockSpec((rows, d_model), lambda i: (start // rows + i, 0))

        q_s, o_s, u_s = spec(qrows, 0), spec(orows, qrows), spec(d_model, qrows + orows)
        g_qkv, g_out, g_up, g_down, loss = pl.pallas_call(
            finish_kernel,
            grid=(steps,),
            out_shape=(f32(qrows, d_model), f32(orows, d_model), f32(d_model, fl), f32(fl, d_model), f32(1)),
            in_specs=[q_s, o_s, u_s, spec(fl, rsum), q_s, o_s, u_s, pl.BlockSpec(memory_space=pltpu.SMEM)],
            out_specs=[spec(qrows, 0), spec(orows, 0), spec(d_model, 0), spec(fl, 0), pl.BlockSpec(memory_space=pltpu.SMEM)],
            name="finish",
        )(part, part, part, part, late, late, late, loss)
        g_qkv = jnp.transpose(g_qkv.reshape(hl, 3, hd, d_model), (3, 0, 1, 2))[None, None]
        return g_qkv, g_out.reshape(1, 1, hl, hd, d_model), g_up[None, None], g_down[None, None], loss

    tok_spec = P(None, "data", None)
    qkv_spec = P("stage", None, None, "model", None, None)
    out_spec = P("stage", None, "model", None, None)
    up_spec = P("stage", None, None, "model")
    down_spec = P("stage", None, "model", None)
    g_qkv_spec = P(("data", "stage"), None, None, "model", None, None)
    g_out_spec = P(("data", "stage"), None, "model", None, None)
    g_up_spec = P(("data", "stage"), None, None, "model")
    g_down_spec = P(("data", "stage"), None, "model", None)
    return jax.shard_map(per_device, mesh=mesh, in_specs=(tok_spec, tok_spec, qkv_spec, out_spec, up_spec, down_spec), out_specs=(g_qkv_spec, g_out_spec, g_up_spec, g_down_spec, P("data")), check_vma=False)
```

```python
import functools
import math

import jax
import jax.numpy as jnp
from jax import lax
from jax.experimental import pallas as pl
from jax.experimental.pallas import tpu as pltpu
from jax.sharding import PartitionSpec as P

F32 = jnp.float32
BF16 = jnp.bfloat16
MESH = pl.DeviceIdType.MESH
CHUNK = 256
NEG = -1e30
GELU_C = math.sqrt(2.0 / math.pi)
GELU_A = 0.044715

W_Q, W_O, W_U, W_D = range(4)


def dot(lhs, rhs):
    return jnp.dot(lhs, rhs, preferred_element_type=F32)


def dot_t(lhs, rhs):
    return lax.dot_general(lhs, rhs, (((1,), (1,)), ((), ())), preferred_element_type=F32)


def inv_rms(x32):
    return lax.rsqrt(jnp.mean(x32 * x32, axis=0, keepdims=True) + 1e-6)


def norm_pull(x32, inv, g32):
    mean_gx = jnp.mean(g32 * x32, axis=0, keepdims=True)
    return g32 * inv - x32 * (inv * inv * inv * mean_gx)


def gelu(u):
    tanh = jnp.tanh(u * (GELU_C + (GELU_C * GELU_A) * (u * u)))
    half = 0.5 * u
    return half + half * tanh


def gelu_grad(u):
    u2 = u * u
    sig = 0.5 + 0.5 * jnp.tanh(u * (GELU_C + (GELU_C * GELU_A) * u2))
    slope = u * (2.0 * GELU_C + (6.0 * GELU_C * GELU_A) * u2)
    return sig * (1.0 + slope * (1.0 - sig))


def step_kernel(cfg, x_hbm, t_hbm, wqT_in, wo_in, wu_in, wd_in,
                sum_out, loss_out, far_p, far_m, near_e, near_l, z_recv, z_fwd, dy_recv,
                wqT, woT, wuT, wdT, wd, wu, wo, wq,
                xin, hbuf, n1buf, qkv, qkvn, obuf, mbuf, n2buf, ubuf, zbuf, pbuf, dybuf, dvacc, dkacc, sscr,
                ybuf, dobuf, losst, lossv, stage_buf, radd, gdacc, zdy,
                ag_send, ag_recv, ag_loc, go_sem, xsem, fsend, frecv, bsend, brecv, lsend, lrecv, lfsend, lfrecv,
                rs_send, rs_recv, ld_sem, out_sem, z_send, z_arr, dy_send, dy_arr):
    ns, nm, nc, tc, dm_, hl, hd, fl = cfg
    heads = nm * hl
    qrows = hl * 3 * hd
    orows = hl * hd
    inv_d = 1.0 / (nm * nc * tc * dm_)
    scale = hd ** -0.5
    exp_c = scale * math.log2(math.e)
    me = lax.axis_index("model")
    st = lax.axis_index("stage")
    nxt = lax.rem(st + 1, ns)
    prv = lax.rem(st + ns - 1, ns)
    first = st == 0
    last = st == ns - 1

    def peer(k):
        return lax.rem(me + k, nm)

    bar = pltpu.get_barrier_semaphore()
    pl.semaphore_signal(bar, inc=1, device_id={"stage": nxt}, device_id_type=MESH)
    pl.semaphore_signal(bar, inc=1, device_id={"stage": prv}, device_id_type=MESH)
    for k in range(1, nm):
        pl.semaphore_signal(bar, inc=1, device_id={"model": peer(k)}, device_id_type=MESH)
    pl.semaphore_wait(bar, 2 + nm - 1)

    def rowsl(start, size, mult):
        return pl.ds(pl.multiple_of(start, mult), size)

    plus, minus, far = 1, nm - 1, 2

    def w_rows(idx, who, half=None):
        size = (qrows, orows, fl, fl)[idx]
        if idx in (W_Q, W_U):
            buf = wqT if idx == W_Q else wuT
            if half is None:
                return buf.at[rowsl(who * size, size, size), :]
            return buf.at[rowsl(who * size + half * (size // 2), size // 2, size // 2), :]
        view = (woT if idx == W_O else wdT).at[:, rowsl(who * size, size, size)]
        return view if half is None else view.at[pl.ds(half * (dm_ // 2), dm_ // 2), :]

    def w_copy(idx, way):
        to = plus if way in (0, 2) else minus
        if way < 2:
            src = wqT_in if idx == W_Q else w_rows(idx, me)
            dst = w_rows(idx, me)
        else:
            src = dst = w_rows(idx, peer(minus if way == 2 else plus), way - 2)
        return pltpu.make_async_remote_copy(
            src_ref=src, dst_ref=dst, send_sem=ag_send.at[idx, way], recv_sem=ag_recv.at[idx, way],
            device_id={"model": peer(to)}, device_id_type=MESH)

    def w_arrival(idx, way):
        who = peer((minus, plus, far, far)[way])
        ref = w_rows(idx, who) if way < 2 else w_rows(idx, who, way - 2)
        return pltpu.make_async_remote_copy(
            src_ref=ref, dst_ref=ref, send_sem=ag_send.at[idx, way], recv_sem=ag_recv.at[idx, way],
            device_id={"model": peer(plus)}, device_id_type=MESH)

    def w_local(idx):
        src = (wqT_in, wo_in, wu_in, wd_in)[idx]
        dst = (w_rows(W_Q, me), wo.at[rowsl(me * orows, orows, orows), :], wu.at[:, rowsl(me * fl, fl, fl)], wd.at[rowsl(me * fl, fl, fl), :])[idx]
        return pltpu.make_async_copy(src, dst, ag_loc.at[idx])

    def w_own(idx):
        for way in range(2):
            w_copy(idx, way).start()

    def w_forward(idx):
        for way in range(2):
            w_arrival(idx, way).wait_recv()
        for way in range(2, 4):
            w_copy(idx, way).start()

    def w_wait(idx):
        for way in range(2, 4):
            w_arrival(idx, way).wait_recv()

    def x_copy(c):
        return pltpu.make_async_copy(x_hbm.at[me, pl.ds(c * tc, tc), :], xin.at[c], xsem.at[c])

    def t_copy(c):
        return pltpu.make_async_copy(t_hbm.at[me, pl.ds(c * tc, tc), :], xin.at[c], xsem.at[c])

    @pl.when(first)
    def _():
        for c in range(nc):
            x_copy(c).start()

    @pl.when(last)
    def _():
        for c in range(nc):
            t_copy(c).start()

    for idx in range(4):
        w_local(idx).start()

    odd = lax.rem(st, 2) == 1
    early = st < 2

    @pl.when(odd)
    def _():
        pl.semaphore_wait(go_sem, 1)

    w_own(W_Q)
    w_local(W_O).wait()
    woT[:, rowsl(me * orows, orows, orows)] = jnp.transpose(wo[rowsl(me * orows, orows, orows), :])
    w_own(W_O)
    w_local(W_U).wait()
    wuT[rowsl(me * fl, fl, fl), :] = jnp.transpose(wu[:, rowsl(me * fl, fl, fl)])
    w_local(W_Q).wait()
    w_forward(W_Q)
    w_own(W_U)
    w_local(W_D).wait()
    wdT[:, rowsl(me * fl, fl, fl)] = jnp.transpose(wd[rowsl(me * fl, fl, fl), :])
    w_forward(W_O)
    w_own(W_D)

    def pass_go():
        @pl.when(jnp.logical_not(odd))
        def _():
            pl.semaphore_signal(go_sem, inc=1, device_id={"stage": nxt}, device_id_type=MESH)

    def natural_weights():
        @pl.loop(0, nm)
        def _(f):
            wu[:, rowsl(f * fl, fl, fl)] = jnp.transpose(wuT[rowsl(f * fl, fl, fl), :])
            wd[rowsl(f * fl, fl, fl), :] = jnp.transpose(wdT[:, rowsl(f * fl, fl, fl)])
            wo[rowsl(f * orows, orows, orows), :] = jnp.transpose(woT[:, rowsl(f * orows, orows, orows)])
            wq[:, rowsl(f * qrows, qrows, qrows)] = jnp.transpose(wqT[rowsl(f * qrows, qrows, qrows), :])

    late = st >= max(2, ns // 2)

    @pl.when(jnp.logical_not(early))
    def _():
        w_forward(W_U)
        w_forward(W_D)
        pass_go()
        for idx in range(4):
            w_wait(idx)

    @pl.when(late)
    def _():
        natural_weights()

    def f_copy(c):
        return pltpu.make_async_remote_copy(
            src_ref=ybuf.at[c], dst_ref=hbuf.at[c], send_sem=fsend.at[c], recv_sem=frecv.at[c],
            device_id={"stage": nxt}, device_id_type=MESH)

    def b_copy(c):
        return pltpu.make_async_remote_copy(
            src_ref=ybuf.at[c], dst_ref=dybuf.at[c], send_sem=bsend.at[c], recv_sem=brecv.at[c],
            device_id={"stage": prv}, device_id_type=MESH)

    def ring_copy(src, dst, send, recv, way):
        return pltpu.make_async_remote_copy(
            src_ref=src, dst_ref=dst, send_sem=send, recv_sem=recv,
            device_id={"model": peer((plus, minus)[way % 2])}, device_id_type=MESH)

    hf = fl // 2

    def z_copy(c, way):
        if way < 2:
            src, dst = zbuf.at[c, rowsl(peer((plus, minus)[way]) * fl, fl, fl), :], z_recv.at[way, c]
        elif way < 4:
            src, dst = zbuf.at[c, rowsl(peer(far) * fl + (way - 2) * hf, hf, hf), :], z_fwd.at[way - 2, c]
        else:
            src, dst = z_fwd.at[way - 4, c], z_recv.at[2, c, pl.ds((way - 4) * hf, hf)]
        return ring_copy(src, dst, z_send.at[way, c], z_arr.at[way, c], way)

    def z_forward(c):
        for way in (2, 3):
            z_copy(c, way).wait_recv()
        for way in (4, 5):
            z_copy(c, way).start()

    def dy_copy(c, way):
        if way < 2:
            src, dst = dybuf.at[c], dy_recv.at[way, c]
        else:
            rows = pl.ds((way - 2) * (dm_ // 2), dm_ // 2)
            src, dst = dy_recv.at[way - 2, c, rows], dy_recv.at[2, c, rows]
        return ring_copy(src, dst, dy_send.at[way, c], dy_arr.at[way, c], way)

    def dy_forward(c):
        for way in (0, 1):
            dy_copy(c, way).wait_recv()
        for way in (2, 3):
            dy_copy(c, way).start()

    lossv[...] = jnp.zeros_like(lossv)

    def head_rows(p, h, part):
        return pl.ds(p * (2 * 3 * hd) + (h * 3 + part) * hd, hd)

    k_lane = (0, 2 * 2 * hd)
    v_lane = (2 * hd, 2 * 2 * hd)
    two = 2 * hd

    def pad_k(val, h):
        zero = jnp.zeros_like(val)
        return jnp.concatenate([zero, val] if h == 0 else [val, zero], axis=0)

    def pad_v(val, h):
        zero = jnp.zeros_like(val)
        return jnp.concatenate([val, zero] if h == 0 else [zero, val], axis=0)

    def causal(shape, row0):
        return lax.broadcasted_iota(jnp.int32, shape, 0) + row0 <= lax.broadcasted_iota(jnp.int32, shape, 1)

    def attention(cc):
        nk = (cc + 1) * tc
        slots = min(heads, sscr.shape[0] // nk)
        ahead = min(4, slots - 1)
        sub = tc // 2

        def front(head):
            p, h = head // 2, head % 2
            base = (head % slots) * nk
            qz = pad_k(qkv[cc, head_rows(p, h, 0), :], h)
            tops, sums = [], []
            for j in range(cc + 1):
                s = dot(qkvn[p, pl.ds(j * tc, tc), pl.ds(k_lane[h], two)], qz)
                for r in range(0, tc, sub):
                    part = s[r:r + sub]
                    if j == cc:
                        part = jnp.where(causal(part.shape, r), part, NEG)
                    top = jnp.max(part, axis=0, keepdims=True)
                    e = jnp.exp2((part - top) * exp_c)
                    sscr[pl.ds(base + j * tc + r, sub), :] = e
                    tops.append(top)
                    sums.append(jnp.sum(e, axis=0, keepdims=True))
            mx = functools.reduce(jnp.maximum, tops)
            scales = [jnp.exp2((top - mx) * exp_c) for top in tops]
            inv = 1.0 / functools.reduce(jnp.add, [a * b for a, b in zip(scales, sums)])
            return [a * inv for a in scales]

        def back(head, factors):
            p, h = head // 2, head % 2
            base = (head % slots) * nk
            o_t = None
            for j in range(cc + 1):
                parts = []
                for i in range(2):
                    pr = (sscr[pl.ds(base + j * tc + i * sub, sub), :] * factors[2 * j + i]).astype(BF16)
                    pbuf[cc * (cc + 1) // 2 + j, head, pl.ds(i * sub, sub), :] = pr
                    parts.append(pr)
                part = dot(qkv[j, head_rows(p, h, 2), :], jnp.concatenate(parts, axis=0))
                o_t = part if o_t is None else o_t + part
            obuf[cc, pl.ds(head * hd, hd), :] = o_t.astype(BF16)

        factors = {}
        for head in range(ahead):
            factors[head] = front(head)
        for head in range(heads):
            if head + ahead < heads:
                factors[head + ahead] = front(head + ahead)
            back(head, factors.pop(head))

    def attention_grad(cc):
        units = [(p, j) for p in range(heads // 2) for j in range(cc + 1)]
        dqs = {}
        held = {}

        def of_head(p, h):
            if (p, h) not in held:
                rows = pl.ds((p * 2 + h) * hd, hd)
                do_t = dobuf[rows, :]
                dsum = jnp.sum(do_t.astype(F32) * obuf[cc, rows, :].astype(F32), axis=0, keepdims=True)
                held[p, h] = (pad_v(do_t, h), dsum)
            return held[p, h]

        def front(p, j):
            out = []
            for h in range(2):
                do_z, dsum = of_head(p, h)
                pr = pbuf[cc * (cc + 1) // 2 + j, p * 2 + h]
                dp = dot(qkvn[p, pl.ds(j * tc, tc), pl.ds(v_lane[h], two)], do_z).astype(BF16).astype(F32)
                out.append((pr.astype(F32) * (dp - dsum)).astype(BF16))
            return out

        def back(p, j, ds):
            dv_new = dk_new = None
            for h in range(2):
                do_z, _ = of_head(p, h)
                dv_h = dot_t(pbuf[cc * (cc + 1) // 2 + j, p * 2 + h], do_z)
                dk_h = dot_t(ds[h], pad_v(qkv[cc, head_rows(p, h, 0), :], h))
                dv_new = dv_h if dv_new is None else dv_new + dv_h
                dk_new = dk_h if dk_new is None else dk_new + dk_h
                dq_h = dot(qkv[j, head_rows(p, h, 1), :], ds[h])
                dqs[p, h] = dq_h if j == 0 else dqs[p, h] + dq_h
            rows = pl.ds(j * tc, tc)
            if cc < nc - 1:
                dv_new = dv_new + dvacc[p, rows, :]
                dk_new = dk_new + dkacc[p, rows, :]
            if j < cc:
                dvacc[p, rows, :] = dv_new
                dkacc[p, rows, :] = dk_new
                return
            dv_t = jnp.transpose(dv_new).astype(BF16)
            dk_t = (jnp.transpose(dk_new) * scale).astype(BF16)
            for h in range(2):
                qkv[cc, head_rows(p, h, 0), :] = (dqs[p, h] * scale).astype(BF16)
                qkv[cc, head_rows(p, h, 1), :] = dk_t[h * hd:(h + 1) * hd, :]
                qkv[cc, head_rows(p, h, 2), :] = dv_t[h * hd:(h + 1) * hd, :]

        ds = front(*units[0])
        for n, unit in enumerate(units):
            later = front(*units[n + 1]) if n + 1 < len(units) else None
            back(*unit, ds)
            ds = later

    def attention_step(c):
        @pl.when(first)
        def _():
            x_copy(c).wait()
            hbuf[c] = jnp.transpose(xin[c])

        @pl.when(jnp.logical_not(first))
        def _():
            f_copy(c).wait_recv()

        @pl.when(early & (c == 0))
        def _():
            w_wait(W_Q)

        h32 = hbuf[c].astype(F32)
        n1 = (h32 * inv_rms(h32)).astype(BF16)
        n1buf[c] = n1
        for r in range(nm):
            rows = pl.ds(r * qrows, qrows)
            blk = dot(wqT[rows, :], n1).astype(BF16)
            qkv[c, rows, :] = blk
            qkvn[r, pl.ds(pl.multiple_of(c * tc, tc), tc), :] = jnp.transpose(blk)

        for cc in range(nc):
            pl.when(c == cc)(functools.partial(attention, cc))

    def mlp_step(c):
        a = dot(woT[...], obuf[c]).astype(BF16)
        m32 = (hbuf[c].astype(F32) + a.astype(F32)).astype(BF16).astype(F32)
        mbuf[c] = m32.astype(BF16)
        n2 = (m32 * inv_rms(m32)).astype(BF16)
        n2buf[c] = n2

        blk = fl // 2
        for f in range(2 * nm):
            rows = pl.ds(f * blk, blk)
            u = dot(wuT[rows, :], n2buf[c]).astype(BF16)
            ubuf[c, rows, :] = u
            zbuf[c, rows, :] = gelu(u.astype(F32)).astype(BF16)
        acc = dot(wdT[...], zbuf[c])
        y32 = (mbuf[c].astype(F32) + acc.astype(BF16).astype(F32)).astype(BF16)
        ybuf[c] = y32

        @pl.when(jnp.logical_not(last))
        def _():
            f_copy(c).start()

        @pl.when(last)
        def _():
            t_copy(c).wait()
            err = ybuf[c].astype(F32) - jnp.transpose(xin[c]).astype(F32)
            lossv[...] += jnp.sum((err * err).reshape(dm_ // 8, 8, tc), axis=0)
            dybuf[c] = (err * inv_d).astype(BF16)

    @pl.loop(0, 2 * nc)
    def _(n):
        attn_turn = jnp.where(early, jnp.where(n < nc, 1, 0), 1 - lax.rem(n, 2))
        c = jnp.where(early, lax.rem(n, nc), n // 2)

        @pl.when(early & (n == 2))
        def _():
            w_forward(W_U)

        @pl.when(early & (n == min(3, nc)))
        def _():
            w_forward(W_D)
            pass_go()

        @pl.when(attn_turn == 1)
        def _():
            attention_step(c)

        @pl.when(early & (n == nc))
        def _():
            w_wait(W_O)
            w_wait(W_U)
            w_wait(W_D)

        @pl.when(attn_turn == 0)
        def _():
            mlp_step(c)

    def z_start():
        for c in range(nc):
            for way in range(4):
                z_copy(c, way).start()

    z_last = st >= ns - 2

    @pl.when(jnp.logical_not(z_last))
    def _():
        z_start()

    @pl.when(jnp.logical_not(late))
    def _():
        natural_weights()
        for c in range(nc):
            z_forward(c)

    def l_copy(k):
        return pltpu.make_async_remote_copy(
            src_ref=losst.at[nm], dst_ref=losst.at[3 - k if nm == 4 else nm - 1 - k], send_sem=lsend.at[k - 1],
            recv_sem=lrecv.at[k - 1], device_id={"model": peer(k)}, device_id_type=MESH)

    def lf_copy():
        return pltpu.make_async_remote_copy(
            src_ref=losst.at[nm + 1], dst_ref=losst.at[nm + 1], send_sem=lfsend, recv_sem=lfrecv,
            device_id={"stage": prv}, device_id_type=MESH)

    @pl.when(last)
    def _():
        tot = jnp.sum(lossv[...]) * (0.5 * inv_d)
        losst[nm] = jnp.full(losst.shape[1:], tot, F32)
        for k in range(1, nm):
            l_copy(k).start()

    @pl.loop(0, nc)
    def _(i):
        c = nc - 1 - i

        @pl.when(jnp.logical_not(last))
        def _():
            b_copy(c).wait_recv()

        for way in range(2):
            dy_copy(c, way).start()

        blk = fl // 4
        for f in range(4 * nm):
            rows = pl.ds(f * blk, blk)
            dz = dot(wd[rows, :], dybuf[c]).astype(BF16).astype(F32)
            ubuf[c, rows, :] = (dz * gelu_grad(ubuf[c, rows, :].astype(F32))).astype(BF16)
        acc = dot(wu[...], ubuf[c])
        dn2 = acc.astype(BF16).astype(F32)
        m32 = mbuf[c].astype(F32)
        pull = norm_pull(m32, inv_rms(m32), dn2).astype(BF16)
        dmid = (dybuf[c].astype(F32) + pull.astype(F32)).astype(BF16)
        mbuf[c] = dmid
        dobuf[...] = dot(wo[...], dmid).astype(BF16)

        for cc in range(nc):
            pl.when(c == cc)(functools.partial(attention_grad, cc))

        dn1 = dot(wq[...], qkv[c]).astype(BF16).astype(F32)
        h32 = hbuf[c].astype(F32)
        pull1 = norm_pull(h32, inv_rms(h32), dn1).astype(BF16)

        @pl.when(jnp.logical_not(last))
        def _():
            f_copy(c).wait_send()

        ybuf[c] = (mbuf[c].astype(F32) + pull1.astype(F32)).astype(BF16)

        @pl.when(jnp.logical_not(first))
        def _():
            b_copy(c).start()

        @pl.when(i > 0)
        def _():
            dy_forward(c + 1)

    dy_forward(0)

    @pl.when(last)
    def _():
        for k in range(1, nm):
            l_copy(k).wait_recv()
        vals = [losst[nm]] + [losst[k - 1] for k in range(1, nm)]
        tot = jnp.zeros_like(vals[0])
        for who in range(nm):
            pick = vals[0]
            for k in range(1, nm):
                pick = jnp.where(peer(k) == who, vals[k], pick)
            tot = tot + pick
        losst[nm + 1] = tot

    @pl.when(jnp.logical_not(last))
    def _():
        lf_copy().wait_recv()

    @pl.when(jnp.logical_not(first))
    def _():
        lf_copy().start()

    loss_out[...] = losst[nm + 1]

    def wgrad(mat, d):
        acc = None
        for c in range(nc):
            if mat == 0:
                part = dot_t(qkv[c, rowsl(d * qrows, qrows, qrows), :], n1buf[c])
            elif mat == 1:
                part = dot_t(obuf[c, rowsl(d * orows, orows, orows), :], mbuf[c])
            elif mat == 2:
                part = dot_t(n2buf[c], ubuf[c, rowsl(d * fl, fl, fl), :])
            else:
                part = dot_t(zbuf[c, rowsl(d * fl, fl, fl), :], dybuf[c])
            acc = part if acc is None else acc + part
        return acc

    sizes = (qrows, orows, dm_)
    offs = (0, qrows, qrows + orows)

    def rows_of(mat):
        return pl.ds(offs[mat], sizes[mat])

    def half_of(mat, half):
        return pl.ds(offs[mat] + half * (sizes[mat] // 2), sizes[mat] // 2)

    def far_copy(mat, half):
        rows = pl.ds(offs[mat] // 2, sizes[mat] // 2)
        return ring_copy(stage_buf.at[0, half_of(mat, half)], (far_p, far_m)[half].at[rows],
                         rs_send.at[mat, half], rs_recv.at[mat, half], half)

    def near_copy(mat, side, half):
        way = 2 + 2 * side + half
        return ring_copy(stage_buf.at[1 + side, half_of(mat, half)], (near_l if side == half else near_e).at[half_of(mat, half)],
                         rs_send.at[mat, way], rs_recv.at[mat, way], side)

    mats = (2, 0, 1)
    for mat in mats:
        stage_buf[0, rows_of(mat)] = wgrad(mat, peer(far))
        for half in range(2):
            far_copy(mat, half).start()
    for mat in mats:
        for side in range(2):
            stage_buf[1 + side, rows_of(mat)] = wgrad(mat, peer((plus, minus)[side]))
            near_copy(mat, side, 1 - side).start()

    @pl.when(z_last)
    def _():
        z_start()

    def load(src, nr):
        return pltpu.make_async_copy(src, radd.at[pl.ds(0, nr)], ld_sem.at[0])

    for mat in mats:
        nr = sizes[mat] // 2
        for half in range(2):
            far_copy(mat, half).wait_recv()
            src = (far_p, far_m)[half].at[pl.ds(offs[mat] // 2, nr)]
            load(src, nr).start()
            load(src, nr).wait()
            stage_buf[1 + half, half_of(mat, half)] += radd[pl.ds(0, nr)]
            near_copy(mat, half, half).start()

    for mat in mats:
        for half in range(2):
            far_copy(mat, half).wait_send()
        stage_buf[0, rows_of(mat)] = wgrad(mat, me)

    def zdy_load(n, buf):
        slot, c = n // nc, lax.rem(n, nc)
        return (pltpu.make_async_copy(z_recv.at[slot, c], zdy.at[buf, pl.ds(0, fl)], ld_sem.at[1 + buf]),
                pltpu.make_async_copy(dy_recv.at[slot, c], zdy.at[buf, pl.ds(fl, dm_)], ld_sem.at[3 + buf]))

    @pl.when(late)
    def _():
        for c in range(nc):
            z_forward(c)

    gdacc[...] = wgrad(3, me)
    for c in range(nc):
        for way in (0, 1, 4, 5):
            z_copy(c, way).wait_recv()
        for way in (2, 3):
            dy_copy(c, way).wait_recv()
    for cp in zdy_load(0, 0):
        cp.start()

    @pl.loop(0, 3 * nc)
    def _(n):
        buf = lax.rem(n, 2)

        @pl.when(n + 1 < 3 * nc)
        def _():
            for cp in zdy_load(n + 1, 1 - buf):
                cp.start()

        for cp in zdy_load(n, buf):
            cp.wait()
        gdacc[...] += dot_t(zdy[buf, pl.ds(0, fl), :], zdy[buf, pl.ds(fl, dm_), :])

    def out_copy(mat):
        if mat == 3:
            return pltpu.make_async_copy(gdacc, sum_out.at[pl.ds(qrows + orows + dm_, fl)], out_sem.at[3])
        return pltpu.make_async_copy(stage_buf.at[0, rows_of(mat)], sum_out.at[rows_of(mat)], out_sem.at[mat])

    out_copy(3).start()
    for mat in mats:
        nr = sizes[mat] // 2
        for side in range(2):
            near_copy(mat, side, 1 - side).wait_recv()
            load(near_e.at[half_of(mat, 1 - side)], nr).start()
            load(near_e.at[half_of(mat, 1 - side)], nr).wait()
            stage_buf[0, half_of(mat, 1 - side)] += radd[pl.ds(0, nr)]
        out_copy(mat).start()
    for mat in mats:
        for side in range(2):
            near_copy(mat, side, side).wait_recv()

    for mat in range(4):
        out_copy(mat).wait()
    for c in range(nc):
        for way in range(6):
            z_copy(c, way).wait_send()
        for way in range(4):
            dy_copy(c, way).wait_send()
    for idx in range(4):
        for way in range(4):
            w_copy(idx, way).wait_send()
    for mat in mats:
        for half in range(2):
            for side in range(2):
                near_copy(mat, side, half).wait_send()

    @pl.when(jnp.logical_not(first))
    def _():
        for c in range(nc):
            b_copy(c).wait_send()
        lf_copy().wait_send()

    @pl.when(last)
    def _():
        for k in range(1, nm):
            l_copy(k).wait_send()


def finish_kernel(sq, so, su, sd, lq, lo, lu, loss, gq, go, gu, gd, loss_out):
    gq[...] = sq[...] + lq[...]
    go[...] = so[...] + lo[...]
    gu[...] = su[...] + lu[...]
    gd[...] = sd[...]
    loss_out[0] = loss[0, 0]


def solution(mesh):
    ns = mesh.shape["stage"]
    nm = mesh.shape["model"]

    def per_device(tokens_in, targets, w_qkv, w_out, w_up, w_down):
        n_micro, seq_len, d_model = tokens_in.shape
        hl, hd, fl = w_qkv.shape[3], w_qkv.shape[5], w_up.shape[3]
        tc = min(CHUNK, seq_len // 2)
        nc = seq_len // tc
        assert n_micro == nm == 4 and w_qkv.shape[1] == 1 and hl == 2
        qrows, orows = hl * 3 * hd, hl * hd
        wqT = jnp.transpose(w_qkv[0, 0], (1, 2, 3, 0)).reshape(qrows, d_model)
        wo = w_out[0, 0].reshape(orows, d_model)
        wu, wd = w_up[0, 0], w_down[0, 0]
        cfg = (ns, nm, nc, tc, d_model, hl, hd, fl)
        heads = nm * hl
        any_spec = pl.BlockSpec(memory_space=pl.ANY)
        f32 = lambda *shape: jax.ShapeDtypeStruct(shape, F32)
        rsum = qrows + orows + d_model
        seqb = nc * tc
        b16 = lambda *shape: jax.ShapeDtypeStruct(shape, BF16)
        out_shape = (f32(rsum + fl, d_model), f32(8, 128), f32(rsum // 2, d_model), f32(rsum // 2, d_model), f32(rsum, d_model),
                     f32(rsum, d_model), b16(3, nc, fl, tc), b16(2, nc, fl // 2, tc), b16(3, nc, d_model, tc))
        vb = lambda *shape: pltpu.VMEM(shape, BF16)
        vf = lambda *shape: pltpu.VMEM(shape, F32)
        dma = lambda *shape: pltpu.SemaphoreType.DMA(shape)
        scratch = [
            vb(nm * qrows, d_model), vb(d_model, nm * orows), vb(nm * fl, d_model), vb(d_model, nm * fl),
            vb(nm * fl, d_model), vb(d_model, nm * fl), vb(nm * orows, d_model), vb(d_model, nm * qrows),
            vb(nc, tc, d_model), vb(nc, d_model, tc), vb(nc, d_model, tc), vb(nc, nm * qrows, tc), vb(nm, seqb, qrows),
            vb(nc, nm * orows, tc), vb(nc, d_model, tc), vb(nc, d_model, tc), vb(nc, nm * fl, tc), vb(nc, nm * fl, tc),
            vb(nc * (nc + 1) // 2, heads, tc, tc), vb(nc, d_model, tc), vf(heads // 2, seqb, 2 * hd), vf(heads // 2, seqb, 2 * hd),
            vf(2 * seqb, tc), vb(nc, d_model, tc), vb(nm * orows, tc), vf(nm + 2, 8, 128), vf(8, tc),
            vf(3, rsum, d_model), vf(256, d_model), vf(fl, d_model), vb(2, fl + d_model, tc),
            dma(4, 4), dma(4, 4), dma(4), pltpu.SemaphoreType.REGULAR, dma(nc), dma(nc), dma(nc), dma(nc), dma(nc),
            dma(nm - 1), dma(nm - 1), pltpu.SemaphoreType.DMA, pltpu.SemaphoreType.DMA,
            dma(3, 6), dma(3, 6), dma(5), dma(4), dma(6, nc), dma(6, nc), dma(4, nc), dma(4, nc),
        ]
        res = pl.pallas_call(
            functools.partial(step_kernel, cfg),
            out_shape=out_shape,
            in_specs=[any_spec] * 6,
            out_specs=[any_spec, pl.BlockSpec(memory_space=pltpu.VMEM)] + [any_spec] * 7,
            scratch_shapes=scratch,
            compiler_params=pltpu.CompilerParams(collective_id=0, has_side_effects=True, vmem_limit_bytes=67043328),
            name="train_step",
        )(tokens_in, targets, wqT, wo, wu, wd)
        part, loss, late = res[0], res[1], res[5]
        steps = 4

        def spec(size, start):
            rows = size // steps
            return pl.BlockSpec((rows, d_model), lambda i: (start // rows + i, 0))

        q_s, o_s, u_s = spec(qrows, 0), spec(orows, qrows), spec(d_model, qrows + orows)
        g_qkv, g_out, g_up, g_down, loss = pl.pallas_call(
            finish_kernel,
            grid=(steps,),
            out_shape=(f32(qrows, d_model), f32(orows, d_model), f32(d_model, fl), f32(fl, d_model), f32(1)),
            in_specs=[q_s, o_s, u_s, spec(fl, rsum), q_s, o_s, u_s, pl.BlockSpec(memory_space=pltpu.SMEM)],
            out_specs=[spec(qrows, 0), spec(orows, 0), spec(d_model, 0), spec(fl, 0), pl.BlockSpec(memory_space=pltpu.SMEM)],
            name="finish",
        )(part, part, part, part, late, late, late, loss)
        g_qkv = jnp.transpose(g_qkv.reshape(hl, 3, hd, d_model), (3, 0, 1, 2))[None, None]
        return g_qkv, g_out.reshape(1, 1, hl, hd, d_model), g_up[None, None], g_down[None, None], loss

    tok_spec = P(None, "data", None)
    qkv_spec = P("stage", None, None, "model", None, None)
    out_spec = P("stage", None, "model", None, None)
    up_spec = P("stage", None, None, "model")
    down_spec = P("stage", None, "model", None)
    g_qkv_spec = P(("data", "stage"), None, None, "model", None, None)
    g_out_spec = P(("data", "stage"), None, "model", None, None)
    g_up_spec = P(("data", "stage"), None, None, "model")
    g_down_spec = P(("data", "stage"), None, "model", None)
    return jax.shard_map(per_device, mesh=mesh, in_specs=(tok_spec, tok_spec, qkv_spec, out_spec, up_spec, down_spec), out_specs=(g_qkv_spec, g_out_spec, g_up_spec, g_down_spec, P("data")), check_vma=False)
```

```python
import functools
import math

import jax
import jax.numpy as jnp
from jax import lax
from jax.experimental import pallas as pl
from jax.experimental.pallas import tpu as pltpu
from jax.sharding import PartitionSpec as P

F32 = jnp.float32
BF16 = jnp.bfloat16
MESH = pl.DeviceIdType.MESH
CHUNK = 256
NEG = -1e30
GELU_C = math.sqrt(2.0 / math.pi)
GELU_A = 0.044715

W_Q, W_O, W_U, W_D = range(4)


def dot(lhs, rhs):
    return jnp.dot(lhs, rhs, preferred_element_type=F32)


def dot_t(lhs, rhs):
    return lax.dot_general(lhs, rhs, (((1,), (1,)), ((), ())), preferred_element_type=F32)


def inv_rms(x32):
    return lax.rsqrt(jnp.mean(x32 * x32, axis=0, keepdims=True) + 1e-6)


def norm_pull(x32, inv, g32):
    mean_gx = jnp.mean(g32 * x32, axis=0, keepdims=True)
    return g32 * inv - x32 * (inv * inv * inv * mean_gx)


def gelu(u):
    tanh = jnp.tanh(u * (GELU_C + (GELU_C * GELU_A) * (u * u)))
    half = 0.5 * u
    return half + half * tanh


def gelu_grad(u):
    u2 = u * u
    sig = 0.5 + 0.5 * jnp.tanh(u * (GELU_C + (GELU_C * GELU_A) * u2))
    slope = u * (2.0 * GELU_C + (6.0 * GELU_C * GELU_A) * u2)
    return sig * (1.0 + slope * (1.0 - sig))


def step_kernel(cfg, x_hbm, t_hbm, wqT_in, wo_in, wu_in, wd_in,
                sum_out, loss_out, far_p, far_m, near_e, near_l, z_recv, z_fwd, dy_recv,
                wqT, woT, wuT, wdT, wd, wu, wo, wq,
                xin, hbuf, n1buf, qkv, qkvn, obuf, mbuf, n2buf, ubuf, zbuf, pbuf, dybuf, dvacc, dkacc, sscr,
                ybuf, dobuf, losst, lossv, stage_buf, radd, gdacc, zdy,
                ag_send, ag_recv, ag_loc, go_sem, xsem, fsend, frecv, bsend, brecv, lsend, lrecv, lfsend, lfrecv,
                rs_send, rs_recv, ld_sem, out_sem, z_send, z_arr, dy_send, dy_arr):
    ns, nm, nc, tc, dm_, hl, hd, fl = cfg
    heads = nm * hl
    qrows = hl * 3 * hd
    orows = hl * hd
    inv_d = 1.0 / (nm * nc * tc * dm_)
    scale = hd ** -0.5
    exp_c = scale * math.log2(math.e)
    me = lax.axis_index("model")
    st = lax.axis_index("stage")
    nxt = lax.rem(st + 1, ns)
    prv = lax.rem(st + ns - 1, ns)
    first = st == 0
    last = st == ns - 1

    def peer(k):
        return lax.rem(me + k, nm)

    bar = pltpu.get_barrier_semaphore()
    pl.semaphore_signal(bar, inc=1, device_id={"stage": nxt}, device_id_type=MESH)
    pl.semaphore_signal(bar, inc=1, device_id={"stage": prv}, device_id_type=MESH)
    for k in range(1, nm):
        pl.semaphore_signal(bar, inc=1, device_id={"model": peer(k)}, device_id_type=MESH)
    pl.semaphore_wait(bar, 2 + nm - 1)

    def rowsl(start, size, mult):
        return pl.ds(pl.multiple_of(start, mult), size)

    plus, minus, far = 1, nm - 1, 2

    def w_rows(idx, who, half=None):
        size = (qrows, orows, fl, fl)[idx]
        if idx in (W_Q, W_U):
            buf = wqT if idx == W_Q else wuT
            if half is None:
                return buf.at[rowsl(who * size, size, size), :]
            return buf.at[rowsl(who * size + half * (size // 2), size // 2, size // 2), :]
        view = (woT if idx == W_O else wdT).at[:, rowsl(who * size, size, size)]
        return view if half is None else view.at[pl.ds(half * (dm_ // 2), dm_ // 2), :]

    def w_copy(idx, way):
        to = plus if way in (0, 2) else minus
        if way < 2:
            src = wqT_in if idx == W_Q else w_rows(idx, me)
            dst = w_rows(idx, me)
        else:
            src = dst = w_rows(idx, peer(minus if way == 2 else plus), way - 2)
        return pltpu.make_async_remote_copy(
            src_ref=src, dst_ref=dst, send_sem=ag_send.at[idx, way], recv_sem=ag_recv.at[idx, way],
            device_id={"model": peer(to)}, device_id_type=MESH)

    def w_arrival(idx, way):
        who = peer((minus, plus, far, far)[way])
        ref = w_rows(idx, who) if way < 2 else w_rows(idx, who, way - 2)
        return pltpu.make_async_remote_copy(
            src_ref=ref, dst_ref=ref, send_sem=ag_send.at[idx, way], recv_sem=ag_recv.at[idx, way],
            device_id={"model": peer(plus)}, device_id_type=MESH)

    def w_local(idx):
        src = (wqT_in, wo_in, wu_in, wd_in)[idx]
        dst = (w_rows(W_Q, me), wo.at[rowsl(me * orows, orows, orows), :], wu.at[:, rowsl(me * fl, fl, fl)], wd.at[rowsl(me * fl, fl, fl), :])[idx]
        return pltpu.make_async_copy(src, dst, ag_loc.at[idx])

    def w_own(idx):
        for way in range(2):
            w_copy(idx, way).start()

    def w_forward(idx):
        for way in range(2):
            w_arrival(idx, way).wait_recv()
        for way in range(2, 4):
            w_copy(idx, way).start()

    def w_wait(idx):
        for way in range(2, 4):
            w_arrival(idx, way).wait_recv()

    def x_copy(c):
        return pltpu.make_async_copy(x_hbm.at[me, pl.ds(c * tc, tc), :], xin.at[c], xsem.at[c])

    def t_copy(c):
        return pltpu.make_async_copy(t_hbm.at[me, pl.ds(c * tc, tc), :], xin.at[c], xsem.at[c])

    @pl.when(first)
    def _():
        for c in range(nc):
            x_copy(c).start()

    @pl.when(last)
    def _():
        for c in range(nc):
            t_copy(c).start()

    for idx in range(4):
        w_local(idx).start()

    odd = lax.rem(st, 2) == 1
    early = st < 2

    @pl.when(odd)
    def _():
        pl.semaphore_wait(go_sem, 1)

    w_own(W_Q)
    w_local(W_O).wait()
    woT[:, rowsl(me * orows, orows, orows)] = jnp.transpose(wo[rowsl(me * orows, orows, orows), :])
    w_own(W_O)
    w_local(W_U).wait()
    wuT[rowsl(me * fl, fl, fl), :] = jnp.transpose(wu[:, rowsl(me * fl, fl, fl)])
    w_local(W_Q).wait()
    w_forward(W_Q)
    w_own(W_U)
    w_local(W_D).wait()
    wdT[:, rowsl(me * fl, fl, fl)] = jnp.transpose(wd[rowsl(me * fl, fl, fl), :])
    w_forward(W_O)
    w_own(W_D)

    @pl.when(jnp.logical_not(odd))
    def _():
        pl.semaphore_signal(go_sem, inc=1, device_id={"stage": nxt}, device_id_type=MESH)

    def natural_weights():
        @pl.loop(0, nm)
        def _(f):
            wu[:, rowsl(f * fl, fl, fl)] = jnp.transpose(wuT[rowsl(f * fl, fl, fl), :])
            wd[rowsl(f * fl, fl, fl), :] = jnp.transpose(wdT[:, rowsl(f * fl, fl, fl)])
            wo[rowsl(f * orows, orows, orows), :] = jnp.transpose(woT[:, rowsl(f * orows, orows, orows)])
            wq[:, rowsl(f * qrows, qrows, qrows)] = jnp.transpose(wqT[rowsl(f * qrows, qrows, qrows), :])

    late = st >= max(2, ns // 2)

    @pl.when(jnp.logical_not(early))
    def _():
        w_forward(W_U)
        w_forward(W_D)
        for idx in range(4):
            w_wait(idx)

    @pl.when(late)
    def _():
        natural_weights()

    def f_copy(c):
        return pltpu.make_async_remote_copy(
            src_ref=ybuf.at[c], dst_ref=hbuf.at[c], send_sem=fsend.at[c], recv_sem=frecv.at[c],
            device_id={"stage": nxt}, device_id_type=MESH)

    def b_copy(c):
        return pltpu.make_async_remote_copy(
            src_ref=ybuf.at[c], dst_ref=dybuf.at[c], send_sem=bsend.at[c], recv_sem=brecv.at[c],
            device_id={"stage": prv}, device_id_type=MESH)

    def ring_copy(src, dst, send, recv, way):
        return pltpu.make_async_remote_copy(
            src_ref=src, dst_ref=dst, send_sem=send, recv_sem=recv,
            device_id={"model": peer((plus, minus)[way % 2])}, device_id_type=MESH)

    hf = fl // 2

    def z_copy(c, way):
        if way < 2:
            src, dst = zbuf.at[c, rowsl(peer((plus, minus)[way]) * fl, fl, fl), :], z_recv.at[way, c]
        elif way < 4:
            src, dst = zbuf.at[c, rowsl(peer(far) * fl + (way - 2) * hf, hf, hf), :], z_fwd.at[way - 2, c]
        else:
            src, dst = z_fwd.at[way - 4, c], z_recv.at[2, c, pl.ds((way - 4) * hf, hf)]
        return ring_copy(src, dst, z_send.at[way, c], z_arr.at[way, c], way)

    def z_forward(c):
        for way in (2, 3):
            z_copy(c, way).wait_recv()
        for way in (4, 5):
            z_copy(c, way).start()

    def dy_copy(c, way):
        if way < 2:
            src, dst = dybuf.at[c], dy_recv.at[way, c]
        else:
            rows = pl.ds((way - 2) * (dm_ // 2), dm_ // 2)
            src, dst = dy_recv.at[way - 2, c, rows], dy_recv.at[2, c, rows]
        return ring_copy(src, dst, dy_send.at[way, c], dy_arr.at[way, c], way)

    def dy_forward(c):
        for way in (0, 1):
            dy_copy(c, way).wait_recv()
        for way in (2, 3):
            dy_copy(c, way).start()

    lossv[...] = jnp.zeros_like(lossv)

    def head_rows(p, h, part):
        return pl.ds(p * (2 * 3 * hd) + (h * 3 + part) * hd, hd)

    k_lane = (0, 2 * 2 * hd)
    v_lane = (2 * hd, 2 * 2 * hd)
    two = 2 * hd

    def pad_k(val, h):
        zero = jnp.zeros_like(val)
        return jnp.concatenate([zero, val] if h == 0 else [val, zero], axis=0)

    def pad_v(val, h):
        zero = jnp.zeros_like(val)
        return jnp.concatenate([val, zero] if h == 0 else [zero, val], axis=0)

    def causal(shape, row0):
        return lax.broadcasted_iota(jnp.int32, shape, 0) + row0 <= lax.broadcasted_iota(jnp.int32, shape, 1)

    def attention(cc):
        nk = (cc + 1) * tc
        slots = min(heads, sscr.shape[0] // nk)
        ahead = min(4, slots - 1)
        sub = tc // 2

        def front(head):
            p, h = head // 2, head % 2
            base = (head % slots) * nk
            qz = pad_k(qkv[cc, head_rows(p, h, 0), :], h)
            tops, sums = [], []
            for j in range(cc + 1):
                s = dot(qkvn[p, pl.ds(j * tc, tc), pl.ds(k_lane[h], two)], qz)
                for r in range(0, tc, sub):
                    part = s[r:r + sub]
                    if j == cc:
                        part = jnp.where(causal(part.shape, r), part, NEG)
                    top = jnp.max(part, axis=0, keepdims=True)
                    e = jnp.exp2((part - top) * exp_c)
                    sscr[pl.ds(base + j * tc + r, sub), :] = e
                    tops.append(top)
                    sums.append(jnp.sum(e, axis=0, keepdims=True))
            mx = functools.reduce(jnp.maximum, tops)
            scales = [jnp.exp2((top - mx) * exp_c) for top in tops]
            inv = 1.0 / functools.reduce(jnp.add, [a * b for a, b in zip(scales, sums)])
            return [a * inv for a in scales]

        def back(head, factors):
            p, h = head // 2, head % 2
            base = (head % slots) * nk
            o_t = None
            for j in range(cc + 1):
                parts = []
                for i in range(2):
                    pr = (sscr[pl.ds(base + j * tc + i * sub, sub), :] * factors[2 * j + i]).astype(BF16)
                    pbuf[cc * (cc + 1) // 2 + j, head, pl.ds(i * sub, sub), :] = pr
                    parts.append(pr)
                part = dot(qkv[j, head_rows(p, h, 2), :], jnp.concatenate(parts, axis=0))
                o_t = part if o_t is None else o_t + part
            obuf[cc, pl.ds(head * hd, hd), :] = o_t.astype(BF16)

        factors = {}
        for head in range(ahead):
            factors[head] = front(head)
        for head in range(heads):
            if head + ahead < heads:
                factors[head + ahead] = front(head + ahead)
            back(head, factors.pop(head))

    def attention_grad(cc):
        units = [(p, j) for p in range(heads // 2) for j in range(cc + 1)]
        dqs = {}
        held = {}

        def of_head(p, h):
            if (p, h) not in held:
                rows = pl.ds((p * 2 + h) * hd, hd)
                do_t = dobuf[rows, :]
                dsum = jnp.sum(do_t.astype(F32) * obuf[cc, rows, :].astype(F32), axis=0, keepdims=True)
                held[p, h] = (pad_v(do_t, h), dsum)
            return held[p, h]

        def front(p, j):
            out = []
            for h in range(2):
                do_z, dsum = of_head(p, h)
                pr = pbuf[cc * (cc + 1) // 2 + j, p * 2 + h]
                dp = dot(qkvn[p, pl.ds(j * tc, tc), pl.ds(v_lane[h], two)], do_z).astype(BF16).astype(F32)
                out.append((pr.astype(F32) * (dp - dsum)).astype(BF16))
            return out

        def back(p, j, ds):
            dv_new = dk_new = None
            for h in range(2):
                do_z, _ = of_head(p, h)
                dv_h = dot_t(pbuf[cc * (cc + 1) // 2 + j, p * 2 + h], do_z)
                dk_h = dot_t(ds[h], pad_v(qkv[cc, head_rows(p, h, 0), :], h))
                dv_new = dv_h if dv_new is None else dv_new + dv_h
                dk_new = dk_h if dk_new is None else dk_new + dk_h
                dq_h = dot(qkv[j, head_rows(p, h, 1), :], ds[h])
                dqs[p, h] = dq_h if j == 0 else dqs[p, h] + dq_h
            rows = pl.ds(j * tc, tc)
            if cc < nc - 1:
                dv_new = dv_new + dvacc[p, rows, :]
                dk_new = dk_new + dkacc[p, rows, :]
            if j < cc:
                dvacc[p, rows, :] = dv_new
                dkacc[p, rows, :] = dk_new
                return
            dv_t = jnp.transpose(dv_new).astype(BF16)
            dk_t = (jnp.transpose(dk_new) * scale).astype(BF16)
            for h in range(2):
                qkv[cc, head_rows(p, h, 0), :] = (dqs[p, h] * scale).astype(BF16)
                qkv[cc, head_rows(p, h, 1), :] = dk_t[h * hd:(h + 1) * hd, :]
                qkv[cc, head_rows(p, h, 2), :] = dv_t[h * hd:(h + 1) * hd, :]

        ds = front(*units[0])
        for n, unit in enumerate(units):
            later = front(*units[n + 1]) if n + 1 < len(units) else None
            back(*unit, ds)
            ds = later

    def attention_step(c):
        @pl.when(first)
        def _():
            x_copy(c).wait()
            hbuf[c] = jnp.transpose(xin[c])

        @pl.when(jnp.logical_not(first))
        def _():
            f_copy(c).wait_recv()

        @pl.when(early & (c == 0))
        def _():
            w_wait(W_Q)

        h32 = hbuf[c].astype(F32)
        n1 = (h32 * inv_rms(h32)).astype(BF16)
        n1buf[c] = n1
        for r in range(nm):
            rows = pl.ds(r * qrows, qrows)
            blk = dot(wqT[rows, :], n1).astype(BF16)
            qkv[c, rows, :] = blk
            qkvn[r, pl.ds(pl.multiple_of(c * tc, tc), tc), :] = jnp.transpose(blk)

        for cc in range(nc):
            pl.when(c == cc)(functools.partial(attention, cc))

    def mlp_step(c):
        a = dot(woT[...], obuf[c]).astype(BF16)
        m32 = (hbuf[c].astype(F32) + a.astype(F32)).astype(BF16).astype(F32)
        mbuf[c] = m32.astype(BF16)
        n2 = (m32 * inv_rms(m32)).astype(BF16)
        n2buf[c] = n2

        blk = fl // 2
        for f in range(2 * nm):
            rows = pl.ds(f * blk, blk)
            u = dot(wuT[rows, :], n2buf[c]).astype(BF16)
            ubuf[c, rows, :] = u
            zbuf[c, rows, :] = gelu(u.astype(F32)).astype(BF16)
        acc = dot(wdT[...], zbuf[c])
        y32 = (mbuf[c].astype(F32) + acc.astype(BF16).astype(F32)).astype(BF16)
        ybuf[c] = y32

        @pl.when(jnp.logical_not(last))
        def _():
            f_copy(c).start()

        @pl.when(last)
        def _():
            t_copy(c).wait()
            err = ybuf[c].astype(F32) - jnp.transpose(xin[c]).astype(F32)
            lossv[...] += jnp.sum((err * err).reshape(dm_ // 8, 8, tc), axis=0)
            dybuf[c] = (err * inv_d).astype(BF16)

    @pl.loop(0, 2 * nc)
    def _(n):
        attn_turn = jnp.where(early, jnp.where(n < nc, 1, 0), 1 - lax.rem(n, 2))
        c = jnp.where(early, lax.rem(n, nc), n // 2)

        @pl.when(early & (n == 1))
        def _():
            w_forward(W_U)

        @pl.when(early & (n == 2))
        def _():
            w_forward(W_D)

        @pl.when(attn_turn == 1)
        def _():
            attention_step(c)

        @pl.when(early & (n == nc))
        def _():
            w_wait(W_O)
            w_wait(W_U)
            w_wait(W_D)

        @pl.when(attn_turn == 0)
        def _():
            mlp_step(c)

    def z_start():
        for c in range(nc):
            for way in range(4):
                z_copy(c, way).start()

    z_last = st >= ns - 2

    @pl.when(jnp.logical_not(z_last))
    def _():
        z_start()

    @pl.when(jnp.logical_not(late))
    def _():
        natural_weights()
        for c in range(nc):
            z_forward(c)

    def l_copy(k):
        return pltpu.make_async_remote_copy(
            src_ref=losst.at[nm], dst_ref=losst.at[3 - k if nm == 4 else nm - 1 - k], send_sem=lsend.at[k - 1],
            recv_sem=lrecv.at[k - 1], device_id={"model": peer(k)}, device_id_type=MESH)

    def lf_copy():
        return pltpu.make_async_remote_copy(
            src_ref=losst.at[nm + 1], dst_ref=losst.at[nm + 1], send_sem=lfsend, recv_sem=lfrecv,
            device_id={"stage": prv}, device_id_type=MESH)

    @pl.when(last)
    def _():
        tot = jnp.sum(lossv[...]) * (0.5 * inv_d)
        losst[nm] = jnp.full(losst.shape[1:], tot, F32)
        for k in range(1, nm):
            l_copy(k).start()

    @pl.loop(0, nc)
    def _(i):
        c = nc - 1 - i

        @pl.when(jnp.logical_not(last))
        def _():
            b_copy(c).wait_recv()

        for way in range(2):
            dy_copy(c, way).start()

        blk = fl // 4
        for f in range(4 * nm):
            rows = pl.ds(f * blk, blk)
            dz = dot(wd[rows, :], dybuf[c]).astype(BF16).astype(F32)
            ubuf[c, rows, :] = (dz * gelu_grad(ubuf[c, rows, :].astype(F32))).astype(BF16)
        acc = dot(wu[...], ubuf[c])
        dn2 = acc.astype(BF16).astype(F32)
        m32 = mbuf[c].astype(F32)
        pull = norm_pull(m32, inv_rms(m32), dn2).astype(BF16)
        dmid = (dybuf[c].astype(F32) + pull.astype(F32)).astype(BF16)
        mbuf[c] = dmid
        dobuf[...] = dot(wo[...], dmid).astype(BF16)

        for cc in range(nc):
            pl.when(c == cc)(functools.partial(attention_grad, cc))

        dn1 = dot(wq[...], qkv[c]).astype(BF16).astype(F32)
        h32 = hbuf[c].astype(F32)
        pull1 = norm_pull(h32, inv_rms(h32), dn1).astype(BF16)

        @pl.when(jnp.logical_not(last))
        def _():
            f_copy(c).wait_send()

        ybuf[c] = (mbuf[c].astype(F32) + pull1.astype(F32)).astype(BF16)

        @pl.when(jnp.logical_not(first))
        def _():
            b_copy(c).start()

        @pl.when(i > 0)
        def _():
            dy_forward(c + 1)

    dy_forward(0)

    @pl.when(last)
    def _():
        for k in range(1, nm):
            l_copy(k).wait_recv()
        vals = [losst[nm]] + [losst[k - 1] for k in range(1, nm)]
        tot = jnp.zeros_like(vals[0])
        for who in range(nm):
            pick = vals[0]
            for k in range(1, nm):
                pick = jnp.where(peer(k) == who, vals[k], pick)
            tot = tot + pick
        losst[nm + 1] = tot

    @pl.when(jnp.logical_not(last))
    def _():
        lf_copy().wait_recv()

    @pl.when(jnp.logical_not(first))
    def _():
        lf_copy().start()

    loss_out[...] = losst[nm + 1]

    def wgrad(mat, d):
        acc = None
        for c in range(nc):
            if mat == 0:
                part = dot_t(qkv[c, rowsl(d * qrows, qrows, qrows), :], n1buf[c])
            elif mat == 1:
                part = dot_t(obuf[c, rowsl(d * orows, orows, orows), :], mbuf[c])
            elif mat == 2:
                part = dot_t(n2buf[c], ubuf[c, rowsl(d * fl, fl, fl), :])
            else:
                part = dot_t(zbuf[c, rowsl(d * fl, fl, fl), :], dybuf[c])
            acc = part if acc is None else acc + part
        return acc

    sizes = (qrows, orows, dm_)
    offs = (0, qrows, qrows + orows)

    def rows_of(mat):
        return pl.ds(offs[mat], sizes[mat])

    def half_of(mat, half):
        return pl.ds(offs[mat] + half * (sizes[mat] // 2), sizes[mat] // 2)

    def far_copy(mat, half):
        rows = pl.ds(offs[mat] // 2, sizes[mat] // 2)
        return ring_copy(stage_buf.at[0, half_of(mat, half)], (far_p, far_m)[half].at[rows],
                         rs_send.at[mat, half], rs_recv.at[mat, half], half)

    def near_copy(mat, side, half):
        way = 2 + 2 * side + half
        return ring_copy(stage_buf.at[1 + side, half_of(mat, half)], (near_l if side == half else near_e).at[half_of(mat, half)],
                         rs_send.at[mat, way], rs_recv.at[mat, way], side)

    mats = (2, 0, 1)
    for mat in mats:
        stage_buf[0, rows_of(mat)] = wgrad(mat, peer(far))
        for half in range(2):
            far_copy(mat, half).start()
    for mat in mats:
        for side in range(2):
            stage_buf[1 + side, rows_of(mat)] = wgrad(mat, peer((plus, minus)[side]))
            near_copy(mat, side, 1 - side).start()

    @pl.when(z_last)
    def _():
        z_start()

    def load(src, nr):
        return pltpu.make_async_copy(src, radd.at[pl.ds(0, nr)], ld_sem.at[0])

    for mat in mats:
        nr = sizes[mat] // 2
        for half in range(2):
            far_copy(mat, half).wait_recv()
            src = (far_p, far_m)[half].at[pl.ds(offs[mat] // 2, nr)]
            load(src, nr).start()
            load(src, nr).wait()
            stage_buf[1 + half, half_of(mat, half)] += radd[pl.ds(0, nr)]
            near_copy(mat, half, half).start()

    for mat in mats:
        for half in range(2):
            far_copy(mat, half).wait_send()
        stage_buf[0, rows_of(mat)] = wgrad(mat, me)

    def zdy_load(n, buf):
        slot, c = n // nc, lax.rem(n, nc)
        return (pltpu.make_async_copy(z_recv.at[slot, c], zdy.at[buf, pl.ds(0, fl)], ld_sem.at[1 + buf]),
                pltpu.make_async_copy(dy_recv.at[slot, c], zdy.at[buf, pl.ds(fl, dm_)], ld_sem.at[3 + buf]))

    @pl.when(late)
    def _():
        for c in range(nc):
            z_forward(c)

    gdacc[...] = wgrad(3, me)
    for c in range(nc):
        for way in (0, 1, 4, 5):
            z_copy(c, way).wait_recv()
        for way in (2, 3):
            dy_copy(c, way).wait_recv()
    for cp in zdy_load(0, 0):
        cp.start()

    @pl.loop(0, 3 * nc)
    def _(n):
        buf = lax.rem(n, 2)

        @pl.when(n + 1 < 3 * nc)
        def _():
            for cp in zdy_load(n + 1, 1 - buf):
                cp.start()

        for cp in zdy_load(n, buf):
            cp.wait()
        gdacc[...] += dot_t(zdy[buf, pl.ds(0, fl), :], zdy[buf, pl.ds(fl, dm_), :])

    def out_copy(mat):
        if mat == 3:
            return pltpu.make_async_copy(gdacc, sum_out.at[pl.ds(qrows + orows + dm_, fl)], out_sem.at[3])
        return pltpu.make_async_copy(stage_buf.at[0, rows_of(mat)], sum_out.at[rows_of(mat)], out_sem.at[mat])

    out_copy(3).start()
    for mat in mats:
        nr = sizes[mat] // 2
        for side in range(2):
            near_copy(mat, side, 1 - side).wait_recv()
            load(near_e.at[half_of(mat, 1 - side)], nr).start()
            load(near_e.at[half_of(mat, 1 - side)], nr).wait()
            stage_buf[0, half_of(mat, 1 - side)] += radd[pl.ds(0, nr)]
        out_copy(mat).start()
    for mat in mats:
        for side in range(2):
            near_copy(mat, side, side).wait_recv()

    for mat in range(4):
        out_copy(mat).wait()
    for c in range(nc):
        for way in range(6):
            z_copy(c, way).wait_send()
        for way in range(4):
            dy_copy(c, way).wait_send()
    for idx in range(4):
        for way in range(4):
            w_copy(idx, way).wait_send()
    for mat in mats:
        for half in range(2):
            for side in range(2):
                near_copy(mat, side, half).wait_send()

    @pl.when(jnp.logical_not(first))
    def _():
        for c in range(nc):
            b_copy(c).wait_send()
        lf_copy().wait_send()

    @pl.when(last)
    def _():
        for k in range(1, nm):
            l_copy(k).wait_send()


def finish_kernel(sq, so, su, sd, lq, lo, lu, loss, gq, go, gu, gd, loss_out):
    gq[...] = sq[...] + lq[...]
    go[...] = so[...] + lo[...]
    gu[...] = su[...] + lu[...]
    gd[...] = sd[...]
    loss_out[0] = loss[0, 0]


def solution(mesh):
    ns = mesh.shape["stage"]
    nm = mesh.shape["model"]

    def per_device(tokens_in, targets, w_qkv, w_out, w_up, w_down):
        n_micro, seq_len, d_model = tokens_in.shape
        hl, hd, fl = w_qkv.shape[3], w_qkv.shape[5], w_up.shape[3]
        tc = min(CHUNK, seq_len // 2)
        nc = seq_len // tc
        assert n_micro == nm == 4 and w_qkv.shape[1] == 1 and hl == 2
        qrows, orows = hl * 3 * hd, hl * hd
        wqT = jnp.transpose(w_qkv[0, 0], (1, 2, 3, 0)).reshape(qrows, d_model)
        wo = w_out[0, 0].reshape(orows, d_model)
        wu, wd = w_up[0, 0], w_down[0, 0]
        cfg = (ns, nm, nc, tc, d_model, hl, hd, fl)
        heads = nm * hl
        any_spec = pl.BlockSpec(memory_space=pl.ANY)
        f32 = lambda *shape: jax.ShapeDtypeStruct(shape, F32)
        rsum = qrows + orows + d_model
        seqb = nc * tc
        b16 = lambda *shape: jax.ShapeDtypeStruct(shape, BF16)
        out_shape = (f32(rsum + fl, d_model), f32(8, 128), f32(rsum // 2, d_model), f32(rsum // 2, d_model), f32(rsum, d_model),
                     f32(rsum, d_model), b16(3, nc, fl, tc), b16(2, nc, fl // 2, tc), b16(3, nc, d_model, tc))
        vb = lambda *shape: pltpu.VMEM(shape, BF16)
        vf = lambda *shape: pltpu.VMEM(shape, F32)
        dma = lambda *shape: pltpu.SemaphoreType.DMA(shape)
        scratch = [
            vb(nm * qrows, d_model), vb(d_model, nm * orows), vb(nm * fl, d_model), vb(d_model, nm * fl),
            vb(nm * fl, d_model), vb(d_model, nm * fl), vb(nm * orows, d_model), vb(d_model, nm * qrows),
            vb(nc, tc, d_model), vb(nc, d_model, tc), vb(nc, d_model, tc), vb(nc, nm * qrows, tc), vb(nm, seqb, qrows),
            vb(nc, nm * orows, tc), vb(nc, d_model, tc), vb(nc, d_model, tc), vb(nc, nm * fl, tc), vb(nc, nm * fl, tc),
            vb(nc * (nc + 1) // 2, heads, tc, tc), vb(nc, d_model, tc), vf(heads // 2, seqb, 2 * hd), vf(heads // 2, seqb, 2 * hd),
            vf(2 * seqb, tc), vb(nc, d_model, tc), vb(nm * orows, tc), vf(nm + 2, 8, 128), vf(8, tc),
            vf(3, rsum, d_model), vf(256, d_model), vf(fl, d_model), vb(2, fl + d_model, tc),
            dma(4, 4), dma(4, 4), dma(4), pltpu.SemaphoreType.REGULAR, dma(nc), dma(nc), dma(nc), dma(nc), dma(nc),
            dma(nm - 1), dma(nm - 1), pltpu.SemaphoreType.DMA, pltpu.SemaphoreType.DMA,
            dma(3, 6), dma(3, 6), dma(5), dma(4), dma(6, nc), dma(6, nc), dma(4, nc), dma(4, nc),
        ]
        res = pl.pallas_call(
            functools.partial(step_kernel, cfg),
            out_shape=out_shape,
            in_specs=[any_spec] * 6,
            out_specs=[any_spec, pl.BlockSpec(memory_space=pltpu.VMEM)] + [any_spec] * 7,
            scratch_shapes=scratch,
            compiler_params=pltpu.CompilerParams(collective_id=0, has_side_effects=True, vmem_limit_bytes=67043328),
            name="train_step",
        )(tokens_in, targets, wqT, wo, wu, wd)
        part, loss, late = res[0], res[1], res[5]
        steps = 4

        def spec(size, start):
            rows = size // steps
            return pl.BlockSpec((rows, d_model), lambda i: (start // rows + i, 0))

        q_s, o_s, u_s = spec(qrows, 0), spec(orows, qrows), spec(d_model, qrows + orows)
        g_qkv, g_out, g_up, g_down, loss = pl.pallas_call(
            finish_kernel,
            grid=(steps,),
            out_shape=(f32(qrows, d_model), f32(orows, d_model), f32(d_model, fl), f32(fl, d_model), f32(1)),
            in_specs=[q_s, o_s, u_s, spec(fl, rsum), q_s, o_s, u_s, pl.BlockSpec(memory_space=pltpu.SMEM)],
            out_specs=[spec(qrows, 0), spec(orows, 0), spec(d_model, 0), spec(fl, 0), pl.BlockSpec(memory_space=pltpu.SMEM)],
            name="finish",
        )(part, part, part, part, late, late, late, loss)
        g_qkv = jnp.transpose(g_qkv.reshape(hl, 3, hd, d_model), (3, 0, 1, 2))[None, None]
        return g_qkv, g_out.reshape(1, 1, hl, hd, d_model), g_up[None, None], g_down[None, None], loss

    tok_spec = P(None, "data", None)
    qkv_spec = P("stage", None, None, "model", None, None)
    out_spec = P("stage", None, "model", None, None)
    up_spec = P("stage", None, None, "model")
    down_spec = P("stage", None, "model", None)
    g_qkv_spec = P(("data", "stage"), None, None, "model", None, None)
    g_out_spec = P(("data", "stage"), None, "model", None, None)
    g_up_spec = P(("data", "stage"), None, None, "model")
    g_down_spec = P(("data", "stage"), None, "model", None)
    return jax.shard_map(per_device, mesh=mesh, in_specs=(tok_spec, tok_spec, qkv_spec, out_spec, up_spec, down_spec), out_specs=(g_qkv_spec, g_out_spec, g_up_spec, g_down_spec, P("data")), check_vma=False)
```

```python
import functools
import math

import jax
import jax.numpy as jnp
from jax import lax
from jax.experimental import pallas as pl
from jax.experimental.pallas import tpu as pltpu
from jax.sharding import PartitionSpec as P

F32 = jnp.float32
BF16 = jnp.bfloat16
MESH = pl.DeviceIdType.MESH
CHUNK = 256
NEG = -1e30
GELU_C = math.sqrt(2.0 / math.pi)
GELU_A = 0.044715

W_Q, W_O, W_U, W_D = range(4)


def dot(lhs, rhs):
    return jnp.dot(lhs, rhs, preferred_element_type=F32)


def dot_t(lhs, rhs):
    return lax.dot_general(lhs, rhs, (((1,), (1,)), ((), ())), preferred_element_type=F32)


def inv_rms(x32):
    return lax.rsqrt(jnp.mean(x32 * x32, axis=0, keepdims=True) + 1e-6)


def norm_pull(x32, inv, g32):
    mean_gx = jnp.mean(g32 * x32, axis=0, keepdims=True)
    return g32 * inv - x32 * (inv * inv * inv * mean_gx)


def gelu(u):
    tanh = jnp.tanh(u * (GELU_C + (GELU_C * GELU_A) * (u * u)))
    half = 0.5 * u
    return half + half * tanh


def gelu_grad(u):
    u2 = u * u
    sig = 0.5 + 0.5 * jnp.tanh(u * (GELU_C + (GELU_C * GELU_A) * u2))
    slope = u * (2.0 * GELU_C + (6.0 * GELU_C * GELU_A) * u2)
    return sig * (1.0 + slope * (1.0 - sig))


def step_kernel(cfg, x_hbm, t_hbm, wqT_in, wo_in, wu_in, wd_in,
                sum_out, loss_out, far_p, far_m, near_e, near_l, z_recv, z_fwd, dy_recv, gd_far, gd_near,
                wqT, woT, wuT, wdT, wd, wu, wo, wq,
                xin, hbuf, n1buf, qkv, qkvn, obuf, mbuf, n2buf, ubuf, zbuf, pbuf, dybuf, dvacc, dkacc, sscr,
                ybuf, dobuf, losst, lossv, stage_buf, radd, gdacc, zdy,
                ag_send, ag_recv, ag_loc, go_sem, xsem, fsend, frecv, bsend, brecv, lsend, lrecv, lfsend, lfrecv,
                rs_send, rs_recv, ld_sem, out_sem, z_send, z_arr, dy_send, dy_arr, gd_send, gd_recv):
    ns, nm, nc, tc, dm_, hl, hd, fl = cfg
    heads = nm * hl
    qrows = hl * 3 * hd
    orows = hl * hd
    inv_d = 1.0 / (nm * nc * tc * dm_)
    scale = hd ** -0.5
    exp_c = scale * math.log2(math.e)
    me = lax.axis_index("model")
    st = lax.axis_index("stage")
    nxt = lax.rem(st + 1, ns)
    prv = lax.rem(st + ns - 1, ns)
    first = st == 0
    last = st == ns - 1

    def peer(k):
        return lax.rem(me + k, nm)

    bar = pltpu.get_barrier_semaphore()
    pl.semaphore_signal(bar, inc=1, device_id={"stage": nxt}, device_id_type=MESH)
    pl.semaphore_signal(bar, inc=1, device_id={"stage": prv}, device_id_type=MESH)
    for k in range(1, nm):
        pl.semaphore_signal(bar, inc=1, device_id={"model": peer(k)}, device_id_type=MESH)
    pl.semaphore_wait(bar, 2 + nm - 1)

    def rowsl(start, size, mult):
        return pl.ds(pl.multiple_of(start, mult), size)

    plus, minus, far = 1, nm - 1, 2

    def w_rows(idx, who, half=None):
        size = (qrows, orows, fl, fl)[idx]
        if idx in (W_Q, W_U):
            buf = wqT if idx == W_Q else wuT
            if half is None:
                return buf.at[rowsl(who * size, size, size), :]
            return buf.at[rowsl(who * size + half * (size // 2), size // 2, size // 2), :]
        view = (woT if idx == W_O else wdT).at[:, rowsl(who * size, size, size)]
        return view if half is None else view.at[pl.ds(half * (dm_ // 2), dm_ // 2), :]

    def w_copy(idx, way):
        to = plus if way in (0, 2) else minus
        if way < 2:
            src = wqT_in if idx == W_Q else w_rows(idx, me)
            dst = w_rows(idx, me)
        else:
            src = dst = w_rows(idx, peer(minus if way == 2 else plus), way - 2)
        return pltpu.make_async_remote_copy(
            src_ref=src, dst_ref=dst, send_sem=ag_send.at[idx, way], recv_sem=ag_recv.at[idx, way],
            device_id={"model": peer(to)}, device_id_type=MESH)

    def w_arrival(idx, way):
        who = peer((minus, plus, far, far)[way])
        ref = w_rows(idx, who) if way < 2 else w_rows(idx, who, way - 2)
        return pltpu.make_async_remote_copy(
            src_ref=ref, dst_ref=ref, send_sem=ag_send.at[idx, way], recv_sem=ag_recv.at[idx, way],
            device_id={"model": peer(plus)}, device_id_type=MESH)

    def w_local(idx):
        src = (wqT_in, wo_in, wu_in, wd_in)[idx]
        dst = (w_rows(W_Q, me), wo.at[rowsl(me * orows, orows, orows), :], wu.at[:, rowsl(me * fl, fl, fl)], wd.at[rowsl(me * fl, fl, fl), :])[idx]
        return pltpu.make_async_copy(src, dst, ag_loc.at[idx])

    def w_own(idx):
        for way in range(2):
            w_copy(idx, way).start()

    def w_forward(idx):
        for way in range(2):
            w_arrival(idx, way).wait_recv()
        for way in range(2, 4):
            w_copy(idx, way).start()

    def w_wait(idx):
        for way in range(2, 4):
            w_arrival(idx, way).wait_recv()

    def x_copy(c):
        return pltpu.make_async_copy(x_hbm.at[me, pl.ds(c * tc, tc), :], xin.at[c], xsem.at[c])

    def t_copy(c):
        return pltpu.make_async_copy(t_hbm.at[me, pl.ds(c * tc, tc), :], xin.at[c], xsem.at[c])

    @pl.when(first)
    def _():
        for c in range(nc):
            x_copy(c).start()

    @pl.when(last)
    def _():
        for c in range(nc):
            t_copy(c).start()

    for idx in range(4):
        w_local(idx).start()

    odd = lax.rem(st, 2) == 1
    early = st < 2

    @pl.when(odd)
    def _():
        pl.semaphore_wait(go_sem, 1)

    w_own(W_Q)
    w_local(W_O).wait()
    woT[:, rowsl(me * orows, orows, orows)] = jnp.transpose(wo[rowsl(me * orows, orows, orows), :])
    w_own(W_O)
    w_local(W_U).wait()
    wuT[rowsl(me * fl, fl, fl), :] = jnp.transpose(wu[:, rowsl(me * fl, fl, fl)])
    w_local(W_Q).wait()
    w_forward(W_Q)
    w_own(W_U)
    w_local(W_D).wait()
    wdT[:, rowsl(me * fl, fl, fl)] = jnp.transpose(wd[rowsl(me * fl, fl, fl), :])
    w_forward(W_O)
    w_own(W_D)

    @pl.when(jnp.logical_not(odd))
    def _():
        pl.semaphore_signal(go_sem, inc=1, device_id={"stage": nxt}, device_id_type=MESH)

    def natural_weights():
        @pl.loop(0, nm)
        def _(f):
            wu[:, rowsl(f * fl, fl, fl)] = jnp.transpose(wuT[rowsl(f * fl, fl, fl), :])
            wd[rowsl(f * fl, fl, fl), :] = jnp.transpose(wdT[:, rowsl(f * fl, fl, fl)])
            wo[rowsl(f * orows, orows, orows), :] = jnp.transpose(woT[:, rowsl(f * orows, orows, orows)])
            wq[:, rowsl(f * qrows, qrows, qrows)] = jnp.transpose(wqT[rowsl(f * qrows, qrows, qrows), :])

    late = st >= max(2, ns // 2)

    @pl.when(jnp.logical_not(early))
    def _():
        w_forward(W_U)
        w_forward(W_D)
        for idx in range(4):
            w_wait(idx)

    @pl.when(late)
    def _():
        natural_weights()

    def f_copy(c):
        return pltpu.make_async_remote_copy(
            src_ref=ybuf.at[c], dst_ref=hbuf.at[c], send_sem=fsend.at[c], recv_sem=frecv.at[c],
            device_id={"stage": nxt}, device_id_type=MESH)

    def b_copy(c):
        return pltpu.make_async_remote_copy(
            src_ref=ybuf.at[c], dst_ref=dybuf.at[c], send_sem=bsend.at[c], recv_sem=brecv.at[c],
            device_id={"stage": prv}, device_id_type=MESH)

    def ring_copy(src, dst, send, recv, way):
        return pltpu.make_async_remote_copy(
            src_ref=src, dst_ref=dst, send_sem=send, recv_sem=recv,
            device_id={"model": peer((plus, minus)[way % 2])}, device_id_type=MESH)

    hf = fl // 2

    def z_copy(c, way):
        if way < 2:
            src, dst = zbuf.at[c, rowsl(peer((plus, minus)[way]) * fl, fl, fl), :], z_recv.at[way, c]
        elif way < 4:
            src, dst = zbuf.at[c, rowsl(peer(far) * fl + (way - 2) * hf, hf, hf), :], z_fwd.at[way - 2, c]
        else:
            src, dst = z_fwd.at[way - 4, c], z_recv.at[2, c, pl.ds((way - 4) * hf, hf)]
        return ring_copy(src, dst, z_send.at[way, c], z_arr.at[way, c], way)

    def z_forward(c):
        for way in (2, 3):
            z_copy(c, way).wait_recv()
        for way in (4, 5):
            z_copy(c, way).start()

    def dy_copy(c, way):
        if way < 2:
            src, dst = dybuf.at[c], dy_recv.at[way, c]
        else:
            rows = pl.ds((way - 2) * (dm_ // 2), dm_ // 2)
            src, dst = dy_recv.at[way - 2, c, rows], dy_recv.at[2, c, rows]
        return ring_copy(src, dst, dy_send.at[way, c], dy_arr.at[way, c], way)

    def dy_forward(c):
        for way in (0, 1):
            dy_copy(c, way).wait_recv()
        for way in (2, 3):
            dy_copy(c, way).start()

    lossv[...] = jnp.zeros_like(lossv)

    def head_rows(p, h, part):
        return pl.ds(p * (2 * 3 * hd) + (h * 3 + part) * hd, hd)

    k_lane = (0, 2 * 2 * hd)
    v_lane = (2 * hd, 2 * 2 * hd)
    two = 2 * hd

    def pad_k(val, h):
        zero = jnp.zeros_like(val)
        return jnp.concatenate([zero, val] if h == 0 else [val, zero], axis=0)

    def pad_v(val, h):
        zero = jnp.zeros_like(val)
        return jnp.concatenate([val, zero] if h == 0 else [zero, val], axis=0)

    def causal(shape, row0):
        return lax.broadcasted_iota(jnp.int32, shape, 0) + row0 <= lax.broadcasted_iota(jnp.int32, shape, 1)

    def attention(cc):
        nk = (cc + 1) * tc
        slots = min(heads, sscr.shape[0] // nk)
        ahead = min(4, slots - 1)
        sub = tc // 2

        def front(head):
            p, h = head // 2, head % 2
            base = (head % slots) * nk
            qz = pad_k(qkv[cc, head_rows(p, h, 0), :], h)
            tops, sums = [], []
            for j in range(cc + 1):
                s = dot(qkvn[p, pl.ds(j * tc, tc), pl.ds(k_lane[h], two)], qz)
                for r in range(0, tc, sub):
                    part = s[r:r + sub]
                    if j == cc:
                        part = jnp.where(causal(part.shape, r), part, NEG)
                    top = jnp.max(part, axis=0, keepdims=True)
                    e = jnp.exp2((part - top) * exp_c)
                    sscr[pl.ds(base + j * tc + r, sub), :] = e
                    tops.append(top)
                    sums.append(jnp.sum(e, axis=0, keepdims=True))
            mx = functools.reduce(jnp.maximum, tops)
            scales = [jnp.exp2((top - mx) * exp_c) for top in tops]
            inv = 1.0 / functools.reduce(jnp.add, [a * b for a, b in zip(scales, sums)])
            return [a * inv for a in scales]

        def back(head, factors):
            p, h = head // 2, head % 2
            base = (head % slots) * nk
            o_t = None
            for j in range(cc + 1):
                parts = []
                for i in range(2):
                    pr = (sscr[pl.ds(base + j * tc + i * sub, sub), :] * factors[2 * j + i]).astype(BF16)
                    pbuf[cc * (cc + 1) // 2 + j, head, pl.ds(i * sub, sub), :] = pr
                    parts.append(pr)
                part = dot(qkv[j, head_rows(p, h, 2), :], jnp.concatenate(parts, axis=0))
                o_t = part if o_t is None else o_t + part
            obuf[cc, pl.ds(head * hd, hd), :] = o_t.astype(BF16)

        factors = {}
        for head in range(ahead):
            factors[head] = front(head)
        for head in range(heads):
            if head + ahead < heads:
                factors[head + ahead] = front(head + ahead)
            back(head, factors.pop(head))

    def attention_grad(cc):
        units = [(p, j) for p in range(heads // 2) for j in range(cc + 1)]
        dqs = {}
        held = {}

        def of_head(p, h):
            if (p, h) not in held:
                rows = pl.ds((p * 2 + h) * hd, hd)
                do_t = dobuf[rows, :]
                dsum = jnp.sum(do_t.astype(F32) * obuf[cc, rows, :].astype(F32), axis=0, keepdims=True)
                held[p, h] = (pad_v(do_t, h), dsum)
            return held[p, h]

        def front(p, j):
            out = []
            for h in range(2):
                do_z, dsum = of_head(p, h)
                pr = pbuf[cc * (cc + 1) // 2 + j, p * 2 + h]
                dp = dot(qkvn[p, pl.ds(j * tc, tc), pl.ds(v_lane[h], two)], do_z).astype(BF16).astype(F32)
                out.append((pr.astype(F32) * (dp - dsum)).astype(BF16))
            return out

        def back(p, j, ds):
            dv_new = dk_new = None
            for h in range(2):
                do_z, _ = of_head(p, h)
                dv_h = dot_t(pbuf[cc * (cc + 1) // 2 + j, p * 2 + h], do_z)
                dk_h = dot_t(ds[h], pad_v(qkv[cc, head_rows(p, h, 0), :], h))
                dv_new = dv_h if dv_new is None else dv_new + dv_h
                dk_new = dk_h if dk_new is None else dk_new + dk_h
                dq_h = dot(qkv[j, head_rows(p, h, 1), :], ds[h])
                dqs[p, h] = dq_h if j == 0 else dqs[p, h] + dq_h
            rows = pl.ds(j * tc, tc)
            if cc < nc - 1:
                dv_new = dv_new + dvacc[p, rows, :]
                dk_new = dk_new + dkacc[p, rows, :]
            if j < cc:
                dvacc[p, rows, :] = dv_new
                dkacc[p, rows, :] = dk_new
                return
            dv_t = jnp.transpose(dv_new).astype(BF16)
            dk_t = (jnp.transpose(dk_new) * scale).astype(BF16)
            for h in range(2):
                qkv[cc, head_rows(p, h, 0), :] = (dqs[p, h] * scale).astype(BF16)
                qkv[cc, head_rows(p, h, 1), :] = dk_t[h * hd:(h + 1) * hd, :]
                qkv[cc, head_rows(p, h, 2), :] = dv_t[h * hd:(h + 1) * hd, :]

        ds = front(*units[0])
        for n, unit in enumerate(units):
            later = front(*units[n + 1]) if n + 1 < len(units) else None
            back(*unit, ds)
            ds = later

    def attention_step(c):
        @pl.when(first)
        def _():
            x_copy(c).wait()
            hbuf[c] = jnp.transpose(xin[c])

        @pl.when(jnp.logical_not(first))
        def _():
            f_copy(c).wait_recv()

        @pl.when(early & (c == 0))
        def _():
            w_wait(W_Q)

        h32 = hbuf[c].astype(F32)
        n1 = (h32 * inv_rms(h32)).astype(BF16)
        n1buf[c] = n1
        for r in range(nm):
            rows = pl.ds(r * qrows, qrows)
            blk = dot(wqT[rows, :], n1).astype(BF16)
            qkv[c, rows, :] = blk
            qkvn[r, pl.ds(pl.multiple_of(c * tc, tc), tc), :] = jnp.transpose(blk)

        for cc in range(nc):
            pl.when(c == cc)(functools.partial(attention, cc))

    def mlp_step(c):
        a = dot(woT[...], obuf[c]).astype(BF16)
        m32 = (hbuf[c].astype(F32) + a.astype(F32)).astype(BF16).astype(F32)
        mbuf[c] = m32.astype(BF16)
        n2 = (m32 * inv_rms(m32)).astype(BF16)
        n2buf[c] = n2

        blk = fl // 2
        for f in range(2 * nm):
            rows = pl.ds(f * blk, blk)
            u = dot(wuT[rows, :], n2buf[c]).astype(BF16)
            ubuf[c, rows, :] = u
            zbuf[c, rows, :] = gelu(u.astype(F32)).astype(BF16)
        acc = dot(wdT[...], zbuf[c])
        y32 = (mbuf[c].astype(F32) + acc.astype(BF16).astype(F32)).astype(BF16)
        ybuf[c] = y32

        @pl.when(jnp.logical_not(last))
        def _():
            f_copy(c).start()

        @pl.when(last)
        def _():
            t_copy(c).wait()
            err = ybuf[c].astype(F32) - jnp.transpose(xin[c]).astype(F32)
            lossv[...] += jnp.sum((err * err).reshape(dm_ // 8, 8, tc), axis=0)
            dybuf[c] = (err * inv_d).astype(BF16)

    @pl.loop(0, 2 * nc)
    def _(n):
        attn_turn = jnp.where(early, jnp.where(n < nc, 1, 0), 1 - lax.rem(n, 2))
        c = jnp.where(early, lax.rem(n, nc), n // 2)

        @pl.when(early & (n == 1))
        def _():
            w_forward(W_U)

        @pl.when(early & (n == 2))
        def _():
            w_forward(W_D)

        @pl.when(attn_turn == 1)
        def _():
            attention_step(c)

        @pl.when(early & (n == nc))
        def _():
            w_wait(W_O)
            w_wait(W_U)
            w_wait(W_D)

        @pl.when(attn_turn == 0)
        def _():
            mlp_step(c)

    def z_start():
        for c in range(nc):
            for way in range(4):
                z_copy(c, way).start()

    @pl.when(jnp.logical_not(late))
    def _():
        z_start()
        natural_weights()
        for c in range(nc):
            z_forward(c)

    def l_copy(k):
        return pltpu.make_async_remote_copy(
            src_ref=losst.at[nm], dst_ref=losst.at[3 - k if nm == 4 else nm - 1 - k], send_sem=lsend.at[k - 1],
            recv_sem=lrecv.at[k - 1], device_id={"model": peer(k)}, device_id_type=MESH)

    def lf_copy():
        return pltpu.make_async_remote_copy(
            src_ref=losst.at[nm + 1], dst_ref=losst.at[nm + 1], send_sem=lfsend, recv_sem=lfrecv,
            device_id={"stage": prv}, device_id_type=MESH)

    @pl.when(last)
    def _():
        tot = jnp.sum(lossv[...]) * (0.5 * inv_d)
        losst[nm] = jnp.full(losst.shape[1:], tot, F32)
        for k in range(1, nm):
            l_copy(k).start()

    @pl.loop(0, nc)
    def _(i):
        c = nc - 1 - i

        @pl.when(jnp.logical_not(last))
        def _():
            b_copy(c).wait_recv()

        @pl.when(jnp.logical_not(late))
        def _():
            for way in range(2):
                dy_copy(c, way).start()

        blk = fl // 4
        for f in range(4 * nm):
            rows = pl.ds(f * blk, blk)
            dz = dot(wd[rows, :], dybuf[c]).astype(BF16).astype(F32)
            ubuf[c, rows, :] = (dz * gelu_grad(ubuf[c, rows, :].astype(F32))).astype(BF16)
        acc = dot(wu[...], ubuf[c])
        dn2 = acc.astype(BF16).astype(F32)
        m32 = mbuf[c].astype(F32)
        pull = norm_pull(m32, inv_rms(m32), dn2).astype(BF16)
        dmid = (dybuf[c].astype(F32) + pull.astype(F32)).astype(BF16)
        mbuf[c] = dmid
        dobuf[...] = dot(wo[...], dmid).astype(BF16)

        for cc in range(nc):
            pl.when(c == cc)(functools.partial(attention_grad, cc))

        dn1 = dot(wq[...], qkv[c]).astype(BF16).astype(F32)
        h32 = hbuf[c].astype(F32)
        pull1 = norm_pull(h32, inv_rms(h32), dn1).astype(BF16)

        @pl.when(jnp.logical_not(last))
        def _():
            f_copy(c).wait_send()

        ybuf[c] = (mbuf[c].astype(F32) + pull1.astype(F32)).astype(BF16)

        @pl.when(jnp.logical_not(first))
        def _():
            b_copy(c).start()

        @pl.when(jnp.logical_not(late) & (i > 0))
        def _():
            dy_forward(c + 1)

    @pl.when(jnp.logical_not(late))
    def _():
        dy_forward(0)

    @pl.when(last)
    def _():
        for k in range(1, nm):
            l_copy(k).wait_recv()
        vals = [losst[nm]] + [losst[k - 1] for k in range(1, nm)]
        tot = jnp.zeros_like(vals[0])
        for who in range(nm):
            pick = vals[0]
            for k in range(1, nm):
                pick = jnp.where(peer(k) == who, vals[k], pick)
            tot = tot + pick
        losst[nm + 1] = tot

    @pl.when(jnp.logical_not(last))
    def _():
        lf_copy().wait_recv()

    @pl.when(jnp.logical_not(first))
    def _():
        lf_copy().start()

    loss_out[...] = losst[nm + 1]

    def wgrad(mat, d):
        acc = None
        for c in range(nc):
            if mat == 0:
                part = dot_t(qkv[c, rowsl(d * qrows, qrows, qrows), :], n1buf[c])
            elif mat == 1:
                part = dot_t(obuf[c, rowsl(d * orows, orows, orows), :], mbuf[c])
            elif mat == 2:
                part = dot_t(n2buf[c], ubuf[c, rowsl(d * fl, fl, fl), :])
            else:
                part = dot_t(zbuf[c, rowsl(d * fl, fl, fl), :], dybuf[c])
            acc = part if acc is None else acc + part
        return acc

    sizes = (qrows, orows, dm_)
    offs = (0, qrows, qrows + orows)

    def rows_of(mat):
        return pl.ds(offs[mat], sizes[mat])

    def half_of(mat, half):
        return pl.ds(offs[mat] + half * (sizes[mat] // 2), sizes[mat] // 2)

    def far_copy(mat, half):
        rows = pl.ds(offs[mat] // 2, sizes[mat] // 2)
        return ring_copy(stage_buf.at[0, half_of(mat, half)], (far_p, far_m)[half].at[rows],
                         rs_send.at[mat, half], rs_recv.at[mat, half], half)

    def near_copy(mat, side, half):
        way = 2 + 2 * side + half
        return ring_copy(stage_buf.at[1 + side, half_of(mat, half)], (near_l if side == half else near_e).at[half_of(mat, half)],
                         rs_send.at[mat, way], rs_recv.at[mat, way], side)

    mats = (2, 0, 1)
    for mat in mats:
        stage_buf[0, rows_of(mat)] = wgrad(mat, peer(far))
        for half in range(2):
            far_copy(mat, half).start()
    for mat in mats:
        for side in range(2):
            stage_buf[1 + side, rows_of(mat)] = wgrad(mat, peer((plus, minus)[side]))
            near_copy(mat, side, 1 - side).start()

    hd2 = dm_ // 2

    def gd_cols(half):
        return pl.ds(half * hd2, hd2)

    def gd_half(d, half):
        return functools.reduce(jnp.add, [
            dot_t(zbuf[c, rowsl(d * fl, fl, fl), :], dybuf[c, gd_cols(half), :]) for c in range(nc)])

    def gd_far_copy(half):
        return ring_copy(gdacc.at[:, gd_cols(half)], gd_far.at[half], gd_send.at[half], gd_recv.at[half], half)

    def gd_slot(side, half):
        return pl.ds((2 * side + half) * fl, fl)

    def gd_near_copy(side, half):
        way = 2 + 2 * side + half
        return ring_copy(sscr.at[gd_slot(side, half)], gd_near.at[1 if side == half else 0, half],
                         gd_send.at[way], gd_recv.at[way], side)

    @pl.when(late)
    def _():
        for half in range(2):
            gdacc[:, gd_cols(half)] = gd_half(peer(far), half)
            gd_far_copy(half).start()
        for side in range(2):
            for half in (1 - side, side):
                sscr[gd_slot(side, half), :] = gd_half(peer((plus, minus)[side]), half)
            gd_near_copy(side, 1 - side).start()

    def load(src, nr):
        return pltpu.make_async_copy(src, radd.at[pl.ds(0, nr)], ld_sem.at[0])

    def gd_add(src, ref):
        nr = min(fl, radd.shape[0])
        for r in range(0, fl, nr):
            copy = pltpu.make_async_copy(src.at[pl.ds(r, nr)], radd.at[pl.ds(0, nr), pl.ds(0, hd2)], ld_sem.at[0])
            copy.start()
            copy.wait()
            ref[pl.ds(r, nr), :] += radd[pl.ds(0, nr), pl.ds(0, hd2)]

    for mat in mats:
        nr = sizes[mat] // 2
        for half in range(2):
            far_copy(mat, half).wait_recv()
            src = (far_p, far_m)[half].at[pl.ds(offs[mat] // 2, nr)]
            load(src, nr).start()
            load(src, nr).wait()
            stage_buf[1 + half, half_of(mat, half)] += radd[pl.ds(0, nr)]
            near_copy(mat, half, half).start()

    @pl.when(late)
    def _():
        for half in range(2):
            gd_far_copy(half).wait_recv()
            gd_add(gd_far.at[half], sscr.at[gd_slot(half, half)])
            gd_near_copy(half, half).start()
            gd_far_copy(half).wait_send()

    for mat in mats:
        for half in range(2):
            far_copy(mat, half).wait_send()
        stage_buf[0, rows_of(mat)] = wgrad(mat, me)

    def zdy_load(n, buf):
        slot, c = n // nc, lax.rem(n, nc)
        return (pltpu.make_async_copy(z_recv.at[slot, c], zdy.at[buf, pl.ds(0, fl)], ld_sem.at[1 + buf]),
                pltpu.make_async_copy(dy_recv.at[slot, c], zdy.at[buf, pl.ds(fl, dm_)], ld_sem.at[3 + buf]))

    gdacc[...] = wgrad(3, me)

    @pl.when(jnp.logical_not(late))
    def _():
        for c in range(nc):
            for way in (0, 1, 4, 5):
                z_copy(c, way).wait_recv()
            for way in (2, 3):
                dy_copy(c, way).wait_recv()
        for cp in zdy_load(0, 0):
            cp.start()

        @pl.loop(0, 3 * nc)
        def _(n):
            buf = lax.rem(n, 2)

            @pl.when(n + 1 < 3 * nc)
            def _():
                for cp in zdy_load(n + 1, 1 - buf):
                    cp.start()

            for cp in zdy_load(n, buf):
                cp.wait()
            gdacc[...] += dot_t(zdy[buf, pl.ds(0, fl), :], zdy[buf, pl.ds(fl, dm_), :])

    @pl.when(late)
    def _():
        for last_half in range(2):
            for half in range(2):
                side = half if last_half else 1 - half
                gd_near_copy(side, half).wait_recv()
                gd_add(gd_near.at[last_half, half], gdacc.at[:, gd_cols(half)])

    def out_copy(mat):
        if mat == 3:
            return pltpu.make_async_copy(gdacc, sum_out.at[pl.ds(qrows + orows + dm_, fl)], out_sem.at[3])
        return pltpu.make_async_copy(stage_buf.at[0, rows_of(mat)], sum_out.at[rows_of(mat)], out_sem.at[mat])

    out_copy(3).start()
    for mat in mats:
        nr = sizes[mat] // 2
        for side in range(2):
            near_copy(mat, side, 1 - side).wait_recv()
            load(near_e.at[half_of(mat, 1 - side)], nr).start()
            load(near_e.at[half_of(mat, 1 - side)], nr).wait()
            stage_buf[0, half_of(mat, 1 - side)] += radd[pl.ds(0, nr)]
        out_copy(mat).start()
    for mat in mats:
        for side in range(2):
            near_copy(mat, side, side).wait_recv()

    for mat in range(4):
        out_copy(mat).wait()

    @pl.when(jnp.logical_not(late))
    def _():
        for c in range(nc):
            for way in range(6):
                z_copy(c, way).wait_send()
            for way in range(4):
                dy_copy(c, way).wait_send()

    @pl.when(late)
    def _():
        for side in range(2):
            for half in range(2):
                gd_near_copy(side, half).wait_send()

    for idx in range(4):
        for way in range(4):
            w_copy(idx, way).wait_send()
    for mat in mats:
        for half in range(2):
            for side in range(2):
                near_copy(mat, side, half).wait_send()

    @pl.when(jnp.logical_not(first))
    def _():
        for c in range(nc):
            b_copy(c).wait_send()
        lf_copy().wait_send()

    @pl.when(last)
    def _():
        for k in range(1, nm):
            l_copy(k).wait_send()


def finish_kernel(sq, so, su, sd, lq, lo, lu, loss, gq, go, gu, gd, loss_out):
    gq[...] = sq[...] + lq[...]
    go[...] = so[...] + lo[...]
    gu[...] = su[...] + lu[...]
    gd[...] = sd[...]
    loss_out[0] = loss[0, 0]


def solution(mesh):
    ns = mesh.shape["stage"]
    nm = mesh.shape["model"]

    def per_device(tokens_in, targets, w_qkv, w_out, w_up, w_down):
        n_micro, seq_len, d_model = tokens_in.shape
        hl, hd, fl = w_qkv.shape[3], w_qkv.shape[5], w_up.shape[3]
        tc = min(CHUNK, seq_len // 2)
        nc = seq_len // tc
        assert n_micro == nm == 4 and w_qkv.shape[1] == 1 and hl == 2 and d_model == 2 * tc
        qrows, orows = hl * 3 * hd, hl * hd
        wqT = jnp.transpose(w_qkv[0, 0], (1, 2, 3, 0)).reshape(qrows, d_model)
        wo = w_out[0, 0].reshape(orows, d_model)
        wu, wd = w_up[0, 0], w_down[0, 0]
        cfg = (ns, nm, nc, tc, d_model, hl, hd, fl)
        heads = nm * hl
        any_spec = pl.BlockSpec(memory_space=pl.ANY)
        f32 = lambda *shape: jax.ShapeDtypeStruct(shape, F32)
        rsum = qrows + orows + d_model
        seqb = nc * tc
        b16 = lambda *shape: jax.ShapeDtypeStruct(shape, BF16)
        out_shape = (f32(rsum + fl, d_model), f32(8, 128), f32(rsum // 2, d_model), f32(rsum // 2, d_model), f32(rsum, d_model),
                     f32(rsum, d_model), b16(3, nc, fl, tc), b16(2, nc, fl // 2, tc), b16(3, nc, d_model, tc),
                     f32(2, fl, d_model // 2), f32(2, 2, fl, d_model // 2))
        vb = lambda *shape: pltpu.VMEM(shape, BF16)
        vf = lambda *shape: pltpu.VMEM(shape, F32)
        dma = lambda *shape: pltpu.SemaphoreType.DMA(shape)
        scratch = [
            vb(nm * qrows, d_model), vb(d_model, nm * orows), vb(nm * fl, d_model), vb(d_model, nm * fl),
            vb(nm * fl, d_model), vb(d_model, nm * fl), vb(nm * orows, d_model), vb(d_model, nm * qrows),
            vb(nc, tc, d_model), vb(nc, d_model, tc), vb(nc, d_model, tc), vb(nc, nm * qrows, tc), vb(nm, seqb, qrows),
            vb(nc, nm * orows, tc), vb(nc, d_model, tc), vb(nc, d_model, tc), vb(nc, nm * fl, tc), vb(nc, nm * fl, tc),
            vb(nc * (nc + 1) // 2, heads, tc, tc), vb(nc, d_model, tc), vf(heads // 2, seqb, 2 * hd), vf(heads // 2, seqb, 2 * hd),
            vf(max(2 * seqb, 4 * fl), tc), vb(nc, d_model, tc), vb(nm * orows, tc), vf(nm + 2, 8, 128), vf(8, tc),
            vf(3, rsum, d_model), vf(256, d_model), vf(fl, d_model), vb(2, fl + d_model, tc),
            dma(4, 4), dma(4, 4), dma(4), pltpu.SemaphoreType.REGULAR, dma(nc), dma(nc), dma(nc), dma(nc), dma(nc),
            dma(nm - 1), dma(nm - 1), pltpu.SemaphoreType.DMA, pltpu.SemaphoreType.DMA,
            dma(3, 6), dma(3, 6), dma(5), dma(4), dma(6, nc), dma(6, nc), dma(4, nc), dma(4, nc), dma(6), dma(6),
        ]
        res = pl.pallas_call(
            functools.partial(step_kernel, cfg),
            out_shape=out_shape,
            in_specs=[any_spec] * 6,
            out_specs=[any_spec, pl.BlockSpec(memory_space=pltpu.VMEM)] + [any_spec] * 9,
            scratch_shapes=scratch,
            compiler_params=pltpu.CompilerParams(collective_id=0, has_side_effects=True, vmem_limit_bytes=67043328),
            name="train_step",
        )(tokens_in, targets, wqT, wo, wu, wd)
        part, loss, late = res[0], res[1], res[5]
        steps = 4

        def spec(size, start):
            rows = size // steps
            return pl.BlockSpec((rows, d_model), lambda i: (start // rows + i, 0))

        q_s, o_s, u_s = spec(qrows, 0), spec(orows, qrows), spec(d_model, qrows + orows)
        g_qkv, g_out, g_up, g_down, loss = pl.pallas_call(
            finish_kernel,
            grid=(steps,),
            out_shape=(f32(qrows, d_model), f32(orows, d_model), f32(d_model, fl), f32(fl, d_model), f32(1)),
            in_specs=[q_s, o_s, u_s, spec(fl, rsum), q_s, o_s, u_s, pl.BlockSpec(memory_space=pltpu.SMEM)],
            out_specs=[spec(qrows, 0), spec(orows, 0), spec(d_model, 0), spec(fl, 0), pl.BlockSpec(memory_space=pltpu.SMEM)],
            name="finish",
        )(part, part, part, part, late, late, late, loss)
        g_qkv = jnp.transpose(g_qkv.reshape(hl, 3, hd, d_model), (3, 0, 1, 2))[None, None]
        return g_qkv, g_out.reshape(1, 1, hl, hd, d_model), g_up[None, None], g_down[None, None], loss

    tok_spec = P(None, "data", None)
    qkv_spec = P("stage", None, None, "model", None, None)
    out_spec = P("stage", None, "model", None, None)
    up_spec = P("stage", None, None, "model")
    down_spec = P("stage", None, "model", None)
    g_qkv_spec = P(("data", "stage"), None, None, "model", None, None)
    g_out_spec = P(("data", "stage"), None, "model", None, None)
    g_up_spec = P(("data", "stage"), None, None, "model")
    g_down_spec = P(("data", "stage"), None, "model", None)
    return jax.shard_map(per_device, mesh=mesh, in_specs=(tok_spec, tok_spec, qkv_spec, out_spec, up_spec, down_spec), out_specs=(g_qkv_spec, g_out_spec, g_up_spec, g_down_spec, P("data")), check_vma=False)
```

```python
import functools
import math

import jax
import jax.numpy as jnp
from jax import lax
from jax.experimental import pallas as pl
from jax.experimental.pallas import tpu as pltpu
from jax.sharding import PartitionSpec as P

F32 = jnp.float32
BF16 = jnp.bfloat16
MESH = pl.DeviceIdType.MESH
CHUNK = 256
NEG = -1e30
GELU_C = math.sqrt(2.0 / math.pi)
GELU_A = 0.044715

W_Q, W_O, W_U, W_D = range(4)


def dot(lhs, rhs):
    return jnp.dot(lhs, rhs, preferred_element_type=F32)


def dot_t(lhs, rhs):
    return lax.dot_general(lhs, rhs, (((1,), (1,)), ((), ())), preferred_element_type=F32)


def inv_rms(x32):
    return lax.rsqrt(jnp.mean(x32 * x32, axis=0, keepdims=True) + 1e-6)


def norm_pull(x32, inv, g32):
    mean_gx = jnp.mean(g32 * x32, axis=0, keepdims=True)
    return g32 * inv - x32 * (inv * inv * inv * mean_gx)


def gelu(u):
    tanh = jnp.tanh(u * (GELU_C + (GELU_C * GELU_A) * (u * u)))
    half = 0.5 * u
    return half + half * tanh


def gelu_grad(u):
    u2 = u * u
    sig = 0.5 + 0.5 * jnp.tanh(u * (GELU_C + (GELU_C * GELU_A) * u2))
    slope = u * (2.0 * GELU_C + (6.0 * GELU_C * GELU_A) * u2)
    return sig * (1.0 + slope * (1.0 - sig))


def step_kernel(cfg, x_hbm, t_hbm, wqT_in, wo_in, wu_in, wd_in,
                sum_out, loss_out, far_p, far_m, near_e, near_l, z_recv, z_fwd, dy_recv, gd_far, gd_near,
                wqT, woT, wuT, wdT, wd, wu, wo, wq,
                xin, hbuf, n1buf, qkv, qkvn, obuf, mbuf, n2buf, ubuf, zbuf, pbuf, dybuf, dvacc, dkacc, sscr,
                ybuf, dobuf, losst, lossv, stage_buf, radd, gdacc, zdy,
                ag_send, ag_recv, ag_loc, go_sem, xsem, fsend, frecv, bsend, brecv, lsend, lrecv, lfsend, lfrecv,
                rs_send, rs_recv, ld_sem, out_sem, z_send, z_arr, dy_send, dy_arr, gd_send, gd_recv):
    ns, nm, nc, tc, dm_, hl, hd, fl = cfg
    heads = nm * hl
    qrows = hl * 3 * hd
    orows = hl * hd
    inv_d = 1.0 / (nm * nc * tc * dm_)
    scale = hd ** -0.5
    exp_c = scale * math.log2(math.e)
    me = lax.axis_index("model")
    st = lax.axis_index("stage")
    nxt = lax.rem(st + 1, ns)
    prv = lax.rem(st + ns - 1, ns)
    first = st == 0
    last = st == ns - 1

    def peer(k):
        return lax.rem(me + k, nm)

    bar = pltpu.get_barrier_semaphore()
    pl.semaphore_signal(bar, inc=1, device_id={"stage": nxt}, device_id_type=MESH)
    pl.semaphore_signal(bar, inc=1, device_id={"stage": prv}, device_id_type=MESH)
    for k in range(1, nm):
        pl.semaphore_signal(bar, inc=1, device_id={"model": peer(k)}, device_id_type=MESH)
    pl.semaphore_wait(bar, 2 + nm - 1)

    def rowsl(start, size, mult):
        return pl.ds(pl.multiple_of(start, mult), size)

    plus, minus, far = 1, nm - 1, 2

    def w_rows(idx, who, half=None):
        size = (qrows, orows, fl, fl)[idx]
        if idx in (W_Q, W_U):
            buf = wqT if idx == W_Q else wuT
            if half is None:
                return buf.at[rowsl(who * size, size, size), :]
            return buf.at[rowsl(who * size + half * (size // 2), size // 2, size // 2), :]
        view = (woT if idx == W_O else wdT).at[:, rowsl(who * size, size, size)]
        return view if half is None else view.at[pl.ds(half * (dm_ // 2), dm_ // 2), :]

    def w_copy(idx, way):
        to = plus if way in (0, 2) else minus
        if way < 2:
            src = wqT_in if idx == W_Q else w_rows(idx, me)
            dst = w_rows(idx, me)
        else:
            src = dst = w_rows(idx, peer(minus if way == 2 else plus), way - 2)
        return pltpu.make_async_remote_copy(
            src_ref=src, dst_ref=dst, send_sem=ag_send.at[idx, way], recv_sem=ag_recv.at[idx, way],
            device_id={"model": peer(to)}, device_id_type=MESH)

    def w_arrival(idx, way):
        who = peer((minus, plus, far, far)[way])
        ref = w_rows(idx, who) if way < 2 else w_rows(idx, who, way - 2)
        return pltpu.make_async_remote_copy(
            src_ref=ref, dst_ref=ref, send_sem=ag_send.at[idx, way], recv_sem=ag_recv.at[idx, way],
            device_id={"model": peer(plus)}, device_id_type=MESH)

    def w_local(idx):
        src = (wqT_in, wo_in, wu_in, wd_in)[idx]
        dst = (w_rows(W_Q, me), wo.at[rowsl(me * orows, orows, orows), :], wu.at[:, rowsl(me * fl, fl, fl)], wd.at[rowsl(me * fl, fl, fl), :])[idx]
        return pltpu.make_async_copy(src, dst, ag_loc.at[idx])

    def w_own(idx):
        for way in range(2):
            w_copy(idx, way).start()

    def w_forward(idx):
        for way in range(2):
            w_arrival(idx, way).wait_recv()
        for way in range(2, 4):
            w_copy(idx, way).start()

    def w_wait(idx):
        for way in range(2, 4):
            w_arrival(idx, way).wait_recv()

    def x_copy(c):
        return pltpu.make_async_copy(x_hbm.at[me, pl.ds(c * tc, tc), :], xin.at[c], xsem.at[c])

    def t_copy(c):
        return pltpu.make_async_copy(t_hbm.at[me, pl.ds(c * tc, tc), :], xin.at[c], xsem.at[c])

    @pl.when(first)
    def _():
        for c in range(nc):
            x_copy(c).start()

    @pl.when(last)
    def _():
        for c in range(nc):
            t_copy(c).start()

    for idx in range(4):
        w_local(idx).start()

    odd = lax.rem(st, 2) == 1
    early = st < 2

    @pl.when(odd)
    def _():
        pl.semaphore_wait(go_sem, 1)

    w_own(W_Q)
    w_local(W_O).wait()
    woT[:, rowsl(me * orows, orows, orows)] = jnp.transpose(wo[rowsl(me * orows, orows, orows), :])
    w_own(W_O)
    w_local(W_U).wait()
    wuT[rowsl(me * fl, fl, fl), :] = jnp.transpose(wu[:, rowsl(me * fl, fl, fl)])
    w_local(W_Q).wait()
    w_forward(W_Q)
    w_own(W_U)
    w_local(W_D).wait()
    wdT[:, rowsl(me * fl, fl, fl)] = jnp.transpose(wd[rowsl(me * fl, fl, fl), :])
    w_forward(W_O)
    w_own(W_D)

    @pl.when(jnp.logical_not(odd))
    def _():
        pl.semaphore_signal(go_sem, inc=1, device_id={"stage": nxt}, device_id_type=MESH)

    def natural_weights():
        @pl.loop(0, nm)
        def _(f):
            wu[:, rowsl(f * fl, fl, fl)] = jnp.transpose(wuT[rowsl(f * fl, fl, fl), :])
            wd[rowsl(f * fl, fl, fl), :] = jnp.transpose(wdT[:, rowsl(f * fl, fl, fl)])
            wo[rowsl(f * orows, orows, orows), :] = jnp.transpose(woT[:, rowsl(f * orows, orows, orows)])
            wq[:, rowsl(f * qrows, qrows, qrows)] = jnp.transpose(wqT[rowsl(f * qrows, qrows, qrows), :])

    late = st >= max(2, ns // 2)

    @pl.when(jnp.logical_not(early))
    def _():
        w_forward(W_U)
        w_forward(W_D)
        for idx in range(4):
            w_wait(idx)

    @pl.when(late)
    def _():
        natural_weights()

    def f_copy(c):
        return pltpu.make_async_remote_copy(
            src_ref=ybuf.at[c], dst_ref=hbuf.at[c], send_sem=fsend.at[c], recv_sem=frecv.at[c],
            device_id={"stage": nxt}, device_id_type=MESH)

    def b_copy(c):
        return pltpu.make_async_remote_copy(
            src_ref=ybuf.at[c], dst_ref=dybuf.at[c], send_sem=bsend.at[c], recv_sem=brecv.at[c],
            device_id={"stage": prv}, device_id_type=MESH)

    def ring_copy(src, dst, send, recv, way):
        return pltpu.make_async_remote_copy(
            src_ref=src, dst_ref=dst, send_sem=send, recv_sem=recv,
            device_id={"model": peer((plus, minus)[way % 2])}, device_id_type=MESH)

    hf = fl // 2

    def z_copy(c, way):
        if way < 2:
            src, dst = zbuf.at[c, rowsl(peer((plus, minus)[way]) * fl, fl, fl), :], z_recv.at[way, c]
        elif way < 4:
            src, dst = zbuf.at[c, rowsl(peer(far) * fl + (way - 2) * hf, hf, hf), :], z_fwd.at[way - 2, c]
        else:
            src, dst = z_fwd.at[way - 4, c], z_recv.at[2, c, pl.ds((way - 4) * hf, hf)]
        return ring_copy(src, dst, z_send.at[way, c], z_arr.at[way, c], way)

    def z_forward(c):
        for way in (2, 3):
            z_copy(c, way).wait_recv()
        for way in (4, 5):
            z_copy(c, way).start()

    def dy_copy(c, way):
        if way < 2:
            src, dst = dybuf.at[c], dy_recv.at[way, c]
        else:
            rows = pl.ds((way - 2) * (dm_ // 2), dm_ // 2)
            src, dst = dy_recv.at[way - 2, c, rows], dy_recv.at[2, c, rows]
        return ring_copy(src, dst, dy_send.at[way, c], dy_arr.at[way, c], way)

    def dy_forward(c):
        for way in (0, 1):
            dy_copy(c, way).wait_recv()
        for way in (2, 3):
            dy_copy(c, way).start()

    lossv[...] = jnp.zeros_like(lossv)

    def head_rows(p, h, part):
        return pl.ds(p * (2 * 3 * hd) + (h * 3 + part) * hd, hd)

    k_lane = (0, 2 * 2 * hd)
    v_lane = (2 * hd, 2 * 2 * hd)
    two = 2 * hd

    def pad_k(val, h):
        zero = jnp.zeros_like(val)
        return jnp.concatenate([zero, val] if h == 0 else [val, zero], axis=0)

    def pad_v(val, h):
        zero = jnp.zeros_like(val)
        return jnp.concatenate([val, zero] if h == 0 else [zero, val], axis=0)

    def causal(shape, row0):
        return lax.broadcasted_iota(jnp.int32, shape, 0) + row0 <= lax.broadcasted_iota(jnp.int32, shape, 1)

    def attention(cc):
        nk = (cc + 1) * tc
        slots = min(heads, sscr.shape[0] // nk)
        ahead = min(4, slots - 1)
        sub = tc // 2

        def front(head):
            p, h = head // 2, head % 2
            base = (head % slots) * nk
            qz = pad_k(qkv[cc, head_rows(p, h, 0), :], h)
            tops, sums = [], []
            for j in range(cc + 1):
                s = dot(qkvn[p, pl.ds(j * tc, tc), pl.ds(k_lane[h], two)], qz)
                for r in range(0, tc, sub):
                    part = s[r:r + sub]
                    if j == cc:
                        part = jnp.where(causal(part.shape, r), part, NEG)
                    top = jnp.max(part, axis=0, keepdims=True)
                    e = jnp.exp2((part - top) * exp_c)
                    sscr[pl.ds(base + j * tc + r, sub), :] = e
                    tops.append(top)
                    sums.append(jnp.sum(e, axis=0, keepdims=True))
            mx = functools.reduce(jnp.maximum, tops)
            scales = [jnp.exp2((top - mx) * exp_c) for top in tops]
            inv = 1.0 / functools.reduce(jnp.add, [a * b for a, b in zip(scales, sums)])
            return [a * inv for a in scales]

        def back(head, factors):
            p, h = head // 2, head % 2
            base = (head % slots) * nk
            o_t = None
            for j in range(cc + 1):
                parts = []
                for i in range(2):
                    pr = (sscr[pl.ds(base + j * tc + i * sub, sub), :] * factors[2 * j + i]).astype(BF16)
                    pbuf[cc * (cc + 1) // 2 + j, head, pl.ds(i * sub, sub), :] = pr
                    parts.append(pr)
                part = dot(qkv[j, head_rows(p, h, 2), :], jnp.concatenate(parts, axis=0))
                o_t = part if o_t is None else o_t + part
            obuf[cc, pl.ds(head * hd, hd), :] = o_t.astype(BF16)

        factors = {}
        for head in range(ahead):
            factors[head] = front(head)
        for head in range(heads):
            if head + ahead < heads:
                factors[head + ahead] = front(head + ahead)
            back(head, factors.pop(head))

    def attention_grad(cc):
        units = [(p, j) for p in range(heads // 2) for j in range(cc + 1)]
        dqs = {}
        held = {}

        def of_head(p, h):
            if (p, h) not in held:
                rows = pl.ds((p * 2 + h) * hd, hd)
                do_t = dobuf[rows, :]
                dsum = jnp.sum(do_t.astype(F32) * obuf[cc, rows, :].astype(F32), axis=0, keepdims=True)
                held[p, h] = (pad_v(do_t, h), dsum)
            return held[p, h]

        def front(p, j):
            out = []
            for h in range(2):
                do_z, dsum = of_head(p, h)
                pr = pbuf[cc * (cc + 1) // 2 + j, p * 2 + h]
                dp = dot(qkvn[p, pl.ds(j * tc, tc), pl.ds(v_lane[h], two)], do_z).astype(BF16).astype(F32)
                out.append((pr.astype(F32) * (dp - dsum)).astype(BF16))
            return out

        def back(p, j, ds):
            dv_new = dk_new = None
            for h in range(2):
                do_z, _ = of_head(p, h)
                dv_h = dot_t(pbuf[cc * (cc + 1) // 2 + j, p * 2 + h], do_z)
                dk_h = dot_t(ds[h], pad_v(qkv[cc, head_rows(p, h, 0), :], h))
                dv_new = dv_h if dv_new is None else dv_new + dv_h
                dk_new = dk_h if dk_new is None else dk_new + dk_h
                dq_h = dot(qkv[j, head_rows(p, h, 1), :], ds[h])
                dqs[p, h] = dq_h if j == 0 else dqs[p, h] + dq_h
            rows = pl.ds(j * tc, tc)
            if cc < nc - 1:
                dv_new = dv_new + dvacc[p, rows, :]
                dk_new = dk_new + dkacc[p, rows, :]
            if j < cc:
                dvacc[p, rows, :] = dv_new
                dkacc[p, rows, :] = dk_new
                return
            dv_t = jnp.transpose(dv_new).astype(BF16)
            dk_t = (jnp.transpose(dk_new) * scale).astype(BF16)
            for h in range(2):
                qkv[cc, head_rows(p, h, 0), :] = (dqs[p, h] * scale).astype(BF16)
                qkv[cc, head_rows(p, h, 1), :] = dk_t[h * hd:(h + 1) * hd, :]
                qkv[cc, head_rows(p, h, 2), :] = dv_t[h * hd:(h + 1) * hd, :]

        ds = front(*units[0])
        for n, unit in enumerate(units):
            later = front(*units[n + 1]) if n + 1 < len(units) else None
            back(*unit, ds)
            ds = later

    def attention_step(c):
        @pl.when(first)
        def _():
            x_copy(c).wait()
            hbuf[c] = jnp.transpose(xin[c])

        @pl.when(jnp.logical_not(first))
        def _():
            f_copy(c).wait_recv()

        @pl.when(early & (c == 0))
        def _():
            w_wait(W_Q)

        h32 = hbuf[c].astype(F32)
        n1 = (h32 * inv_rms(h32)).astype(BF16)
        n1buf[c] = n1
        for r in range(nm):
            rows = pl.ds(r * qrows, qrows)
            blk = dot(wqT[rows, :], n1).astype(BF16)
            qkv[c, rows, :] = blk
            qkvn[r, pl.ds(pl.multiple_of(c * tc, tc), tc), :] = jnp.transpose(blk)

        for cc in range(nc):
            pl.when(c == cc)(functools.partial(attention, cc))

    def mlp_step(c):
        a = dot(woT[...], obuf[c]).astype(BF16)
        m32 = (hbuf[c].astype(F32) + a.astype(F32)).astype(BF16).astype(F32)
        mbuf[c] = m32.astype(BF16)
        n2 = (m32 * inv_rms(m32)).astype(BF16)
        n2buf[c] = n2

        blk = fl // 2
        for f in range(2 * nm):
            rows = pl.ds(f * blk, blk)
            u = dot(wuT[rows, :], n2buf[c]).astype(BF16)
            ubuf[c, rows, :] = u
            zbuf[c, rows, :] = gelu(u.astype(F32)).astype(BF16)
        acc = dot(wdT[...], zbuf[c])
        y32 = (mbuf[c].astype(F32) + acc.astype(BF16).astype(F32)).astype(BF16)
        ybuf[c] = y32

        @pl.when(jnp.logical_not(last))
        def _():
            f_copy(c).start()

        @pl.when(last)
        def _():
            t_copy(c).wait()
            err = ybuf[c].astype(F32) - jnp.transpose(xin[c]).astype(F32)
            lossv[...] += jnp.sum((err * err).reshape(dm_ // 8, 8, tc), axis=0)
            dybuf[c] = (err * inv_d).astype(BF16)

    @pl.loop(0, 2 * nc)
    def _(n):
        attn_turn = jnp.where(early, jnp.where(n < nc, 1, 0), 1 - lax.rem(n, 2))
        c = jnp.where(early, lax.rem(n, nc), n // 2)

        @pl.when(early & (n == 1))
        def _():
            w_forward(W_U)

        @pl.when(early & (n == 2))
        def _():
            w_forward(W_D)

        @pl.when(attn_turn == 1)
        def _():
            attention_step(c)

        @pl.when(early & (n == nc))
        def _():
            w_wait(W_O)
            w_wait(W_U)
            w_wait(W_D)

        @pl.when(attn_turn == 0)
        def _():
            mlp_step(c)

    def z_start():
        for c in range(nc):
            for way in range(4):
                z_copy(c, way).start()

    @pl.when(jnp.logical_not(late))
    def _():
        for c in range(nc):
            f_copy(c).wait_send()
        z_start()
        natural_weights()
        for c in range(nc):
            z_forward(c)

    def l_copy(k):
        return pltpu.make_async_remote_copy(
            src_ref=losst.at[nm], dst_ref=losst.at[3 - k if nm == 4 else nm - 1 - k], send_sem=lsend.at[k - 1],
            recv_sem=lrecv.at[k - 1], device_id={"model": peer(k)}, device_id_type=MESH)

    def lf_copy():
        return pltpu.make_async_remote_copy(
            src_ref=losst.at[nm + 1], dst_ref=losst.at[nm + 1], send_sem=lfsend, recv_sem=lfrecv,
            device_id={"stage": prv}, device_id_type=MESH)

    @pl.when(last)
    def _():
        tot = jnp.sum(lossv[...]) * (0.5 * inv_d)
        losst[nm] = jnp.full(losst.shape[1:], tot, F32)
        for k in range(1, nm):
            l_copy(k).start()

    @pl.loop(0, nc)
    def _(i):
        c = nc - 1 - i

        @pl.when(jnp.logical_not(last))
        def _():
            b_copy(c).wait_recv()

        @pl.when(jnp.logical_not(late) & (i == 0))
        def _():
            for way in range(2):
                dy_copy(c, way).start()

        blk = fl // 4
        for f in range(4 * nm):
            rows = pl.ds(f * blk, blk)
            dz = dot(wd[rows, :], dybuf[c]).astype(BF16).astype(F32)
            ubuf[c, rows, :] = (dz * gelu_grad(ubuf[c, rows, :].astype(F32))).astype(BF16)
        acc = dot(wu[...], ubuf[c])
        dn2 = acc.astype(BF16).astype(F32)
        m32 = mbuf[c].astype(F32)
        pull = norm_pull(m32, inv_rms(m32), dn2).astype(BF16)
        dmid = (dybuf[c].astype(F32) + pull.astype(F32)).astype(BF16)
        mbuf[c] = dmid
        dobuf[...] = dot(wo[...], dmid).astype(BF16)

        @pl.when(jnp.logical_not(late) & (i > 0))
        def _():
            for way in range(2):
                dy_copy(c, way).start()

        @pl.when(first & (i > 0))
        def _():
            dy_forward(c + 1)

        for cc in range(nc):
            pl.when(c == cc)(functools.partial(attention_grad, cc))

        dn1 = dot(wq[...], qkv[c]).astype(BF16).astype(F32)
        h32 = hbuf[c].astype(F32)
        pull1 = norm_pull(h32, inv_rms(h32), dn1).astype(BF16)

        @pl.when(late & jnp.logical_not(last))
        def _():
            f_copy(c).wait_send()

        ybuf[c] = (mbuf[c].astype(F32) + pull1.astype(F32)).astype(BF16)

        @pl.when(jnp.logical_not(first))
        def _():
            b_copy(c).start()

    @pl.when(last)
    def _():
        for k in range(1, nm):
            l_copy(k).wait_recv()
        vals = [losst[nm]] + [losst[k - 1] for k in range(1, nm)]
        tot = jnp.zeros_like(vals[0])
        for who in range(nm):
            pick = vals[0]
            for k in range(1, nm):
                pick = jnp.where(peer(k) == who, vals[k], pick)
            tot = tot + pick
        losst[nm + 1] = tot

    @pl.when(jnp.logical_not(last))
    def _():
        lf_copy().wait_recv()

    @pl.when(jnp.logical_not(first))
    def _():
        lf_copy().start()

    loss_out[...] = losst[nm + 1]

    def wgrad(mat, d):
        acc = None
        for c in range(nc):
            if mat == 0:
                part = dot_t(qkv[c, rowsl(d * qrows, qrows, qrows), :], n1buf[c])
            elif mat == 1:
                part = dot_t(obuf[c, rowsl(d * orows, orows, orows), :], mbuf[c])
            elif mat == 2:
                part = dot_t(n2buf[c], ubuf[c, rowsl(d * fl, fl, fl), :])
            else:
                part = dot_t(zbuf[c, rowsl(d * fl, fl, fl), :], dybuf[c])
            acc = part if acc is None else acc + part
        return acc

    sizes = (qrows, orows, dm_)
    offs = (0, qrows, qrows + orows)

    def rows_of(mat):
        return pl.ds(offs[mat], sizes[mat])

    def half_of(mat, half):
        return pl.ds(offs[mat] + half * (sizes[mat] // 2), sizes[mat] // 2)

    def far_copy(mat, half):
        rows = pl.ds(offs[mat] // 2, sizes[mat] // 2)
        return ring_copy(stage_buf.at[0, half_of(mat, half)], (far_p, far_m)[half].at[rows],
                         rs_send.at[mat, half], rs_recv.at[mat, half], half)

    def near_copy(mat, side, half):
        way = 2 + 2 * side + half
        return ring_copy(stage_buf.at[1 + side, half_of(mat, half)], (near_l if side == half else near_e).at[half_of(mat, half)],
                         rs_send.at[mat, way], rs_recv.at[mat, way], side)

    mats = (2, 0, 1)
    for mat in mats:
        stage_buf[0, rows_of(mat)] = wgrad(mat, peer(far))
        for half in range(2):
            far_copy(mat, half).start()
    for mat in mats:
        for side in range(2):
            stage_buf[1 + side, rows_of(mat)] = wgrad(mat, peer((plus, minus)[side]))
            near_copy(mat, side, 1 - side).start()

    @pl.when(first)
    def _():
        dy_forward(0)

    @pl.when(jnp.logical_not(late | first))
    def _():
        for c in reversed(range(nc)):
            dy_forward(c)

    hd2 = dm_ // 2

    def gd_cols(half):
        return pl.ds(half * hd2, hd2)

    def gd_half(d, half):
        return functools.reduce(jnp.add, [
            dot_t(zbuf[c, rowsl(d * fl, fl, fl), :], dybuf[c, gd_cols(half), :]) for c in range(nc)])

    def gd_far_copy(half):
        return ring_copy(gdacc.at[:, gd_cols(half)], gd_far.at[half], gd_send.at[half], gd_recv.at[half], half)

    def gd_slot(side, half):
        return pl.ds((2 * side + half) * fl, fl)

    def gd_near_copy(side, half):
        way = 2 + 2 * side + half
        return ring_copy(sscr.at[gd_slot(side, half)], gd_near.at[1 if side == half else 0, half],
                         gd_send.at[way], gd_recv.at[way], side)

    @pl.when(late)
    def _():
        for half in range(2):
            gdacc[:, gd_cols(half)] = gd_half(peer(far), half)
            gd_far_copy(half).start()
        for side in range(2):
            for half in (1 - side, side):
                sscr[gd_slot(side, half), :] = gd_half(peer((plus, minus)[side]), half)
            gd_near_copy(side, 1 - side).start()

    def load(src, nr):
        return pltpu.make_async_copy(src, radd.at[pl.ds(0, nr)], ld_sem.at[0])

    def gd_add(src, ref):
        nr = min(fl, radd.shape[0])
        for r in range(0, fl, nr):
            copy = pltpu.make_async_copy(src.at[pl.ds(r, nr)], radd.at[pl.ds(0, nr), pl.ds(0, hd2)], ld_sem.at[0])
            copy.start()
            copy.wait()
            ref[pl.ds(r, nr), :] += radd[pl.ds(0, nr), pl.ds(0, hd2)]

    for mat in mats:
        nr = sizes[mat] // 2
        for half in range(2):
            far_copy(mat, half).wait_recv()
            src = (far_p, far_m)[half].at[pl.ds(offs[mat] // 2, nr)]
            load(src, nr).start()
            load(src, nr).wait()
            stage_buf[1 + half, half_of(mat, half)] += radd[pl.ds(0, nr)]
            near_copy(mat, half, half).start()

    @pl.when(late)
    def _():
        for half in range(2):
            gd_far_copy(half).wait_recv()
            gd_add(gd_far.at[half], sscr.at[gd_slot(half, half)])
            gd_near_copy(half, half).start()
            gd_far_copy(half).wait_send()

    for mat in mats:
        for half in range(2):
            far_copy(mat, half).wait_send()
        stage_buf[0, rows_of(mat)] = wgrad(mat, me)

    def zdy_load(n, buf):
        slot, c = n // nc, lax.rem(n, nc)
        return (pltpu.make_async_copy(z_recv.at[slot, c], zdy.at[buf, pl.ds(0, fl)], ld_sem.at[1 + buf]),
                pltpu.make_async_copy(dy_recv.at[slot, c], zdy.at[buf, pl.ds(fl, dm_)], ld_sem.at[3 + buf]))

    gdacc[...] = wgrad(3, me)

    @pl.when(jnp.logical_not(late))
    def _():
        for c in range(nc):
            for way in (0, 1, 4, 5):
                z_copy(c, way).wait_recv()
            for way in (2, 3):
                dy_copy(c, way).wait_recv()
        for cp in zdy_load(0, 0):
            cp.start()

        @pl.loop(0, 3 * nc)
        def _(n):
            buf = lax.rem(n, 2)

            @pl.when(n + 1 < 3 * nc)
            def _():
                for cp in zdy_load(n + 1, 1 - buf):
                    cp.start()

            for cp in zdy_load(n, buf):
                cp.wait()
            gdacc[...] += dot_t(zdy[buf, pl.ds(0, fl), :], zdy[buf, pl.ds(fl, dm_), :])

    @pl.when(late)
    def _():
        for last_half in range(2):
            for half in range(2):
                side = half if last_half else 1 - half
                gd_near_copy(side, half).wait_recv()
                gd_add(gd_near.at[last_half, half], gdacc.at[:, gd_cols(half)])

    def out_copy(mat):
        if mat == 3:
            return pltpu.make_async_copy(gdacc, sum_out.at[pl.ds(qrows + orows + dm_, fl)], out_sem.at[3])
        return pltpu.make_async_copy(stage_buf.at[0, rows_of(mat)], sum_out.at[rows_of(mat)], out_sem.at[mat])

    out_copy(3).start()
    for mat in mats:
        nr = sizes[mat] // 2
        for side in range(2):
            near_copy(mat, side, 1 - side).wait_recv()
            load(near_e.at[half_of(mat, 1 - side)], nr).start()
            load(near_e.at[half_of(mat, 1 - side)], nr).wait()
            stage_buf[0, half_of(mat, 1 - side)] += radd[pl.ds(0, nr)]
        out_copy(mat).start()
    for mat in mats:
        for side in range(2):
            near_copy(mat, side, side).wait_recv()

    for mat in range(4):
        out_copy(mat).wait()

    @pl.when(jnp.logical_not(late))
    def _():
        for c in range(nc):
            for way in range(6):
                z_copy(c, way).wait_send()
            for way in range(4):
                dy_copy(c, way).wait_send()

    @pl.when(late)
    def _():
        for side in range(2):
            for half in range(2):
                gd_near_copy(side, half).wait_send()

    for idx in range(4):
        for way in range(4):
            w_copy(idx, way).wait_send()
    for mat in mats:
        for half in range(2):
            for side in range(2):
                near_copy(mat, side, half).wait_send()

    @pl.when(jnp.logical_not(first))
    def _():
        for c in range(nc):
            b_copy(c).wait_send()
        lf_copy().wait_send()

    @pl.when(last)
    def _():
        for k in range(1, nm):
            l_copy(k).wait_send()


def finish_kernel(sq, so, su, sd, lq, lo, lu, loss, gq, go, gu, gd, loss_out):
    gq[...] = sq[...] + lq[...]
    go[...] = so[...] + lo[...]
    gu[...] = su[...] + lu[...]
    gd[...] = sd[...]
    loss_out[0] = loss[0, 0]


def solution(mesh):
    ns = mesh.shape["stage"]
    nm = mesh.shape["model"]

    def per_device(tokens_in, targets, w_qkv, w_out, w_up, w_down):
        n_micro, seq_len, d_model = tokens_in.shape
        hl, hd, fl = w_qkv.shape[3], w_qkv.shape[5], w_up.shape[3]
        tc = min(CHUNK, seq_len // 2)
        nc = seq_len // tc
        assert n_micro == nm == 4 and w_qkv.shape[1] == 1 and hl == 2 and d_model == 2 * tc
        qrows, orows = hl * 3 * hd, hl * hd
        wqT = jnp.transpose(w_qkv[0, 0], (1, 2, 3, 0)).reshape(qrows, d_model)
        wo = w_out[0, 0].reshape(orows, d_model)
        wu, wd = w_up[0, 0], w_down[0, 0]
        cfg = (ns, nm, nc, tc, d_model, hl, hd, fl)
        heads = nm * hl
        any_spec = pl.BlockSpec(memory_space=pl.ANY)
        f32 = lambda *shape: jax.ShapeDtypeStruct(shape, F32)
        rsum = qrows + orows + d_model
        seqb = nc * tc
        b16 = lambda *shape: jax.ShapeDtypeStruct(shape, BF16)
        out_shape = (f32(rsum + fl, d_model), f32(8, 128), f32(rsum // 2, d_model), f32(rsum // 2, d_model), f32(rsum, d_model),
                     f32(rsum, d_model), b16(3, nc, fl, tc), b16(2, nc, fl // 2, tc), b16(3, nc, d_model, tc),
                     f32(2, fl, d_model // 2), f32(2, 2, fl, d_model // 2))
        vb = lambda *shape: pltpu.VMEM(shape, BF16)
        vf = lambda *shape: pltpu.VMEM(shape, F32)
        dma = lambda *shape: pltpu.SemaphoreType.DMA(shape)
        scratch = [
            vb(nm * qrows, d_model), vb(d_model, nm * orows), vb(nm * fl, d_model), vb(d_model, nm * fl),
            vb(nm * fl, d_model), vb(d_model, nm * fl), vb(nm * orows, d_model), vb(d_model, nm * qrows),
            vb(nc, tc, d_model), vb(nc, d_model, tc), vb(nc, d_model, tc), vb(nc, nm * qrows, tc), vb(nm, seqb, qrows),
            vb(nc, nm * orows, tc), vb(nc, d_model, tc), vb(nc, d_model, tc), vb(nc, nm * fl, tc), vb(nc, nm * fl, tc),
            vb(nc * (nc + 1) // 2, heads, tc, tc), vb(nc, d_model, tc), vf(heads // 2, seqb, 2 * hd), vf(heads // 2, seqb, 2 * hd),
            vf(max(2 * seqb, 4 * fl), tc), vb(nc, d_model, tc), vb(nm * orows, tc), vf(nm + 2, 8, 128), vf(8, tc),
            vf(3, rsum, d_model), vf(256, d_model), vf(fl, d_model), vb(2, fl + d_model, tc),
            dma(4, 4), dma(4, 4), dma(4), pltpu.SemaphoreType.REGULAR, dma(nc), dma(nc), dma(nc), dma(nc), dma(nc),
            dma(nm - 1), dma(nm - 1), pltpu.SemaphoreType.DMA, pltpu.SemaphoreType.DMA,
            dma(3, 6), dma(3, 6), dma(5), dma(4), dma(6, nc), dma(6, nc), dma(4, nc), dma(4, nc), dma(6), dma(6),
        ]
        res = pl.pallas_call(
            functools.partial(step_kernel, cfg),
            out_shape=out_shape,
            in_specs=[any_spec] * 6,
            out_specs=[any_spec, pl.BlockSpec(memory_space=pltpu.VMEM)] + [any_spec] * 9,
            scratch_shapes=scratch,
            compiler_params=pltpu.CompilerParams(collective_id=0, has_side_effects=True, vmem_limit_bytes=67043328),
            name="train_step",
        )(tokens_in, targets, wqT, wo, wu, wd)
        part, loss, late = res[0], res[1], res[5]
        steps = 4

        def spec(size, start):
            rows = size // steps
            return pl.BlockSpec((rows, d_model), lambda i: (start // rows + i, 0))

        q_s, o_s, u_s = spec(qrows, 0), spec(orows, qrows), spec(d_model, qrows + orows)
        g_qkv, g_out, g_up, g_down, loss = pl.pallas_call(
            finish_kernel,
            grid=(steps,),
            out_shape=(f32(qrows, d_model), f32(orows, d_model), f32(d_model, fl), f32(fl, d_model), f32(1)),
            in_specs=[q_s, o_s, u_s, spec(fl, rsum), q_s, o_s, u_s, pl.BlockSpec(memory_space=pltpu.SMEM)],
            out_specs=[spec(qrows, 0), spec(orows, 0), spec(d_model, 0), spec(fl, 0), pl.BlockSpec(memory_space=pltpu.SMEM)],
            name="finish",
        )(part, part, part, part, late, late, late, loss)
        g_qkv = jnp.transpose(g_qkv.reshape(hl, 3, hd, d_model), (3, 0, 1, 2))[None, None]
        return g_qkv, g_out.reshape(1, 1, hl, hd, d_model), g_up[None, None], g_down[None, None], loss

    tok_spec = P(None, "data", None)
    qkv_spec = P("stage", None, None, "model", None, None)
    out_spec = P("stage", None, "model", None, None)
    up_spec = P("stage", None, None, "model")
    down_spec = P("stage", None, "model", None)
    g_qkv_spec = P(("data", "stage"), None, None, "model", None, None)
    g_out_spec = P(("data", "stage"), None, "model", None, None)
    g_up_spec = P(("data", "stage"), None, None, "model")
    g_down_spec = P(("data", "stage"), None, "model", None)
    return jax.shard_map(per_device, mesh=mesh, in_specs=(tok_spec, tok_spec, qkv_spec, out_spec, up_spec, down_spec), out_specs=(g_qkv_spec, g_out_spec, g_up_spec, g_down_spec, P("data")), check_vma=False)
```

```python
import functools
import math

import jax
import jax.numpy as jnp
from jax import lax
from jax.experimental import pallas as pl
from jax.experimental.pallas import tpu as pltpu
from jax.sharding import PartitionSpec as P

F32 = jnp.float32
BF16 = jnp.bfloat16
MESH = pl.DeviceIdType.MESH
CHUNK = 256
NEG = -1e30
GELU_C = math.sqrt(2.0 / math.pi)
GELU_A = 0.044715

W_Q, W_O, W_U, W_D = range(4)


def dot(lhs, rhs):
    return jnp.dot(lhs, rhs, preferred_element_type=F32)


def dot_t(lhs, rhs):
    return lax.dot_general(lhs, rhs, (((1,), (1,)), ((), ())), preferred_element_type=F32)


def inv_rms(x32):
    return lax.rsqrt(jnp.mean(x32 * x32, axis=0, keepdims=True) + 1e-6)


def norm_pull(x32, inv, g32):
    mean_gx = jnp.mean(g32 * x32, axis=0, keepdims=True)
    return g32 * inv - x32 * (inv * inv * inv * mean_gx)


def gelu(u):
    tanh = jnp.tanh(u * (GELU_C + (GELU_C * GELU_A) * (u * u)))
    half = 0.5 * u
    return half + half * tanh


def gelu_grad(u):
    u2 = u * u
    sig = 0.5 + 0.5 * jnp.tanh(u * (GELU_C + (GELU_C * GELU_A) * u2))
    slope = u * (2.0 * GELU_C + (6.0 * GELU_C * GELU_A) * u2)
    return sig * (1.0 + slope * (1.0 - sig))


def step_kernel(cfg, x_hbm, t_hbm, wqT_in, wo_in, wu_in, wd_in,
                sum_out, loss_out, far_p, far_m, near_e, near_l, z_recv, z_fwd, dy_recv, gd_far, gd_near,
                wqT, woT, wuT, wdT, wd, wu, wo, wq,
                xin, hbuf, n1buf, qkv, kn, vn, obuf, mbuf, n2buf, ubuf, zbuf, pbuf, dybuf, dvacc, dkacc, sscr,
                ybuf, dobuf, losst, lossv, stage_buf, radd, gdacc, dsbuf, qsave,
                ag_send, ag_recv, ag_loc, go_sem, xsem, fsend, frecv, bsend, brecv, lsend, lrecv, lfsend, lfrecv,
                rs_send, rs_recv, ld_sem, out_sem, z_send, z_arr, dy_send, dy_arr, gd_send, gd_recv):
    ns, nm, nc, tc, dm_, hl, hd, fl = cfg
    heads = nm * hl
    qrows = hl * 3 * hd
    orows = hl * hd
    inv_d = 1.0 / (nm * nc * tc * dm_)
    scale = hd ** -0.5
    exp_c = scale * math.log2(math.e)
    me = lax.axis_index("model")
    st = lax.axis_index("stage")
    nxt = lax.rem(st + 1, ns)
    prv = lax.rem(st + ns - 1, ns)
    first = st == 0
    last = st == ns - 1

    def peer(k):
        return lax.rem(me + k, nm)

    bar = pltpu.get_barrier_semaphore()
    pl.semaphore_signal(bar, inc=1, device_id={"stage": nxt}, device_id_type=MESH)
    pl.semaphore_signal(bar, inc=1, device_id={"stage": prv}, device_id_type=MESH)
    for k in range(1, nm):
        pl.semaphore_signal(bar, inc=1, device_id={"model": peer(k)}, device_id_type=MESH)
    pl.semaphore_wait(bar, 2 + nm - 1)

    def rowsl(start, size, mult):
        return pl.ds(pl.multiple_of(start, mult), size)

    plus, minus, far = 1, nm - 1, 2

    def w_rows(idx, who, half=None):
        size = (qrows, orows, fl, fl)[idx]
        if idx in (W_Q, W_U):
            buf = wqT if idx == W_Q else wuT
            if half is None:
                return buf.at[rowsl(who * size, size, size), :]
            return buf.at[rowsl(who * size + half * (size // 2), size // 2, size // 2), :]
        view = (woT if idx == W_O else wdT).at[:, rowsl(who * size, size, size)]
        return view if half is None else view.at[pl.ds(half * (dm_ // 2), dm_ // 2), :]

    def w_copy(idx, way):
        to = plus if way in (0, 2) else minus
        if way < 2:
            src = wqT_in if idx == W_Q else w_rows(idx, me)
            dst = w_rows(idx, me)
        else:
            src = dst = w_rows(idx, peer(minus if way == 2 else plus), way - 2)
        return pltpu.make_async_remote_copy(
            src_ref=src, dst_ref=dst, send_sem=ag_send.at[idx, way], recv_sem=ag_recv.at[idx, way],
            device_id={"model": peer(to)}, device_id_type=MESH)

    def w_arrival(idx, way):
        who = peer((minus, plus, far, far)[way])
        ref = w_rows(idx, who) if way < 2 else w_rows(idx, who, way - 2)
        return pltpu.make_async_remote_copy(
            src_ref=ref, dst_ref=ref, send_sem=ag_send.at[idx, way], recv_sem=ag_recv.at[idx, way],
            device_id={"model": peer(plus)}, device_id_type=MESH)

    def w_local(idx):
        src = (wqT_in, wo_in, wu_in, wd_in)[idx]
        dst = (w_rows(W_Q, me), wo.at[rowsl(me * orows, orows, orows), :], wu.at[:, rowsl(me * fl, fl, fl)], wd.at[rowsl(me * fl, fl, fl), :])[idx]
        return pltpu.make_async_copy(src, dst, ag_loc.at[idx])

    def w_own(idx):
        for way in range(2):
            w_copy(idx, way).start()

    def w_forward(idx):
        for way in range(2):
            w_arrival(idx, way).wait_recv()
        for way in range(2, 4):
            w_copy(idx, way).start()

    def w_wait(idx):
        for way in range(2, 4):
            w_arrival(idx, way).wait_recv()

    def x_copy(c):
        return pltpu.make_async_copy(x_hbm.at[me, pl.ds(c * tc, tc), :], xin.at[c], xsem.at[c])

    def t_copy(c):
        return pltpu.make_async_copy(t_hbm.at[me, pl.ds(c * tc, tc), :], xin.at[c], xsem.at[c])

    @pl.when(first)
    def _():
        for c in range(nc):
            x_copy(c).start()

    @pl.when(last)
    def _():
        for c in range(nc):
            t_copy(c).start()

    for idx in range(4):
        w_local(idx).start()

    odd = lax.rem(st, 2) == 1
    early = st < 2

    @pl.when(odd)
    def _():
        pl.semaphore_wait(go_sem, 1)

    w_own(W_Q)
    w_local(W_O).wait()
    woT[:, rowsl(me * orows, orows, orows)] = jnp.transpose(wo[rowsl(me * orows, orows, orows), :])
    w_own(W_O)
    w_local(W_U).wait()
    wuT[rowsl(me * fl, fl, fl), :] = jnp.transpose(wu[:, rowsl(me * fl, fl, fl)])
    w_local(W_Q).wait()
    w_forward(W_Q)
    w_own(W_U)
    w_local(W_D).wait()
    wdT[:, rowsl(me * fl, fl, fl)] = jnp.transpose(wd[rowsl(me * fl, fl, fl), :])
    w_forward(W_O)
    w_own(W_D)

    @pl.when(jnp.logical_not(odd))
    def _():
        pl.semaphore_signal(go_sem, inc=1, device_id={"stage": nxt}, device_id_type=MESH)

    def natural_weights():
        @pl.loop(0, nm)
        def _(f):
            wu[:, rowsl(f * fl, fl, fl)] = jnp.transpose(wuT[rowsl(f * fl, fl, fl), :])
            wd[rowsl(f * fl, fl, fl), :] = jnp.transpose(wdT[:, rowsl(f * fl, fl, fl)])
            wo[rowsl(f * orows, orows, orows), :] = jnp.transpose(woT[:, rowsl(f * orows, orows, orows)])
            wq[:, rowsl(f * qrows, qrows, qrows)] = jnp.transpose(wqT[rowsl(f * qrows, qrows, qrows), :])

    late = st >= max(2, ns // 2)

    @pl.when(jnp.logical_not(early))
    def _():
        w_forward(W_U)
        w_forward(W_D)
        for idx in range(4):
            w_wait(idx)

    @pl.when(late)
    def _():
        natural_weights()

    def f_copy(c):
        return pltpu.make_async_remote_copy(
            src_ref=ybuf.at[c], dst_ref=hbuf.at[c], send_sem=fsend.at[c], recv_sem=frecv.at[c],
            device_id={"stage": nxt}, device_id_type=MESH)

    def b_copy(c):
        return pltpu.make_async_remote_copy(
            src_ref=ybuf.at[c], dst_ref=dybuf.at[c], send_sem=bsend.at[c], recv_sem=brecv.at[c],
            device_id={"stage": prv}, device_id_type=MESH)

    def ring_copy(src, dst, send, recv, way):
        return pltpu.make_async_remote_copy(
            src_ref=src, dst_ref=dst, send_sem=send, recv_sem=recv,
            device_id={"model": peer((plus, minus)[way % 2])}, device_id_type=MESH)

    hf = fl // 2

    def z_copy(c, way):
        if way < 2:
            src, dst = zbuf.at[c, rowsl(peer((plus, minus)[way]) * fl, fl, fl), :], z_recv.at[way, c]
        elif way < 4:
            src, dst = zbuf.at[c, rowsl(peer(far) * fl + (way - 2) * hf, hf, hf), :], z_fwd.at[way - 2, c]
        else:
            src, dst = z_fwd.at[way - 4, c], z_recv.at[2, c, pl.ds((way - 4) * hf, hf)]
        return ring_copy(src, dst, z_send.at[way, c], z_arr.at[way, c], way)

    def z_forward(c):
        for way in (2, 3):
            z_copy(c, way).wait_recv()
        for way in (4, 5):
            z_copy(c, way).start()

    def dy_copy(c, way):
        if way < 2:
            src, dst = dybuf.at[c], dy_recv.at[way, c]
        else:
            rows = pl.ds((way - 2) * (dm_ // 2), dm_ // 2)
            src, dst = dy_recv.at[way - 2, c, rows], dy_recv.at[2, c, rows]
        return ring_copy(src, dst, dy_send.at[way, c], dy_arr.at[way, c], way)

    def dy_forward(c):
        for way in (0, 1):
            dy_copy(c, way).wait_recv()
        for way in (2, 3):
            dy_copy(c, way).start()

    lossv[...] = jnp.zeros_like(lossv)

    def head_rows(p, h, part):
        return pl.ds(p * (2 * 3 * hd) + (h * 3 + part) * hd, hd)

    def pad_head(val, h):
        zero = jnp.zeros_like(val)
        return jnp.concatenate([val, zero] if h == 0 else [zero, val], axis=0)

    def causal(shape, row0):
        return lax.broadcasted_iota(jnp.int32, shape, 0) + row0 <= lax.broadcasted_iota(jnp.int32, shape, 1)

    def attention(cc):
        nk = (cc + 1) * tc
        slots = min(heads, sscr.shape[0] // nk)
        ahead = min(4, slots - 1)
        sub = tc // 2

        def front(head):
            p, h = head // 2, head % 2
            base = (head % slots) * nk
            qz = pad_head(qkv[cc, head_rows(p, h, 0), :], h)
            tops, sums = [], []
            for j in range(cc + 1):
                s = dot(kn[p, pl.ds(j * tc, tc), :], qz)
                for r in range(0, tc, sub):
                    part = s[r:r + sub]
                    if j == cc:
                        part = jnp.where(causal(part.shape, r), part, NEG)
                    top = jnp.max(part, axis=0, keepdims=True)
                    e = jnp.exp2((part - top) * exp_c)
                    sscr[pl.ds(base + j * tc + r, sub), :] = e
                    tops.append(top)
                    sums.append(jnp.sum(e, axis=0, keepdims=True))
            mx = functools.reduce(jnp.maximum, tops)
            scales = [jnp.exp2((top - mx) * exp_c) for top in tops]
            inv = 1.0 / functools.reduce(jnp.add, [a * b for a, b in zip(scales, sums)])
            return [a * inv for a in scales]

        def back(head, factors):
            p, h = head // 2, head % 2
            base = (head % slots) * nk
            o_t = None
            for j in range(cc + 1):
                parts = []
                for i in range(2):
                    pr = (sscr[pl.ds(base + j * tc + i * sub, sub), :] * factors[2 * j + i]).astype(BF16)
                    pbuf[cc * (cc + 1) // 2 + j, head, pl.ds(i * sub, sub), :] = pr
                    parts.append(pr)
                part = dot(qkv[j, head_rows(p, h, 2), :], jnp.concatenate(parts, axis=0))
                o_t = part if o_t is None else o_t + part
            obuf[cc, pl.ds(head * hd, hd), :] = o_t.astype(BF16)

        factors = {}
        for head in range(ahead):
            factors[head] = front(head)
        for head in range(heads):
            if head + ahead < heads:
                factors[head + ahead] = front(head + ahead)
            back(head, factors.pop(head))

    def attention_grad(cc):
        units = [(p, j) for p in range(heads // 2) for j in range(cc + 1)]
        dqs = {}
        held = {}

        def of_head(p, h):
            if (p, h) not in held:
                rows = pl.ds((p * 2 + h) * hd, hd)
                do_t = dobuf[rows, :]
                dsum = jnp.sum(do_t.astype(F32) * obuf[cc, rows, :].astype(F32), axis=0, keepdims=True)
                held[p, h] = (pad_head(do_t, h), dsum)
            return held[p, h]

        def front(p, j):
            out = []
            for h in range(2):
                do_z, dsum = of_head(p, h)
                pr = pbuf[cc * (cc + 1) // 2 + j, p * 2 + h]
                dp = dot(vn[p, pl.ds(j * tc, tc), :], do_z).astype(BF16).astype(F32)
                ds = (pr.astype(F32) * (dp - dsum)).astype(BF16)
                if j < cc:
                    dsbuf[p * 2 + h, pl.ds(j * tc, tc), :] = ds
                out.append(ds)
            return out

        def back(p, j, ds):
            for h in range(2):
                dq_h = dot(qkv[j, head_rows(p, h, 1), :], ds[h])
                dqs[p, h] = dq_h if j == 0 else dqs[p, h] + dq_h
            if j < cc:
                return
            dv_new, dk_new = kv_grad(cc, p, j, [of_head(p, h)[0] for h in range(2)], ds,
                                     [qkv[cc, head_rows(p, h, 0), :] for h in range(2)])
            dv_t = jnp.transpose(dv_new).astype(BF16)
            dk_t = (jnp.transpose(dk_new) * scale).astype(BF16)
            for h in range(2):
                qsave[pl.ds((p * 2 + h) * hd, hd), :] = qkv[cc, head_rows(p, h, 0), :]
                qkv[cc, head_rows(p, h, 0), :] = (dqs[p, h] * scale).astype(BF16)
                qkv[cc, head_rows(p, h, 1), :] = dk_t[h * hd:(h + 1) * hd, :]
                qkv[cc, head_rows(p, h, 2), :] = dv_t[h * hd:(h + 1) * hd, :]

        ds = front(*units[0])
        for n, unit in enumerate(units):
            later = front(*units[n + 1]) if n + 1 < len(units) else None
            back(*unit, ds)
            ds = later

    def kv_grad(cc, p, j, do_z, ds, q_t):
        dv_new = dk_new = None
        for h in range(2):
            dv_h = dot_t(pbuf[cc * (cc + 1) // 2 + j, p * 2 + h], do_z[h])
            dk_h = dot_t(ds[h], pad_head(q_t[h], h))
            dv_new = dv_h if dv_new is None else dv_new + dv_h
            dk_new = dk_h if dk_new is None else dk_new + dk_h
        rows = pl.ds(j * tc, tc)
        if cc < nc - 1:
            dv_new = dv_new + dvacc[p, rows, :]
            dk_new = dk_new + dkacc[p, rows, :]
        return dv_new, dk_new

    def earlier_keys(cc):
        for p in range(heads // 2):
            heads_of = [pl.ds((p * 2 + h) * hd, hd) for h in range(2)]
            do_z = [pad_head(dobuf[heads_of[h], :], h) for h in range(2)]
            q_t = [qsave[heads_of[h], :] for h in range(2)]
            for j in range(cc):
                rows = pl.ds(j * tc, tc)
                dv_new, dk_new = kv_grad(cc, p, j, do_z, [dsbuf[p * 2 + h, rows, :] for h in range(2)], q_t)
                dvacc[p, rows, :] = dv_new
                dkacc[p, rows, :] = dk_new

    def attention_step(c):
        @pl.when(first)
        def _():
            x_copy(c).wait()
            hbuf[c] = jnp.transpose(xin[c])

        @pl.when(jnp.logical_not(first))
        def _():
            f_copy(c).wait_recv()

        @pl.when(early & (c == 0))
        def _():
            w_wait(W_Q)

        h32 = hbuf[c].astype(F32)
        n1 = (h32 * inv_rms(h32)).astype(BF16)
        n1buf[c] = n1
        for r in range(nm):
            rows = pl.ds(r * qrows, qrows)
            blk = dot(wqT[rows, :], n1).astype(BF16)
            qkv[c, rows, :] = blk
            for part, ref in ((1, kn), (2, vn)):
                both = jnp.concatenate([blk[(3 * h + part) * hd:(3 * h + part + 1) * hd] for h in range(2)], axis=0)
                ref[r, pl.ds(pl.multiple_of(c * tc, tc), tc), :] = jnp.transpose(both)

        for cc in range(nc):
            pl.when(c == cc)(functools.partial(attention, cc))

    def mlp_step(c):
        a = dot(woT[...], obuf[c]).astype(BF16)
        m32 = (hbuf[c].astype(F32) + a.astype(F32)).astype(BF16).astype(F32)
        mbuf[c] = m32.astype(BF16)
        n2 = (m32 * inv_rms(m32)).astype(BF16)
        n2buf[c] = n2

        blk = fl // 2
        for f in range(2 * nm):
            rows = pl.ds(f * blk, blk)
            u = dot(wuT[rows, :], n2buf[c]).astype(BF16)
            ubuf[c, rows, :] = u
            zbuf[c, rows, :] = gelu(u.astype(F32)).astype(BF16)
        acc = dot(wdT[...], zbuf[c])
        y32 = (mbuf[c].astype(F32) + acc.astype(BF16).astype(F32)).astype(BF16)
        ybuf[c] = y32

        @pl.when(jnp.logical_not(last))
        def _():
            f_copy(c).start()

        @pl.when(last)
        def _():
            t_copy(c).wait()
            err = ybuf[c].astype(F32) - jnp.transpose(xin[c]).astype(F32)
            lossv[...] += jnp.sum((err * err).reshape(dm_ // 8, 8, tc), axis=0)
            dybuf[c] = (err * inv_d).astype(BF16)

    @pl.loop(0, 2 * nc)
    def _(n):
        attn_turn = jnp.where(early, jnp.where(n < nc, 1, 0), 1 - lax.rem(n, 2))
        c = jnp.where(early, lax.rem(n, nc), n // 2)

        @pl.when(early & (n == 1))
        def _():
            w_forward(W_U)

        @pl.when(early & (n == 2))
        def _():
            w_forward(W_D)

        @pl.when(attn_turn == 1)
        def _():
            attention_step(c)

        @pl.when(early & (n == nc))
        def _():
            w_wait(W_O)
            w_wait(W_U)
            w_wait(W_D)

        @pl.when(attn_turn == 0)
        def _():
            mlp_step(c)

    def z_start():
        for c in range(nc):
            for way in range(4):
                z_copy(c, way).start()

    @pl.when(jnp.logical_not(late))
    def _():
        for c in range(nc):
            f_copy(c).wait_send()
        z_start()
        natural_weights()
        for c in range(nc):
            z_forward(c)

    def l_copy(k):
        return pltpu.make_async_remote_copy(
            src_ref=losst.at[nm], dst_ref=losst.at[3 - k if nm == 4 else nm - 1 - k], send_sem=lsend.at[k - 1],
            recv_sem=lrecv.at[k - 1], device_id={"model": peer(k)}, device_id_type=MESH)

    def lf_copy():
        return pltpu.make_async_remote_copy(
            src_ref=losst.at[nm + 1], dst_ref=losst.at[nm + 1], send_sem=lfsend, recv_sem=lfrecv,
            device_id={"stage": prv}, device_id_type=MESH)

    @pl.when(last)
    def _():
        tot = jnp.sum(lossv[...]) * (0.5 * inv_d)
        losst[nm] = jnp.full(losst.shape[1:], tot, F32)
        for k in range(1, nm):
            l_copy(k).start()

    dy_inside = jnp.logical_not(late) & (first | odd)

    @pl.loop(0, nc)
    def _(i):
        c = nc - 1 - i

        @pl.when(jnp.logical_not(last))
        def _():
            b_copy(c).wait_recv()

        @pl.when(jnp.logical_not(late) & (i == 0))
        def _():
            for way in range(2):
                dy_copy(c, way).start()

        blk = fl // 4
        for f in range(4 * nm):
            rows = pl.ds(f * blk, blk)
            dz = dot(wd[rows, :], dybuf[c]).astype(BF16).astype(F32)
            ubuf[c, rows, :] = (dz * gelu_grad(ubuf[c, rows, :].astype(F32))).astype(BF16)
        acc = dot(wu[...], ubuf[c])
        dn2 = acc.astype(BF16).astype(F32)
        m32 = mbuf[c].astype(F32)
        pull = norm_pull(m32, inv_rms(m32), dn2).astype(BF16)
        dmid = (dybuf[c].astype(F32) + pull.astype(F32)).astype(BF16)
        mbuf[c] = dmid
        dobuf[...] = dot(wo[...], dmid).astype(BF16)

        @pl.when(jnp.logical_not(late) & (i > 0))
        def _():
            for way in range(2):
                dy_copy(c, way).start()

        @pl.when(dy_inside & (i > 0))
        def _():
            dy_forward(c + 1)

        for cc in range(nc):
            pl.when(c == cc)(functools.partial(attention_grad, cc))

        dn1 = dot(wq[...], qkv[c]).astype(BF16).astype(F32)
        h32 = hbuf[c].astype(F32)
        pull1 = norm_pull(h32, inv_rms(h32), dn1).astype(BF16)

        @pl.when(late & jnp.logical_not(last))
        def _():
            f_copy(c).wait_send()

        ybuf[c] = (mbuf[c].astype(F32) + pull1.astype(F32)).astype(BF16)

        @pl.when(jnp.logical_not(first))
        def _():
            b_copy(c).start()

        for cc in range(1, nc):
            pl.when(c == cc)(functools.partial(earlier_keys, cc))

    @pl.when(last)
    def _():
        for k in range(1, nm):
            l_copy(k).wait_recv()
        vals = [losst[nm]] + [losst[k - 1] for k in range(1, nm)]
        tot = jnp.zeros_like(vals[0])
        for who in range(nm):
            pick = vals[0]
            for k in range(1, nm):
                pick = jnp.where(peer(k) == who, vals[k], pick)
            tot = tot + pick
        losst[nm + 1] = tot

    @pl.when(jnp.logical_not(last))
    def _():
        lf_copy().wait_recv()

    @pl.when(jnp.logical_not(first))
    def _():
        lf_copy().start()

    loss_out[...] = losst[nm + 1]

    def wgrad(mat, d):
        acc = None
        for c in range(nc):
            if mat == 0:
                part = dot_t(qkv[c, rowsl(d * qrows, qrows, qrows), :], n1buf[c])
            elif mat == 1:
                part = dot_t(obuf[c, rowsl(d * orows, orows, orows), :], mbuf[c])
            elif mat == 2:
                part = dot_t(n2buf[c], ubuf[c, rowsl(d * fl, fl, fl), :])
            else:
                part = dot_t(zbuf[c, rowsl(d * fl, fl, fl), :], dybuf[c])
            acc = part if acc is None else acc + part
        return acc

    sizes = (qrows, orows, dm_)
    offs = (0, qrows, qrows + orows)

    def rows_of(mat):
        return pl.ds(offs[mat], sizes[mat])

    def half_of(mat, half):
        return pl.ds(offs[mat] + half * (sizes[mat] // 2), sizes[mat] // 2)

    def far_copy(mat, half):
        rows = pl.ds(offs[mat] // 2, sizes[mat] // 2)
        return ring_copy(stage_buf.at[0, half_of(mat, half)], (far_p, far_m)[half].at[rows],
                         rs_send.at[mat, half], rs_recv.at[mat, half], half)

    def near_copy(mat, side, half):
        way = 2 + 2 * side + half
        return ring_copy(stage_buf.at[1 + side, half_of(mat, half)], (near_l if side == half else near_e).at[half_of(mat, half)],
                         rs_send.at[mat, way], rs_recv.at[mat, way], side)

    mats = (2, 0, 1)
    for mat in mats:
        stage_buf[0, rows_of(mat)] = wgrad(mat, peer(far))
        for half in range(2):
            far_copy(mat, half).start()
    for mat in mats:
        for side in range(2):
            stage_buf[1 + side, rows_of(mat)] = wgrad(mat, peer((plus, minus)[side]))
            near_copy(mat, side, 1 - side).start()

    @pl.when(dy_inside)
    def _():
        dy_forward(0)

    @pl.when(jnp.logical_not(late | dy_inside))
    def _():
        for c in reversed(range(nc)):
            dy_forward(c)

    hd2 = dm_ // 2

    def gd_cols(half):
        return pl.ds(half * hd2, hd2)

    def gd_half(d, half):
        return functools.reduce(jnp.add, [
            dot_t(zbuf[c, rowsl(d * fl, fl, fl), :], dybuf[c, gd_cols(half), :]) for c in range(nc)])

    def gd_far_copy(half):
        return ring_copy(gdacc.at[:, gd_cols(half)], gd_far.at[half], gd_send.at[half], gd_recv.at[half], half)

    def gd_slot(side, half):
        return pl.ds((2 * side + half) * fl, fl)

    def gd_near_copy(side, half):
        way = 2 + 2 * side + half
        return ring_copy(sscr.at[gd_slot(side, half)], gd_near.at[1 if side == half else 0, half],
                         gd_send.at[way], gd_recv.at[way], side)

    @pl.when(late)
    def _():
        for half in range(2):
            gdacc[:, gd_cols(half)] = gd_half(peer(far), half)
            gd_far_copy(half).start()
        for side in range(2):
            for half in (1 - side, side):
                sscr[gd_slot(side, half), :] = gd_half(peer((plus, minus)[side]), half)
            gd_near_copy(side, 1 - side).start()

    def load(src, nr):
        return pltpu.make_async_copy(src, radd.at[pl.ds(0, nr)], ld_sem.at[0])

    def gd_add(src, ref):
        nr = min(fl, radd.shape[0])
        for r in range(0, fl, nr):
            copy = pltpu.make_async_copy(src.at[pl.ds(r, nr)], radd.at[pl.ds(0, nr), pl.ds(0, hd2)], ld_sem.at[0])
            copy.start()
            copy.wait()
            ref[pl.ds(r, nr), :] += radd[pl.ds(0, nr), pl.ds(0, hd2)]

    for mat in mats:
        nr = sizes[mat] // 2
        for half in range(2):
            far_copy(mat, half).wait_recv()
            src = (far_p, far_m)[half].at[pl.ds(offs[mat] // 2, nr)]
            load(src, nr).start()
            load(src, nr).wait()
            stage_buf[1 + half, half_of(mat, half)] += radd[pl.ds(0, nr)]
            near_copy(mat, half, half).start()

    @pl.when(late)
    def _():
        for half in range(2):
            gd_far_copy(half).wait_recv()
            gd_add(gd_far.at[half], sscr.at[gd_slot(half, half)])
            gd_near_copy(half, half).start()
            gd_far_copy(half).wait_send()

    for mat in mats:
        for half in range(2):
            far_copy(mat, half).wait_send()
        stage_buf[0, rows_of(mat)] = wgrad(mat, me)

    def zdy_load(n, buf):
        slot, c = n // nc, lax.rem(n, nc)
        return (pltpu.make_async_copy(z_recv.at[slot, c], dsbuf.at[2 * buf, pl.ds(0, fl)], ld_sem.at[1 + buf]),
                pltpu.make_async_copy(dy_recv.at[slot, c], dsbuf.at[2 * buf + 1, pl.ds(0, dm_)], ld_sem.at[3 + buf]))

    gdacc[...] = wgrad(3, me)

    @pl.when(jnp.logical_not(late))
    def _():
        for c in range(nc):
            for way in (0, 1, 4, 5):
                z_copy(c, way).wait_recv()
            for way in (2, 3):
                dy_copy(c, way).wait_recv()
        for cp in zdy_load(0, 0):
            cp.start()

        @pl.loop(0, 3 * nc)
        def _(n):
            buf = lax.rem(n, 2)

            @pl.when(n + 1 < 3 * nc)
            def _():
                for cp in zdy_load(n + 1, 1 - buf):
                    cp.start()

            for cp in zdy_load(n, buf):
                cp.wait()
            gdacc[...] += dot_t(dsbuf[2 * buf, pl.ds(0, fl), :], dsbuf[2 * buf + 1, pl.ds(0, dm_), :])

    def gd_arrivals(last_half):
        for half in range(2):
            side = half if last_half else 1 - half
            gd_near_copy(side, half).wait_recv()
            gd_add(gd_near.at[last_half, half], gdacc.at[:, gd_cols(half)])

    def out_copy(mat):
        if mat == 3:
            return pltpu.make_async_copy(gdacc, sum_out.at[pl.ds(qrows + orows + dm_, fl)], out_sem.at[3])
        return pltpu.make_async_copy(stage_buf.at[0, rows_of(mat)], sum_out.at[rows_of(mat)], out_sem.at[mat])

    for mat in mats:
        nr = sizes[mat] // 2
        for side in range(2):
            near_copy(mat, side, 1 - side).wait_recv()
            load(near_e.at[half_of(mat, 1 - side)], nr).start()
            load(near_e.at[half_of(mat, 1 - side)], nr).wait()
            stage_buf[0, half_of(mat, 1 - side)] += radd[pl.ds(0, nr)]
        out_copy(mat).start()

    @pl.when(late)
    def _():
        gd_arrivals(0)
        gd_arrivals(1)

    out_copy(3).start()
    for mat in mats:
        for side in range(2):
            near_copy(mat, side, side).wait_recv()

    for mat in range(4):
        out_copy(mat).wait()

    @pl.when(jnp.logical_not(late))
    def _():
        for c in range(nc):
            for way in range(6):
                z_copy(c, way).wait_send()
            for way in range(4):
                dy_copy(c, way).wait_send()

    @pl.when(late)
    def _():
        for side in range(2):
            for half in range(2):
                gd_near_copy(side, half).wait_send()

    for idx in range(4):
        for way in range(4):
            w_copy(idx, way).wait_send()
    for mat in mats:
        for half in range(2):
            for side in range(2):
                near_copy(mat, side, half).wait_send()

    @pl.when(jnp.logical_not(first))
    def _():
        for c in range(nc):
            b_copy(c).wait_send()
        lf_copy().wait_send()

    @pl.when(last)
    def _():
        for k in range(1, nm):
            l_copy(k).wait_send()


def finish_kernel(sq, so, su, sd, lq, lo, lu, loss, gq, go, gu, gd, loss_out):
    gq[...] = sq[...] + lq[...]
    go[...] = so[...] + lo[...]
    gu[...] = su[...] + lu[...]
    gd[...] = sd[...]
    loss_out[0] = loss[0, 0]


def solution(mesh):
    ns = mesh.shape["stage"]
    nm = mesh.shape["model"]

    def per_device(tokens_in, targets, w_qkv, w_out, w_up, w_down):
        n_micro, seq_len, d_model = tokens_in.shape
        hl, hd, fl = w_qkv.shape[3], w_qkv.shape[5], w_up.shape[3]
        tc = min(CHUNK, seq_len // 2)
        nc = seq_len // tc
        assert n_micro == nm == 4 and w_qkv.shape[1] == 1 and hl == 2 and d_model == 2 * tc
        qrows, orows = hl * 3 * hd, hl * hd
        wqT = jnp.transpose(w_qkv[0, 0], (1, 2, 3, 0)).reshape(qrows, d_model)
        wo = w_out[0, 0].reshape(orows, d_model)
        wu, wd = w_up[0, 0], w_down[0, 0]
        cfg = (ns, nm, nc, tc, d_model, hl, hd, fl)
        heads = nm * hl
        any_spec = pl.BlockSpec(memory_space=pl.ANY)
        f32 = lambda *shape: jax.ShapeDtypeStruct(shape, F32)
        rsum = qrows + orows + d_model
        seqb = nc * tc
        b16 = lambda *shape: jax.ShapeDtypeStruct(shape, BF16)
        out_shape = (f32(rsum + fl, d_model), f32(8, 128), f32(rsum // 2, d_model), f32(rsum // 2, d_model), f32(rsum, d_model),
                     f32(rsum, d_model), b16(3, nc, fl, tc), b16(2, nc, fl // 2, tc), b16(3, nc, d_model, tc),
                     f32(2, fl, d_model // 2), f32(2, 2, fl, d_model // 2))
        vb = lambda *shape: pltpu.VMEM(shape, BF16)
        vf = lambda *shape: pltpu.VMEM(shape, F32)
        dma = lambda *shape: pltpu.SemaphoreType.DMA(shape)
        scratch = [
            vb(nm * qrows, d_model), vb(d_model, nm * orows), vb(nm * fl, d_model), vb(d_model, nm * fl),
            vb(nm * fl, d_model), vb(d_model, nm * fl), vb(nm * orows, d_model), vb(d_model, nm * qrows),
            vb(nc, tc, d_model), vb(nc, d_model, tc), vb(nc, d_model, tc), vb(nc, nm * qrows, tc), vb(nm, seqb, orows), vb(nm, seqb, orows),
            vb(nc, nm * orows, tc), vb(nc, d_model, tc), vb(nc, d_model, tc), vb(nc, nm * fl, tc), vb(nc, nm * fl, tc),
            vb(nc * (nc + 1) // 2, heads, tc, tc), vb(nc, d_model, tc), vf(heads // 2, seqb, 2 * hd), vf(heads // 2, seqb, 2 * hd),
            vf(max(2 * seqb, 4 * fl), tc), vb(nc, d_model, tc), vb(nm * orows, tc), vf(nm + 2, 8, 128), vf(8, tc),
            vf(3, rsum, d_model), vf(256, d_model), vf(fl, d_model), vb(heads, max((nc - 1) * tc, fl), tc), vb(nm * orows, tc),
            dma(4, 4), dma(4, 4), dma(4), pltpu.SemaphoreType.REGULAR, dma(nc), dma(nc), dma(nc), dma(nc), dma(nc),
            dma(nm - 1), dma(nm - 1), pltpu.SemaphoreType.DMA, pltpu.SemaphoreType.DMA,
            dma(3, 6), dma(3, 6), dma(5), dma(4), dma(6, nc), dma(6, nc), dma(4, nc), dma(4, nc), dma(6), dma(6),
        ]
        res = pl.pallas_call(
            functools.partial(step_kernel, cfg),
            out_shape=out_shape,
            in_specs=[any_spec] * 6,
            out_specs=[any_spec, pl.BlockSpec(memory_space=pltpu.VMEM)] + [any_spec] * 9,
            scratch_shapes=scratch,
            compiler_params=pltpu.CompilerParams(collective_id=0, has_side_effects=True, vmem_limit_bytes=67043328),
            name="train_step",
        )(tokens_in, targets, wqT, wo, wu, wd)
        part, loss, late = res[0], res[1], res[5]
        steps = 4

        def spec(size, start):
            rows = size // steps
            return pl.BlockSpec((rows, d_model), lambda i: (start // rows + i, 0))

        q_s, o_s, u_s = spec(qrows, 0), spec(orows, qrows), spec(d_model, qrows + orows)
        g_qkv, g_out, g_up, g_down, loss = pl.pallas_call(
            finish_kernel,
            grid=(steps,),
            out_shape=(f32(qrows, d_model), f32(orows, d_model), f32(d_model, fl), f32(fl, d_model), f32(1)),
            in_specs=[q_s, o_s, u_s, spec(fl, rsum), q_s, o_s, u_s, pl.BlockSpec(memory_space=pltpu.SMEM)],
            out_specs=[spec(qrows, 0), spec(orows, 0), spec(d_model, 0), spec(fl, 0), pl.BlockSpec(memory_space=pltpu.SMEM)],
            name="finish",
        )(part, part, part, part, late, late, late, loss)
        g_qkv = jnp.transpose(g_qkv.reshape(hl, 3, hd, d_model), (3, 0, 1, 2))[None, None]
        return g_qkv, g_out.reshape(1, 1, hl, hd, d_model), g_up[None, None], g_down[None, None], loss

    tok_spec = P(None, "data", None)
    qkv_spec = P("stage", None, None, "model", None, None)
    out_spec = P("stage", None, "model", None, None)
    up_spec = P("stage", None, None, "model")
    down_spec = P("stage", None, "model", None)
    g_qkv_spec = P(("data", "stage"), None, None, "model", None, None)
    g_out_spec = P(("data", "stage"), None, "model", None, None)
    g_up_spec = P(("data", "stage"), None, None, "model")
    g_down_spec = P(("data", "stage"), None, "model", None)
    return jax.shard_map(per_device, mesh=mesh, in_specs=(tok_spec, tok_spec, qkv_spec, out_spec, up_spec, down_spec), out_specs=(g_qkv_spec, g_out_spec, g_up_spec, g_down_spec, P("data")), check_vma=False)
```

```python
import functools
import math

import jax
import jax.numpy as jnp
from jax import lax
from jax.experimental import pallas as pl
from jax.experimental.pallas import tpu as pltpu
from jax.sharding import PartitionSpec as P

F32 = jnp.float32
BF16 = jnp.bfloat16
MESH = pl.DeviceIdType.MESH
CHUNK = 256
NEG = -1e30
GELU_C = math.sqrt(2.0 / math.pi)
GELU_A = 0.044715

W_Q, W_O, W_U, W_D = range(4)


def dot(lhs, rhs):
    return jnp.dot(lhs, rhs, preferred_element_type=F32)


def dot_t(lhs, rhs):
    return lax.dot_general(lhs, rhs, (((1,), (1,)), ((), ())), preferred_element_type=F32)


def inv_rms(x32):
    return lax.rsqrt(jnp.mean(x32 * x32, axis=0, keepdims=True) + 1e-6)


def norm_pull(x32, inv, g32):
    mean_gx = jnp.mean(g32 * x32, axis=0, keepdims=True)
    return g32 * inv - x32 * (inv * inv * inv * mean_gx)


def gelu(u):
    tanh = jnp.tanh(u * (GELU_C + (GELU_C * GELU_A) * (u * u)))
    half = 0.5 * u
    return half + half * tanh


def gelu_grad(u):
    u2 = u * u
    sig = 0.5 + 0.5 * jnp.tanh(u * (GELU_C + (GELU_C * GELU_A) * u2))
    slope = u * (2.0 * GELU_C + (6.0 * GELU_C * GELU_A) * u2)
    return sig * (1.0 + slope * (1.0 - sig))


def step_kernel(cfg, x_hbm, t_hbm, wqT_in, wo_in, wu_in, wd_in,
                sum_out, loss_out, far_p, far_m, near_e, near_l, z_recv, z_fwd, dy_recv, gd_far, gd_near,
                wqT, woT, wuT, wdT, wd, wu, wo, wq,
                xin, hbuf, n1buf, qkv, kn, vn, obuf, mbuf, n2buf, ubuf, zbuf, pbuf, dybuf, dvacc, dkacc, sscr,
                ybuf, dobuf, losst, lossv, stage_buf, radd, gdacc, dsbuf, qsave,
                ag_send, ag_recv, ag_loc, go_sem, xsem, fsend, frecv, bsend, brecv, lsend, lrecv, lfsend, lfrecv,
                rs_send, rs_recv, ld_sem, out_sem, z_send, z_arr, dy_send, dy_arr, gd_send, gd_recv):
    ns, nm, nc, tc, dm_, hl, hd, fl = cfg
    heads = nm * hl
    qrows = hl * 3 * hd
    orows = hl * hd
    inv_d = 1.0 / (nm * nc * tc * dm_)
    scale = hd ** -0.5
    exp_c = scale * math.log2(math.e)
    me = lax.axis_index("model")
    st = lax.axis_index("stage")
    nxt = lax.rem(st + 1, ns)
    prv = lax.rem(st + ns - 1, ns)
    first = st == 0
    last = st == ns - 1

    def peer(k):
        return lax.rem(me + k, nm)

    bar = pltpu.get_barrier_semaphore()
    pl.semaphore_signal(bar, inc=1, device_id={"stage": nxt}, device_id_type=MESH)
    pl.semaphore_signal(bar, inc=1, device_id={"stage": prv}, device_id_type=MESH)
    for k in range(1, nm):
        pl.semaphore_signal(bar, inc=1, device_id={"model": peer(k)}, device_id_type=MESH)
    pl.semaphore_wait(bar, 2 + nm - 1)

    def rowsl(start, size, mult):
        return pl.ds(pl.multiple_of(start, mult), size)

    plus, minus, far = 1, nm - 1, 2

    def w_rows(idx, who, half=None):
        size = (qrows, orows, fl, fl)[idx]
        if idx in (W_Q, W_U):
            buf = wqT if idx == W_Q else wuT
            if half is None:
                return buf.at[rowsl(who * size, size, size), :]
            return buf.at[rowsl(who * size + half * (size // 2), size // 2, size // 2), :]
        view = (woT if idx == W_O else wdT).at[:, rowsl(who * size, size, size)]
        return view if half is None else view.at[pl.ds(half * (dm_ // 2), dm_ // 2), :]

    def w_copy(idx, way):
        to = plus if way in (0, 2) else minus
        if way < 2:
            src = wqT_in if idx == W_Q else w_rows(idx, me)
            dst = w_rows(idx, me)
        else:
            src = dst = w_rows(idx, peer(minus if way == 2 else plus), way - 2)
        return pltpu.make_async_remote_copy(
            src_ref=src, dst_ref=dst, send_sem=ag_send.at[idx, way], recv_sem=ag_recv.at[idx, way],
            device_id={"model": peer(to)}, device_id_type=MESH)

    def w_arrival(idx, way):
        who = peer((minus, plus, far, far)[way])
        ref = w_rows(idx, who) if way < 2 else w_rows(idx, who, way - 2)
        return pltpu.make_async_remote_copy(
            src_ref=ref, dst_ref=ref, send_sem=ag_send.at[idx, way], recv_sem=ag_recv.at[idx, way],
            device_id={"model": peer(plus)}, device_id_type=MESH)

    def w_local(idx):
        src = (wqT_in, wo_in, wu_in, wd_in)[idx]
        dst = (w_rows(W_Q, me), wo.at[rowsl(me * orows, orows, orows), :], wu.at[:, rowsl(me * fl, fl, fl)], wd.at[rowsl(me * fl, fl, fl), :])[idx]
        return pltpu.make_async_copy(src, dst, ag_loc.at[idx])

    def w_own(idx):
        for way in range(2):
            w_copy(idx, way).start()

    def w_forward(idx):
        for way in range(2):
            w_arrival(idx, way).wait_recv()
        for way in range(2, 4):
            w_copy(idx, way).start()

    def w_wait(idx):
        for way in range(2, 4):
            w_arrival(idx, way).wait_recv()

    def x_copy(c):
        return pltpu.make_async_copy(x_hbm.at[me, pl.ds(c * tc, tc), :], xin.at[c], xsem.at[c])

    def t_copy(c):
        return pltpu.make_async_copy(t_hbm.at[me, pl.ds(c * tc, tc), :], xin.at[c], xsem.at[c])

    @pl.when(first)
    def _():
        for c in range(nc):
            x_copy(c).start()

    @pl.when(last)
    def _():
        for c in range(nc):
            t_copy(c).start()

    for idx in range(4):
        w_local(idx).start()

    odd = lax.rem(st, 2) == 1
    early = st < 2

    @pl.when(odd)
    def _():
        pl.semaphore_wait(go_sem, 1)

    w_own(W_Q)
    w_local(W_O).wait()
    woT[:, rowsl(me * orows, orows, orows)] = jnp.transpose(wo[rowsl(me * orows, orows, orows), :])
    w_own(W_O)
    w_local(W_U).wait()
    wuT[rowsl(me * fl, fl, fl), :] = jnp.transpose(wu[:, rowsl(me * fl, fl, fl)])
    w_local(W_Q).wait()
    w_forward(W_Q)
    w_own(W_U)
    w_local(W_D).wait()
    wdT[:, rowsl(me * fl, fl, fl)] = jnp.transpose(wd[rowsl(me * fl, fl, fl), :])
    w_forward(W_O)
    w_own(W_D)

    @pl.when(jnp.logical_not(odd))
    def _():
        pl.semaphore_signal(go_sem, inc=1, device_id={"stage": nxt}, device_id_type=MESH)

    def natural_weights():
        @pl.loop(0, nm)
        def _(f):
            wu[:, rowsl(f * fl, fl, fl)] = jnp.transpose(wuT[rowsl(f * fl, fl, fl), :])
            wd[rowsl(f * fl, fl, fl), :] = jnp.transpose(wdT[:, rowsl(f * fl, fl, fl)])
            wo[rowsl(f * orows, orows, orows), :] = jnp.transpose(woT[:, rowsl(f * orows, orows, orows)])
            wq[:, rowsl(f * qrows, qrows, qrows)] = jnp.transpose(wqT[rowsl(f * qrows, qrows, qrows), :])

    late = st >= max(2, ns // 2)

    @pl.when(jnp.logical_not(early))
    def _():
        w_forward(W_U)
        w_forward(W_D)
        for idx in range(4):
            w_wait(idx)

    @pl.when(late)
    def _():
        natural_weights()

    def f_copy(c):
        return pltpu.make_async_remote_copy(
            src_ref=ybuf.at[c], dst_ref=hbuf.at[c], send_sem=fsend.at[c], recv_sem=frecv.at[c],
            device_id={"stage": nxt}, device_id_type=MESH)

    def b_copy(c):
        return pltpu.make_async_remote_copy(
            src_ref=ybuf.at[c], dst_ref=dybuf.at[c], send_sem=bsend.at[c], recv_sem=brecv.at[c],
            device_id={"stage": prv}, device_id_type=MESH)

    def ring_copy(src, dst, send, recv, way):
        return pltpu.make_async_remote_copy(
            src_ref=src, dst_ref=dst, send_sem=send, recv_sem=recv,
            device_id={"model": peer((plus, minus)[way % 2])}, device_id_type=MESH)

    hf = fl // 2

    def z_copy(c, way):
        if way < 2:
            src, dst = zbuf.at[c, rowsl(peer((plus, minus)[way]) * fl, fl, fl), :], z_recv.at[way, c]
        elif way < 4:
            src, dst = zbuf.at[c, rowsl(peer(far) * fl + (way - 2) * hf, hf, hf), :], z_fwd.at[way - 2, c]
        else:
            src, dst = z_fwd.at[way - 4, c], z_recv.at[2, c, pl.ds((way - 4) * hf, hf)]
        return ring_copy(src, dst, z_send.at[way, c], z_arr.at[way, c], way)

    def z_forward(c):
        for way in (2, 3):
            z_copy(c, way).wait_recv()
        for way in (4, 5):
            z_copy(c, way).start()

    def dy_copy(c, way):
        if way < 2:
            src, dst = dybuf.at[c], dy_recv.at[way, c]
        else:
            rows = pl.ds((way - 2) * (dm_ // 2), dm_ // 2)
            src, dst = dy_recv.at[way - 2, c, rows], dy_recv.at[2, c, rows]
        return ring_copy(src, dst, dy_send.at[way, c], dy_arr.at[way, c], way)

    def dy_forward(c):
        for way in (0, 1):
            dy_copy(c, way).wait_recv()
        for way in (2, 3):
            dy_copy(c, way).start()

    lossv[...] = jnp.zeros_like(lossv)

    def head_rows(p, h, part):
        return pl.ds(p * (2 * 3 * hd) + (h * 3 + part) * hd, hd)

    def pad_head(val, h):
        zero = jnp.zeros_like(val)
        return jnp.concatenate([val, zero] if h == 0 else [zero, val], axis=0)

    def causal(shape, row0):
        return lax.broadcasted_iota(jnp.int32, shape, 0) + row0 <= lax.broadcasted_iota(jnp.int32, shape, 1)

    def attention(cc):
        nk = (cc + 1) * tc
        slots = min(heads, sscr.shape[0] // nk)
        ahead = min(4, slots - 1)
        sub = tc // 2

        def front(head):
            p, h = head // 2, head % 2
            base = (head % slots) * nk
            qz = pad_head(qkv[cc, head_rows(p, h, 0), :], h)
            tops, sums = [], []
            for j in range(cc + 1):
                s = dot(kn[p, pl.ds(j * tc, tc), :], qz)
                for r in range(0, tc, sub):
                    part = s[r:r + sub]
                    if j == cc:
                        part = jnp.where(causal(part.shape, r), part, NEG)
                    top = jnp.max(part, axis=0, keepdims=True)
                    e = jnp.exp2((part - top) * exp_c)
                    sscr[pl.ds(base + j * tc + r, sub), :] = e
                    tops.append(top)
                    sums.append(jnp.sum(e, axis=0, keepdims=True))
            mx = functools.reduce(jnp.maximum, tops)
            scales = [jnp.exp2((top - mx) * exp_c) for top in tops]
            inv = 1.0 / functools.reduce(jnp.add, [a * b for a, b in zip(scales, sums)])
            return [a * inv for a in scales]

        def back(head, factors):
            p, h = head // 2, head % 2
            base = (head % slots) * nk
            o_t = None
            for j in range(cc + 1):
                parts = []
                for i in range(2):
                    pr = (sscr[pl.ds(base + j * tc + i * sub, sub), :] * factors[2 * j + i]).astype(BF16)
                    pbuf[cc * (cc + 1) // 2 + j, head, pl.ds(i * sub, sub), :] = pr
                    parts.append(pr)
                part = dot(qkv[j, head_rows(p, h, 2), :], jnp.concatenate(parts, axis=0))
                o_t = part if o_t is None else o_t + part
            obuf[cc, pl.ds(head * hd, hd), :] = o_t.astype(BF16)

        factors = {}
        for head in range(ahead):
            factors[head] = front(head)
        for head in range(heads):
            if head + ahead < heads:
                factors[head + ahead] = front(head + ahead)
            back(head, factors.pop(head))

    def attention_grad(cc):
        units = [(p, j) for p in range(heads // 2) for j in range(cc + 1)]
        dqs = {}
        held = {}

        def of_head(p, h):
            if (p, h) not in held:
                rows = pl.ds((p * 2 + h) * hd, hd)
                do_t = dobuf[rows, :]
                dsum = jnp.sum(do_t.astype(F32) * obuf[cc, rows, :].astype(F32), axis=0, keepdims=True)
                held[p, h] = (pad_head(do_t, h), dsum)
            return held[p, h]

        def front(p, j):
            out = []
            for h in range(2):
                do_z, dsum = of_head(p, h)
                pr = pbuf[cc * (cc + 1) // 2 + j, p * 2 + h]
                dp = dot(vn[p, pl.ds(j * tc, tc), :], do_z).astype(BF16).astype(F32)
                ds = (pr.astype(F32) * (dp - dsum)).astype(BF16)
                if j < cc:
                    dsbuf[p * 2 + h, pl.ds(j * tc, tc), :] = ds
                out.append(ds)
            return out

        def back(p, j, ds):
            for h in range(2):
                dq_h = dot(qkv[j, head_rows(p, h, 1), :], ds[h])
                dqs[p, h] = dq_h if j == 0 else dqs[p, h] + dq_h
            if j < cc:
                return
            dv_new, dk_new = kv_grad(cc, p, j, [of_head(p, h)[0] for h in range(2)], ds,
                                     [qkv[cc, head_rows(p, h, 0), :] for h in range(2)])
            dv_t = jnp.transpose(dv_new).astype(BF16)
            dk_t = (jnp.transpose(dk_new) * scale).astype(BF16)
            for h in range(2):
                qsave[pl.ds((p * 2 + h) * hd, hd), :] = qkv[cc, head_rows(p, h, 0), :]
                qkv[cc, head_rows(p, h, 0), :] = (dqs[p, h] * scale).astype(BF16)
                qkv[cc, head_rows(p, h, 1), :] = dk_t[h * hd:(h + 1) * hd, :]
                qkv[cc, head_rows(p, h, 2), :] = dv_t[h * hd:(h + 1) * hd, :]

        ds = front(*units[0])
        for n, unit in enumerate(units):
            later = front(*units[n + 1]) if n + 1 < len(units) else None
            back(*unit, ds)
            ds = later

    def kv_grad(cc, p, j, do_z, ds, q_t):
        dv_new = dk_new = None
        for h in range(2):
            dv_h = dot_t(pbuf[cc * (cc + 1) // 2 + j, p * 2 + h], do_z[h])
            dk_h = dot_t(ds[h], pad_head(q_t[h], h))
            dv_new = dv_h if dv_new is None else dv_new + dv_h
            dk_new = dk_h if dk_new is None else dk_new + dk_h
        rows = pl.ds(j * tc, tc)
        if cc < nc - 1:
            dv_new = dv_new + dvacc[p, rows, :]
            dk_new = dk_new + dkacc[p, rows, :]
        return dv_new, dk_new

    def earlier_keys(cc):
        for p in range(heads // 2):
            heads_of = [pl.ds((p * 2 + h) * hd, hd) for h in range(2)]
            do_z = [pad_head(dobuf[heads_of[h], :], h) for h in range(2)]
            q_t = [qsave[heads_of[h], :] for h in range(2)]
            for j in range(cc):
                rows = pl.ds(j * tc, tc)
                dv_new, dk_new = kv_grad(cc, p, j, do_z, [dsbuf[p * 2 + h, rows, :] for h in range(2)], q_t)
                dvacc[p, rows, :] = dv_new
                dkacc[p, rows, :] = dk_new

    def attention_step(c):
        @pl.when(first)
        def _():
            x_copy(c).wait()
            hbuf[c] = jnp.transpose(xin[c])

        @pl.when(jnp.logical_not(first))
        def _():
            f_copy(c).wait_recv()

        @pl.when(early & (c == 0))
        def _():
            w_wait(W_Q)

        h32 = hbuf[c].astype(F32)
        n1 = (h32 * inv_rms(h32)).astype(BF16)
        n1buf[c] = n1
        for r in range(nm):
            rows = pl.ds(r * qrows, qrows)
            blk = dot(wqT[rows, :], n1).astype(BF16)
            qkv[c, rows, :] = blk
            for part, ref in ((1, kn), (2, vn)):
                both = jnp.concatenate([blk[(3 * h + part) * hd:(3 * h + part + 1) * hd] for h in range(2)], axis=0)
                ref[r, pl.ds(pl.multiple_of(c * tc, tc), tc), :] = jnp.transpose(both)

        for cc in range(nc):
            pl.when(c == cc)(functools.partial(attention, cc))

    def mlp_step(c):
        a = dot(woT[...], obuf[c]).astype(BF16)
        m32 = (hbuf[c].astype(F32) + a.astype(F32)).astype(BF16).astype(F32)
        mbuf[c] = m32.astype(BF16)
        n2 = (m32 * inv_rms(m32)).astype(BF16)
        n2buf[c] = n2

        blk = fl // 2
        for f in range(2 * nm):
            rows = pl.ds(f * blk, blk)
            u = dot(wuT[rows, :], n2buf[c]).astype(BF16)
            ubuf[c, rows, :] = u
            zbuf[c, rows, :] = gelu(u.astype(F32)).astype(BF16)
        acc = dot(wdT[...], zbuf[c])
        y32 = (mbuf[c].astype(F32) + acc.astype(BF16).astype(F32)).astype(BF16)
        ybuf[c] = y32

        @pl.when(jnp.logical_not(last))
        def _():
            f_copy(c).start()

        @pl.when(last)
        def _():
            t_copy(c).wait()
            err = ybuf[c].astype(F32) - jnp.transpose(xin[c]).astype(F32)
            lossv[...] += jnp.sum((err * err).reshape(dm_ // 8, 8, tc), axis=0)
            dybuf[c] = (err * inv_d).astype(BF16)

    @pl.loop(0, 2 * nc)
    def _(n):
        attn_turn = jnp.where(early, jnp.where(n < nc, 1, 0), 1 - lax.rem(n, 2))
        c = jnp.where(early, lax.rem(n, nc), n // 2)

        @pl.when(early & (n == 1))
        def _():
            w_forward(W_U)

        @pl.when(early & (n == 2))
        def _():
            w_forward(W_D)

        @pl.when(attn_turn == 1)
        def _():
            attention_step(c)

        @pl.when(early & (n == nc))
        def _():
            w_wait(W_O)
            w_wait(W_U)
            w_wait(W_D)

        @pl.when(attn_turn == 0)
        def _():
            mlp_step(c)

    def z_start():
        for c in range(nc):
            for way in range(4):
                z_copy(c, way).start()

    @pl.when(jnp.logical_not(late))
    def _():
        for c in range(nc):
            f_copy(c).wait_send()
        z_start()
        natural_weights()
        for c in range(nc):
            z_forward(c)

    def l_copy(k):
        return pltpu.make_async_remote_copy(
            src_ref=losst.at[nm], dst_ref=losst.at[3 - k if nm == 4 else nm - 1 - k], send_sem=lsend.at[k - 1],
            recv_sem=lrecv.at[k - 1], device_id={"model": peer(k)}, device_id_type=MESH)

    def lf_copy():
        return pltpu.make_async_remote_copy(
            src_ref=losst.at[nm + 1], dst_ref=losst.at[nm + 1], send_sem=lfsend, recv_sem=lfrecv,
            device_id={"stage": prv}, device_id_type=MESH)

    @pl.when(last)
    def _():
        tot = jnp.sum(lossv[...]) * (0.5 * inv_d)
        losst[nm] = jnp.full(losst.shape[1:], tot, F32)
        for k in range(1, nm):
            l_copy(k).start()

    dy_inside = jnp.logical_not(late) & (first | odd)

    @pl.loop(0, nc)
    def _(i):
        c = nc - 1 - i

        @pl.when(jnp.logical_not(last))
        def _():
            b_copy(c).wait_recv()

        @pl.when(jnp.logical_not(late) & (i == 0))
        def _():
            for way in range(2):
                dy_copy(c, way).start()

        blk = fl // 4
        for f in range(4 * nm):
            rows = pl.ds(f * blk, blk)
            dz = dot(wd[rows, :], dybuf[c]).astype(BF16).astype(F32)
            ubuf[c, rows, :] = (dz * gelu_grad(ubuf[c, rows, :].astype(F32))).astype(BF16)
        acc = dot(wu[...], ubuf[c])
        dn2 = acc.astype(BF16).astype(F32)
        m32 = mbuf[c].astype(F32)
        pull = norm_pull(m32, inv_rms(m32), dn2).astype(BF16)
        dmid = (dybuf[c].astype(F32) + pull.astype(F32)).astype(BF16)
        mbuf[c] = dmid
        dobuf[...] = dot(wo[...], dmid).astype(BF16)

        @pl.when(jnp.logical_not(late) & (i > 0))
        def _():
            for way in range(2):
                dy_copy(c, way).start()

        @pl.when(dy_inside & (i > 0))
        def _():
            dy_forward(c + 1)

        for cc in range(nc):
            pl.when(c == cc)(functools.partial(attention_grad, cc))

        dn1 = dot(wq[...], qkv[c]).astype(BF16).astype(F32)
        h32 = hbuf[c].astype(F32)
        pull1 = norm_pull(h32, inv_rms(h32), dn1).astype(BF16)

        @pl.when(late & jnp.logical_not(last))
        def _():
            f_copy(c).wait_send()

        ybuf[c] = (mbuf[c].astype(F32) + pull1.astype(F32)).astype(BF16)

        @pl.when(jnp.logical_not(first))
        def _():
            b_copy(c).start()

        for cc in range(1, nc):
            pl.when(c == cc)(functools.partial(earlier_keys, cc))

    @pl.when(last)
    def _():
        for k in range(1, nm):
            l_copy(k).wait_recv()
        vals = [losst[nm]] + [losst[k - 1] for k in range(1, nm)]
        tot = jnp.zeros_like(vals[0])
        for who in range(nm):
            pick = vals[0]
            for k in range(1, nm):
                pick = jnp.where(peer(k) == who, vals[k], pick)
            tot = tot + pick
        losst[nm + 1] = tot

    @pl.when(jnp.logical_not(last))
    def _():
        lf_copy().wait_recv()

    @pl.when(jnp.logical_not(first))
    def _():
        lf_copy().start()

    loss_out[...] = losst[nm + 1]

    def wgrad(mat, d):
        acc = None
        for c in range(nc):
            if mat == 0:
                part = dot_t(qkv[c, rowsl(d * qrows, qrows, qrows), :], n1buf[c])
            elif mat == 1:
                part = dot_t(obuf[c, rowsl(d * orows, orows, orows), :], mbuf[c])
            elif mat == 2:
                part = dot_t(n2buf[c], ubuf[c, rowsl(d * fl, fl, fl), :])
            else:
                part = dot_t(zbuf[c, rowsl(d * fl, fl, fl), :], dybuf[c])
            acc = part if acc is None else acc + part
        return acc

    sizes = (qrows, orows, dm_)
    offs = (0, qrows, qrows + orows)

    def rows_of(mat):
        return pl.ds(offs[mat], sizes[mat])

    def half_of(mat, half):
        return pl.ds(offs[mat] + half * (sizes[mat] // 2), sizes[mat] // 2)

    def far_copy(mat, half):
        rows = pl.ds(offs[mat] // 2, sizes[mat] // 2)
        return ring_copy(stage_buf.at[0, half_of(mat, half)], (far_p, far_m)[half].at[rows],
                         rs_send.at[mat, half], rs_recv.at[mat, half], half)

    def near_copy(mat, side, half):
        way = 2 + 2 * side + half
        return ring_copy(stage_buf.at[1 + side, half_of(mat, half)], (near_l if side == half else near_e).at[half_of(mat, half)],
                         rs_send.at[mat, way], rs_recv.at[mat, way], side)

    hd2 = dm_ // 2

    def gd_cols(half):
        return pl.ds(half * hd2, hd2)

    def gd_half(d, half):
        return functools.reduce(jnp.add, [
            dot_t(zbuf[c, rowsl(d * fl, fl, fl), :], dybuf[c, gd_cols(half), :]) for c in range(nc)])

    def gd_far_copy(half):
        return ring_copy(gdacc.at[:, gd_cols(half)], gd_far.at[half], gd_send.at[half], gd_recv.at[half], half)

    def gd_slot(side, half):
        return pl.ds((2 * side + half) * fl, fl)

    def gd_near_copy(side, half):
        way = 2 + 2 * side + half
        return ring_copy(sscr.at[gd_slot(side, half)], gd_near.at[1 if side == half else 0, half],
                         gd_send.at[way], gd_recv.at[way], side)

    def load(src, nr):
        return pltpu.make_async_copy(src, radd.at[pl.ds(0, nr)], ld_sem.at[0])

    def gd_add(src, ref):
        nr = min(fl, radd.shape[0])
        for r in range(0, fl, nr):
            copy = pltpu.make_async_copy(src.at[pl.ds(r, nr)], radd.at[pl.ds(0, nr), pl.ds(0, hd2)], ld_sem.at[0])
            copy.start()
            copy.wait()
            ref[pl.ds(r, nr), :] += radd[pl.ds(0, nr), pl.ds(0, hd2)]

    mats = (1, 0, 2)
    for mat in mats:
        stage_buf[0, rows_of(mat)] = wgrad(mat, peer(far))
        for half in range(2):
            far_copy(mat, half).start()

    @pl.when(late)
    def _():
        for half in range(2):
            gdacc[:, gd_cols(half)] = gd_half(peer(far), half)
            gd_far_copy(half).start()

    for mat in mats:
        for side in range(2):
            stage_buf[1 + side, rows_of(mat)] = wgrad(mat, peer((plus, minus)[side]))

    @pl.when(late)
    def _():
        for side in range(2):
            for half in range(2):
                sscr[gd_slot(side, half), :] = gd_half(peer((plus, minus)[side]), half)

    for mat in mats:
        nr = sizes[mat] // 2
        for half in range(2):
            far_copy(mat, half).wait_recv()
            src = (far_p, far_m)[half].at[pl.ds(offs[mat] // 2, nr)]
            load(src, nr).start()
            load(src, nr).wait()
            stage_buf[1 + half, half_of(mat, half)] += radd[pl.ds(0, nr)]
            near_copy(mat, half, half).start()
        for side in range(2):
            near_copy(mat, side, 1 - side).start()

    @pl.when(late)
    def _():
        for half in range(2):
            gd_far_copy(half).wait_recv()
            gd_add(gd_far.at[half], sscr.at[gd_slot(half, half)])
            gd_near_copy(half, half).start()
            gd_near_copy(1 - half, half).start()
            gd_far_copy(half).wait_send()

    @pl.when(dy_inside)
    def _():
        dy_forward(0)

    @pl.when(jnp.logical_not(late | dy_inside))
    def _():
        for c in reversed(range(nc)):
            dy_forward(c)

    for mat in mats:
        for half in range(2):
            far_copy(mat, half).wait_send()
        stage_buf[0, rows_of(mat)] = wgrad(mat, me)

    def zdy_load(n, buf):
        slot, c = n // nc, lax.rem(n, nc)
        return (pltpu.make_async_copy(z_recv.at[slot, c], dsbuf.at[2 * buf, pl.ds(0, fl)], ld_sem.at[1 + buf]),
                pltpu.make_async_copy(dy_recv.at[slot, c], dsbuf.at[2 * buf + 1, pl.ds(0, dm_)], ld_sem.at[3 + buf]))

    gdacc[...] = wgrad(3, me)

    @pl.when(jnp.logical_not(late))
    def _():
        for c in range(nc):
            for way in (0, 1, 4, 5):
                z_copy(c, way).wait_recv()
            for way in (2, 3):
                dy_copy(c, way).wait_recv()
        for cp in zdy_load(0, 0):
            cp.start()

        @pl.loop(0, 3 * nc)
        def _(n):
            buf = lax.rem(n, 2)

            @pl.when(n + 1 < 3 * nc)
            def _():
                for cp in zdy_load(n + 1, 1 - buf):
                    cp.start()

            for cp in zdy_load(n, buf):
                cp.wait()
            gdacc[...] += dot_t(dsbuf[2 * buf, pl.ds(0, fl), :], dsbuf[2 * buf + 1, pl.ds(0, dm_), :])

    def gd_arrivals(last_half):
        for half in range(2):
            side = half if last_half else 1 - half
            gd_near_copy(side, half).wait_recv()
            gd_add(gd_near.at[last_half, half], gdacc.at[:, gd_cols(half)])

    def out_copy(mat):
        if mat == 3:
            return pltpu.make_async_copy(gdacc, sum_out.at[pl.ds(qrows + orows + dm_, fl)], out_sem.at[3])
        return pltpu.make_async_copy(stage_buf.at[0, rows_of(mat)], sum_out.at[rows_of(mat)], out_sem.at[mat])

    for mat in mats:
        nr = sizes[mat] // 2
        for side in range(2):
            near_copy(mat, side, 1 - side).wait_recv()
            load(near_e.at[half_of(mat, 1 - side)], nr).start()
            load(near_e.at[half_of(mat, 1 - side)], nr).wait()
            stage_buf[0, half_of(mat, 1 - side)] += radd[pl.ds(0, nr)]
        out_copy(mat).start()

    @pl.when(late)
    def _():
        gd_arrivals(0)
        gd_arrivals(1)

    out_copy(3).start()
    for mat in mats:
        for side in range(2):
            near_copy(mat, side, side).wait_recv()

    for mat in range(4):
        out_copy(mat).wait()

    @pl.when(jnp.logical_not(late))
    def _():
        for c in range(nc):
            for way in range(6):
                z_copy(c, way).wait_send()
            for way in range(4):
                dy_copy(c, way).wait_send()

    @pl.when(late)
    def _():
        for side in range(2):
            for half in range(2):
                gd_near_copy(side, half).wait_send()

    for idx in range(4):
        for way in range(4):
            w_copy(idx, way).wait_send()
    for mat in mats:
        for half in range(2):
            for side in range(2):
                near_copy(mat, side, half).wait_send()

    @pl.when(jnp.logical_not(first))
    def _():
        for c in range(nc):
            b_copy(c).wait_send()
        lf_copy().wait_send()

    @pl.when(last)
    def _():
        for k in range(1, nm):
            l_copy(k).wait_send()


def finish_kernel(sq, so, su, sd, lq, lo, lu, loss, gq, go, gu, gd, loss_out):
    gq[...] = sq[...] + lq[...]
    go[...] = so[...] + lo[...]
    gu[...] = su[...] + lu[...]
    gd[...] = sd[...]
    loss_out[0] = loss[0, 0]


def solution(mesh):
    ns = mesh.shape["stage"]
    nm = mesh.shape["model"]

    def per_device(tokens_in, targets, w_qkv, w_out, w_up, w_down):
        n_micro, seq_len, d_model = tokens_in.shape
        hl, hd, fl = w_qkv.shape[3], w_qkv.shape[5], w_up.shape[3]
        tc = min(CHUNK, seq_len // 2)
        nc = seq_len // tc
        assert n_micro == nm == 4 and w_qkv.shape[1] == 1 and hl == 2 and d_model == 2 * tc
        qrows, orows = hl * 3 * hd, hl * hd
        wqT = jnp.transpose(w_qkv[0, 0], (1, 2, 3, 0)).reshape(qrows, d_model)
        wo = w_out[0, 0].reshape(orows, d_model)
        wu, wd = w_up[0, 0], w_down[0, 0]
        cfg = (ns, nm, nc, tc, d_model, hl, hd, fl)
        heads = nm * hl
        any_spec = pl.BlockSpec(memory_space=pl.ANY)
        f32 = lambda *shape: jax.ShapeDtypeStruct(shape, F32)
        rsum = qrows + orows + d_model
        seqb = nc * tc
        b16 = lambda *shape: jax.ShapeDtypeStruct(shape, BF16)
        out_shape = (f32(rsum + fl, d_model), f32(8, 128), f32(rsum // 2, d_model), f32(rsum // 2, d_model), f32(rsum, d_model),
                     f32(rsum, d_model), b16(3, nc, fl, tc), b16(2, nc, fl // 2, tc), b16(3, nc, d_model, tc),
                     f32(2, fl, d_model // 2), f32(2, 2, fl, d_model // 2))
        vb = lambda *shape: pltpu.VMEM(shape, BF16)
        vf = lambda *shape: pltpu.VMEM(shape, F32)
        dma = lambda *shape: pltpu.SemaphoreType.DMA(shape)
        scratch = [
            vb(nm * qrows, d_model), vb(d_model, nm * orows), vb(nm * fl, d_model), vb(d_model, nm * fl),
            vb(nm * fl, d_model), vb(d_model, nm * fl), vb(nm * orows, d_model), vb(d_model, nm * qrows),
            vb(nc, tc, d_model), vb(nc, d_model, tc), vb(nc, d_model, tc), vb(nc, nm * qrows, tc), vb(nm, seqb, orows), vb(nm, seqb, orows),
            vb(nc, nm * orows, tc), vb(nc, d_model, tc), vb(nc, d_model, tc), vb(nc, nm * fl, tc), vb(nc, nm * fl, tc),
            vb(nc * (nc + 1) // 2, heads, tc, tc), vb(nc, d_model, tc), vf(heads // 2, seqb, 2 * hd), vf(heads // 2, seqb, 2 * hd),
            vf(max(2 * seqb, 4 * fl), tc), vb(nc, d_model, tc), vb(nm * orows, tc), vf(nm + 2, 8, 128), vf(8, tc),
            vf(3, rsum, d_model), vf(256, d_model), vf(fl, d_model), vb(heads, max((nc - 1) * tc, fl), tc), vb(nm * orows, tc),
            dma(4, 4), dma(4, 4), dma(4), pltpu.SemaphoreType.REGULAR, dma(nc), dma(nc), dma(nc), dma(nc), dma(nc),
            dma(nm - 1), dma(nm - 1), pltpu.SemaphoreType.DMA, pltpu.SemaphoreType.DMA,
            dma(3, 6), dma(3, 6), dma(5), dma(4), dma(6, nc), dma(6, nc), dma(4, nc), dma(4, nc), dma(6), dma(6),
        ]
        res = pl.pallas_call(
            functools.partial(step_kernel, cfg),
            out_shape=out_shape,
            in_specs=[any_spec] * 6,
            out_specs=[any_spec, pl.BlockSpec(memory_space=pltpu.VMEM)] + [any_spec] * 9,
            scratch_shapes=scratch,
            compiler_params=pltpu.CompilerParams(collective_id=0, has_side_effects=True, vmem_limit_bytes=67043328),
            name="train_step",
        )(tokens_in, targets, wqT, wo, wu, wd)
        part, loss, late = res[0], res[1], res[5]
        steps = 4

        def spec(size, start):
            rows = size // steps
            return pl.BlockSpec((rows, d_model), lambda i: (start // rows + i, 0))

        q_s, o_s, u_s = spec(qrows, 0), spec(orows, qrows), spec(d_model, qrows + orows)
        g_qkv, g_out, g_up, g_down, loss = pl.pallas_call(
            finish_kernel,
            grid=(steps,),
            out_shape=(f32(qrows, d_model), f32(orows, d_model), f32(d_model, fl), f32(fl, d_model), f32(1)),
            in_specs=[q_s, o_s, u_s, spec(fl, rsum), q_s, o_s, u_s, pl.BlockSpec(memory_space=pltpu.SMEM)],
            out_specs=[spec(qrows, 0), spec(orows, 0), spec(d_model, 0), spec(fl, 0), pl.BlockSpec(memory_space=pltpu.SMEM)],
            name="finish",
        )(part, part, part, part, late, late, late, loss)
        g_qkv = jnp.transpose(g_qkv.reshape(hl, 3, hd, d_model), (3, 0, 1, 2))[None, None]
        return g_qkv, g_out.reshape(1, 1, hl, hd, d_model), g_up[None, None], g_down[None, None], loss

    tok_spec = P(None, "data", None)
    qkv_spec = P("stage", None, None, "model", None, None)
    out_spec = P("stage", None, "model", None, None)
    up_spec = P("stage", None, None, "model")
    down_spec = P("stage", None, "model", None)
    g_qkv_spec = P(("data", "stage"), None, None, "model", None, None)
    g_out_spec = P(("data", "stage"), None, "model", None, None)
    g_up_spec = P(("data", "stage"), None, None, "model")
    g_down_spec = P(("data", "stage"), None, "model", None)
    return jax.shard_map(per_device, mesh=mesh, in_specs=(tok_spec, tok_spec, qkv_spec, out_spec, up_spec, down_spec), out_specs=(g_qkv_spec, g_out_spec, g_up_spec, g_down_spec, P("data")), check_vma=False)
```

```python
import functools
import math

import jax
import jax.numpy as jnp
from jax import lax
from jax.experimental import pallas as pl
from jax.experimental.pallas import tpu as pltpu
from jax.sharding import PartitionSpec as P

F32 = jnp.float32
BF16 = jnp.bfloat16
MESH = pl.DeviceIdType.MESH
CHUNK = 256
NEG = -1e30
GELU_C = math.sqrt(2.0 / math.pi)
GELU_A = 0.044715

W_Q, W_O, W_U, W_D = range(4)


def dot(lhs, rhs):
    return jnp.dot(lhs, rhs, preferred_element_type=F32)


def dot_t(lhs, rhs):
    return lax.dot_general(lhs, rhs, (((1,), (1,)), ((), ())), preferred_element_type=F32)


def inv_rms(x32):
    return lax.rsqrt(jnp.mean(x32 * x32, axis=0, keepdims=True) + 1e-6)


def norm_pull(x32, inv, g32):
    mean_gx = jnp.mean(g32 * x32, axis=0, keepdims=True)
    return g32 * inv - x32 * (inv * inv * inv * mean_gx)


def gelu(u):
    tanh = jnp.tanh(u * (GELU_C + (GELU_C * GELU_A) * (u * u)))
    half = 0.5 * u
    return half + half * tanh


def gelu_grad(u):
    u2 = u * u
    sig = 0.5 + 0.5 * jnp.tanh(u * (GELU_C + (GELU_C * GELU_A) * u2))
    slope = u * (2.0 * GELU_C + (6.0 * GELU_C * GELU_A) * u2)
    return sig * (1.0 + slope * (1.0 - sig))


def step_kernel(cfg, x_hbm, t_hbm, wqT_in, wo_in, wu_in, wd_in,
                sum_out, loss_out, far_p, far_m, near_e, near_l, z_recv, z_fwd, dy_recv, gd_far, gd_near,
                wqT, woT, wuT, wdT, wd, wu, wo, wq,
                xin, hbuf, n1buf, qkv, kn, vn, obuf, mbuf, n2buf, ubuf, zbuf, pbuf, dybuf, dvacc, dkacc, sscr,
                ybuf, dobuf, losst, lossv, stage_buf, radd, gdacc, dsbuf, qsave,
                ag_send, ag_recv, ag_loc, go_sem, xsem, fsend, frecv, bsend, brecv, lsend, lrecv, lfsend, lfrecv,
                rs_send, rs_recv, ld_sem, out_sem, z_send, z_arr, dy_send, dy_arr, gd_send, gd_recv, pl_sem):
    ns, nm, nc, tc, dm_, hl, hd, fl = cfg
    heads = nm * hl
    qrows = hl * 3 * hd
    orows = hl * hd
    inv_d = 1.0 / (nm * nc * tc * dm_)
    scale = hd ** -0.5
    exp_c = scale * math.log2(math.e)
    me = lax.axis_index("model")
    st = lax.axis_index("stage")
    nxt = lax.rem(st + 1, ns)
    prv = lax.rem(st + ns - 1, ns)
    first = st == 0
    last = st == ns - 1

    def peer(k):
        return lax.rem(me + k, nm)

    bar = pltpu.get_barrier_semaphore()
    pl.semaphore_signal(bar, inc=1, device_id={"stage": nxt}, device_id_type=MESH)
    pl.semaphore_signal(bar, inc=1, device_id={"stage": prv}, device_id_type=MESH)
    for k in range(1, nm):
        pl.semaphore_signal(bar, inc=1, device_id={"model": peer(k)}, device_id_type=MESH)
    pl.semaphore_wait(bar, 2 + nm - 1)

    def rowsl(start, size, mult):
        return pl.ds(pl.multiple_of(start, mult), size)

    plus, minus, far = 1, nm - 1, 2

    def w_rows(idx, who, half=None):
        size = (qrows, orows, fl, fl)[idx]
        if idx in (W_Q, W_U):
            buf = wqT if idx == W_Q else wuT
            if half is None:
                return buf.at[rowsl(who * size, size, size), :]
            return buf.at[rowsl(who * size + half * (size // 2), size // 2, size // 2), :]
        view = (woT if idx == W_O else wdT).at[:, rowsl(who * size, size, size)]
        return view if half is None else view.at[pl.ds(half * (dm_ // 2), dm_ // 2), :]

    def w_copy(idx, way):
        to = plus if way in (0, 2) else minus
        if way < 2:
            src = wqT_in if idx == W_Q else w_rows(idx, me)
            dst = w_rows(idx, me)
        else:
            src = dst = w_rows(idx, peer(minus if way == 2 else plus), way - 2)
        return pltpu.make_async_remote_copy(
            src_ref=src, dst_ref=dst, send_sem=ag_send.at[idx, way], recv_sem=ag_recv.at[idx, way],
            device_id={"model": peer(to)}, device_id_type=MESH)

    def w_arrival(idx, way):
        who = peer((minus, plus, far, far)[way])
        ref = w_rows(idx, who) if way < 2 else w_rows(idx, who, way - 2)
        return pltpu.make_async_remote_copy(
            src_ref=ref, dst_ref=ref, send_sem=ag_send.at[idx, way], recv_sem=ag_recv.at[idx, way],
            device_id={"model": peer(plus)}, device_id_type=MESH)

    def w_local(idx):
        src = (wqT_in, wo_in, wu_in, wd_in)[idx]
        dst = (w_rows(W_Q, me), wo.at[rowsl(me * orows, orows, orows), :], wu.at[:, rowsl(me * fl, fl, fl)], wd.at[rowsl(me * fl, fl, fl), :])[idx]
        return pltpu.make_async_copy(src, dst, ag_loc.at[idx])

    def w_own(idx):
        for way in range(2):
            w_copy(idx, way).start()

    def w_forward(idx):
        for way in range(2):
            w_arrival(idx, way).wait_recv()
        for way in range(2, 4):
            w_copy(idx, way).start()

    def w_wait(idx):
        for way in range(2, 4):
            w_arrival(idx, way).wait_recv()

    def x_copy(c):
        return pltpu.make_async_copy(x_hbm.at[me, pl.ds(c * tc, tc), :], xin.at[c], xsem.at[c])

    def t_copy(c):
        return pltpu.make_async_copy(t_hbm.at[me, pl.ds(c * tc, tc), :], xin.at[c], xsem.at[c])

    @pl.when(first)
    def _():
        for c in range(nc):
            x_copy(c).start()

    @pl.when(last)
    def _():
        for c in range(nc):
            t_copy(c).start()

    for idx in range(4):
        w_local(idx).start()

    odd = lax.rem(st, 2) == 1
    early = st < 2

    @pl.when(odd)
    def _():
        pl.semaphore_wait(go_sem, 1)

    w_own(W_Q)
    w_local(W_O).wait()
    woT[:, rowsl(me * orows, orows, orows)] = jnp.transpose(wo[rowsl(me * orows, orows, orows), :])
    w_own(W_O)
    w_local(W_U).wait()
    wuT[rowsl(me * fl, fl, fl), :] = jnp.transpose(wu[:, rowsl(me * fl, fl, fl)])
    w_own(W_U)
    w_local(W_D).wait()
    wdT[:, rowsl(me * fl, fl, fl)] = jnp.transpose(wd[rowsl(me * fl, fl, fl), :])
    w_own(W_D)
    w_local(W_Q).wait()
    w_forward(W_Q)
    w_forward(W_O)

    @pl.when(jnp.logical_not(odd))
    def _():
        pl.semaphore_signal(go_sem, inc=1, device_id={"stage": nxt}, device_id_type=MESH)

    def natural_weights():
        @pl.loop(0, nm)
        def _(f):
            wu[:, rowsl(f * fl, fl, fl)] = jnp.transpose(wuT[rowsl(f * fl, fl, fl), :])
            wd[rowsl(f * fl, fl, fl), :] = jnp.transpose(wdT[:, rowsl(f * fl, fl, fl)])
            wo[rowsl(f * orows, orows, orows), :] = jnp.transpose(woT[:, rowsl(f * orows, orows, orows)])
            wq[:, rowsl(f * qrows, qrows, qrows)] = jnp.transpose(wqT[rowsl(f * qrows, qrows, qrows), :])

    late = st >= max(2, ns // 2)

    @pl.when(jnp.logical_not(early))
    def _():
        w_forward(W_U)
        w_forward(W_D)
        for idx in range(4):
            w_wait(idx)

    @pl.when(late)
    def _():
        natural_weights()

    def f_copy(c):
        return pltpu.make_async_remote_copy(
            src_ref=ybuf.at[c], dst_ref=hbuf.at[c], send_sem=fsend.at[c], recv_sem=frecv.at[c],
            device_id={"stage": nxt}, device_id_type=MESH)

    def b_copy(c):
        return pltpu.make_async_remote_copy(
            src_ref=ybuf.at[c], dst_ref=dybuf.at[c], send_sem=bsend.at[c], recv_sem=brecv.at[c],
            device_id={"stage": prv}, device_id_type=MESH)

    def ring_copy(src, dst, send, recv, way):
        return pltpu.make_async_remote_copy(
            src_ref=src, dst_ref=dst, send_sem=send, recv_sem=recv,
            device_id={"model": peer((plus, minus)[way % 2])}, device_id_type=MESH)

    hf = fl // 2

    def z_copy(c, way):
        if way < 2:
            src, dst = zbuf.at[c, rowsl(peer((plus, minus)[way]) * fl, fl, fl), :], z_recv.at[way, c]
        elif way < 4:
            src, dst = zbuf.at[c, rowsl(peer(far) * fl + (way - 2) * hf, hf, hf), :], z_fwd.at[way - 2, c]
        else:
            src, dst = z_fwd.at[way - 4, c], z_recv.at[2, c, pl.ds((way - 4) * hf, hf)]
        return ring_copy(src, dst, z_send.at[way, c], z_arr.at[way, c], way)

    def z_forward(c):
        for way in (2, 3):
            z_copy(c, way).wait_recv()
        for way in (4, 5):
            z_copy(c, way).start()

    def dy_copy(c, way):
        if way < 2:
            src, dst = dybuf.at[c], dy_recv.at[way, c]
        else:
            rows = pl.ds((way - 2) * (dm_ // 2), dm_ // 2)
            src, dst = dy_recv.at[way - 2, c, rows], dy_recv.at[2, c, rows]
        return ring_copy(src, dst, dy_send.at[way, c], dy_arr.at[way, c], way)

    def dy_forward(c):
        for way in (0, 1):
            dy_copy(c, way).wait_recv()
        for way in (2, 3):
            dy_copy(c, way).start()

    lossv[...] = jnp.zeros_like(lossv)

    def head_rows(p, h, part):
        return pl.ds(p * (2 * 3 * hd) + (h * 3 + part) * hd, hd)

    def pad_head(val, h):
        zero = jnp.zeros_like(val)
        return jnp.concatenate([val, zero] if h == 0 else [zero, val], axis=0)

    def causal(shape, row0):
        return lax.broadcasted_iota(jnp.int32, shape, 0) + row0 <= lax.broadcasted_iota(jnp.int32, shape, 1)

    def attention(cc):
        nk = (cc + 1) * tc
        slots = min(heads, sscr.shape[0] // nk)
        ahead = min(4, slots - 1)
        sub = tc // 2

        def front(head):
            p, h = head // 2, head % 2
            base = (head % slots) * nk
            qz = pad_head(qkv[cc, head_rows(p, h, 0), :], h)
            tops, sums = [], []
            for j in range(cc + 1):
                s = dot(kn[p, pl.ds(j * tc, tc), :], qz)
                for r in range(0, tc, sub):
                    part = s[r:r + sub]
                    if j == cc:
                        part = jnp.where(causal(part.shape, r), part, NEG)
                    top = jnp.max(part, axis=0, keepdims=True)
                    e = jnp.exp2((part - top) * exp_c)
                    sscr[pl.ds(base + j * tc + r, sub), :] = e
                    tops.append(top)
                    sums.append(jnp.sum(e, axis=0, keepdims=True))
            mx = functools.reduce(jnp.maximum, tops)
            scales = [jnp.exp2((top - mx) * exp_c) for top in tops]
            inv = 1.0 / functools.reduce(jnp.add, [a * b for a, b in zip(scales, sums)])
            return [a * inv for a in scales]

        def back(head, factors):
            p, h = head // 2, head % 2
            base = (head % slots) * nk
            o_t = None
            for j in range(cc + 1):
                parts = []
                for i in range(2):
                    pr = (sscr[pl.ds(base + j * tc + i * sub, sub), :] * factors[2 * j + i]).astype(BF16)
                    pbuf[cc * (cc + 1) // 2 + j, head, pl.ds(i * sub, sub), :] = pr
                    parts.append(pr)
                part = dot(qkv[j, head_rows(p, h, 2), :], jnp.concatenate(parts, axis=0))
                o_t = part if o_t is None else o_t + part
            obuf[cc, pl.ds(head * hd, hd), :] = o_t.astype(BF16)

        factors = {}
        for head in range(ahead):
            factors[head] = front(head)
        for head in range(heads):
            if head + ahead < heads:
                factors[head + ahead] = front(head + ahead)
            back(head, factors.pop(head))

    def attention_grad(cc):
        units = [(p, j) for p in range(heads // 2) for j in range(cc + 1)]
        dqs = {}
        held = {}

        def of_head(p, h):
            if (p, h) not in held:
                rows = pl.ds((p * 2 + h) * hd, hd)
                do_t = dobuf[rows, :]
                dsum = jnp.sum(do_t.astype(F32) * obuf[cc, rows, :].astype(F32), axis=0, keepdims=True)
                held[p, h] = (pad_head(do_t, h), dsum)
            return held[p, h]

        def front(p, j):
            out = []
            for h in range(2):
                do_z, dsum = of_head(p, h)
                pr = pbuf[cc * (cc + 1) // 2 + j, p * 2 + h]
                dp = dot(vn[p, pl.ds(j * tc, tc), :], do_z).astype(BF16).astype(F32)
                ds = (pr.astype(F32) * (dp - dsum)).astype(BF16)
                if j < cc:
                    dsbuf[p * 2 + h, pl.ds(j * tc, tc), :] = ds
                out.append(ds)
            return out

        def back(p, j, ds):
            for h in range(2):
                dq_h = dot(qkv[j, head_rows(p, h, 1), :], ds[h])
                dqs[p, h] = dq_h if j == 0 else dqs[p, h] + dq_h
            if j < cc:
                return
            dv_new, dk_new = kv_grad(cc, p, j, [of_head(p, h)[0] for h in range(2)], ds,
                                     [qkv[cc, head_rows(p, h, 0), :] for h in range(2)])
            dv_t = jnp.transpose(dv_new).astype(BF16)
            dk_t = (jnp.transpose(dk_new) * scale).astype(BF16)
            for h in range(2):
                qsave[pl.ds((p * 2 + h) * hd, hd), :] = qkv[cc, head_rows(p, h, 0), :]
                qkv[cc, head_rows(p, h, 0), :] = (dqs[p, h] * scale).astype(BF16)
                qkv[cc, head_rows(p, h, 1), :] = dk_t[h * hd:(h + 1) * hd, :]
                qkv[cc, head_rows(p, h, 2), :] = dv_t[h * hd:(h + 1) * hd, :]

        ds = front(*units[0])
        for n, unit in enumerate(units):
            later = front(*units[n + 1]) if n + 1 < len(units) else None
            back(*unit, ds)
            ds = later

    def kv_grad(cc, p, j, do_z, ds, q_t):
        dv_new = dk_new = None
        for h in range(2):
            dv_h = dot_t(pbuf[cc * (cc + 1) // 2 + j, p * 2 + h], do_z[h])
            dk_h = dot_t(ds[h], pad_head(q_t[h], h))
            dv_new = dv_h if dv_new is None else dv_new + dv_h
            dk_new = dk_h if dk_new is None else dk_new + dk_h
        rows = pl.ds(j * tc, tc)
        if cc < nc - 1:
            dv_new = dv_new + dvacc[p, rows, :]
            dk_new = dk_new + dkacc[p, rows, :]
        return dv_new, dk_new

    def earlier_keys(cc):
        for p in range(heads // 2):
            heads_of = [pl.ds((p * 2 + h) * hd, hd) for h in range(2)]
            do_z = [pad_head(dobuf[heads_of[h], :], h) for h in range(2)]
            q_t = [qsave[heads_of[h], :] for h in range(2)]
            for j in range(cc):
                rows = pl.ds(j * tc, tc)
                dv_new, dk_new = kv_grad(cc, p, j, do_z, [dsbuf[p * 2 + h, rows, :] for h in range(2)], q_t)
                dvacc[p, rows, :] = dv_new
                dkacc[p, rows, :] = dk_new

    def attention_step(c):
        @pl.when(first)
        def _():
            x_copy(c).wait()
            hbuf[c] = jnp.transpose(xin[c])

        @pl.when(jnp.logical_not(first))
        def _():
            f_copy(c).wait_recv()

        @pl.when(early & (c == 0))
        def _():
            w_wait(W_Q)

        h32 = hbuf[c].astype(F32)
        n1 = (h32 * inv_rms(h32)).astype(BF16)
        n1buf[c] = n1
        for r in range(nm):
            rows = pl.ds(r * qrows, qrows)
            blk = dot(wqT[rows, :], n1).astype(BF16)
            qkv[c, rows, :] = blk
            for part, ref in ((1, kn), (2, vn)):
                both = jnp.concatenate([blk[(3 * h + part) * hd:(3 * h + part + 1) * hd] for h in range(2)], axis=0)
                ref[r, pl.ds(pl.multiple_of(c * tc, tc), tc), :] = jnp.transpose(both)

        for cc in range(nc):
            pl.when(c == cc)(functools.partial(attention, cc))

    def mlp_step(c):
        a = dot(woT[...], obuf[c]).astype(BF16)
        m32 = (hbuf[c].astype(F32) + a.astype(F32)).astype(BF16).astype(F32)
        mbuf[c] = m32.astype(BF16)
        n2 = (m32 * inv_rms(m32)).astype(BF16)
        n2buf[c] = n2

        blk = fl // 2
        for f in range(2 * nm):
            rows = pl.ds(f * blk, blk)
            u = dot(wuT[rows, :], n2buf[c]).astype(BF16)
            ubuf[c, rows, :] = u
            zbuf[c, rows, :] = gelu(u.astype(F32)).astype(BF16)
        acc = dot(wdT[...], zbuf[c])
        y32 = (mbuf[c].astype(F32) + acc.astype(BF16).astype(F32)).astype(BF16)
        ybuf[c] = y32

        @pl.when(jnp.logical_not(last))
        def _():
            f_copy(c).start()

        @pl.when(last)
        def _():
            t_copy(c).wait()
            err = ybuf[c].astype(F32) - jnp.transpose(xin[c]).astype(F32)
            lossv[...] += jnp.sum((err * err).reshape(dm_ // 8, 8, tc), axis=0)
            dybuf[c] = (err * inv_d).astype(BF16)

    @pl.loop(0, 2 * nc)
    def _(n):
        attn_turn = jnp.where(early, jnp.where(n < nc, 1, 0), 1 - lax.rem(n, 2))
        c = jnp.where(early, lax.rem(n, nc), n // 2)

        @pl.when(early & (n == 1))
        def _():
            w_forward(W_U)

        @pl.when(early & (n == 2))
        def _():
            w_forward(W_D)

        @pl.when(attn_turn == 1)
        def _():
            attention_step(c)

        @pl.when(early & (n == nc))
        def _():
            w_wait(W_O)
            w_wait(W_U)
            w_wait(W_D)

        @pl.when(attn_turn == 0)
        def _():
            mlp_step(c)

    def z_start():
        for c in range(nc):
            for way in range(4):
                z_copy(c, way).start()

    @pl.when(jnp.logical_not(late))
    def _():
        for c in range(nc):
            f_copy(c).wait_send()
        z_start()
        natural_weights()
        for c in range(nc):
            z_forward(c)

    def l_copy(k):
        return pltpu.make_async_remote_copy(
            src_ref=losst.at[nm], dst_ref=losst.at[3 - k if nm == 4 else nm - 1 - k], send_sem=lsend.at[k - 1],
            recv_sem=lrecv.at[k - 1], device_id={"model": peer(k)}, device_id_type=MESH)

    def lf_copy():
        return pltpu.make_async_remote_copy(
            src_ref=losst.at[nm + 1], dst_ref=losst.at[nm + 1], send_sem=lfsend, recv_sem=lfrecv,
            device_id={"stage": prv}, device_id_type=MESH)

    @pl.when(last)
    def _():
        tot = jnp.sum(lossv[...]) * (0.5 * inv_d)
        losst[nm] = jnp.full(losst.shape[1:], tot, F32)
        for k in range(1, nm):
            l_copy(k).start()

    dy_inside = jnp.logical_not(late) & (first | odd)

    @pl.loop(0, nc)
    def _(i):
        c = nc - 1 - i

        @pl.when(jnp.logical_not(last))
        def _():
            b_copy(c).wait_recv()

        @pl.when(jnp.logical_not(late) & (i == 0))
        def _():
            for way in range(2):
                dy_copy(c, way).start()

        blk = fl // 4
        for f in range(4 * nm):
            rows = pl.ds(f * blk, blk)
            dz = dot(wd[rows, :], dybuf[c]).astype(BF16).astype(F32)
            ubuf[c, rows, :] = (dz * gelu_grad(ubuf[c, rows, :].astype(F32))).astype(BF16)
        acc = dot(wu[...], ubuf[c])
        dn2 = acc.astype(BF16).astype(F32)
        m32 = mbuf[c].astype(F32)
        pull = norm_pull(m32, inv_rms(m32), dn2).astype(BF16)
        dmid = (dybuf[c].astype(F32) + pull.astype(F32)).astype(BF16)
        mbuf[c] = dmid
        dobuf[...] = dot(wo[...], dmid).astype(BF16)

        @pl.when(jnp.logical_not(late) & (i > 0))
        def _():
            for way in range(2):
                dy_copy(c, way).start()

        @pl.when(dy_inside & (i > 0))
        def _():
            dy_forward(c + 1)

        for cc in range(nc):
            pl.when(c == cc)(functools.partial(attention_grad, cc))

        dn1 = dot(wq[...], qkv[c]).astype(BF16).astype(F32)
        h32 = hbuf[c].astype(F32)
        pull1 = norm_pull(h32, inv_rms(h32), dn1).astype(BF16)

        @pl.when(late & jnp.logical_not(last))
        def _():
            f_copy(c).wait_send()

        ybuf[c] = (mbuf[c].astype(F32) + pull1.astype(F32)).astype(BF16)

        @pl.when(jnp.logical_not(first))
        def _():
            b_copy(c).start()

        for cc in range(1, nc):
            pl.when(c == cc)(functools.partial(earlier_keys, cc))

    @pl.when(last)
    def _():
        for k in range(1, nm):
            l_copy(k).wait_recv()
        vals = [losst[nm]] + [losst[k - 1] for k in range(1, nm)]
        tot = jnp.zeros_like(vals[0])
        for who in range(nm):
            pick = vals[0]
            for k in range(1, nm):
                pick = jnp.where(peer(k) == who, vals[k], pick)
            tot = tot + pick
        losst[nm + 1] = tot

    @pl.when(jnp.logical_not(last))
    def _():
        lf_copy().wait_recv()

    @pl.when(jnp.logical_not(first))
    def _():
        lf_copy().start()

    loss_out[...] = losst[nm + 1]

    def wgrad(mat, d):
        acc = None
        for c in range(nc):
            if mat == 0:
                part = dot_t(qkv[c, rowsl(d * qrows, qrows, qrows), :], n1buf[c])
            elif mat == 1:
                part = dot_t(obuf[c, rowsl(d * orows, orows, orows), :], mbuf[c])
            elif mat == 2:
                part = dot_t(n2buf[c], ubuf[c, rowsl(d * fl, fl, fl), :])
            else:
                part = dot_t(zbuf[c, rowsl(d * fl, fl, fl), :], dybuf[c])
            acc = part if acc is None else acc + part
        return acc

    sizes = (qrows, orows, dm_)
    offs = (0, qrows, qrows + orows)

    def rows_of(mat):
        return pl.ds(offs[mat], sizes[mat])

    def half_of(mat, half):
        return pl.ds(offs[mat] + half * (sizes[mat] // 2), sizes[mat] // 2)

    def far_copy(mat, half):
        rows = pl.ds(offs[mat] // 2, sizes[mat] // 2)
        return ring_copy(stage_buf.at[0, half_of(mat, half)], (far_p, far_m)[half].at[rows],
                         rs_send.at[mat, half], rs_recv.at[mat, half], half)

    def near_copy(mat, side, half):
        way = 2 + 2 * side + half
        return ring_copy(stage_buf.at[1 + side, half_of(mat, half)], (near_l if side == half else near_e).at[half_of(mat, half)],
                         rs_send.at[mat, way], rs_recv.at[mat, way], side)

    mats = (2, 0, 1)
    for mat in mats:
        stage_buf[0, rows_of(mat)] = wgrad(mat, peer(far))
        for half in range(2):
            far_copy(mat, half).start()
    for mat in mats:
        for side in range(2):
            stage_buf[1 + side, rows_of(mat)] = wgrad(mat, peer((plus, minus)[side]))
            near_copy(mat, side, 1 - side).start()

    @pl.when(dy_inside)
    def _():
        dy_forward(0)

    @pl.when(jnp.logical_not(late | dy_inside))
    def _():
        for c in reversed(range(nc)):
            dy_forward(c)

    hd2 = dm_ // 2

    def gd_cols(half):
        return pl.ds(half * hd2, hd2)

    def gd_half(d, half):
        return functools.reduce(jnp.add, [
            dot_t(zbuf[c, rowsl(d * fl, fl, fl), :], dybuf[c, gd_cols(half), :]) for c in range(nc)])

    def gd_far_copy(half):
        return ring_copy(gdacc.at[:, gd_cols(half)], gd_far.at[half], gd_send.at[half], gd_recv.at[half], half)

    def gd_slot(side, half):
        return pl.ds((2 * side + half) * fl, fl)

    def gd_near_copy(side, half):
        way = 2 + 2 * side + half
        return ring_copy(sscr.at[gd_slot(side, half)], gd_near.at[1 if side == half else 0, half],
                         gd_send.at[way], gd_recv.at[way], side)

    @pl.when(late)
    def _():
        for half in range(2):
            gdacc[:, gd_cols(half)] = gd_half(peer(far), half)
            gd_far_copy(half).start()
        for side in range(2):
            for half in (1 - side, side):
                sscr[gd_slot(side, half), :] = gd_half(peer((plus, minus)[side]), half)
            gd_near_copy(side, 1 - side).start()

    def gd_add(src, ref):
        nr = min(fl, radd.shape[0])
        for r in range(0, fl, nr):
            copy = pltpu.make_async_copy(src.at[pl.ds(r, nr)], radd.at[pl.ds(0, nr), pl.ds(0, hd2)], ld_sem.at[0])
            copy.start()
            copy.wait()
            ref[pl.ds(r, nr), :] += radd[pl.ds(0, nr), pl.ds(0, hd2)]

    pieces = [(mat, half) for mat in mats for half in range(2)]
    cols = dvacc.shape[2]
    n_cols = dm_ // cols

    def piece_loads(n, kind):
        mat, half = pieces[n]
        nr = sizes[mat] // 2
        r0 = sum(sizes[m] // 2 for m, _ in pieces[:n])
        src = near_e.at[half_of(mat, half)] if kind else (far_p, far_m)[half].at[pl.ds(offs[mat] // 2, nr)]
        dst = dkacc if kind else dvacc
        return [pltpu.make_async_copy(src.at[:, pl.ds(k * cols, cols)], dst.at[k, pl.ds(r0, nr), :], pl_sem.at[kind, n])
                for k in range(n_cols)], dst, r0, nr

    def piece_start(n, kind):
        mat, half = pieces[n]
        if kind:
            near_copy(mat, 1 - half, half).wait_recv()
        else:
            far_copy(mat, half).wait_recv()
        for copy in piece_loads(n, kind)[0]:
            copy.start()

    def piece_add(n, kind, slot):
        mat, half = pieces[n]
        copies, src, r0, nr = piece_loads(n, kind)
        for copy in copies:
            copy.wait()
        rows = half_of(mat, half)
        for k in range(n_cols):
            stage_buf[slot, rows, pl.ds(k * cols, cols)] += src[k, pl.ds(r0, nr), :]

    piece_start(0, 0)
    for n, (mat, half) in enumerate(pieces):
        if n + 1 < len(pieces):
            piece_start(n + 1, 0)
        piece_add(n, 0, 1 + half)
        near_copy(mat, half, half).start()

    @pl.when(late)
    def _():
        for half in range(2):
            gd_far_copy(half).wait_recv()
            gd_add(gd_far.at[half], sscr.at[gd_slot(half, half)])
            gd_near_copy(half, half).start()
            gd_far_copy(half).wait_send()

    for mat in mats:
        for half in range(2):
            far_copy(mat, half).wait_send()
        stage_buf[0, rows_of(mat)] = wgrad(mat, me)

    def zdy_load(n, buf):
        slot, c = n // nc, lax.rem(n, nc)
        return (pltpu.make_async_copy(z_recv.at[slot, c], dsbuf.at[2 * buf, pl.ds(0, fl)], ld_sem.at[1 + buf]),
                pltpu.make_async_copy(dy_recv.at[slot, c], dsbuf.at[2 * buf + 1, pl.ds(0, dm_)], ld_sem.at[3 + buf]))

    gdacc[...] = wgrad(3, me)

    @pl.when(jnp.logical_not(late))
    def _():
        for c in range(nc):
            for way in (0, 1, 4, 5):
                z_copy(c, way).wait_recv()
            for way in (2, 3):
                dy_copy(c, way).wait_recv()
        for cp in zdy_load(0, 0):
            cp.start()

        @pl.loop(0, 3 * nc)
        def _(n):
            buf = lax.rem(n, 2)

            @pl.when(n + 1 < 3 * nc)
            def _():
                for cp in zdy_load(n + 1, 1 - buf):
                    cp.start()

            for cp in zdy_load(n, buf):
                cp.wait()
            gdacc[...] += dot_t(dsbuf[2 * buf, pl.ds(0, fl), :], dsbuf[2 * buf + 1, pl.ds(0, dm_), :])

    def gd_arrivals(last_half):
        for half in range(2):
            side = half if last_half else 1 - half
            gd_near_copy(side, half).wait_recv()
            gd_add(gd_near.at[last_half, half], gdacc.at[:, gd_cols(half)])

    def out_copy(mat):
        if mat == 3:
            return pltpu.make_async_copy(gdacc, sum_out.at[pl.ds(qrows + orows + dm_, fl)], out_sem.at[3])
        return pltpu.make_async_copy(stage_buf.at[0, rows_of(mat)], sum_out.at[rows_of(mat)], out_sem.at[mat])

    piece_start(0, 1)
    for n, (mat, half) in enumerate(pieces):
        if n + 1 < len(pieces):
            piece_start(n + 1, 1)
        piece_add(n, 1, 0)
        if half:
            out_copy(mat).start()

    @pl.when(late)
    def _():
        gd_arrivals(0)
        gd_arrivals(1)

    out_copy(3).start()
    for mat in mats:
        for side in range(2):
            near_copy(mat, side, side).wait_recv()

    for mat in range(4):
        out_copy(mat).wait()

    @pl.when(jnp.logical_not(late))
    def _():
        for c in range(nc):
            for way in range(6):
                z_copy(c, way).wait_send()
            for way in range(4):
                dy_copy(c, way).wait_send()

    @pl.when(late)
    def _():
        for side in range(2):
            for half in range(2):
                gd_near_copy(side, half).wait_send()

    for idx in range(4):
        for way in range(4):
            w_copy(idx, way).wait_send()
    for mat in mats:
        for half in range(2):
            for side in range(2):
                near_copy(mat, side, half).wait_send()

    @pl.when(jnp.logical_not(first))
    def _():
        for c in range(nc):
            b_copy(c).wait_send()
        lf_copy().wait_send()

    @pl.when(last)
    def _():
        for k in range(1, nm):
            l_copy(k).wait_send()


def finish_kernel(sq, so, su, sd, lq, lo, lu, loss, gq, go, gu, gd, loss_out):
    gq[...] = sq[...] + lq[...]
    go[...] = so[...] + lo[...]
    gu[...] = su[...] + lu[...]
    gd[...] = sd[...]
    loss_out[0] = loss[0, 0]


def solution(mesh):
    ns = mesh.shape["stage"]
    nm = mesh.shape["model"]

    def per_device(tokens_in, targets, w_qkv, w_out, w_up, w_down):
        n_micro, seq_len, d_model = tokens_in.shape
        hl, hd, fl = w_qkv.shape[3], w_qkv.shape[5], w_up.shape[3]
        tc = min(CHUNK, seq_len // 2)
        nc = seq_len // tc
        qrows, orows = hl * 3 * hd, hl * hd
        assert n_micro == nm == 4 and w_qkv.shape[1] == 1 and hl == 2 and d_model == 2 * tc and qrows + orows + d_model <= seq_len
        wqT = jnp.transpose(w_qkv[0, 0], (1, 2, 3, 0)).reshape(qrows, d_model)
        wo = w_out[0, 0].reshape(orows, d_model)
        wu, wd = w_up[0, 0], w_down[0, 0]
        cfg = (ns, nm, nc, tc, d_model, hl, hd, fl)
        heads = nm * hl
        any_spec = pl.BlockSpec(memory_space=pl.ANY)
        f32 = lambda *shape: jax.ShapeDtypeStruct(shape, F32)
        rsum = qrows + orows + d_model
        seqb = nc * tc
        b16 = lambda *shape: jax.ShapeDtypeStruct(shape, BF16)
        out_shape = (f32(rsum + fl, d_model), f32(8, 128), f32(rsum // 2, d_model), f32(rsum // 2, d_model), f32(rsum, d_model),
                     f32(rsum, d_model), b16(3, nc, fl, tc), b16(2, nc, fl // 2, tc), b16(3, nc, d_model, tc),
                     f32(2, fl, d_model // 2), f32(2, 2, fl, d_model // 2))
        vb = lambda *shape: pltpu.VMEM(shape, BF16)
        vf = lambda *shape: pltpu.VMEM(shape, F32)
        dma = lambda *shape: pltpu.SemaphoreType.DMA(shape)
        scratch = [
            vb(nm * qrows, d_model), vb(d_model, nm * orows), vb(nm * fl, d_model), vb(d_model, nm * fl),
            vb(nm * fl, d_model), vb(d_model, nm * fl), vb(nm * orows, d_model), vb(d_model, nm * qrows),
            vb(nc, tc, d_model), vb(nc, d_model, tc), vb(nc, d_model, tc), vb(nc, nm * qrows, tc), vb(nm, seqb, orows), vb(nm, seqb, orows),
            vb(nc, nm * orows, tc), vb(nc, d_model, tc), vb(nc, d_model, tc), vb(nc, nm * fl, tc), vb(nc, nm * fl, tc),
            vb(nc * (nc + 1) // 2, heads, tc, tc), vb(nc, d_model, tc), vf(heads // 2, seqb, 2 * hd), vf(heads // 2, seqb, 2 * hd),
            vf(max(2 * seqb, 4 * fl), tc), vb(nc, d_model, tc), vb(nm * orows, tc), vf(nm + 2, 8, 128), vf(8, tc),
            vf(3, rsum, d_model), vf(256, d_model), vf(fl, d_model), vb(heads, max((nc - 1) * tc, fl), tc), vb(nm * orows, tc),
            dma(4, 4), dma(4, 4), dma(4), pltpu.SemaphoreType.REGULAR, dma(nc), dma(nc), dma(nc), dma(nc), dma(nc),
            dma(nm - 1), dma(nm - 1), pltpu.SemaphoreType.DMA, pltpu.SemaphoreType.DMA,
            dma(3, 6), dma(3, 6), dma(5), dma(4), dma(6, nc), dma(6, nc), dma(4, nc), dma(4, nc), dma(6), dma(6), dma(2, 6),
        ]
        res = pl.pallas_call(
            functools.partial(step_kernel, cfg),
            out_shape=out_shape,
            in_specs=[any_spec] * 6,
            out_specs=[any_spec, pl.BlockSpec(memory_space=pltpu.VMEM)] + [any_spec] * 9,
            scratch_shapes=scratch,
            compiler_params=pltpu.CompilerParams(collective_id=0, has_side_effects=True, vmem_limit_bytes=67043328),
            name="train_step",
        )(tokens_in, targets, wqT, wo, wu, wd)
        part, loss, late = res[0], res[1], res[5]
        steps = 4

        def spec(size, start):
            rows = size // steps
            return pl.BlockSpec((rows, d_model), lambda i: (start // rows + i, 0))

        q_s, o_s, u_s = spec(qrows, 0), spec(orows, qrows), spec(d_model, qrows + orows)
        g_qkv, g_out, g_up, g_down, loss = pl.pallas_call(
            finish_kernel,
            grid=(steps,),
            out_shape=(f32(qrows, d_model), f32(orows, d_model), f32(d_model, fl), f32(fl, d_model), f32(1)),
            in_specs=[q_s, o_s, u_s, spec(fl, rsum), q_s, o_s, u_s, pl.BlockSpec(memory_space=pltpu.SMEM)],
            out_specs=[spec(qrows, 0), spec(orows, 0), spec(d_model, 0), spec(fl, 0), pl.BlockSpec(memory_space=pltpu.SMEM)],
            name="finish",
        )(part, part, part, part, late, late, late, loss)
        g_qkv = jnp.transpose(g_qkv.reshape(hl, 3, hd, d_model), (3, 0, 1, 2))[None, None]
        return g_qkv, g_out.reshape(1, 1, hl, hd, d_model), g_up[None, None], g_down[None, None], loss

    tok_spec = P(None, "data", None)
    qkv_spec = P("stage", None, None, "model", None, None)
    out_spec = P("stage", None, "model", None, None)
    up_spec = P("stage", None, None, "model")
    down_spec = P("stage", None, "model", None)
    g_qkv_spec = P(("data", "stage"), None, None, "model", None, None)
    g_out_spec = P(("data", "stage"), None, "model", None, None)
    g_up_spec = P(("data", "stage"), None, None, "model")
    g_down_spec = P(("data", "stage"), None, "model", None)
    return jax.shard_map(per_device, mesh=mesh, in_specs=(tok_spec, tok_spec, qkv_spec, out_spec, up_spec, down_spec), out_specs=(g_qkv_spec, g_out_spec, g_up_spec, g_down_spec, P("data")), check_vma=False)
```

```python
import functools
import math

import jax
import jax.numpy as jnp
from jax import lax
from jax.experimental import pallas as pl
from jax.experimental.pallas import tpu as pltpu
from jax.sharding import PartitionSpec as P

F32 = jnp.float32
BF16 = jnp.bfloat16
MESH = pl.DeviceIdType.MESH
CHUNK = 256
NEG = -1e30
GELU_C = math.sqrt(2.0 / math.pi)
GELU_A = 0.044715

W_Q, W_O, W_U, W_D = range(4)


def dot(lhs, rhs):
    return jnp.dot(lhs, rhs, preferred_element_type=F32)


def dot_t(lhs, rhs):
    return lax.dot_general(lhs, rhs, (((1,), (1,)), ((), ())), preferred_element_type=F32)


def inv_rms(x32):
    return lax.rsqrt(jnp.mean(x32 * x32, axis=0, keepdims=True) + 1e-6)


def norm_pull(x32, inv, g32):
    mean_gx = jnp.mean(g32 * x32, axis=0, keepdims=True)
    return g32 * inv - x32 * (inv * inv * inv * mean_gx)


def gelu(u):
    tanh = jnp.tanh(u * (GELU_C + (GELU_C * GELU_A) * (u * u)))
    half = 0.5 * u
    return half + half * tanh


def gelu_grad(u):
    u2 = u * u
    sig = 0.5 + 0.5 * jnp.tanh(u * (GELU_C + (GELU_C * GELU_A) * u2))
    slope = u * (2.0 * GELU_C + (6.0 * GELU_C * GELU_A) * u2)
    return sig * (1.0 + slope * (1.0 - sig))


def step_kernel(cfg, x_hbm, t_hbm, wqT_in, wo_in, wu_in, wd_in,
                sum_out, loss_out, far_p, far_m, near_e, near_l, z_recv, z_fwd, dy_recv, gd_far, gd_near,
                wqT, woT, wuT, wdT, wd, wu, wo, wq,
                xin, hbuf, n1buf, qkv, kn, vn, obuf, mbuf, n2buf, ubuf, zbuf, pbuf, dybuf, dvacc, dkacc,
                ybuf, dobuf, losst, lossv, stage_buf, radd, gdacc, dsbuf, qsave,
                ag_send, ag_recv, ag_loc, go_sem, xsem, fsend, frecv, bsend, brecv, lsend, lrecv, lfsend, lfrecv,
                rs_send, rs_recv, ld_sem, out_sem, z_send, z_arr, dy_send, dy_arr, gd_send, gd_recv, pl_sem):
    ns, nm, nc, tc, dm_, hl, hd, fl = cfg
    heads = nm * hl
    qrows = hl * 3 * hd
    orows = hl * hd
    inv_d = 1.0 / (nm * nc * tc * dm_)
    scale = hd ** -0.5
    exp_c = scale * math.log2(math.e)
    me = lax.axis_index("model")
    st = lax.axis_index("stage")
    nxt = lax.rem(st + 1, ns)
    prv = lax.rem(st + ns - 1, ns)
    first = st == 0
    last = st == ns - 1

    def peer(k):
        return lax.rem(me + k, nm)

    bar = pltpu.get_barrier_semaphore()
    pl.semaphore_signal(bar, inc=1, device_id={"stage": nxt}, device_id_type=MESH)
    pl.semaphore_signal(bar, inc=1, device_id={"stage": prv}, device_id_type=MESH)
    for k in range(1, nm):
        pl.semaphore_signal(bar, inc=1, device_id={"model": peer(k)}, device_id_type=MESH)
    pl.semaphore_wait(bar, 2 + nm - 1)

    def rowsl(start, size, mult):
        return pl.ds(pl.multiple_of(start, mult), size)

    plus, minus, far = 1, nm - 1, 2

    def w_rows(idx, who, half=None):
        size = (qrows, orows, fl, fl)[idx]
        if idx in (W_Q, W_U):
            buf = wqT if idx == W_Q else wuT
            if half is None:
                return buf.at[rowsl(who * size, size, size), :]
            return buf.at[rowsl(who * size + half * (size // 2), size // 2, size // 2), :]
        view = (woT if idx == W_O else wdT).at[:, rowsl(who * size, size, size)]
        return view if half is None else view.at[pl.ds(half * (dm_ // 2), dm_ // 2), :]

    def w_copy(idx, way):
        to = plus if way in (0, 2) else minus
        if way < 2:
            src = wqT_in if idx == W_Q else w_rows(idx, me)
            dst = w_rows(idx, me)
        else:
            src = dst = w_rows(idx, peer(minus if way == 2 else plus), way - 2)
        return pltpu.make_async_remote_copy(
            src_ref=src, dst_ref=dst, send_sem=ag_send.at[idx, way], recv_sem=ag_recv.at[idx, way],
            device_id={"model": peer(to)}, device_id_type=MESH)

    def w_arrival(idx, way):
        who = peer((minus, plus, far, far)[way])
        ref = w_rows(idx, who) if way < 2 else w_rows(idx, who, way - 2)
        return pltpu.make_async_remote_copy(
            src_ref=ref, dst_ref=ref, send_sem=ag_send.at[idx, way], recv_sem=ag_recv.at[idx, way],
            device_id={"model": peer(plus)}, device_id_type=MESH)

    def w_local(idx):
        src = (wqT_in, wo_in, wu_in, wd_in)[idx]
        dst = (w_rows(W_Q, me), wo.at[rowsl(me * orows, orows, orows), :], wu.at[:, rowsl(me * fl, fl, fl)], wd.at[rowsl(me * fl, fl, fl), :])[idx]
        return pltpu.make_async_copy(src, dst, ag_loc.at[idx])

    def w_own(idx):
        for way in range(2):
            w_copy(idx, way).start()

    def w_forward(idx):
        for way in range(2):
            w_arrival(idx, way).wait_recv()
        for way in range(2, 4):
            w_copy(idx, way).start()

    def w_wait(idx):
        for way in range(2, 4):
            w_arrival(idx, way).wait_recv()

    def x_copy(c):
        return pltpu.make_async_copy(x_hbm.at[me, pl.ds(c * tc, tc), :], xin.at[c], xsem.at[c])

    def t_copy(c):
        return pltpu.make_async_copy(t_hbm.at[me, pl.ds(c * tc, tc), :], xin.at[c], xsem.at[c])

    @pl.when(first)
    def _():
        for c in range(nc):
            x_copy(c).start()

    @pl.when(last)
    def _():
        for c in range(nc):
            t_copy(c).start()

    for idx in range(4):
        w_local(idx).start()

    odd = lax.rem(st, 2) == 1
    early = st < 2

    @pl.when(odd)
    def _():
        pl.semaphore_wait(go_sem, 1)

    w_own(W_Q)
    w_local(W_O).wait()
    woT[:, rowsl(me * orows, orows, orows)] = jnp.transpose(wo[rowsl(me * orows, orows, orows), :])
    w_own(W_O)
    w_local(W_U).wait()
    wuT[rowsl(me * fl, fl, fl), :] = jnp.transpose(wu[:, rowsl(me * fl, fl, fl)])
    w_own(W_U)
    w_local(W_D).wait()
    wdT[:, rowsl(me * fl, fl, fl)] = jnp.transpose(wd[rowsl(me * fl, fl, fl), :])
    w_own(W_D)
    w_local(W_Q).wait()
    w_forward(W_Q)
    w_forward(W_O)

    @pl.when(jnp.logical_not(odd))
    def _():
        pl.semaphore_signal(go_sem, inc=1, device_id={"stage": nxt}, device_id_type=MESH)

    def natural_weights():
        @pl.loop(0, nm)
        def _(f):
            wu[:, rowsl(f * fl, fl, fl)] = jnp.transpose(wuT[rowsl(f * fl, fl, fl), :])
            wd[rowsl(f * fl, fl, fl), :] = jnp.transpose(wdT[:, rowsl(f * fl, fl, fl)])
            wo[rowsl(f * orows, orows, orows), :] = jnp.transpose(woT[:, rowsl(f * orows, orows, orows)])
            wq[:, rowsl(f * qrows, qrows, qrows)] = jnp.transpose(wqT[rowsl(f * qrows, qrows, qrows), :])

    late = st >= max(2, ns // 2)

    @pl.when(jnp.logical_not(early))
    def _():
        w_forward(W_U)
        w_forward(W_D)
        for idx in range(4):
            w_wait(idx)

    @pl.when(late)
    def _():
        natural_weights()

    def f_copy(c):
        return pltpu.make_async_remote_copy(
            src_ref=ybuf.at[c], dst_ref=hbuf.at[c], send_sem=fsend.at[c], recv_sem=frecv.at[c],
            device_id={"stage": nxt}, device_id_type=MESH)

    def b_copy(c):
        return pltpu.make_async_remote_copy(
            src_ref=ybuf.at[c], dst_ref=dybuf.at[c], send_sem=bsend.at[c], recv_sem=brecv.at[c],
            device_id={"stage": prv}, device_id_type=MESH)

    def ring_copy(src, dst, send, recv, way):
        return pltpu.make_async_remote_copy(
            src_ref=src, dst_ref=dst, send_sem=send, recv_sem=recv,
            device_id={"model": peer((plus, minus)[way % 2])}, device_id_type=MESH)

    hf = fl // 2

    def z_copy(c, way):
        if way < 2:
            src, dst = zbuf.at[c, rowsl(peer((plus, minus)[way]) * fl, fl, fl), :], z_recv.at[way, c]
        elif way < 4:
            src, dst = zbuf.at[c, rowsl(peer(far) * fl + (way - 2) * hf, hf, hf), :], z_fwd.at[way - 2, c]
        else:
            src, dst = z_fwd.at[way - 4, c], z_recv.at[2, c, pl.ds((way - 4) * hf, hf)]
        return ring_copy(src, dst, z_send.at[way, c], z_arr.at[way, c], way)

    def z_forward(c):
        for way in (2, 3):
            z_copy(c, way).wait_recv()
        for way in (4, 5):
            z_copy(c, way).start()

    def dy_copy(c, way):
        if way < 2:
            src, dst = dybuf.at[c], dy_recv.at[way, c]
        else:
            rows = pl.ds((way - 2) * (dm_ // 2), dm_ // 2)
            src, dst = dy_recv.at[way - 2, c, rows], dy_recv.at[2, c, rows]
        return ring_copy(src, dst, dy_send.at[way, c], dy_arr.at[way, c], way)

    def dy_forward(c):
        for way in (0, 1):
            dy_copy(c, way).wait_recv()
        for way in (2, 3):
            dy_copy(c, way).start()

    lossv[...] = jnp.zeros_like(lossv)

    def head_rows(p, h, part):
        return pl.ds(p * (2 * 3 * hd) + (h * 3 + part) * hd, hd)

    def pad_head(val, h):
        zero = jnp.zeros_like(val)
        return jnp.concatenate([val, zero] if h == 0 else [zero, val], axis=0)

    def causal(shape, row0):
        return lax.broadcasted_iota(jnp.int32, shape, 0) + row0 <= lax.broadcasted_iota(jnp.int32, shape, 1)

    n_st = stage_buf.shape[0]

    def folded(slot, row, n):
        fold = stage_buf.shape[1]
        return stage_buf.at[slot, pl.ds(row % fold, n), pl.ds((row // fold) * tc, tc)]

    def slope(c):
        blk = fl // 2
        for f in range(2 * nm):
            folded(nc - 1 - c, f * blk, blk)[...] = gelu_grad(ubuf[c, pl.ds(f * blk, blk), :].astype(F32))

    def attention(cc):
        nk = (cc + 1) * tc
        slots = min(heads, 2 * nc * tc // nk)
        ahead = min(4, slots - 1)
        sub = tc // 2

        def front(head):
            p, h = head // 2, head % 2
            base = (head % slots) * nk
            qz = pad_head(qkv[cc, head_rows(p, h, 0), :], h)
            tops, sums = [], []
            for j in range(cc + 1):
                s = dot(kn[p, pl.ds(j * tc, tc), :], qz)
                for r in range(0, tc, sub):
                    part = s[r:r + sub]
                    if j == cc:
                        part = jnp.where(causal(part.shape, r), part, NEG)
                    top = jnp.max(part, axis=0, keepdims=True)
                    e = jnp.exp2((part - top) * exp_c)
                    folded(n_st - 1, base + j * tc + r, sub)[...] = e
                    tops.append(top)
                    sums.append(jnp.sum(e, axis=0, keepdims=True))
            mx = functools.reduce(jnp.maximum, tops)
            scales = [jnp.exp2((top - mx) * exp_c) for top in tops]
            inv = 1.0 / functools.reduce(jnp.add, [a * b for a, b in zip(scales, sums)])
            return [a * inv for a in scales]

        def back(head, factors):
            p, h = head // 2, head % 2
            base = (head % slots) * nk
            o_t = None
            for j in range(cc + 1):
                parts = []
                for i in range(2):
                    pr = (folded(n_st - 1, base + j * tc + i * sub, sub)[...] * factors[2 * j + i]).astype(BF16)
                    pbuf[cc * (cc + 1) // 2 + j, head, pl.ds(i * sub, sub), :] = pr
                    parts.append(pr)
                part = dot(qkv[j, head_rows(p, h, 2), :], jnp.concatenate(parts, axis=0))
                o_t = part if o_t is None else o_t + part
            obuf[cc, pl.ds(head * hd, hd), :] = o_t.astype(BF16)

        factors = {}
        for head in range(ahead):
            factors[head] = front(head)
        for head in range(heads):
            if head + ahead < heads:
                factors[head + ahead] = front(head + ahead)
            back(head, factors.pop(head))

    def attention_grad(cc):
        units = [(p, j) for p in range(heads // 2) for j in range(cc + 1)]
        dqs = {}
        held = {}

        def of_head(p, h):
            if (p, h) not in held:
                rows = pl.ds((p * 2 + h) * hd, hd)
                do_t = dobuf[rows, :]
                dsum = jnp.sum(do_t.astype(F32) * obuf[cc, rows, :].astype(F32), axis=0, keepdims=True)
                held[p, h] = (pad_head(do_t, h), dsum)
            return held[p, h]

        def front(p, j):
            out = []
            for h in range(2):
                do_z, dsum = of_head(p, h)
                pr = pbuf[cc * (cc + 1) // 2 + j, p * 2 + h]
                dp = dot(vn[p, pl.ds(j * tc, tc), :], do_z).astype(BF16).astype(F32)
                ds = (pr.astype(F32) * (dp - dsum)).astype(BF16)
                if j < cc:
                    dsbuf[p * 2 + h, pl.ds(j * tc, tc), :] = ds
                out.append(ds)
            return out

        def back(p, j, ds):
            for h in range(2):
                dq_h = dot(qkv[j, head_rows(p, h, 1), :], ds[h])
                dqs[p, h] = dq_h if j == 0 else dqs[p, h] + dq_h
            if j < cc:
                return
            dv_new, dk_new = kv_grad(cc, p, j, [of_head(p, h)[0] for h in range(2)], ds,
                                     [qkv[cc, head_rows(p, h, 0), :] for h in range(2)])
            dv_t = jnp.transpose(dv_new).astype(BF16)
            dk_t = (jnp.transpose(dk_new) * scale).astype(BF16)
            for h in range(2):
                qsave[pl.ds((p * 2 + h) * hd, hd), :] = qkv[cc, head_rows(p, h, 0), :]
                qkv[cc, head_rows(p, h, 0), :] = (dqs[p, h] * scale).astype(BF16)
                qkv[cc, head_rows(p, h, 1), :] = dk_t[h * hd:(h + 1) * hd, :]
                qkv[cc, head_rows(p, h, 2), :] = dv_t[h * hd:(h + 1) * hd, :]

        ds = front(*units[0])
        for n, unit in enumerate(units):
            later = front(*units[n + 1]) if n + 1 < len(units) else None
            back(*unit, ds)
            ds = later

    def kv_grad(cc, p, j, do_z, ds, q_t):
        dv_new = dk_new = None
        for h in range(2):
            dv_h = dot_t(pbuf[cc * (cc + 1) // 2 + j, p * 2 + h], do_z[h])
            dk_h = dot_t(ds[h], pad_head(q_t[h], h))
            dv_new = dv_h if dv_new is None else dv_new + dv_h
            dk_new = dk_h if dk_new is None else dk_new + dk_h
        rows = pl.ds(j * tc, tc)
        if cc < nc - 1:
            dv_new = dv_new + dvacc[p, rows, :]
            dk_new = dk_new + dkacc[p, rows, :]
        return dv_new, dk_new

    def earlier_keys(cc):
        for p in range(heads // 2):
            heads_of = [pl.ds((p * 2 + h) * hd, hd) for h in range(2)]
            do_z = [pad_head(dobuf[heads_of[h], :], h) for h in range(2)]
            q_t = [qsave[heads_of[h], :] for h in range(2)]
            for j in range(cc):
                rows = pl.ds(j * tc, tc)
                dv_new, dk_new = kv_grad(cc, p, j, do_z, [dsbuf[p * 2 + h, rows, :] for h in range(2)], q_t)
                dvacc[p, rows, :] = dv_new
                dkacc[p, rows, :] = dk_new

    def attention_step(c):
        @pl.when(first)
        def _():
            x_copy(c).wait()
            hbuf[c] = jnp.transpose(xin[c])

        @pl.when(jnp.logical_not(first))
        def _():
            f_copy(c).wait_recv()

        @pl.when(early & (c == 0))
        def _():
            w_wait(W_Q)

        h32 = hbuf[c].astype(F32)
        n1 = (h32 * inv_rms(h32)).astype(BF16)
        n1buf[c] = n1
        for r in range(nm):
            rows = pl.ds(r * qrows, qrows)
            blk = dot(wqT[rows, :], n1).astype(BF16)
            qkv[c, rows, :] = blk
            for part, ref in ((1, kn), (2, vn)):
                both = jnp.concatenate([blk[(3 * h + part) * hd:(3 * h + part + 1) * hd] for h in range(2)], axis=0)
                ref[r, pl.ds(pl.multiple_of(c * tc, tc), tc), :] = jnp.transpose(both)

        for cc in range(nc):
            pl.when(c == cc)(functools.partial(attention, cc))

    def mlp_step(c):
        a = dot(woT[...], obuf[c]).astype(BF16)
        m32 = (hbuf[c].astype(F32) + a.astype(F32)).astype(BF16).astype(F32)
        mbuf[c] = m32.astype(BF16)
        n2 = (m32 * inv_rms(m32)).astype(BF16)
        n2buf[c] = n2

        blk = fl // 2
        for f in range(2 * nm):
            rows = pl.ds(f * blk, blk)
            u = dot(wuT[rows, :], n2buf[c]).astype(BF16)
            ubuf[c, rows, :] = u
            zbuf[c, rows, :] = gelu(u.astype(F32)).astype(BF16)
        acc = dot(wdT[...], zbuf[c])
        y32 = (mbuf[c].astype(F32) + acc.astype(BF16).astype(F32)).astype(BF16)
        ybuf[c] = y32

        @pl.when(jnp.logical_not(last))
        def _():
            f_copy(c).start()

        @pl.when(last)
        def _():
            t_copy(c).wait()
            err = ybuf[c].astype(F32) - jnp.transpose(xin[c]).astype(F32)
            lossv[...] += jnp.sum((err * err).reshape(dm_ // 8, 8, tc), axis=0)
            dybuf[c] = (err * inv_d).astype(BF16)

        @pl.when(last & (c > 0))
        def _():
            slope(c)

    @pl.loop(0, 2 * nc)
    def _(n):
        attn_turn = jnp.where(early, jnp.where(n < nc, 1, 0), 1 - lax.rem(n, 2))
        c = jnp.where(early, lax.rem(n, nc), n // 2)

        @pl.when(early & (n == 1))
        def _():
            w_forward(W_U)

        @pl.when(early & (n == 2))
        def _():
            w_forward(W_D)

        @pl.when(attn_turn == 1)
        def _():
            attention_step(c)

        @pl.when(early & (n == nc))
        def _():
            w_wait(W_O)
            w_wait(W_U)
            w_wait(W_D)

        @pl.when(attn_turn == 0)
        def _():
            mlp_step(c)

    def z_start():
        for c in range(nc):
            for way in range(4):
                z_copy(c, way).start()

    def slopes():
        @pl.loop(0, nc)
        def _(c):
            slope(c)

    @pl.when(jnp.logical_not(late))
    def _():
        for c in range(nc):
            f_copy(c).wait_send()
        z_start()
        natural_weights()
        slopes()
        for c in range(nc):
            z_forward(c)

    @pl.when(late & jnp.logical_not(last))
    def _():
        slopes()

    def l_copy(k):
        return pltpu.make_async_remote_copy(
            src_ref=losst.at[nm], dst_ref=losst.at[3 - k if nm == 4 else nm - 1 - k], send_sem=lsend.at[k - 1],
            recv_sem=lrecv.at[k - 1], device_id={"model": peer(k)}, device_id_type=MESH)

    def lf_copy():
        return pltpu.make_async_remote_copy(
            src_ref=losst.at[nm + 1], dst_ref=losst.at[nm + 1], send_sem=lfsend, recv_sem=lfrecv,
            device_id={"stage": prv}, device_id_type=MESH)

    @pl.when(last)
    def _():
        tot = jnp.sum(lossv[...]) * (0.5 * inv_d)
        losst[nm] = jnp.full(losst.shape[1:], tot, F32)
        for k in range(1, nm):
            l_copy(k).start()

    dy_inside = jnp.logical_not(late) & (first | odd)

    @pl.loop(0, nc)
    def _(i):
        c = nc - 1 - i

        @pl.when(jnp.logical_not(last))
        def _():
            b_copy(c).wait_recv()

        @pl.when(jnp.logical_not(late) & (i == 0))
        def _():
            for way in range(2):
                dy_copy(c, way).start()

        @pl.when(last & (c == 0))
        def _():
            slope(c)

        blk = fl // 4
        for f in range(4 * nm):
            rows = pl.ds(f * blk, blk)
            dz = dot(wd[rows, :], dybuf[c]).astype(BF16).astype(F32)
            ubuf[c, rows, :] = (dz * folded(i, f * blk, blk)[...]).astype(BF16)
        acc = dot(wu[...], ubuf[c])
        dn2 = acc.astype(BF16).astype(F32)
        m32 = mbuf[c].astype(F32)
        pull = norm_pull(m32, inv_rms(m32), dn2).astype(BF16)
        dmid = (dybuf[c].astype(F32) + pull.astype(F32)).astype(BF16)
        mbuf[c] = dmid
        dobuf[...] = dot(wo[...], dmid).astype(BF16)

        @pl.when(jnp.logical_not(late) & (i > 0))
        def _():
            for way in range(2):
                dy_copy(c, way).start()

        @pl.when(dy_inside & (i > 0))
        def _():
            dy_forward(c + 1)

        for cc in range(nc):
            pl.when(c == cc)(functools.partial(attention_grad, cc))

        dn1 = dot(wq[...], qkv[c]).astype(BF16).astype(F32)
        h32 = hbuf[c].astype(F32)
        pull1 = norm_pull(h32, inv_rms(h32), dn1).astype(BF16)

        @pl.when(late & jnp.logical_not(last))
        def _():
            f_copy(c).wait_send()

        ybuf[c] = (mbuf[c].astype(F32) + pull1.astype(F32)).astype(BF16)

        @pl.when(jnp.logical_not(first))
        def _():
            b_copy(c).start()

        for cc in range(1, nc):
            pl.when(c == cc)(functools.partial(earlier_keys, cc))

    @pl.when(last)
    def _():
        for k in range(1, nm):
            l_copy(k).wait_recv()
        vals = [losst[nm]] + [losst[k - 1] for k in range(1, nm)]
        tot = jnp.zeros_like(vals[0])
        for who in range(nm):
            pick = vals[0]
            for k in range(1, nm):
                pick = jnp.where(peer(k) == who, vals[k], pick)
            tot = tot + pick
        losst[nm + 1] = tot

    @pl.when(jnp.logical_not(last))
    def _():
        lf_copy().wait_recv()

    @pl.when(jnp.logical_not(first))
    def _():
        lf_copy().start()

    loss_out[...] = losst[nm + 1]

    def wgrad(mat, d):
        acc = None
        for c in range(nc):
            if mat == 0:
                part = dot_t(qkv[c, rowsl(d * qrows, qrows, qrows), :], n1buf[c])
            elif mat == 1:
                part = dot_t(obuf[c, rowsl(d * orows, orows, orows), :], mbuf[c])
            elif mat == 2:
                part = dot_t(n2buf[c], ubuf[c, rowsl(d * fl, fl, fl), :])
            else:
                part = dot_t(zbuf[c, rowsl(d * fl, fl, fl), :], dybuf[c])
            acc = part if acc is None else acc + part
        return acc

    sizes = (qrows, orows, dm_)
    offs = (0, qrows, qrows + orows)

    def rows_of(mat):
        return pl.ds(offs[mat], sizes[mat])

    def half_of(mat, half):
        return pl.ds(offs[mat] + half * (sizes[mat] // 2), sizes[mat] // 2)

    def far_copy(mat, half):
        rows = pl.ds(offs[mat] // 2, sizes[mat] // 2)
        return ring_copy(stage_buf.at[0, half_of(mat, half)], (far_p, far_m)[half].at[rows],
                         rs_send.at[mat, half], rs_recv.at[mat, half], half)

    def near_copy(mat, side, half):
        way = 2 + 2 * side + half
        return ring_copy(stage_buf.at[1 + side, half_of(mat, half)], (near_l if side == half else near_e).at[half_of(mat, half)],
                         rs_send.at[mat, way], rs_recv.at[mat, way], side)

    mats = (2, 0, 1)
    for mat in mats:
        stage_buf[0, rows_of(mat)] = wgrad(mat, peer(far))
        for half in range(2):
            far_copy(mat, half).start()
    for mat in mats:
        for side in range(2):
            stage_buf[1 + side, rows_of(mat)] = wgrad(mat, peer((plus, minus)[side]))
            near_copy(mat, side, 1 - side).start()

    @pl.when(dy_inside)
    def _():
        dy_forward(0)

    @pl.when(jnp.logical_not(late | dy_inside))
    def _():
        for c in reversed(range(nc)):
            dy_forward(c)

    hd2 = dm_ // 2

    def gd_cols(half):
        return pl.ds(half * hd2, hd2)

    def gd_half(d, half):
        return functools.reduce(jnp.add, [
            dot_t(zbuf[c, rowsl(d * fl, fl, fl), :], dybuf[c, gd_cols(half), :]) for c in range(nc)])

    def gd_far_copy(half):
        return ring_copy(gdacc.at[:, gd_cols(half)], gd_far.at[half], gd_send.at[half], gd_recv.at[half], half)

    def gd_slot(side, half):
        return folded(n_st - 1, (2 * side + half) * fl, fl)

    def gd_near_copy(side, half):
        way = 2 + 2 * side + half
        return ring_copy(gd_slot(side, half), gd_near.at[1 if side == half else 0, half],
                         gd_send.at[way], gd_recv.at[way], side)

    @pl.when(late)
    def _():
        for half in range(2):
            gdacc[:, gd_cols(half)] = gd_half(peer(far), half)
            gd_far_copy(half).start()
        for side in range(2):
            for half in (1 - side, side):
                gd_slot(side, half)[...] = gd_half(peer((plus, minus)[side]), half)
            gd_near_copy(side, 1 - side).start()

    def gd_add(src, ref):
        nr = min(fl, radd.shape[0])
        for r in range(0, fl, nr):
            copy = pltpu.make_async_copy(src.at[pl.ds(r, nr)], radd.at[pl.ds(0, nr), pl.ds(0, hd2)], ld_sem.at[0])
            copy.start()
            copy.wait()
            ref[pl.ds(r, nr), :] += radd[pl.ds(0, nr), pl.ds(0, hd2)]

    pieces = [(mat, half) for mat in mats for half in range(2)]
    cols = dvacc.shape[2]
    n_cols = dm_ // cols

    def piece_loads(n, kind):
        mat, half = pieces[n]
        nr = sizes[mat] // 2
        r0 = sum(sizes[m] // 2 for m, _ in pieces[:n])
        src = near_e.at[half_of(mat, half)] if kind else (far_p, far_m)[half].at[pl.ds(offs[mat] // 2, nr)]
        dst = dkacc if kind else dvacc
        return [pltpu.make_async_copy(src.at[:, pl.ds(k * cols, cols)], dst.at[k, pl.ds(r0, nr), :], pl_sem.at[kind, n])
                for k in range(n_cols)], dst, r0, nr

    def piece_start(n, kind):
        mat, half = pieces[n]
        if kind:
            near_copy(mat, 1 - half, half).wait_recv()
        else:
            far_copy(mat, half).wait_recv()
        for copy in piece_loads(n, kind)[0]:
            copy.start()

    def piece_add(n, kind, slot):
        mat, half = pieces[n]
        copies, src, r0, nr = piece_loads(n, kind)
        for copy in copies:
            copy.wait()
        rows = half_of(mat, half)
        for k in range(n_cols):
            stage_buf[slot, rows, pl.ds(k * cols, cols)] += src[k, pl.ds(r0, nr), :]

    piece_start(0, 0)
    for n, (mat, half) in enumerate(pieces):
        if n + 1 < len(pieces):
            piece_start(n + 1, 0)
        piece_add(n, 0, 1 + half)
        near_copy(mat, half, half).start()

    @pl.when(late)
    def _():
        for half in range(2):
            gd_far_copy(half).wait_recv()
            gd_add(gd_far.at[half], gd_slot(half, half))
            gd_near_copy(half, half).start()
            gd_far_copy(half).wait_send()

    for mat in mats:
        for half in range(2):
            far_copy(mat, half).wait_send()
        stage_buf[0, rows_of(mat)] = wgrad(mat, me)

    def zdy_load(n, buf):
        slot, c = n // nc, lax.rem(n, nc)
        return (pltpu.make_async_copy(z_recv.at[slot, c], dsbuf.at[2 * buf, pl.ds(0, fl)], ld_sem.at[1 + buf]),
                pltpu.make_async_copy(dy_recv.at[slot, c], dsbuf.at[2 * buf + 1, pl.ds(0, dm_)], ld_sem.at[3 + buf]))

    gdacc[...] = wgrad(3, me)

    @pl.when(jnp.logical_not(late))
    def _():
        for c in range(nc):
            for way in (0, 1, 4, 5):
                z_copy(c, way).wait_recv()
            for way in (2, 3):
                dy_copy(c, way).wait_recv()
        for cp in zdy_load(0, 0):
            cp.start()

        @pl.loop(0, 3 * nc)
        def _(n):
            buf = lax.rem(n, 2)

            @pl.when(n + 1 < 3 * nc)
            def _():
                for cp in zdy_load(n + 1, 1 - buf):
                    cp.start()

            for cp in zdy_load(n, buf):
                cp.wait()
            gdacc[...] += dot_t(dsbuf[2 * buf, pl.ds(0, fl), :], dsbuf[2 * buf + 1, pl.ds(0, dm_), :])

    def gd_arrivals(last_half):
        for half in range(2):
            side = half if last_half else 1 - half
            gd_near_copy(side, half).wait_recv()
            gd_add(gd_near.at[last_half, half], gdacc.at[:, gd_cols(half)])

    def out_copy(mat):
        if mat == 3:
            return pltpu.make_async_copy(gdacc, sum_out.at[pl.ds(qrows + orows + dm_, fl)], out_sem.at[3])
        return pltpu.make_async_copy(stage_buf.at[0, rows_of(mat)], sum_out.at[rows_of(mat)], out_sem.at[mat])

    piece_start(0, 1)
    for n, (mat, half) in enumerate(pieces):
        if n + 1 < len(pieces):
            piece_start(n + 1, 1)
        piece_add(n, 1, 0)
        if half:
            out_copy(mat).start()

    @pl.when(late)
    def _():
        gd_arrivals(0)
        gd_arrivals(1)

    out_copy(3).start()
    for mat in mats:
        for side in range(2):
            near_copy(mat, side, side).wait_recv()

    for mat in range(4):
        out_copy(mat).wait()

    @pl.when(jnp.logical_not(late))
    def _():
        for c in range(nc):
            for way in range(6):
                z_copy(c, way).wait_send()
            for way in range(4):
                dy_copy(c, way).wait_send()

    @pl.when(late)
    def _():
        for side in range(2):
            for half in range(2):
                gd_near_copy(side, half).wait_send()

    for idx in range(4):
        for way in range(4):
            w_copy(idx, way).wait_send()
    for mat in mats:
        for half in range(2):
            for side in range(2):
                near_copy(mat, side, half).wait_send()

    @pl.when(jnp.logical_not(first))
    def _():
        for c in range(nc):
            b_copy(c).wait_send()
        lf_copy().wait_send()

    @pl.when(last)
    def _():
        for k in range(1, nm):
            l_copy(k).wait_send()


def finish_kernel(sq, so, su, sd, lq, lo, lu, loss, gq, go, gu, gd, loss_out):
    gq[...] = sq[...] + lq[...]
    go[...] = so[...] + lo[...]
    gu[...] = su[...] + lu[...]
    gd[...] = sd[...]
    loss_out[0] = loss[0, 0]


def solution(mesh):
    ns = mesh.shape["stage"]
    nm = mesh.shape["model"]

    def per_device(tokens_in, targets, w_qkv, w_out, w_up, w_down):
        n_micro, seq_len, d_model = tokens_in.shape
        hl, hd, fl = w_qkv.shape[3], w_qkv.shape[5], w_up.shape[3]
        tc = min(CHUNK, seq_len // 2)
        nc = seq_len // tc
        qrows, orows = hl * 3 * hd, hl * hd
        assert n_micro == nm == 4 and w_qkv.shape[1] == 1 and hl == 2 and d_model == 2 * tc and qrows + orows + d_model == seq_len == 2 * fl and nc == 4
        wqT = jnp.transpose(w_qkv[0, 0], (1, 2, 3, 0)).reshape(qrows, d_model)
        wo = w_out[0, 0].reshape(orows, d_model)
        wu, wd = w_up[0, 0], w_down[0, 0]
        cfg = (ns, nm, nc, tc, d_model, hl, hd, fl)
        heads = nm * hl
        any_spec = pl.BlockSpec(memory_space=pl.ANY)
        f32 = lambda *shape: jax.ShapeDtypeStruct(shape, F32)
        rsum = qrows + orows + d_model
        seqb = nc * tc
        b16 = lambda *shape: jax.ShapeDtypeStruct(shape, BF16)
        out_shape = (f32(rsum + fl, d_model), f32(8, 128), f32(rsum // 2, d_model), f32(rsum // 2, d_model), f32(rsum, d_model),
                     f32(rsum, d_model), b16(3, nc, fl, tc), b16(2, nc, fl // 2, tc), b16(3, nc, d_model, tc),
                     f32(2, fl, d_model // 2), f32(2, 2, fl, d_model // 2))
        vb = lambda *shape: pltpu.VMEM(shape, BF16)
        vf = lambda *shape: pltpu.VMEM(shape, F32)
        dma = lambda *shape: pltpu.SemaphoreType.DMA(shape)
        scratch = [
            vb(nm * qrows, d_model), vb(d_model, nm * orows), vb(nm * fl, d_model), vb(d_model, nm * fl),
            vb(nm * fl, d_model), vb(d_model, nm * fl), vb(nm * orows, d_model), vb(d_model, nm * qrows),
            vb(nc, tc, d_model), vb(nc, d_model, tc), vb(nc, d_model, tc), vb(nc, nm * qrows, tc), vb(nm, seqb, orows), vb(nm, seqb, orows),
            vb(nc, nm * orows, tc), vb(nc, d_model, tc), vb(nc, d_model, tc), vb(nc, nm * fl, tc), vb(nc, nm * fl, tc),
            vb(nc * (nc + 1) // 2, heads, tc, tc), vb(nc, d_model, tc), vf(heads // 2, seqb, 2 * hd), vf(heads // 2, seqb, 2 * hd),
            vb(nc, d_model, tc), vb(nm * orows, tc), vf(nm + 2, 8, 128), vf(8, tc),
            vf(4, rsum, d_model), vf(256, d_model), vf(fl, d_model), vb(heads, max((nc - 1) * tc, fl), tc), vb(nm * orows, tc),
            dma(4, 4), dma(4, 4), dma(4), pltpu.SemaphoreType.REGULAR, dma(nc), dma(nc), dma(nc), dma(nc), dma(nc),
            dma(nm - 1), dma(nm - 1), pltpu.SemaphoreType.DMA, pltpu.SemaphoreType.DMA,
            dma(3, 6), dma(3, 6), dma(5), dma(4), dma(6, nc), dma(6, nc), dma(4, nc), dma(4, nc), dma(6), dma(6), dma(2, 6),
        ]
        res = pl.pallas_call(
            functools.partial(step_kernel, cfg),
            out_shape=out_shape,
            in_specs=[any_spec] * 6,
            out_specs=[any_spec, pl.BlockSpec(memory_space=pltpu.VMEM)] + [any_spec] * 9,
            scratch_shapes=scratch,
            compiler_params=pltpu.CompilerParams(collective_id=0, has_side_effects=True, vmem_limit_bytes=67043328),
            name="train_step",
        )(tokens_in, targets, wqT, wo, wu, wd)
        part, loss, late = res[0], res[1], res[5]
        steps = 4

        def spec(size, start):
            rows = size // steps
            return pl.BlockSpec((rows, d_model), lambda i: (start // rows + i, 0))

        q_s, o_s, u_s = spec(qrows, 0), spec(orows, qrows), spec(d_model, qrows + orows)
        g_qkv, g_out, g_up, g_down, loss = pl.pallas_call(
            finish_kernel,
            grid=(steps,),
            out_shape=(f32(qrows, d_model), f32(orows, d_model), f32(d_model, fl), f32(fl, d_model), f32(1)),
            in_specs=[q_s, o_s, u_s, spec(fl, rsum), q_s, o_s, u_s, pl.BlockSpec(memory_space=pltpu.SMEM)],
            out_specs=[spec(qrows, 0), spec(orows, 0), spec(d_model, 0), spec(fl, 0), pl.BlockSpec(memory_space=pltpu.SMEM)],
            name="finish",
        )(part, part, part, part, late, late, late, loss)
        g_qkv = jnp.transpose(g_qkv.reshape(hl, 3, hd, d_model), (3, 0, 1, 2))[None, None]
        return g_qkv, g_out.reshape(1, 1, hl, hd, d_model), g_up[None, None], g_down[None, None], loss

    tok_spec = P(None, "data", None)
    qkv_spec = P("stage", None, None, "model", None, None)
    out_spec = P("stage", None, "model", None, None)
    up_spec = P("stage", None, None, "model")
    down_spec = P("stage", None, "model", None)
    g_qkv_spec = P(("data", "stage"), None, None, "model", None, None)
    g_out_spec = P(("data", "stage"), None, "model", None, None)
    g_up_spec = P(("data", "stage"), None, None, "model")
    g_down_spec = P(("data", "stage"), None, "model", None)
    return jax.shard_map(per_device, mesh=mesh, in_specs=(tok_spec, tok_spec, qkv_spec, out_spec, up_spec, down_spec), out_specs=(g_qkv_spec, g_out_spec, g_up_spec, g_down_spec, P("data")), check_vma=False)
```

```python
import functools
import math

import jax
import jax.numpy as jnp
from jax import lax
from jax.experimental import pallas as pl
from jax.experimental.pallas import tpu as pltpu
from jax.sharding import PartitionSpec as P

F32 = jnp.float32
BF16 = jnp.bfloat16
MESH = pl.DeviceIdType.MESH
CHUNK = 256
NEG = -1e30
GELU_C = math.sqrt(2.0 / math.pi)
GELU_A = 0.044715

W_Q, W_O, W_U, W_D = range(4)


def dot(lhs, rhs):
    return jnp.dot(lhs, rhs, preferred_element_type=F32)


def dot_t(lhs, rhs):
    return lax.dot_general(lhs, rhs, (((1,), (1,)), ((), ())), preferred_element_type=F32)


def inv_rms(x32):
    return lax.rsqrt(jnp.mean(x32 * x32, axis=0, keepdims=True) + 1e-6)


def norm_pull(x32, inv, g32):
    mean_gx = jnp.mean(g32 * x32, axis=0, keepdims=True)
    return g32 * inv - x32 * (inv * inv * inv * mean_gx)


def gelu(u):
    tanh = jnp.tanh(u * (GELU_C + (GELU_C * GELU_A) * (u * u)))
    half = 0.5 * u
    return half + half * tanh


def gelu_grad(u):
    u2 = u * u
    sig = 0.5 + 0.5 * jnp.tanh(u * (GELU_C + (GELU_C * GELU_A) * u2))
    slope = u * (2.0 * GELU_C + (6.0 * GELU_C * GELU_A) * u2)
    return sig * (1.0 + slope * (1.0 - sig))


def step_kernel(cfg, x_hbm, t_hbm, wqT_in, wo_in, wu_in, wd_in,
                sum_out, loss_out, far_p, far_m, near_e, near_l, z_recv, z_fwd, dy_recv, gd_far, gd_near,
                wqT, woT, wuT, wdT, wd, wu, wo, wq,
                xin, hbuf, n1buf, qkv, kn, vn, obuf, mbuf, n2buf, ubuf, zbuf, pbuf, dybuf, dvacc, dkacc,
                ybuf, dobuf, losst, lossv, stage_buf, radd, gdacc, dsbuf, qsave,
                ag_send, ag_recv, ag_loc, go_sem, xsem, fsend, frecv, bsend, brecv, lsend, lrecv, lfsend, lfrecv,
                rs_send, rs_recv, ld_sem, out_sem, z_send, z_arr, dy_send, dy_arr, gd_send, gd_recv, pl_sem):
    ns, nm, nc, tc, dm_, hl, hd, fl = cfg
    heads = nm * hl
    qrows = hl * 3 * hd
    orows = hl * hd
    inv_d = 1.0 / (nm * nc * tc * dm_)
    scale = hd ** -0.5
    exp_c = scale * math.log2(math.e)
    me = lax.axis_index("model")
    st = lax.axis_index("stage")
    nxt = lax.rem(st + 1, ns)
    prv = lax.rem(st + ns - 1, ns)
    first = st == 0
    last = st == ns - 1

    def peer(k):
        return lax.rem(me + k, nm)

    bar = pltpu.get_barrier_semaphore()
    pl.semaphore_signal(bar, inc=1, device_id={"stage": nxt}, device_id_type=MESH)
    pl.semaphore_signal(bar, inc=1, device_id={"stage": prv}, device_id_type=MESH)
    for k in range(1, nm):
        pl.semaphore_signal(bar, inc=1, device_id={"model": peer(k)}, device_id_type=MESH)
    pl.semaphore_wait(bar, 2 + nm - 1)

    def rowsl(start, size, mult):
        return pl.ds(pl.multiple_of(start, mult), size)

    plus, minus, far = 1, nm - 1, 2

    def w_rows(idx, who, half=None):
        size = (qrows, orows, fl, fl)[idx]
        if idx in (W_Q, W_U):
            buf = wqT if idx == W_Q else wuT
            if half is None:
                return buf.at[rowsl(who * size, size, size), :]
            return buf.at[rowsl(who * size + half * (size // 2), size // 2, size // 2), :]
        view = (woT if idx == W_O else wdT).at[:, rowsl(who * size, size, size)]
        return view if half is None else view.at[pl.ds(half * (dm_ // 2), dm_ // 2), :]

    def w_copy(idx, way):
        to = plus if way in (0, 2) else minus
        if way < 2:
            src = wqT_in if idx == W_Q else w_rows(idx, me)
            dst = w_rows(idx, me)
        else:
            src = dst = w_rows(idx, peer(minus if way == 2 else plus), way - 2)
        return pltpu.make_async_remote_copy(
            src_ref=src, dst_ref=dst, send_sem=ag_send.at[idx, way], recv_sem=ag_recv.at[idx, way],
            device_id={"model": peer(to)}, device_id_type=MESH)

    def w_arrival(idx, way):
        who = peer((minus, plus, far, far)[way])
        ref = w_rows(idx, who) if way < 2 else w_rows(idx, who, way - 2)
        return pltpu.make_async_remote_copy(
            src_ref=ref, dst_ref=ref, send_sem=ag_send.at[idx, way], recv_sem=ag_recv.at[idx, way],
            device_id={"model": peer(plus)}, device_id_type=MESH)

    def w_local(idx):
        src = (wqT_in, wo_in, wu_in, wd_in)[idx]
        dst = (w_rows(W_Q, me), wo.at[rowsl(me * orows, orows, orows), :], wu.at[:, rowsl(me * fl, fl, fl)], wd.at[rowsl(me * fl, fl, fl), :])[idx]
        return pltpu.make_async_copy(src, dst, ag_loc.at[idx])

    def w_own(idx):
        for way in range(2):
            w_copy(idx, way).start()

    def w_forward(idx):
        for way in range(2):
            w_arrival(idx, way).wait_recv()
        for way in range(2, 4):
            w_copy(idx, way).start()

    def w_wait(idx):
        for way in range(2, 4):
            w_arrival(idx, way).wait_recv()

    def x_copy(c):
        return pltpu.make_async_copy(x_hbm.at[me, pl.ds(c * tc, tc), :], xin.at[c], xsem.at[c])

    def t_copy(c):
        return pltpu.make_async_copy(t_hbm.at[me, pl.ds(c * tc, tc), :], xin.at[c], xsem.at[c])

    @pl.when(first)
    def _():
        for c in range(nc):
            x_copy(c).start()

    @pl.when(last)
    def _():
        for c in range(nc):
            t_copy(c).start()

    for idx in range(4):
        w_local(idx).start()

    odd = lax.rem(st, 2) == 1
    early = st < 2

    @pl.when(odd)
    def _():
        pl.semaphore_wait(go_sem, 1)

    w_own(W_Q)
    w_local(W_O).wait()
    woT[:, rowsl(me * orows, orows, orows)] = jnp.transpose(wo[rowsl(me * orows, orows, orows), :])
    w_own(W_O)
    w_local(W_U).wait()
    wuT[rowsl(me * fl, fl, fl), :] = jnp.transpose(wu[:, rowsl(me * fl, fl, fl)])
    w_own(W_U)
    w_local(W_D).wait()
    wdT[:, rowsl(me * fl, fl, fl)] = jnp.transpose(wd[rowsl(me * fl, fl, fl), :])
    w_own(W_D)
    w_local(W_Q).wait()
    w_forward(W_Q)
    w_forward(W_O)

    @pl.when(jnp.logical_not(odd))
    def _():
        pl.semaphore_signal(go_sem, inc=1, device_id={"stage": nxt}, device_id_type=MESH)

    def natural_weights():
        @pl.loop(0, nm)
        def _(f):
            wu[:, rowsl(f * fl, fl, fl)] = jnp.transpose(wuT[rowsl(f * fl, fl, fl), :])
            wd[rowsl(f * fl, fl, fl), :] = jnp.transpose(wdT[:, rowsl(f * fl, fl, fl)])
            wo[rowsl(f * orows, orows, orows), :] = jnp.transpose(woT[:, rowsl(f * orows, orows, orows)])
            wq[:, rowsl(f * qrows, qrows, qrows)] = jnp.transpose(wqT[rowsl(f * qrows, qrows, qrows), :])

    late = st >= max(2, ns // 2)

    @pl.when(jnp.logical_not(early))
    def _():
        w_forward(W_U)
        w_forward(W_D)
        for idx in range(4):
            w_wait(idx)

    @pl.when(late)
    def _():
        natural_weights()

    def f_copy(c):
        return pltpu.make_async_remote_copy(
            src_ref=ybuf.at[c], dst_ref=hbuf.at[c], send_sem=fsend.at[c], recv_sem=frecv.at[c],
            device_id={"stage": nxt}, device_id_type=MESH)

    def b_copy(c):
        return pltpu.make_async_remote_copy(
            src_ref=ybuf.at[c], dst_ref=dybuf.at[c], send_sem=bsend.at[c], recv_sem=brecv.at[c],
            device_id={"stage": prv}, device_id_type=MESH)

    def ring_copy(src, dst, send, recv, way):
        return pltpu.make_async_remote_copy(
            src_ref=src, dst_ref=dst, send_sem=send, recv_sem=recv,
            device_id={"model": peer((plus, minus)[way % 2])}, device_id_type=MESH)

    hf = fl // 2

    def z_copy(c, way):
        if way < 2:
            src, dst = zbuf.at[c, rowsl(peer((plus, minus)[way]) * fl, fl, fl), :], z_recv.at[way, c]
        elif way < 4:
            src, dst = zbuf.at[c, rowsl(peer(far) * fl + (way - 2) * hf, hf, hf), :], z_fwd.at[way - 2, c]
        else:
            src, dst = z_fwd.at[way - 4, c], z_recv.at[2, c, pl.ds((way - 4) * hf, hf)]
        return ring_copy(src, dst, z_send.at[way, c], z_arr.at[way, c], way)

    def z_forward(c):
        for way in (2, 3):
            z_copy(c, way).wait_recv()
        for way in (4, 5):
            z_copy(c, way).start()

    def dy_copy(c, way):
        if way < 2:
            src, dst = dybuf.at[c], dy_recv.at[way, c]
        else:
            rows = pl.ds((way - 2) * (dm_ // 2), dm_ // 2)
            src, dst = dy_recv.at[way - 2, c, rows], dy_recv.at[2, c, rows]
        return ring_copy(src, dst, dy_send.at[way, c], dy_arr.at[way, c], way)

    def dy_forward(c):
        for way in (0, 1):
            dy_copy(c, way).wait_recv()
        for way in (2, 3):
            dy_copy(c, way).start()

    lossv[...] = jnp.zeros_like(lossv)

    def head_rows(p, h, part):
        return pl.ds(p * (2 * 3 * hd) + (h * 3 + part) * hd, hd)

    def pad_head(val, h):
        zero = jnp.zeros_like(val)
        return jnp.concatenate([val, zero] if h == 0 else [zero, val], axis=0)

    def causal(shape, row0):
        return lax.broadcasted_iota(jnp.int32, shape, 0) + row0 <= lax.broadcasted_iota(jnp.int32, shape, 1)

    n_st = stage_buf.shape[0]

    def folded(slot, row, n):
        fold = stage_buf.shape[1]
        return stage_buf.at[slot, pl.ds(row % fold, n), pl.ds((row // fold) * tc, tc)]

    def slope(c):
        blk = fl // 4
        per = stage_buf.shape[1] // blk

        @pl.loop(0, 4 * nm)
        def _(f):
            half = f // per
            rows = pl.ds(pl.multiple_of((f - half * per) * blk, blk), blk)
            cols = pl.ds(pl.multiple_of(half * tc, tc), tc)
            u = ubuf[c, pl.ds(pl.multiple_of(f * blk, blk), blk), :].astype(F32)
            stage_buf[nc - 1 - c, rows, cols] = gelu_grad(u)

    def attention(cc):
        nk = (cc + 1) * tc
        slots = min(heads, 2 * nc * tc // nk)
        ahead = min(4, slots - 1)
        sub = tc // 2

        def front(head):
            p, h = head // 2, head % 2
            base = (head % slots) * nk
            qz = pad_head(qkv[cc, head_rows(p, h, 0), :], h)
            tops, sums = [], []
            for j in range(cc + 1):
                s = dot(kn[p, pl.ds(j * tc, tc), :], qz)
                for r in range(0, tc, sub):
                    part = s[r:r + sub]
                    if j == cc:
                        part = jnp.where(causal(part.shape, r), part, NEG)
                    top = jnp.max(part, axis=0, keepdims=True)
                    e = jnp.exp2((part - top) * exp_c)
                    folded(n_st - 1, base + j * tc + r, sub)[...] = e
                    tops.append(top)
                    sums.append(jnp.sum(e, axis=0, keepdims=True))
            mx = functools.reduce(jnp.maximum, tops)
            scales = [jnp.exp2((top - mx) * exp_c) for top in tops]
            inv = 1.0 / functools.reduce(jnp.add, [a * b for a, b in zip(scales, sums)])
            return [a * inv for a in scales]

        def back(head, factors):
            p, h = head // 2, head % 2
            base = (head % slots) * nk
            o_t = None
            for j in range(cc + 1):
                parts = []
                for i in range(2):
                    pr = (folded(n_st - 1, base + j * tc + i * sub, sub)[...] * factors[2 * j + i]).astype(BF16)
                    pbuf[cc * (cc + 1) // 2 + j, head, pl.ds(i * sub, sub), :] = pr
                    parts.append(pr)
                part = dot(qkv[j, head_rows(p, h, 2), :], jnp.concatenate(parts, axis=0))
                o_t = part if o_t is None else o_t + part
            obuf[cc, pl.ds(head * hd, hd), :] = o_t.astype(BF16)

        factors = {}
        for head in range(ahead):
            factors[head] = front(head)
        for head in range(heads):
            if head + ahead < heads:
                factors[head + ahead] = front(head + ahead)
            back(head, factors.pop(head))

    def attention_grad(cc):
        units = [(p, j) for p in range(heads // 2) for j in range(cc + 1)]
        dqs = {}
        held = {}

        def of_head(p, h):
            if (p, h) not in held:
                rows = pl.ds((p * 2 + h) * hd, hd)
                do_t = dobuf[rows, :]
                dsum = jnp.sum(do_t.astype(F32) * obuf[cc, rows, :].astype(F32), axis=0, keepdims=True)
                held[p, h] = (pad_head(do_t, h), dsum)
            return held[p, h]

        def front(p, j):
            out = []
            for h in range(2):
                do_z, dsum = of_head(p, h)
                pr = pbuf[cc * (cc + 1) // 2 + j, p * 2 + h]
                dp = dot(vn[p, pl.ds(j * tc, tc), :], do_z).astype(BF16).astype(F32)
                ds = (pr.astype(F32) * (dp - dsum)).astype(BF16)
                if j < cc:
                    dsbuf[p * 2 + h, pl.ds(j * tc, tc), :] = ds
                out.append(ds)
            return out

        def back(p, j, ds):
            for h in range(2):
                dq_h = dot(qkv[j, head_rows(p, h, 1), :], ds[h])
                dqs[p, h] = dq_h if j == 0 else dqs[p, h] + dq_h
            if j < cc:
                return
            dv_new, dk_new = kv_grad(cc, p, j, [of_head(p, h)[0] for h in range(2)], ds,
                                     [qkv[cc, head_rows(p, h, 0), :] for h in range(2)])
            dv_t = jnp.transpose(dv_new).astype(BF16)
            dk_t = (jnp.transpose(dk_new) * scale).astype(BF16)
            for h in range(2):
                qsave[pl.ds((p * 2 + h) * hd, hd), :] = qkv[cc, head_rows(p, h, 0), :]
                qkv[cc, head_rows(p, h, 0), :] = (dqs[p, h] * scale).astype(BF16)
                qkv[cc, head_rows(p, h, 1), :] = dk_t[h * hd:(h + 1) * hd, :]
                qkv[cc, head_rows(p, h, 2), :] = dv_t[h * hd:(h + 1) * hd, :]

        ds = front(*units[0])
        for n, unit in enumerate(units):
            later = front(*units[n + 1]) if n + 1 < len(units) else None
            back(*unit, ds)
            ds = later

    def kv_grad(cc, p, j, do_z, ds, q_t):
        dv_new = dk_new = None
        for h in range(2):
            dv_h = dot_t(pbuf[cc * (cc + 1) // 2 + j, p * 2 + h], do_z[h])
            dk_h = dot_t(ds[h], pad_head(q_t[h], h))
            dv_new = dv_h if dv_new is None else dv_new + dv_h
            dk_new = dk_h if dk_new is None else dk_new + dk_h
        rows = pl.ds(j * tc, tc)
        if cc < nc - 1:
            dv_new = dv_new + dvacc[p, rows, :]
            dk_new = dk_new + dkacc[p, rows, :]
        return dv_new, dk_new

    def earlier_keys(cc):
        for p in range(heads // 2):
            heads_of = [pl.ds((p * 2 + h) * hd, hd) for h in range(2)]
            do_z = [pad_head(dobuf[heads_of[h], :], h) for h in range(2)]
            q_t = [qsave[heads_of[h], :] for h in range(2)]
            for j in range(cc):
                rows = pl.ds(j * tc, tc)
                dv_new, dk_new = kv_grad(cc, p, j, do_z, [dsbuf[p * 2 + h, rows, :] for h in range(2)], q_t)
                dvacc[p, rows, :] = dv_new
                dkacc[p, rows, :] = dk_new

    def attention_step(c):
        @pl.when(first)
        def _():
            x_copy(c).wait()
            hbuf[c] = jnp.transpose(xin[c])

        @pl.when(jnp.logical_not(first))
        def _():
            f_copy(c).wait_recv()

        @pl.when(early & (c == 0))
        def _():
            w_wait(W_Q)

        h32 = hbuf[c].astype(F32)
        n1 = (h32 * inv_rms(h32)).astype(BF16)
        n1buf[c] = n1
        for r in range(nm):
            rows = pl.ds(r * qrows, qrows)
            blk = dot(wqT[rows, :], n1).astype(BF16)
            qkv[c, rows, :] = blk
            for part, ref in ((1, kn), (2, vn)):
                both = jnp.concatenate([blk[(3 * h + part) * hd:(3 * h + part + 1) * hd] for h in range(2)], axis=0)
                ref[r, pl.ds(pl.multiple_of(c * tc, tc), tc), :] = jnp.transpose(both)

        for cc in range(nc):
            pl.when(c == cc)(functools.partial(attention, cc))

    def mlp_step(c):
        a = dot(woT[...], obuf[c]).astype(BF16)
        m32 = (hbuf[c].astype(F32) + a.astype(F32)).astype(BF16).astype(F32)
        mbuf[c] = m32.astype(BF16)
        n2 = (m32 * inv_rms(m32)).astype(BF16)
        n2buf[c] = n2

        blk = fl // 2
        for f in range(2 * nm):
            rows = pl.ds(f * blk, blk)
            u = dot(wuT[rows, :], n2buf[c]).astype(BF16)
            ubuf[c, rows, :] = u
            zbuf[c, rows, :] = gelu(u.astype(F32)).astype(BF16)
        acc = dot(wdT[...], zbuf[c])
        y32 = (mbuf[c].astype(F32) + acc.astype(BF16).astype(F32)).astype(BF16)
        ybuf[c] = y32

        @pl.when(jnp.logical_not(last))
        def _():
            f_copy(c).start()

        @pl.when(last)
        def _():
            t_copy(c).wait()
            err = ybuf[c].astype(F32) - jnp.transpose(xin[c]).astype(F32)
            lossv[...] += jnp.sum((err * err).reshape(dm_ // 8, 8, tc), axis=0)
            dybuf[c] = (err * inv_d).astype(BF16)

        @pl.when(last & (c > 0))
        def _():
            slope(c)

    @pl.loop(0, 2 * nc)
    def _(n):
        attn_turn = jnp.where(early, jnp.where(n < nc, 1, 0), 1 - lax.rem(n, 2))
        c = jnp.where(early, lax.rem(n, nc), n // 2)

        @pl.when(early & (n == 1))
        def _():
            w_forward(W_U)

        @pl.when(early & (n == 2))
        def _():
            w_forward(W_D)

        @pl.when(attn_turn == 1)
        def _():
            attention_step(c)

        @pl.when(early & (n == nc))
        def _():
            w_wait(W_O)
            w_wait(W_U)
            w_wait(W_D)

        @pl.when(attn_turn == 0)
        def _():
            mlp_step(c)

    def z_start():
        for c in range(nc):
            for way in range(4):
                z_copy(c, way).start()

    @pl.when(jnp.logical_not(late))
    def _():
        for c in range(nc):
            f_copy(c).wait_send()
        z_start()
        natural_weights()

    @pl.when(jnp.logical_not(last))
    def _():
        @pl.loop(0, nc)
        def _(c):
            slope(c)

    @pl.when(jnp.logical_not(late))
    def _():
        @pl.loop(0, nc)
        def _(c):
            z_forward(c)

    def l_copy(k):
        return pltpu.make_async_remote_copy(
            src_ref=losst.at[nm], dst_ref=losst.at[3 - k if nm == 4 else nm - 1 - k], send_sem=lsend.at[k - 1],
            recv_sem=lrecv.at[k - 1], device_id={"model": peer(k)}, device_id_type=MESH)

    def lf_copy():
        return pltpu.make_async_remote_copy(
            src_ref=losst.at[nm + 1], dst_ref=losst.at[nm + 1], send_sem=lfsend, recv_sem=lfrecv,
            device_id={"stage": prv}, device_id_type=MESH)

    @pl.when(last)
    def _():
        tot = jnp.sum(lossv[...]) * (0.5 * inv_d)
        losst[nm] = jnp.full(losst.shape[1:], tot, F32)
        for k in range(1, nm):
            l_copy(k).start()

    dy_inside = jnp.logical_not(late) & (first | odd)

    @pl.loop(0, nc)
    def _(i):
        c = nc - 1 - i

        @pl.when(jnp.logical_not(last))
        def _():
            b_copy(c).wait_recv()

        @pl.when(jnp.logical_not(late) & (i == 0))
        def _():
            for way in range(2):
                dy_copy(c, way).start()

        @pl.when(last & (c == 0))
        def _():
            slope(c)

        blk = fl // 4
        for f in range(4 * nm):
            rows = pl.ds(f * blk, blk)
            dz = dot(wd[rows, :], dybuf[c]).astype(BF16).astype(F32)
            ubuf[c, rows, :] = (dz * folded(i, f * blk, blk)[...]).astype(BF16)
        acc = dot(wu[...], ubuf[c])
        dn2 = acc.astype(BF16).astype(F32)
        m32 = mbuf[c].astype(F32)
        pull = norm_pull(m32, inv_rms(m32), dn2).astype(BF16)
        dmid = (dybuf[c].astype(F32) + pull.astype(F32)).astype(BF16)
        mbuf[c] = dmid
        dobuf[...] = dot(wo[...], dmid).astype(BF16)

        @pl.when(jnp.logical_not(late) & (i > 0))
        def _():
            for way in range(2):
                dy_copy(c, way).start()

        @pl.when(dy_inside & (i > 0))
        def _():
            dy_forward(c + 1)

        for cc in range(nc):
            pl.when(c == cc)(functools.partial(attention_grad, cc))

        dn1 = dot(wq[...], qkv[c]).astype(BF16).astype(F32)
        h32 = hbuf[c].astype(F32)
        pull1 = norm_pull(h32, inv_rms(h32), dn1).astype(BF16)

        @pl.when(late & jnp.logical_not(last))
        def _():
            f_copy(c).wait_send()

        ybuf[c] = (mbuf[c].astype(F32) + pull1.astype(F32)).astype(BF16)

        @pl.when(jnp.logical_not(first))
        def _():
            b_copy(c).start()

        for cc in range(1, nc):
            pl.when(c == cc)(functools.partial(earlier_keys, cc))

    @pl.when(last)
    def _():
        for k in range(1, nm):
            l_copy(k).wait_recv()
        vals = [losst[nm]] + [losst[k - 1] for k in range(1, nm)]
        tot = jnp.zeros_like(vals[0])
        for who in range(nm):
            pick = vals[0]
            for k in range(1, nm):
                pick = jnp.where(peer(k) == who, vals[k], pick)
            tot = tot + pick
        losst[nm + 1] = tot

    @pl.when(jnp.logical_not(last))
    def _():
        lf_copy().wait_recv()

    @pl.when(jnp.logical_not(first))
    def _():
        lf_copy().start()

    loss_out[...] = losst[nm + 1]

    def wgrad(mat, d):
        acc = None
        for c in range(nc):
            if mat == 0:
                part = dot_t(qkv[c, rowsl(d * qrows, qrows, qrows), :], n1buf[c])
            elif mat == 1:
                part = dot_t(obuf[c, rowsl(d * orows, orows, orows), :], mbuf[c])
            elif mat == 2:
                part = dot_t(n2buf[c], ubuf[c, rowsl(d * fl, fl, fl), :])
            else:
                part = dot_t(zbuf[c, rowsl(d * fl, fl, fl), :], dybuf[c])
            acc = part if acc is None else acc + part
        return acc

    sizes = (qrows, orows, dm_)
    offs = (0, qrows, qrows + orows)

    def rows_of(mat):
        return pl.ds(offs[mat], sizes[mat])

    def half_of(mat, half):
        return pl.ds(offs[mat] + half * (sizes[mat] // 2), sizes[mat] // 2)

    def far_copy(mat, half):
        rows = pl.ds(offs[mat] // 2, sizes[mat] // 2)
        return ring_copy(stage_buf.at[0, half_of(mat, half)], (far_p, far_m)[half].at[rows],
                         rs_send.at[mat, half], rs_recv.at[mat, half], half)

    def near_copy(mat, side, half):
        way = 2 + 2 * side + half
        return ring_copy(stage_buf.at[1 + side, half_of(mat, half)], (near_l if side == half else near_e).at[half_of(mat, half)],
                         rs_send.at[mat, way], rs_recv.at[mat, way], side)

    mats = (2, 0, 1)
    for mat in mats:
        stage_buf[0, rows_of(mat)] = wgrad(mat, peer(far))
        for half in range(2):
            far_copy(mat, half).start()
    for mat in mats:
        for side in range(2):
            stage_buf[1 + side, rows_of(mat)] = wgrad(mat, peer((plus, minus)[side]))
            near_copy(mat, side, 1 - side).start()

    @pl.when(dy_inside)
    def _():
        dy_forward(0)

    @pl.when(jnp.logical_not(late | dy_inside))
    def _():
        for c in reversed(range(nc)):
            dy_forward(c)

    hd2 = dm_ // 2

    def gd_cols(half):
        return pl.ds(half * hd2, hd2)

    def gd_half(d, half):
        return functools.reduce(jnp.add, [
            dot_t(zbuf[c, rowsl(d * fl, fl, fl), :], dybuf[c, gd_cols(half), :]) for c in range(nc)])

    def gd_far_copy(half):
        return ring_copy(gdacc.at[:, gd_cols(half)], gd_far.at[half], gd_send.at[half], gd_recv.at[half], half)

    def gd_slot(side, half):
        return folded(n_st - 1, (2 * side + half) * fl, fl)

    def gd_near_copy(side, half):
        way = 2 + 2 * side + half
        return ring_copy(gd_slot(side, half), gd_near.at[1 if side == half else 0, half],
                         gd_send.at[way], gd_recv.at[way], side)

    @pl.when(late)
    def _():
        for half in range(2):
            gdacc[:, gd_cols(half)] = gd_half(peer(far), half)
            gd_far_copy(half).start()
        for side in range(2):
            for half in (1 - side, side):
                gd_slot(side, half)[...] = gd_half(peer((plus, minus)[side]), half)
            gd_near_copy(side, 1 - side).start()

    def gd_add(src, ref):
        nr = min(fl, radd.shape[0])
        for r in range(0, fl, nr):
            copy = pltpu.make_async_copy(src.at[pl.ds(r, nr)], radd.at[pl.ds(0, nr), pl.ds(0, hd2)], ld_sem.at[0])
            copy.start()
            copy.wait()
            ref[pl.ds(r, nr), :] += radd[pl.ds(0, nr), pl.ds(0, hd2)]

    pieces = [(mat, half) for mat in mats for half in range(2)]
    cols = dvacc.shape[2]
    n_cols = dm_ // cols

    def piece_loads(n, kind):
        mat, half = pieces[n]
        nr = sizes[mat] // 2
        r0 = sum(sizes[m] // 2 for m, _ in pieces[:n])
        src = near_e.at[half_of(mat, half)] if kind else (far_p, far_m)[half].at[pl.ds(offs[mat] // 2, nr)]
        dst = dkacc if kind else dvacc
        return [pltpu.make_async_copy(src.at[:, pl.ds(k * cols, cols)], dst.at[k, pl.ds(r0, nr), :], pl_sem.at[kind, n])
                for k in range(n_cols)], dst, r0, nr

    def piece_start(n, kind):
        mat, half = pieces[n]
        if kind:
            near_copy(mat, 1 - half, half).wait_recv()
        else:
            far_copy(mat, half).wait_recv()
        for copy in piece_loads(n, kind)[0]:
            copy.start()

    def piece_add(n, kind, slot):
        mat, half = pieces[n]
        copies, src, r0, nr = piece_loads(n, kind)
        for copy in copies:
            copy.wait()
        rows = half_of(mat, half)
        for k in range(n_cols):
            stage_buf[slot, rows, pl.ds(k * cols, cols)] += src[k, pl.ds(r0, nr), :]

    piece_start(0, 0)
    for n, (mat, half) in enumerate(pieces):
        if n + 1 < len(pieces):
            piece_start(n + 1, 0)
        piece_add(n, 0, 1 + half)
        near_copy(mat, half, half).start()

    @pl.when(late)
    def _():
        for half in range(2):
            gd_far_copy(half).wait_recv()
            gd_add(gd_far.at[half], gd_slot(half, half))
            gd_near_copy(half, half).start()
            gd_far_copy(half).wait_send()

    for mat in mats:
        for half in range(2):
            far_copy(mat, half).wait_send()
        stage_buf[0, rows_of(mat)] = wgrad(mat, me)

    def zdy_load(n, buf):
        slot, c = n // nc, lax.rem(n, nc)
        return (pltpu.make_async_copy(z_recv.at[slot, c], dsbuf.at[2 * buf, pl.ds(0, fl)], ld_sem.at[1 + buf]),
                pltpu.make_async_copy(dy_recv.at[slot, c], dsbuf.at[2 * buf + 1, pl.ds(0, dm_)], ld_sem.at[3 + buf]))

    gdacc[...] = wgrad(3, me)

    @pl.when(jnp.logical_not(late))
    def _():
        for c in range(nc):
            for way in (0, 1, 4, 5):
                z_copy(c, way).wait_recv()
            for way in (2, 3):
                dy_copy(c, way).wait_recv()
        for cp in zdy_load(0, 0):
            cp.start()

        @pl.loop(0, 3 * nc)
        def _(n):
            buf = lax.rem(n, 2)

            @pl.when(n + 1 < 3 * nc)
            def _():
                for cp in zdy_load(n + 1, 1 - buf):
                    cp.start()

            for cp in zdy_load(n, buf):
                cp.wait()
            gdacc[...] += dot_t(dsbuf[2 * buf, pl.ds(0, fl), :], dsbuf[2 * buf + 1, pl.ds(0, dm_), :])

    def gd_arrivals(last_half):
        for half in range(2):
            side = half if last_half else 1 - half
            gd_near_copy(side, half).wait_recv()
            gd_add(gd_near.at[last_half, half], gdacc.at[:, gd_cols(half)])

    def out_copy(mat):
        if mat == 3:
            return pltpu.make_async_copy(gdacc, sum_out.at[pl.ds(qrows + orows + dm_, fl)], out_sem.at[3])
        return pltpu.make_async_copy(stage_buf.at[0, rows_of(mat)], sum_out.at[rows_of(mat)], out_sem.at[mat])

    piece_start(0, 1)
    for n, (mat, half) in enumerate(pieces):
        if n + 1 < len(pieces):
            piece_start(n + 1, 1)
        piece_add(n, 1, 0)
        if half:
            out_copy(mat).start()

    @pl.when(late)
    def _():
        gd_arrivals(0)
        gd_arrivals(1)

    out_copy(3).start()
    for mat in mats:
        for side in range(2):
            near_copy(mat, side, side).wait_recv()

    for mat in range(4):
        out_copy(mat).wait()

    @pl.when(jnp.logical_not(late))
    def _():
        for c in range(nc):
            for way in range(6):
                z_copy(c, way).wait_send()
            for way in range(4):
                dy_copy(c, way).wait_send()

    @pl.when(late)
    def _():
        for side in range(2):
            for half in range(2):
                gd_near_copy(side, half).wait_send()

    for idx in range(4):
        for way in range(4):
            w_copy(idx, way).wait_send()
    for mat in mats:
        for half in range(2):
            for side in range(2):
                near_copy(mat, side, half).wait_send()

    @pl.when(jnp.logical_not(first))
    def _():
        for c in range(nc):
            b_copy(c).wait_send()
        lf_copy().wait_send()

    @pl.when(last)
    def _():
        for k in range(1, nm):
            l_copy(k).wait_send()


def finish_kernel(sq, so, su, sd, lq, lo, lu, loss, gq, go, gu, gd, loss_out):
    gq[...] = sq[...] + lq[...]
    go[...] = so[...] + lo[...]
    gu[...] = su[...] + lu[...]
    gd[...] = sd[...]
    loss_out[0] = loss[0, 0]


def solution(mesh):
    ns = mesh.shape["stage"]
    nm = mesh.shape["model"]

    def per_device(tokens_in, targets, w_qkv, w_out, w_up, w_down):
        n_micro, seq_len, d_model = tokens_in.shape
        hl, hd, fl = w_qkv.shape[3], w_qkv.shape[5], w_up.shape[3]
        tc = min(CHUNK, seq_len // 2)
        nc = seq_len // tc
        qrows, orows = hl * 3 * hd, hl * hd
        assert n_micro == nm == 4 and w_qkv.shape[1] == 1 and hl == 2 and d_model == 2 * tc and qrows + orows + d_model == seq_len == 2 * fl and nc == 4
        wqT = jnp.transpose(w_qkv[0, 0], (1, 2, 3, 0)).reshape(qrows, d_model)
        wo = w_out[0, 0].reshape(orows, d_model)
        wu, wd = w_up[0, 0], w_down[0, 0]
        cfg = (ns, nm, nc, tc, d_model, hl, hd, fl)
        heads = nm * hl
        any_spec = pl.BlockSpec(memory_space=pl.ANY)
        f32 = lambda *shape: jax.ShapeDtypeStruct(shape, F32)
        rsum = qrows + orows + d_model
        seqb = nc * tc
        b16 = lambda *shape: jax.ShapeDtypeStruct(shape, BF16)
        out_shape = (f32(rsum + fl, d_model), f32(8, 128), f32(rsum // 2, d_model), f32(rsum // 2, d_model), f32(rsum, d_model),
                     f32(rsum, d_model), b16(3, nc, fl, tc), b16(2, nc, fl // 2, tc), b16(3, nc, d_model, tc),
                     f32(2, fl, d_model // 2), f32(2, 2, fl, d_model // 2))
        vb = lambda *shape: pltpu.VMEM(shape, BF16)
        vf = lambda *shape: pltpu.VMEM(shape, F32)
        dma = lambda *shape: pltpu.SemaphoreType.DMA(shape)
        scratch = [
            vb(nm * qrows, d_model), vb(d_model, nm * orows), vb(nm * fl, d_model), vb(d_model, nm * fl),
            vb(nm * fl, d_model), vb(d_model, nm * fl), vb(nm * orows, d_model), vb(d_model, nm * qrows),
            vb(nc, tc, d_model), vb(nc, d_model, tc), vb(nc, d_model, tc), vb(nc, nm * qrows, tc), vb(nm, seqb, orows), vb(nm, seqb, orows),
            vb(nc, nm * orows, tc), vb(nc, d_model, tc), vb(nc, d_model, tc), vb(nc, nm * fl, tc), vb(nc, nm * fl, tc),
            vb(nc * (nc + 1) // 2, heads, tc, tc), vb(nc, d_model, tc), vf(heads // 2, seqb, 2 * hd), vf(heads // 2, seqb, 2 * hd),
            vb(nc, d_model, tc), vb(nm * orows, tc), vf(nm + 2, 8, 128), vf(8, tc),
            vf(4, rsum, d_model), vf(256, d_model), vf(fl, d_model), vb(heads, max((nc - 1) * tc, fl), tc), vb(nm * orows, tc),
            dma(4, 4), dma(4, 4), dma(4), pltpu.SemaphoreType.REGULAR, dma(nc), dma(nc), dma(nc), dma(nc), dma(nc),
            dma(nm - 1), dma(nm - 1), pltpu.SemaphoreType.DMA, pltpu.SemaphoreType.DMA,
            dma(3, 6), dma(3, 6), dma(5), dma(4), dma(6, nc), dma(6, nc), dma(4, nc), dma(4, nc), dma(6), dma(6), dma(2, 6),
        ]
        res = pl.pallas_call(
            functools.partial(step_kernel, cfg),
            out_shape=out_shape,
            in_specs=[any_spec] * 6,
            out_specs=[any_spec, pl.BlockSpec(memory_space=pltpu.VMEM)] + [any_spec] * 9,
            scratch_shapes=scratch,
            compiler_params=pltpu.CompilerParams(collective_id=0, has_side_effects=True, vmem_limit_bytes=67043328),
            name="train_step",
        )(tokens_in, targets, wqT, wo, wu, wd)
        part, loss, late = res[0], res[1], res[5]
        steps = 4

        def spec(size, start):
            rows = size // steps
            return pl.BlockSpec((rows, d_model), lambda i: (start // rows + i, 0))

        q_s, o_s, u_s = spec(qrows, 0), spec(orows, qrows), spec(d_model, qrows + orows)
        g_qkv, g_out, g_up, g_down, loss = pl.pallas_call(
            finish_kernel,
            grid=(steps,),
            out_shape=(f32(qrows, d_model), f32(orows, d_model), f32(d_model, fl), f32(fl, d_model), f32(1)),
            in_specs=[q_s, o_s, u_s, spec(fl, rsum), q_s, o_s, u_s, pl.BlockSpec(memory_space=pltpu.SMEM)],
            out_specs=[spec(qrows, 0), spec(orows, 0), spec(d_model, 0), spec(fl, 0), pl.BlockSpec(memory_space=pltpu.SMEM)],
            name="finish",
        )(part, part, part, part, late, late, late, loss)
        g_qkv = jnp.transpose(g_qkv.reshape(hl, 3, hd, d_model), (3, 0, 1, 2))[None, None]
        return g_qkv, g_out.reshape(1, 1, hl, hd, d_model), g_up[None, None], g_down[None, None], loss

    tok_spec = P(None, "data", None)
    qkv_spec = P("stage", None, None, "model", None, None)
    out_spec = P("stage", None, "model", None, None)
    up_spec = P("stage", None, None, "model")
    down_spec = P("stage", None, "model", None)
    g_qkv_spec = P(("data", "stage"), None, None, "model", None, None)
    g_out_spec = P(("data", "stage"), None, "model", None, None)
    g_up_spec = P(("data", "stage"), None, None, "model")
    g_down_spec = P(("data", "stage"), None, "model", None)
    return jax.shard_map(per_device, mesh=mesh, in_specs=(tok_spec, tok_spec, qkv_spec, out_spec, up_spec, down_spec), out_specs=(g_qkv_spec, g_out_spec, g_up_spec, g_down_spec, P("data")), check_vma=False)
```

```python
import functools
import math

import jax
import jax.numpy as jnp
from jax import lax
from jax.experimental import pallas as pl
from jax.experimental.pallas import tpu as pltpu
from jax.sharding import PartitionSpec as P

F32 = jnp.float32
BF16 = jnp.bfloat16
MESH = pl.DeviceIdType.MESH
CHUNK = 256
NEG = -1e30
GELU_C = math.sqrt(2.0 / math.pi)
GELU_A = 0.044715

W_Q, W_O, W_U, W_D = range(4)


def dot(lhs, rhs):
    return jnp.dot(lhs, rhs, preferred_element_type=F32)


def dot_t(lhs, rhs):
    return lax.dot_general(lhs, rhs, (((1,), (1,)), ((), ())), preferred_element_type=F32)


def inv_rms(x32):
    return lax.rsqrt(jnp.mean(x32 * x32, axis=0, keepdims=True) + 1e-6)


def norm_pull(x32, inv, g32):
    mean_gx = jnp.mean(g32 * x32, axis=0, keepdims=True)
    return g32 * inv - x32 * (inv * inv * inv * mean_gx)


def gelu(u):
    tanh = jnp.tanh(u * (GELU_C + (GELU_C * GELU_A) * (u * u)))
    half = 0.5 * u
    return half + half * tanh


def gelu_grad(u):
    u2 = u * u
    sig = 0.5 + 0.5 * jnp.tanh(u * (GELU_C + (GELU_C * GELU_A) * u2))
    slope = u * (2.0 * GELU_C + (6.0 * GELU_C * GELU_A) * u2)
    return sig * (1.0 + slope * (1.0 - sig))


def step_kernel(cfg, x_hbm, t_hbm, wqT_in, wo_in, wu_in, wd_in,
                sum_out, loss_out, far_p, far_m, near_e, near_l, z_recv, z_fwd, dy_recv, gd_far, gd_near,
                wqT, woT, wuT, wdT, wd, wu, wo, wq,
                xin, hbuf, n1buf, qkv, kn, vn, obuf, mbuf, n2buf, ubuf, zbuf, pbuf, dybuf, dvacc, dkacc,
                ybuf, dobuf, losst, lossv, stage_buf, radd, gdacc, dsbuf, qsave,
                ag_send, ag_recv, ag_loc, go_sem, xsem, fsend, frecv, bsend, brecv, lsend, lrecv, lfsend, lfrecv,
                rs_send, rs_recv, ld_sem, out_sem, z_send, z_arr, dy_send, dy_arr, gd_send, gd_recv, pl_sem):
    ns, nm, nc, tc, dm_, hl, hd, fl = cfg
    heads = nm * hl
    qrows = hl * 3 * hd
    orows = hl * hd
    inv_d = 1.0 / (nm * nc * tc * dm_)
    scale = hd ** -0.5
    exp_c = scale * math.log2(math.e)
    me = lax.axis_index("model")
    st = lax.axis_index("stage")
    nxt = lax.rem(st + 1, ns)
    prv = lax.rem(st + ns - 1, ns)
    first = st == 0
    last = st == ns - 1

    def peer(k):
        return lax.rem(me + k, nm)

    bar = pltpu.get_barrier_semaphore()
    pl.semaphore_signal(bar, inc=1, device_id={"stage": nxt}, device_id_type=MESH)
    pl.semaphore_signal(bar, inc=1, device_id={"stage": prv}, device_id_type=MESH)
    for k in range(1, nm):
        pl.semaphore_signal(bar, inc=1, device_id={"model": peer(k)}, device_id_type=MESH)
    pl.semaphore_wait(bar, 2 + nm - 1)

    def rowsl(start, size, mult):
        return pl.ds(pl.multiple_of(start, mult), size)

    plus, minus, far = 1, nm - 1, 2

    def w_rows(idx, who, half=None):
        size = (qrows, orows, fl, fl)[idx]
        if idx in (W_Q, W_U):
            buf = wqT if idx == W_Q else wuT
            if half is None:
                return buf.at[rowsl(who * size, size, size), :]
            return buf.at[rowsl(who * size + half * (size // 2), size // 2, size // 2), :]
        view = (woT if idx == W_O else wdT).at[:, rowsl(who * size, size, size)]
        return view if half is None else view.at[pl.ds(half * (dm_ // 2), dm_ // 2), :]

    def w_copy(idx, way):
        to = plus if way in (0, 2) else minus
        if way < 2:
            src = wqT_in if idx == W_Q else w_rows(idx, me)
            dst = w_rows(idx, me)
        else:
            src = dst = w_rows(idx, peer(minus if way == 2 else plus), way - 2)
        return pltpu.make_async_remote_copy(
            src_ref=src, dst_ref=dst, send_sem=ag_send.at[idx, way], recv_sem=ag_recv.at[idx, way],
            device_id={"model": peer(to)}, device_id_type=MESH)

    def w_arrival(idx, way):
        who = peer((minus, plus, far, far)[way])
        ref = w_rows(idx, who) if way < 2 else w_rows(idx, who, way - 2)
        return pltpu.make_async_remote_copy(
            src_ref=ref, dst_ref=ref, send_sem=ag_send.at[idx, way], recv_sem=ag_recv.at[idx, way],
            device_id={"model": peer(plus)}, device_id_type=MESH)

    def w_local(idx):
        src = (wqT_in, wo_in, wu_in, wd_in)[idx]
        dst = (w_rows(W_Q, me), wo.at[rowsl(me * orows, orows, orows), :], wu.at[:, rowsl(me * fl, fl, fl)], wd.at[rowsl(me * fl, fl, fl), :])[idx]
        return pltpu.make_async_copy(src, dst, ag_loc.at[idx])

    def w_own(idx):
        for way in range(2):
            w_copy(idx, way).start()

    def w_forward(idx):
        for way in range(2):
            w_arrival(idx, way).wait_recv()
        for way in range(2, 4):
            w_copy(idx, way).start()

    def w_wait(idx):
        for way in range(2, 4):
            w_arrival(idx, way).wait_recv()

    def x_copy(c):
        return pltpu.make_async_copy(x_hbm.at[me, pl.ds(c * tc, tc), :], xin.at[c], xsem.at[c])

    def t_copy(c):
        return pltpu.make_async_copy(t_hbm.at[me, pl.ds(c * tc, tc), :], xin.at[c], xsem.at[c])

    @pl.when(first)
    def _():
        for c in range(nc):
            x_copy(c).start()

    @pl.when(last)
    def _():
        for c in range(nc):
            t_copy(c).start()

    for idx in range(4):
        w_local(idx).start()

    odd = lax.rem(st, 2) == 1
    early = st < 2

    @pl.when(odd)
    def _():
        pl.semaphore_wait(go_sem, 1)

    w_own(W_Q)
    w_local(W_O).wait()
    woT[:, rowsl(me * orows, orows, orows)] = jnp.transpose(wo[rowsl(me * orows, orows, orows), :])
    w_own(W_O)
    w_local(W_U).wait()
    wuT[rowsl(me * fl, fl, fl), :] = jnp.transpose(wu[:, rowsl(me * fl, fl, fl)])
    w_own(W_U)
    w_local(W_D).wait()
    wdT[:, rowsl(me * fl, fl, fl)] = jnp.transpose(wd[rowsl(me * fl, fl, fl), :])
    w_own(W_D)
    w_local(W_Q).wait()
    w_forward(W_Q)
    w_forward(W_O)

    @pl.when(jnp.logical_not(odd))
    def _():
        pl.semaphore_signal(go_sem, inc=1, device_id={"stage": nxt}, device_id_type=MESH)

    def natural_weights():
        @pl.loop(0, nm)
        def _(f):
            wu[:, rowsl(f * fl, fl, fl)] = jnp.transpose(wuT[rowsl(f * fl, fl, fl), :])
            wd[rowsl(f * fl, fl, fl), :] = jnp.transpose(wdT[:, rowsl(f * fl, fl, fl)])
            wo[rowsl(f * orows, orows, orows), :] = jnp.transpose(woT[:, rowsl(f * orows, orows, orows)])
            wq[:, rowsl(f * qrows, qrows, qrows)] = jnp.transpose(wqT[rowsl(f * qrows, qrows, qrows), :])

    late = st >= max(2, ns // 2)

    @pl.when(jnp.logical_not(early))
    def _():
        w_forward(W_U)
        w_forward(W_D)
        for idx in range(4):
            w_wait(idx)

    @pl.when(late)
    def _():
        natural_weights()

    def f_copy(c):
        return pltpu.make_async_remote_copy(
            src_ref=ybuf.at[c], dst_ref=hbuf.at[c], send_sem=fsend.at[c], recv_sem=frecv.at[c],
            device_id={"stage": nxt}, device_id_type=MESH)

    def b_copy(c):
        return pltpu.make_async_remote_copy(
            src_ref=ybuf.at[c], dst_ref=dybuf.at[c], send_sem=bsend.at[c], recv_sem=brecv.at[c],
            device_id={"stage": prv}, device_id_type=MESH)

    def ring_copy(src, dst, send, recv, way):
        return pltpu.make_async_remote_copy(
            src_ref=src, dst_ref=dst, send_sem=send, recv_sem=recv,
            device_id={"model": peer((plus, minus)[way % 2])}, device_id_type=MESH)

    hf = fl // 2

    def z_copy(c, way):
        if way < 2:
            src, dst = zbuf.at[c, rowsl(peer((plus, minus)[way]) * fl, fl, fl), :], z_recv.at[way, c]
        elif way < 4:
            src, dst = zbuf.at[c, rowsl(peer(far) * fl + (way - 2) * hf, hf, hf), :], z_fwd.at[way - 2, c]
        else:
            src, dst = z_fwd.at[way - 4, c], z_recv.at[2, c, pl.ds((way - 4) * hf, hf)]
        return ring_copy(src, dst, z_send.at[way, c], z_arr.at[way, c], way)

    def z_forward(c):
        for way in (2, 3):
            z_copy(c, way).wait_recv()
        for way in (4, 5):
            z_copy(c, way).start()

    def dy_copy(c, way):
        if way < 2:
            src, dst = dybuf.at[c], dy_recv.at[way, c]
        else:
            rows = pl.ds((way - 2) * (dm_ // 2), dm_ // 2)
            src, dst = dy_recv.at[way - 2, c, rows], dy_recv.at[2, c, rows]
        return ring_copy(src, dst, dy_send.at[way, c], dy_arr.at[way, c], way)

    def dy_forward(c):
        for way in (0, 1):
            dy_copy(c, way).wait_recv()
        for way in (2, 3):
            dy_copy(c, way).start()

    lossv[...] = jnp.zeros_like(lossv)

    def head_rows(p, h, part):
        return pl.ds(p * (2 * 3 * hd) + (h * 3 + part) * hd, hd)

    def pad_head(val, h):
        zero = jnp.zeros_like(val)
        return jnp.concatenate([val, zero] if h == 0 else [zero, val], axis=0)

    def causal(shape, row0):
        return lax.broadcasted_iota(jnp.int32, shape, 0) + row0 <= lax.broadcasted_iota(jnp.int32, shape, 1)

    n_st = stage_buf.shape[0]

    def folded(slot, row, n):
        fold = stage_buf.shape[1]
        return stage_buf.at[slot, pl.ds(row % fold, n), pl.ds((row // fold) * tc, tc)]

    def slope(c):
        blk = fl // 4
        per = stage_buf.shape[1] // blk

        @pl.loop(0, 4 * nm)
        def _(f):
            half = f // per
            rows = pl.ds(pl.multiple_of((f - half * per) * blk, blk), blk)
            cols = pl.ds(pl.multiple_of(half * tc, tc), tc)
            u = ubuf[c, pl.ds(pl.multiple_of(f * blk, blk), blk), :].astype(F32)
            stage_buf[nc - 1 - c, rows, cols] = gelu_grad(u)

    def attention(cc):
        nk = (cc + 1) * tc
        slots = min(heads, 2 * nc * tc // nk)
        ahead = min(4, slots - 1)
        sub = tc // 2

        def front(head):
            p, h = head // 2, head % 2
            base = (head % slots) * nk
            qz = pad_head(qkv[cc, head_rows(p, h, 0), :], h)
            tops, sums = [], []
            for j in range(cc + 1):
                s = dot(kn[p, pl.ds(j * tc, tc), :], qz)
                for r in range(0, tc, sub):
                    part = s[r:r + sub]
                    if j == cc:
                        part = jnp.where(causal(part.shape, r), part, NEG)
                    top = jnp.max(part, axis=0, keepdims=True)
                    e = jnp.exp2((part - top) * exp_c)
                    folded(n_st - 1, base + j * tc + r, sub)[...] = e
                    tops.append(top)
                    sums.append(jnp.sum(e, axis=0, keepdims=True))
            mx = functools.reduce(jnp.maximum, tops)
            scales = [jnp.exp2((top - mx) * exp_c) for top in tops]
            inv = 1.0 / functools.reduce(jnp.add, [a * b for a, b in zip(scales, sums)])
            return [a * inv for a in scales]

        def back(head, factors):
            p, h = head // 2, head % 2
            base = (head % slots) * nk
            o_t = None
            for j in range(cc + 1):
                parts = []
                for i in range(2):
                    pr = (folded(n_st - 1, base + j * tc + i * sub, sub)[...] * factors[2 * j + i]).astype(BF16)
                    pbuf[cc * (cc + 1) // 2 + j, head, pl.ds(i * sub, sub), :] = pr
                    parts.append(pr)
                part = dot(qkv[j, head_rows(p, h, 2), :], jnp.concatenate(parts, axis=0))
                o_t = part if o_t is None else o_t + part
            obuf[cc, pl.ds(head * hd, hd), :] = o_t.astype(BF16)

        factors = {}
        for head in range(ahead):
            factors[head] = front(head)
        for head in range(heads):
            if head + ahead < heads:
                factors[head + ahead] = front(head + ahead)
            back(head, factors.pop(head))

    def attention_grad(cc):
        units = [(p, j) for p in range(heads // 2) for j in range(cc + 1)]
        dqs = {}
        held = {}

        def of_head(p, h):
            if (p, h) not in held:
                rows = pl.ds((p * 2 + h) * hd, hd)
                do_t = dobuf[rows, :]
                dsum = jnp.sum(do_t.astype(F32) * obuf[cc, rows, :].astype(F32), axis=0, keepdims=True)
                held[p, h] = (pad_head(do_t, h), dsum)
            return held[p, h]

        def front(p, j):
            out = []
            for h in range(2):
                do_z, dsum = of_head(p, h)
                pr = pbuf[cc * (cc + 1) // 2 + j, p * 2 + h]
                dp = dot(vn[p, pl.ds(j * tc, tc), :], do_z).astype(BF16).astype(F32)
                ds = (pr.astype(F32) * (dp - dsum)).astype(BF16)
                if j < cc:
                    dsbuf[p * 2 + h, pl.ds(j * tc, tc), :] = ds
                out.append(ds)
            return out

        def back(p, j, ds):
            for h in range(2):
                dq_h = dot(qkv[j, head_rows(p, h, 1), :], ds[h])
                dqs[p, h] = dq_h if j == 0 else dqs[p, h] + dq_h
            if j < cc:
                return
            dv_new, dk_new = kv_grad(cc, p, j, [of_head(p, h)[0] for h in range(2)], ds,
                                     [qkv[cc, head_rows(p, h, 0), :] for h in range(2)])
            dv_t = jnp.transpose(dv_new).astype(BF16)
            dk_t = (jnp.transpose(dk_new) * scale).astype(BF16)
            for h in range(2):
                qsave[pl.ds((p * 2 + h) * hd, hd), :] = qkv[cc, head_rows(p, h, 0), :]
                qkv[cc, head_rows(p, h, 0), :] = (dqs[p, h] * scale).astype(BF16)
                qkv[cc, head_rows(p, h, 1), :] = dk_t[h * hd:(h + 1) * hd, :]
                qkv[cc, head_rows(p, h, 2), :] = dv_t[h * hd:(h + 1) * hd, :]

        ds = front(*units[0])
        for n, unit in enumerate(units):
            later = front(*units[n + 1]) if n + 1 < len(units) else None
            back(*unit, ds)
            ds = later

    def kv_grad(cc, p, j, do_z, ds, q_t):
        dv_new = dk_new = None
        for h in range(2):
            dv_h = dot_t(pbuf[cc * (cc + 1) // 2 + j, p * 2 + h], do_z[h])
            dk_h = dot_t(ds[h], pad_head(q_t[h], h))
            dv_new = dv_h if dv_new is None else dv_new + dv_h
            dk_new = dk_h if dk_new is None else dk_new + dk_h
        rows = pl.ds(j * tc, tc)
        if cc < nc - 1:
            dv_new = dv_new + dvacc[p, rows, :]
            dk_new = dk_new + dkacc[p, rows, :]
        return dv_new, dk_new

    def earlier_keys(cc):
        for p in range(heads // 2):
            heads_of = [pl.ds((p * 2 + h) * hd, hd) for h in range(2)]
            do_z = [pad_head(dobuf[heads_of[h], :], h) for h in range(2)]
            q_t = [qsave[heads_of[h], :] for h in range(2)]
            for j in range(cc):
                rows = pl.ds(j * tc, tc)
                dv_new, dk_new = kv_grad(cc, p, j, do_z, [dsbuf[p * 2 + h, rows, :] for h in range(2)], q_t)
                dvacc[p, rows, :] = dv_new
                dkacc[p, rows, :] = dk_new

    def attention_step(c):
        @pl.when(first)
        def _():
            x_copy(c).wait()
            hbuf[c] = jnp.transpose(xin[c])

        @pl.when(jnp.logical_not(first))
        def _():
            f_copy(c).wait_recv()

        @pl.when(early & (c == 0))
        def _():
            w_wait(W_Q)

        h32 = hbuf[c].astype(F32)
        n1 = (h32 * inv_rms(h32)).astype(BF16)
        n1buf[c] = n1
        for r in range(nm):
            rows = pl.ds(r * qrows, qrows)
            blk = dot(wqT[rows, :], n1).astype(BF16)
            qkv[c, rows, :] = blk
            for part, ref in ((1, kn), (2, vn)):
                both = jnp.concatenate([blk[(3 * h + part) * hd:(3 * h + part + 1) * hd] for h in range(2)], axis=0)
                ref[r, pl.ds(pl.multiple_of(c * tc, tc), tc), :] = jnp.transpose(both)

        for cc in range(nc):
            pl.when(c == cc)(functools.partial(attention, cc))

    def mlp_step(c):
        a = dot(woT[...], obuf[c]).astype(BF16)
        m32 = (hbuf[c].astype(F32) + a.astype(F32)).astype(BF16).astype(F32)
        mbuf[c] = m32.astype(BF16)
        n2 = (m32 * inv_rms(m32)).astype(BF16)
        n2buf[c] = n2

        blk = fl // 2
        for f in range(2 * nm):
            rows = pl.ds(f * blk, blk)
            u = dot(wuT[rows, :], n2buf[c]).astype(BF16)
            ubuf[c, rows, :] = u
            zbuf[c, rows, :] = gelu(u.astype(F32)).astype(BF16)
        acc = dot(wdT[...], zbuf[c])
        y32 = (mbuf[c].astype(F32) + acc.astype(BF16).astype(F32)).astype(BF16)
        ybuf[c] = y32

        @pl.when(jnp.logical_not(last))
        def _():
            f_copy(c).start()

        @pl.when(last)
        def _():
            t_copy(c).wait()
            err = ybuf[c].astype(F32) - jnp.transpose(xin[c]).astype(F32)
            lossv[...] += jnp.sum((err * err).reshape(dm_ // 8, 8, tc), axis=0)
            dybuf[c] = (err * inv_d).astype(BF16)


    @pl.loop(0, 2 * nc)
    def _(n):
        attn_turn = jnp.where(early, jnp.where(n < nc, 1, 0), 1 - lax.rem(n, 2))
        c = jnp.where(early, lax.rem(n, nc), n // 2)

        @pl.when(early & (n == 1))
        def _():
            w_forward(W_U)

        @pl.when(early & (n == 2))
        def _():
            w_forward(W_D)

        @pl.when(attn_turn == 1)
        def _():
            attention_step(c)

        @pl.when(early & (n == nc))
        def _():
            w_wait(W_O)
            w_wait(W_U)
            w_wait(W_D)

        @pl.when(attn_turn == 0)
        def _():
            mlp_step(c)

    def z_start():
        for c in range(nc):
            for way in range(4):
                z_copy(c, way).start()

    @pl.when(jnp.logical_not(late))
    def _():
        for c in range(nc):
            f_copy(c).wait_send()
        z_start()
        natural_weights()

    @pl.when(jnp.logical_not(last))
    def _():
        @pl.loop(0, nc)
        def _(c):
            slope(c)

    @pl.when(jnp.logical_not(late))
    def _():
        @pl.loop(0, nc)
        def _(c):
            z_forward(c)

    def l_copy(k):
        return pltpu.make_async_remote_copy(
            src_ref=losst.at[nm], dst_ref=losst.at[3 - k if nm == 4 else nm - 1 - k], send_sem=lsend.at[k - 1],
            recv_sem=lrecv.at[k - 1], device_id={"model": peer(k)}, device_id_type=MESH)

    def lf_copy():
        return pltpu.make_async_remote_copy(
            src_ref=losst.at[nm + 1], dst_ref=losst.at[nm + 1], send_sem=lfsend, recv_sem=lfrecv,
            device_id={"stage": prv}, device_id_type=MESH)

    @pl.when(last)
    def _():
        tot = jnp.sum(lossv[...]) * (0.5 * inv_d)
        losst[nm] = jnp.full(losst.shape[1:], tot, F32)
        for k in range(1, nm):
            l_copy(k).start()

    dy_inside = jnp.logical_not(late) & (first | odd)

    @pl.loop(0, nc)
    def _(i):
        c = nc - 1 - i

        @pl.when(jnp.logical_not(last))
        def _():
            b_copy(c).wait_recv()

        @pl.when(jnp.logical_not(late) & (i == 0))
        def _():
            for way in range(2):
                dy_copy(c, way).start()

        @pl.when(last)
        def _():
            slope(c)

        blk = fl // 4
        for f in range(4 * nm):
            rows = pl.ds(f * blk, blk)
            dz = dot(wd[rows, :], dybuf[c]).astype(BF16).astype(F32)
            ubuf[c, rows, :] = (dz * folded(i, f * blk, blk)[...]).astype(BF16)
        acc = dot(wu[...], ubuf[c])
        dn2 = acc.astype(BF16).astype(F32)
        m32 = mbuf[c].astype(F32)
        pull = norm_pull(m32, inv_rms(m32), dn2).astype(BF16)
        dmid = (dybuf[c].astype(F32) + pull.astype(F32)).astype(BF16)
        mbuf[c] = dmid
        dobuf[...] = dot(wo[...], dmid).astype(BF16)

        @pl.when(jnp.logical_not(late) & (i > 0))
        def _():
            for way in range(2):
                dy_copy(c, way).start()

        @pl.when(dy_inside & (i > 0))
        def _():
            dy_forward(c + 1)

        for cc in range(nc):
            pl.when(c == cc)(functools.partial(attention_grad, cc))

        dn1 = dot(wq[...], qkv[c]).astype(BF16).astype(F32)
        h32 = hbuf[c].astype(F32)
        pull1 = norm_pull(h32, inv_rms(h32), dn1).astype(BF16)

        @pl.when(late & jnp.logical_not(last))
        def _():
            f_copy(c).wait_send()

        ybuf[c] = (mbuf[c].astype(F32) + pull1.astype(F32)).astype(BF16)

        @pl.when(jnp.logical_not(first))
        def _():
            b_copy(c).start()

        for cc in range(1, nc):
            pl.when(c == cc)(functools.partial(earlier_keys, cc))

    @pl.when(last)
    def _():
        for k in range(1, nm):
            l_copy(k).wait_recv()
        vals = [losst[nm]] + [losst[k - 1] for k in range(1, nm)]
        tot = jnp.zeros_like(vals[0])
        for who in range(nm):
            pick = vals[0]
            for k in range(1, nm):
                pick = jnp.where(peer(k) == who, vals[k], pick)
            tot = tot + pick
        losst[nm + 1] = tot

    @pl.when(jnp.logical_not(last))
    def _():
        lf_copy().wait_recv()

    @pl.when(jnp.logical_not(first))
    def _():
        lf_copy().start()

    loss_out[...] = losst[nm + 1]

    def wgrad(mat, d):
        acc = None
        for c in range(nc):
            if mat == 0:
                part = dot_t(qkv[c, rowsl(d * qrows, qrows, qrows), :], n1buf[c])
            elif mat == 1:
                part = dot_t(obuf[c, rowsl(d * orows, orows, orows), :], mbuf[c])
            elif mat == 2:
                part = dot_t(n2buf[c], ubuf[c, rowsl(d * fl, fl, fl), :])
            else:
                part = dot_t(zbuf[c, rowsl(d * fl, fl, fl), :], dybuf[c])
            acc = part if acc is None else acc + part
        return acc

    sizes = (qrows, orows, dm_)
    offs = (0, qrows, qrows + orows)

    def rows_of(mat):
        return pl.ds(offs[mat], sizes[mat])

    def half_of(mat, half):
        return pl.ds(offs[mat] + half * (sizes[mat] // 2), sizes[mat] // 2)

    def far_copy(mat, half):
        rows = pl.ds(offs[mat] // 2, sizes[mat] // 2)
        return ring_copy(stage_buf.at[0, half_of(mat, half)], (far_p, far_m)[half].at[rows],
                         rs_send.at[mat, half], rs_recv.at[mat, half], half)

    def near_copy(mat, side, half):
        way = 2 + 2 * side + half
        return ring_copy(stage_buf.at[1 + side, half_of(mat, half)], (near_l if side == half else near_e).at[half_of(mat, half)],
                         rs_send.at[mat, way], rs_recv.at[mat, way], side)

    mats = (2, 0, 1)

    @pl.loop(0, 3)
    def _(slot):
        who = lax.rem(me + jnp.where(slot == 0, far, jnp.where(slot == 1, plus, minus)), nm)
        for mat in mats:
            stage_buf[slot, rows_of(mat)] = wgrad(mat, who)

            @pl.when(slot == 0)
            def _():
                for half in range(2):
                    far_copy(mat, half).start()

            for side in range(2):
                @pl.when(slot == 1 + side)
                def _():
                    near_copy(mat, side, 1 - side).start()

    @pl.when(dy_inside)
    def _():
        dy_forward(0)

    @pl.when(jnp.logical_not(late | dy_inside))
    def _():
        for c in reversed(range(nc)):
            dy_forward(c)

    hd2 = dm_ // 2

    def gd_cols(half):
        return pl.ds(half * hd2, hd2) if isinstance(half, int) else pl.ds(pl.multiple_of(half * hd2, hd2), hd2)

    def gd_half(d, half):
        return functools.reduce(jnp.add, [
            dot_t(zbuf[c, rowsl(d * fl, fl, fl), :], dybuf[c, gd_cols(half), :]) for c in range(nc)])

    def gd_far_copy(half):
        return ring_copy(gdacc.at[:, gd_cols(half)], gd_far.at[half], gd_send.at[half], gd_recv.at[half], half)

    def gd_slot(side, half):
        return folded(n_st - 1, (2 * side + half) * fl, fl)

    def gd_near_copy(side, half):
        way = 2 + 2 * side + half
        return ring_copy(gd_slot(side, half), gd_near.at[1 if side == half else 0, half],
                         gd_send.at[way], gd_recv.at[way], side)

    @pl.when(late)
    def _():
        @pl.loop(0, 2)
        def _(half):
            gdacc[:, gd_cols(half)] = gd_half(peer(far), half)

        for half in range(2):
            gd_far_copy(half).start()

        @pl.loop(0, 4)
        def _(n):
            rows, cols = lax.rem(n, 2) * fl, (n // 2) * tc
            stage_buf[n_st - 1, pl.ds(pl.multiple_of(rows, fl), fl), pl.ds(pl.multiple_of(cols, tc), tc)] = gd_half(
                lax.rem(me + 1 + 2 * (n // 2), nm), lax.rem(n, 2))

        for side in range(2):
            gd_near_copy(side, 1 - side).start()

    def gd_add(src, ref):
        nr = min(fl, radd.shape[0])
        for r in range(0, fl, nr):
            copy = pltpu.make_async_copy(src.at[pl.ds(r, nr)], radd.at[pl.ds(0, nr), pl.ds(0, hd2)], ld_sem.at[0])
            copy.start()
            copy.wait()
            ref[pl.ds(r, nr), :] += radd[pl.ds(0, nr), pl.ds(0, hd2)]

    pieces = [(mat, half) for mat in mats for half in range(2)]
    cols = dvacc.shape[2]
    n_cols = dm_ // cols

    def piece_loads(n, kind):
        mat, half = pieces[n]
        nr = sizes[mat] // 2
        r0 = sum(sizes[m] // 2 for m, _ in pieces[:n])
        src = near_e.at[half_of(mat, half)] if kind else (far_p, far_m)[half].at[pl.ds(offs[mat] // 2, nr)]
        dst = dkacc if kind else dvacc
        return [pltpu.make_async_copy(src.at[:, pl.ds(k * cols, cols)], dst.at[k, pl.ds(r0, nr), :], pl_sem.at[kind, n])
                for k in range(n_cols)], dst, r0, nr

    def piece_start(n, kind):
        mat, half = pieces[n]
        if kind:
            near_copy(mat, 1 - half, half).wait_recv()
        else:
            far_copy(mat, half).wait_recv()
        for copy in piece_loads(n, kind)[0]:
            copy.start()

    def piece_add(n, kind, slot):
        mat, half = pieces[n]
        copies, src, r0, nr = piece_loads(n, kind)
        for copy in copies:
            copy.wait()
        rows = half_of(mat, half)
        for k in range(n_cols):
            stage_buf[slot, rows, pl.ds(k * cols, cols)] += src[k, pl.ds(r0, nr), :]

    piece_start(0, 0)
    for n, (mat, half) in enumerate(pieces):
        if n + 1 < len(pieces):
            piece_start(n + 1, 0)
        piece_add(n, 0, 1 + half)
        near_copy(mat, half, half).start()

    @pl.when(late)
    def _():
        for half in range(2):
            gd_far_copy(half).wait_recv()
            gd_add(gd_far.at[half], gd_slot(half, half))
            gd_near_copy(half, half).start()
            gd_far_copy(half).wait_send()

    for mat in mats:
        for half in range(2):
            far_copy(mat, half).wait_send()
        stage_buf[0, rows_of(mat)] = wgrad(mat, me)

    def zdy_load(n, buf):
        slot, c = n // nc, lax.rem(n, nc)
        return (pltpu.make_async_copy(z_recv.at[slot, c], dsbuf.at[2 * buf, pl.ds(0, fl)], ld_sem.at[1 + buf]),
                pltpu.make_async_copy(dy_recv.at[slot, c], dsbuf.at[2 * buf + 1, pl.ds(0, dm_)], ld_sem.at[3 + buf]))

    gdacc[...] = wgrad(3, me)

    @pl.when(jnp.logical_not(late))
    def _():
        for c in range(nc):
            for way in (0, 1, 4, 5):
                z_copy(c, way).wait_recv()
            for way in (2, 3):
                dy_copy(c, way).wait_recv()
        for cp in zdy_load(0, 0):
            cp.start()

        @pl.loop(0, 3 * nc)
        def _(n):
            buf = lax.rem(n, 2)

            @pl.when(n + 1 < 3 * nc)
            def _():
                for cp in zdy_load(n + 1, 1 - buf):
                    cp.start()

            for cp in zdy_load(n, buf):
                cp.wait()
            gdacc[...] += dot_t(dsbuf[2 * buf, pl.ds(0, fl), :], dsbuf[2 * buf + 1, pl.ds(0, dm_), :])

    def gd_arrivals(last_half):
        for half in range(2):
            side = half if last_half else 1 - half
            gd_near_copy(side, half).wait_recv()
            gd_add(gd_near.at[last_half, half], gdacc.at[:, gd_cols(half)])

    def out_copy(mat):
        if mat == 3:
            return pltpu.make_async_copy(gdacc, sum_out.at[pl.ds(qrows + orows + dm_, fl)], out_sem.at[3])
        return pltpu.make_async_copy(stage_buf.at[0, rows_of(mat)], sum_out.at[rows_of(mat)], out_sem.at[mat])

    piece_start(0, 1)
    for n, (mat, half) in enumerate(pieces):
        if n + 1 < len(pieces):
            piece_start(n + 1, 1)
        piece_add(n, 1, 0)
        if half:
            out_copy(mat).start()

    @pl.when(late)
    def _():
        gd_arrivals(0)
        gd_arrivals(1)

    out_copy(3).start()
    for mat in mats:
        for side in range(2):
            near_copy(mat, side, side).wait_recv()

    for mat in range(4):
        out_copy(mat).wait()

    @pl.when(jnp.logical_not(late))
    def _():
        for c in range(nc):
            for way in range(6):
                z_copy(c, way).wait_send()
            for way in range(4):
                dy_copy(c, way).wait_send()

    @pl.when(late)
    def _():
        for side in range(2):
            for half in range(2):
                gd_near_copy(side, half).wait_send()

    for idx in range(4):
        for way in range(4):
            w_copy(idx, way).wait_send()
    for mat in mats:
        for half in range(2):
            for side in range(2):
                near_copy(mat, side, half).wait_send()

    @pl.when(jnp.logical_not(first))
    def _():
        for c in range(nc):
            b_copy(c).wait_send()
        lf_copy().wait_send()

    @pl.when(last)
    def _():
        for k in range(1, nm):
            l_copy(k).wait_send()


def finish_kernel(sq, so, su, sd, lq, lo, lu, loss, gq, go, gu, gd, loss_out):
    gq[...] = sq[...] + lq[...]
    go[...] = so[...] + lo[...]
    gu[...] = su[...] + lu[...]
    gd[...] = sd[...]
    loss_out[0] = loss[0, 0]


def solution(mesh):
    ns = mesh.shape["stage"]
    nm = mesh.shape["model"]

    def per_device(tokens_in, targets, w_qkv, w_out, w_up, w_down):
        n_micro, seq_len, d_model = tokens_in.shape
        hl, hd, fl = w_qkv.shape[3], w_qkv.shape[5], w_up.shape[3]
        tc = min(CHUNK, seq_len // 2)
        nc = seq_len // tc
        qrows, orows = hl * 3 * hd, hl * hd
        assert n_micro == nm == 4 and w_qkv.shape[1] == 1 and hl == 2 and d_model == 2 * tc and qrows + orows + d_model == seq_len == 2 * fl and nc == 4
        wqT = jnp.transpose(w_qkv[0, 0], (1, 2, 3, 0)).reshape(qrows, d_model)
        wo = w_out[0, 0].reshape(orows, d_model)
        wu, wd = w_up[0, 0], w_down[0, 0]
        cfg = (ns, nm, nc, tc, d_model, hl, hd, fl)
        heads = nm * hl
        any_spec = pl.BlockSpec(memory_space=pl.ANY)
        f32 = lambda *shape: jax.ShapeDtypeStruct(shape, F32)
        rsum = qrows + orows + d_model
        seqb = nc * tc
        b16 = lambda *shape: jax.ShapeDtypeStruct(shape, BF16)
        out_shape = (f32(rsum + fl, d_model), f32(8, 128), f32(rsum // 2, d_model), f32(rsum // 2, d_model), f32(rsum, d_model),
                     f32(rsum, d_model), b16(3, nc, fl, tc), b16(2, nc, fl // 2, tc), b16(3, nc, d_model, tc),
                     f32(2, fl, d_model // 2), f32(2, 2, fl, d_model // 2))
        vb = lambda *shape: pltpu.VMEM(shape, BF16)
        vf = lambda *shape: pltpu.VMEM(shape, F32)
        dma = lambda *shape: pltpu.SemaphoreType.DMA(shape)
        scratch = [
            vb(nm * qrows, d_model), vb(d_model, nm * orows), vb(nm * fl, d_model), vb(d_model, nm * fl),
            vb(nm * fl, d_model), vb(d_model, nm * fl), vb(nm * orows, d_model), vb(d_model, nm * qrows),
            vb(nc, tc, d_model), vb(nc, d_model, tc), vb(nc, d_model, tc), vb(nc, nm * qrows, tc), vb(nm, seqb, orows), vb(nm, seqb, orows),
            vb(nc, nm * orows, tc), vb(nc, d_model, tc), vb(nc, d_model, tc), vb(nc, nm * fl, tc), vb(nc, nm * fl, tc),
            vb(nc * (nc + 1) // 2, heads, tc, tc), vb(nc, d_model, tc), vf(heads // 2, seqb, 2 * hd), vf(heads // 2, seqb, 2 * hd),
            vb(nc, d_model, tc), vb(nm * orows, tc), vf(nm + 2, 8, 128), vf(8, tc),
            vf(4, rsum, d_model), vf(256, d_model), vf(fl, d_model), vb(heads, max((nc - 1) * tc, fl), tc), vb(nm * orows, tc),
            dma(4, 4), dma(4, 4), dma(4), pltpu.SemaphoreType.REGULAR, dma(nc), dma(nc), dma(nc), dma(nc), dma(nc),
            dma(nm - 1), dma(nm - 1), pltpu.SemaphoreType.DMA, pltpu.SemaphoreType.DMA,
            dma(3, 6), dma(3, 6), dma(5), dma(4), dma(6, nc), dma(6, nc), dma(4, nc), dma(4, nc), dma(6), dma(6), dma(2, 6),
        ]
        res = pl.pallas_call(
            functools.partial(step_kernel, cfg),
            out_shape=out_shape,
            in_specs=[any_spec] * 6,
            out_specs=[any_spec, pl.BlockSpec(memory_space=pltpu.VMEM)] + [any_spec] * 9,
            scratch_shapes=scratch,
            compiler_params=pltpu.CompilerParams(collective_id=0, has_side_effects=True, vmem_limit_bytes=67043328),
            name="train_step",
        )(tokens_in, targets, wqT, wo, wu, wd)
        part, loss, late = res[0], res[1], res[5]
        steps = 2

        def spec(size, start):
            rows = size // steps
            return pl.BlockSpec((rows, d_model), lambda i: (start // rows + i, 0))

        q_s, o_s, u_s = spec(qrows, 0), spec(orows, qrows), spec(d_model, qrows + orows)
        g_qkv, g_out, g_up, g_down, loss = pl.pallas_call(
            finish_kernel,
            grid=(steps,),
            out_shape=(f32(qrows, d_model), f32(orows, d_model), f32(d_model, fl), f32(fl, d_model), f32(1)),
            in_specs=[q_s, o_s, u_s, spec(fl, rsum), q_s, o_s, u_s, pl.BlockSpec(memory_space=pltpu.SMEM)],
            out_specs=[spec(qrows, 0), spec(orows, 0), spec(d_model, 0), spec(fl, 0), pl.BlockSpec(memory_space=pltpu.SMEM)],
            name="finish",
        )(part, part, part, part, late, late, late, loss)
        g_qkv = jnp.transpose(g_qkv.reshape(hl, 3, hd, d_model), (3, 0, 1, 2))[None, None]
        return g_qkv, g_out.reshape(1, 1, hl, hd, d_model), g_up[None, None], g_down[None, None], loss

    tok_spec = P(None, "data", None)
    qkv_spec = P("stage", None, None, "model", None, None)
    out_spec = P("stage", None, "model", None, None)
    up_spec = P("stage", None, None, "model")
    down_spec = P("stage", None, "model", None)
    g_qkv_spec = P(("data", "stage"), None, None, "model", None, None)
    g_out_spec = P(("data", "stage"), None, "model", None, None)
    g_up_spec = P(("data", "stage"), None, None, "model")
    g_down_spec = P(("data", "stage"), None, "model", None)
    return jax.shard_map(per_device, mesh=mesh, in_specs=(tok_spec, tok_spec, qkv_spec, out_spec, up_spec, down_spec), out_specs=(g_qkv_spec, g_out_spec, g_up_spec, g_down_spec, P("data")), check_vma=False)
```

```python
import functools
import math

import jax
import jax.numpy as jnp
from jax import lax
from jax.experimental import pallas as pl
from jax.experimental.pallas import tpu as pltpu
from jax.sharding import PartitionSpec as P

F32 = jnp.float32
BF16 = jnp.bfloat16
MESH = pl.DeviceIdType.MESH
CHUNK = 256
NEG = -1e30
GELU_C = math.sqrt(2.0 / math.pi)
GELU_A = 0.044715

W_Q, W_O, W_U, W_D = range(4)


def dot(lhs, rhs):
    return jnp.dot(lhs, rhs, preferred_element_type=F32)


def dot_t(lhs, rhs):
    return lax.dot_general(lhs, rhs, (((1,), (1,)), ((), ())), preferred_element_type=F32)


def inv_rms(x32):
    return lax.rsqrt(jnp.mean(x32 * x32, axis=0, keepdims=True) + 1e-6)


def norm_pull(x32, inv, g32):
    mean_gx = jnp.mean(g32 * x32, axis=0, keepdims=True)
    return g32 * inv - x32 * (inv * inv * inv * mean_gx)


def gelu(u):
    tanh = jnp.tanh(u * (GELU_C + (GELU_C * GELU_A) * (u * u)))
    half = 0.5 * u
    return half + half * tanh


def gelu_grad(u):
    u2 = u * u
    sig = 0.5 + 0.5 * jnp.tanh(u * (GELU_C + (GELU_C * GELU_A) * u2))
    slope = u * (2.0 * GELU_C + (6.0 * GELU_C * GELU_A) * u2)
    return sig * (1.0 + slope * (1.0 - sig))


def step_kernel(cfg, x_hbm, t_hbm, wqT_in, wo_in, wu_in, wd_in,
                sum_out, loss_out, far_p, far_m, near_e, near_l, z_recv, z_fwd, dy_recv, gd_far, gd_near,
                wqT, woT, wuT, wdT, wd, wu, wo, wq,
                xin, hbuf, n1buf, qkv, kn, vn, obuf, mbuf, n2buf, ubuf, zbuf, pbuf, dybuf, dvacc, dkacc,
                ybuf, dobuf, losst, lossv, stage_buf, radd, gdacc, dsbuf, qsave,
                ag_send, ag_recv, ag_loc, go_sem, xsem, fsend, frecv, bsend, brecv, lsend, lrecv, lfsend, lfrecv,
                rs_send, rs_recv, ld_sem, out_sem, z_send, z_arr, dy_send, dy_arr, gd_send, gd_recv, pl_sem):
    ns, nm, nc, tc, dm_, hl, hd, fl = cfg
    heads = nm * hl
    qrows = hl * 3 * hd
    orows = hl * hd
    inv_d = 1.0 / (nm * nc * tc * dm_)
    scale = hd ** -0.5
    exp_c = scale * math.log2(math.e)
    me = lax.axis_index("model")
    st = lax.axis_index("stage")
    nxt = lax.rem(st + 1, ns)
    prv = lax.rem(st + ns - 1, ns)
    first = st == 0
    last = st == ns - 1

    def peer(k):
        return lax.rem(me + k, nm)

    bar = pltpu.get_barrier_semaphore()
    pl.semaphore_signal(bar, inc=1, device_id={"stage": nxt}, device_id_type=MESH)
    pl.semaphore_signal(bar, inc=1, device_id={"stage": prv}, device_id_type=MESH)
    for k in range(1, nm):
        pl.semaphore_signal(bar, inc=1, device_id={"model": peer(k)}, device_id_type=MESH)
    pl.semaphore_wait(bar, 2 + nm - 1)

    def rowsl(start, size, mult):
        return pl.ds(pl.multiple_of(start, mult), size)

    plus, minus, far = 1, nm - 1, 2

    def w_rows(idx, who, half=None):
        size = (qrows, orows, fl, fl)[idx]
        if idx in (W_Q, W_U):
            buf = wqT if idx == W_Q else wuT
            if half is None:
                return buf.at[rowsl(who * size, size, size), :]
            return buf.at[rowsl(who * size + half * (size // 2), size // 2, size // 2), :]
        view = (woT if idx == W_O else wdT).at[:, rowsl(who * size, size, size)]
        return view if half is None else view.at[pl.ds(half * (dm_ // 2), dm_ // 2), :]

    def w_copy(idx, way):
        to = plus if way in (0, 2) else minus
        if way < 2:
            src = wqT_in if idx == W_Q else w_rows(idx, me)
            dst = w_rows(idx, me)
        else:
            src = dst = w_rows(idx, peer(minus if way == 2 else plus), way - 2)
        return pltpu.make_async_remote_copy(
            src_ref=src, dst_ref=dst, send_sem=ag_send.at[idx, way], recv_sem=ag_recv.at[idx, way],
            device_id={"model": peer(to)}, device_id_type=MESH)

    def w_arrival(idx, way):
        who = peer((minus, plus, far, far)[way])
        ref = w_rows(idx, who) if way < 2 else w_rows(idx, who, way - 2)
        return pltpu.make_async_remote_copy(
            src_ref=ref, dst_ref=ref, send_sem=ag_send.at[idx, way], recv_sem=ag_recv.at[idx, way],
            device_id={"model": peer(plus)}, device_id_type=MESH)

    def w_local(idx):
        src = (wqT_in, wo_in, wu_in, wd_in)[idx]
        dst = (w_rows(W_Q, me), wo.at[rowsl(me * orows, orows, orows), :], wu.at[:, rowsl(me * fl, fl, fl)], wd.at[rowsl(me * fl, fl, fl), :])[idx]
        return pltpu.make_async_copy(src, dst, ag_loc.at[idx])

    def w_own(idx):
        for way in range(2):
            w_copy(idx, way).start()

    def w_forward(idx):
        for way in range(2):
            w_arrival(idx, way).wait_recv()
        for way in range(2, 4):
            w_copy(idx, way).start()

    def w_wait(idx):
        for way in range(2, 4):
            w_arrival(idx, way).wait_recv()

    def x_copy(c):
        return pltpu.make_async_copy(x_hbm.at[me, pl.ds(c * tc, tc), :], xin.at[c], xsem.at[c])

    def t_copy(c):
        return pltpu.make_async_copy(t_hbm.at[me, pl.ds(c * tc, tc), :], xin.at[c], xsem.at[c])

    @pl.when(first)
    def _():
        for c in range(nc):
            x_copy(c).start()

    @pl.when(last)
    def _():
        for c in range(nc):
            t_copy(c).start()

    for idx in range(4):
        w_local(idx).start()

    odd = lax.rem(st, 2) == 1
    early = st < 2

    @pl.when(odd)
    def _():
        pl.semaphore_wait(go_sem, 1)

    w_own(W_Q)
    w_local(W_O).wait()
    woT[:, rowsl(me * orows, orows, orows)] = jnp.transpose(wo[rowsl(me * orows, orows, orows), :])
    w_own(W_O)
    w_local(W_U).wait()
    wuT[rowsl(me * fl, fl, fl), :] = jnp.transpose(wu[:, rowsl(me * fl, fl, fl)])
    w_own(W_U)
    w_local(W_D).wait()
    wdT[:, rowsl(me * fl, fl, fl)] = jnp.transpose(wd[rowsl(me * fl, fl, fl), :])
    w_own(W_D)

    @pl.when(jnp.logical_not(odd))
    def _():
        pl.semaphore_signal(go_sem, inc=1, device_id={"stage": nxt}, device_id_type=MESH)

    w_local(W_Q).wait()
    w_forward(W_Q)
    w_forward(W_O)

    def natural_weights():
        @pl.loop(0, nm)
        def _(f):
            wu[:, rowsl(f * fl, fl, fl)] = jnp.transpose(wuT[rowsl(f * fl, fl, fl), :])
            wd[rowsl(f * fl, fl, fl), :] = jnp.transpose(wdT[:, rowsl(f * fl, fl, fl)])
            wo[rowsl(f * orows, orows, orows), :] = jnp.transpose(woT[:, rowsl(f * orows, orows, orows)])
            wq[:, rowsl(f * qrows, qrows, qrows)] = jnp.transpose(wqT[rowsl(f * qrows, qrows, qrows), :])

    late = st >= max(2, ns // 2)

    @pl.when(jnp.logical_not(early))
    def _():
        w_forward(W_U)
        w_forward(W_D)
        for idx in range(4):
            w_wait(idx)

    @pl.when(late)
    def _():
        natural_weights()

    def f_copy(c):
        return pltpu.make_async_remote_copy(
            src_ref=ybuf.at[c], dst_ref=hbuf.at[c], send_sem=fsend.at[c], recv_sem=frecv.at[c],
            device_id={"stage": nxt}, device_id_type=MESH)

    def b_copy(c):
        return pltpu.make_async_remote_copy(
            src_ref=ybuf.at[c], dst_ref=dybuf.at[c], send_sem=bsend.at[c], recv_sem=brecv.at[c],
            device_id={"stage": prv}, device_id_type=MESH)

    def ring_copy(src, dst, send, recv, way):
        return pltpu.make_async_remote_copy(
            src_ref=src, dst_ref=dst, send_sem=send, recv_sem=recv,
            device_id={"model": peer((plus, minus)[way % 2])}, device_id_type=MESH)

    hf = fl // 2

    def z_copy(c, way):
        if way < 2:
            src, dst = zbuf.at[c, rowsl(peer((plus, minus)[way]) * fl, fl, fl), :], z_recv.at[way, c]
        elif way < 4:
            src, dst = zbuf.at[c, rowsl(peer(far) * fl + (way - 2) * hf, hf, hf), :], z_fwd.at[way - 2, c]
        else:
            src, dst = z_fwd.at[way - 4, c], z_recv.at[2, c, pl.ds((way - 4) * hf, hf)]
        return ring_copy(src, dst, z_send.at[way, c], z_arr.at[way, c], way)

    def z_forward(c):
        for way in (2, 3):
            z_copy(c, way).wait_recv()
        for way in (4, 5):
            z_copy(c, way).start()

    def dy_copy(c, way):
        if way < 2:
            src, dst = dybuf.at[c], dy_recv.at[way, c]
        else:
            rows = pl.ds((way - 2) * (dm_ // 2), dm_ // 2)
            src, dst = dy_recv.at[way - 2, c, rows], dy_recv.at[2, c, rows]
        return ring_copy(src, dst, dy_send.at[way, c], dy_arr.at[way, c], way)

    def dy_forward(c):
        for way in (0, 1):
            dy_copy(c, way).wait_recv()
        for way in (2, 3):
            dy_copy(c, way).start()

    lossv[...] = jnp.zeros_like(lossv)

    def head_rows(p, h, part):
        return pl.ds(p * (2 * 3 * hd) + (h * 3 + part) * hd, hd)

    def pad_head(val, h):
        zero = jnp.zeros_like(val)
        return jnp.concatenate([val, zero] if h == 0 else [zero, val], axis=0)

    def causal(shape, row0):
        return lax.broadcasted_iota(jnp.int32, shape, 0) + row0 <= lax.broadcasted_iota(jnp.int32, shape, 1)

    n_st = stage_buf.shape[0]

    def folded(slot, row, n):
        fold = stage_buf.shape[1]
        return stage_buf.at[slot, pl.ds(row % fold, n), pl.ds((row // fold) * tc, tc)]

    def slope(c):
        blk = fl // 4
        per = stage_buf.shape[1] // blk

        @pl.loop(0, 4 * nm)
        def _(f):
            half = f // per
            rows = pl.ds(pl.multiple_of((f - half * per) * blk, blk), blk)
            cols = pl.ds(pl.multiple_of(half * tc, tc), tc)
            u = ubuf[c, pl.ds(pl.multiple_of(f * blk, blk), blk), :].astype(F32)
            stage_buf[nc - 1 - c, rows, cols] = gelu_grad(u)

    def attention(cc):
        nk = (cc + 1) * tc
        slots = min(heads, 2 * nc * tc // nk)
        ahead = min(4, slots - 1)
        sub = tc // 2

        def front(head):
            p, h = head // 2, head % 2
            base = (head % slots) * nk
            qz = pad_head(qkv[cc, head_rows(p, h, 0), :], h)
            tops, sums = [], []
            for j in range(cc + 1):
                s = dot(kn[p, pl.ds(j * tc, tc), :], qz)
                for r in range(0, tc, sub):
                    part = s[r:r + sub]
                    if j == cc:
                        part = jnp.where(causal(part.shape, r), part, NEG)
                    top = jnp.max(part, axis=0, keepdims=True)
                    e = jnp.exp2((part - top) * exp_c)
                    folded(n_st - 1, base + j * tc + r, sub)[...] = e
                    tops.append(top)
                    sums.append(jnp.sum(e, axis=0, keepdims=True))
            mx = functools.reduce(jnp.maximum, tops)
            scales = [jnp.exp2((top - mx) * exp_c) for top in tops]
            inv = 1.0 / functools.reduce(jnp.add, [a * b for a, b in zip(scales, sums)])
            return [a * inv for a in scales]

        def back(head, factors):
            p, h = head // 2, head % 2
            base = (head % slots) * nk
            o_t = None
            for j in range(cc + 1):
                parts = []
                for i in range(2):
                    pr = (folded(n_st - 1, base + j * tc + i * sub, sub)[...] * factors[2 * j + i]).astype(BF16)
                    pbuf[cc * (cc + 1) // 2 + j, head, pl.ds(i * sub, sub), :] = pr
                    parts.append(pr)
                part = dot(qkv[j, head_rows(p, h, 2), :], jnp.concatenate(parts, axis=0))
                o_t = part if o_t is None else o_t + part
            obuf[cc, pl.ds(head * hd, hd), :] = o_t.astype(BF16)

        factors = {}
        for head in range(ahead):
            factors[head] = front(head)
        for head in range(heads):
            if head + ahead < heads:
                factors[head + ahead] = front(head + ahead)
            back(head, factors.pop(head))

    def attention_grad(cc):
        units = [(p, j) for p in range(heads // 2) for j in range(cc + 1)]
        dqs = {}
        held = {}

        def of_head(p, h):
            if (p, h) not in held:
                rows = pl.ds((p * 2 + h) * hd, hd)
                do_t = dobuf[rows, :]
                dsum = jnp.sum(do_t.astype(F32) * obuf[cc, rows, :].astype(F32), axis=0, keepdims=True)
                held[p, h] = (pad_head(do_t, h), dsum)
            return held[p, h]

        def front(p, j):
            out = []
            for h in range(2):
                do_z, dsum = of_head(p, h)
                pr = pbuf[cc * (cc + 1) // 2 + j, p * 2 + h]
                dp = dot(vn[p, pl.ds(j * tc, tc), :], do_z).astype(BF16).astype(F32)
                ds = (pr.astype(F32) * (dp - dsum)).astype(BF16)
                if j < cc:
                    dsbuf[p * 2 + h, pl.ds(j * tc, tc), :] = ds
                out.append(ds)
            return out

        def back(p, j, ds):
            for h in range(2):
                dq_h = dot(qkv[j, head_rows(p, h, 1), :], ds[h])
                dqs[p, h] = dq_h if j == 0 else dqs[p, h] + dq_h
            if j < cc:
                return
            dv_new, dk_new = kv_grad(cc, p, j, [of_head(p, h)[0] for h in range(2)], ds,
                                     [qkv[cc, head_rows(p, h, 0), :] for h in range(2)])
            dv_t = jnp.transpose(dv_new).astype(BF16)
            dk_t = (jnp.transpose(dk_new) * scale).astype(BF16)
            for h in range(2):
                qsave[pl.ds((p * 2 + h) * hd, hd), :] = qkv[cc, head_rows(p, h, 0), :]
                qkv[cc, head_rows(p, h, 0), :] = (dqs[p, h] * scale).astype(BF16)
                qkv[cc, head_rows(p, h, 1), :] = dk_t[h * hd:(h + 1) * hd, :]
                qkv[cc, head_rows(p, h, 2), :] = dv_t[h * hd:(h + 1) * hd, :]

        ds = front(*units[0])
        for n, unit in enumerate(units):
            later = front(*units[n + 1]) if n + 1 < len(units) else None
            back(*unit, ds)
            ds = later

    def kv_grad(cc, p, j, do_z, ds, q_t):
        dv_new = dk_new = None
        for h in range(2):
            dv_h = dot_t(pbuf[cc * (cc + 1) // 2 + j, p * 2 + h], do_z[h])
            dk_h = dot_t(ds[h], pad_head(q_t[h], h))
            dv_new = dv_h if dv_new is None else dv_new + dv_h
            dk_new = dk_h if dk_new is None else dk_new + dk_h
        rows = pl.ds(j * tc, tc)
        if cc < nc - 1:
            dv_new = dv_new + dvacc[p, rows, :]
            dk_new = dk_new + dkacc[p, rows, :]
        return dv_new, dk_new

    def earlier_keys(cc):
        for p in range(heads // 2):
            heads_of = [pl.ds((p * 2 + h) * hd, hd) for h in range(2)]
            do_z = [pad_head(dobuf[heads_of[h], :], h) for h in range(2)]
            q_t = [qsave[heads_of[h], :] for h in range(2)]
            for j in range(cc):
                rows = pl.ds(j * tc, tc)
                dv_new, dk_new = kv_grad(cc, p, j, do_z, [dsbuf[p * 2 + h, rows, :] for h in range(2)], q_t)
                dvacc[p, rows, :] = dv_new
                dkacc[p, rows, :] = dk_new

    def attention_step(c):
        @pl.when(first)
        def _():
            x_copy(c).wait()
            hbuf[c] = jnp.transpose(xin[c])

        @pl.when(jnp.logical_not(first))
        def _():
            f_copy(c).wait_recv()

        @pl.when(early & (c == 0))
        def _():
            w_wait(W_Q)

        h32 = hbuf[c].astype(F32)
        n1 = (h32 * inv_rms(h32)).astype(BF16)
        n1buf[c] = n1
        for r in range(nm):
            rows = pl.ds(r * qrows, qrows)
            blk = dot(wqT[rows, :], n1).astype(BF16)
            qkv[c, rows, :] = blk
            for part, ref in ((1, kn), (2, vn)):
                both = jnp.concatenate([blk[(3 * h + part) * hd:(3 * h + part + 1) * hd] for h in range(2)], axis=0)
                ref[r, pl.ds(pl.multiple_of(c * tc, tc), tc), :] = jnp.transpose(both)

        for cc in range(nc):
            pl.when(c == cc)(functools.partial(attention, cc))

    def mlp_step(c):
        a = dot(woT[...], obuf[c]).astype(BF16)
        m32 = (hbuf[c].astype(F32) + a.astype(F32)).astype(BF16).astype(F32)
        mbuf[c] = m32.astype(BF16)
        n2 = (m32 * inv_rms(m32)).astype(BF16)
        n2buf[c] = n2

        blk = fl // 2
        for f in range(2 * nm):
            rows = pl.ds(f * blk, blk)
            u = dot(wuT[rows, :], n2buf[c]).astype(BF16)
            ubuf[c, rows, :] = u
            zbuf[c, rows, :] = gelu(u.astype(F32)).astype(BF16)
        acc = dot(wdT[...], zbuf[c])
        y32 = (mbuf[c].astype(F32) + acc.astype(BF16).astype(F32)).astype(BF16)
        ybuf[c] = y32

        @pl.when(jnp.logical_not(last))
        def _():
            f_copy(c).start()

        @pl.when(last)
        def _():
            t_copy(c).wait()
            err = ybuf[c].astype(F32) - jnp.transpose(xin[c]).astype(F32)
            lossv[...] += jnp.sum((err * err).reshape(dm_ // 8, 8, tc), axis=0)
            dybuf[c] = (err * inv_d).astype(BF16)


    @pl.loop(0, 2 * nc)
    def _(n):
        attn_turn = jnp.where(early, jnp.where(n < nc, 1, 0), 1 - lax.rem(n, 2))
        c = jnp.where(early, lax.rem(n, nc), n // 2)

        @pl.when(early & (n == 1))
        def _():
            w_forward(W_U)

        @pl.when(early & (n == 2))
        def _():
            w_forward(W_D)

        @pl.when(attn_turn == 1)
        def _():
            attention_step(c)

        @pl.when(early & (n == nc))
        def _():
            w_wait(W_O)
            w_wait(W_U)
            w_wait(W_D)

        @pl.when(attn_turn == 0)
        def _():
            mlp_step(c)

    def z_start():
        for c in range(nc):
            for way in range(4):
                z_copy(c, way).start()

    @pl.when(jnp.logical_not(late))
    def _():
        for c in range(nc):
            f_copy(c).wait_send()
        z_start()
        natural_weights()

    @pl.when(jnp.logical_not(last))
    def _():
        @pl.loop(0, nc)
        def _(c):
            slope(c)

    @pl.when(jnp.logical_not(late))
    def _():
        @pl.loop(0, nc)
        def _(c):
            z_forward(c)

    def l_copy(k):
        return pltpu.make_async_remote_copy(
            src_ref=losst.at[nm], dst_ref=losst.at[3 - k if nm == 4 else nm - 1 - k], send_sem=lsend.at[k - 1],
            recv_sem=lrecv.at[k - 1], device_id={"model": peer(k)}, device_id_type=MESH)

    def lf_copy():
        return pltpu.make_async_remote_copy(
            src_ref=losst.at[nm + 1], dst_ref=losst.at[nm + 1], send_sem=lfsend, recv_sem=lfrecv,
            device_id={"stage": prv}, device_id_type=MESH)

    @pl.when(last)
    def _():
        tot = jnp.sum(lossv[...]) * (0.5 * inv_d)
        losst[nm] = jnp.full(losst.shape[1:], tot, F32)
        for k in range(1, nm):
            l_copy(k).start()

    dy_inside = jnp.logical_not(late) & (first | odd)

    @pl.loop(0, nc)
    def _(i):
        c = nc - 1 - i

        @pl.when(jnp.logical_not(last))
        def _():
            b_copy(c).wait_recv()

        @pl.when(jnp.logical_not(late) & (i == 0))
        def _():
            for way in range(2):
                dy_copy(c, way).start()

        @pl.when(last)
        def _():
            slope(c)

        blk = fl // 4
        for f in range(4 * nm):
            rows = pl.ds(f * blk, blk)
            dz = dot(wd[rows, :], dybuf[c]).astype(BF16).astype(F32)
            ubuf[c, rows, :] = (dz * folded(i, f * blk, blk)[...]).astype(BF16)
        acc = dot(wu[...], ubuf[c])
        dn2 = acc.astype(BF16).astype(F32)
        m32 = mbuf[c].astype(F32)
        pull = norm_pull(m32, inv_rms(m32), dn2).astype(BF16)
        dmid = (dybuf[c].astype(F32) + pull.astype(F32)).astype(BF16)
        mbuf[c] = dmid
        dobuf[...] = dot(wo[...], dmid).astype(BF16)

        @pl.when(jnp.logical_not(late) & (i > 0))
        def _():
            for way in range(2):
                dy_copy(c, way).start()

        @pl.when(dy_inside & (i > 0))
        def _():
            dy_forward(c + 1)

        for cc in range(nc):
            pl.when(c == cc)(functools.partial(attention_grad, cc))

        dn1 = dot(wq[...], qkv[c]).astype(BF16).astype(F32)
        h32 = hbuf[c].astype(F32)
        pull1 = norm_pull(h32, inv_rms(h32), dn1).astype(BF16)

        @pl.when(late & jnp.logical_not(last))
        def _():
            f_copy(c).wait_send()

        ybuf[c] = (mbuf[c].astype(F32) + pull1.astype(F32)).astype(BF16)

        @pl.when(jnp.logical_not(first))
        def _():
            b_copy(c).start()

        for cc in range(1, nc):
            pl.when(c == cc)(functools.partial(earlier_keys, cc))

    @pl.when(last)
    def _():
        for k in range(1, nm):
            l_copy(k).wait_recv()
        vals = [losst[nm]] + [losst[k - 1] for k in range(1, nm)]
        tot = jnp.zeros_like(vals[0])
        for who in range(nm):
            pick = vals[0]
            for k in range(1, nm):
                pick = jnp.where(peer(k) == who, vals[k], pick)
            tot = tot + pick
        losst[nm + 1] = tot

    @pl.when(jnp.logical_not(last))
    def _():
        lf_copy().wait_recv()

    @pl.when(jnp.logical_not(first))
    def _():
        lf_copy().start()

    loss_out[...] = losst[nm + 1]

    def wgrad(mat, d):
        acc = None
        for c in range(nc):
            if mat == 0:
                part = dot_t(qkv[c, rowsl(d * qrows, qrows, qrows), :], n1buf[c])
            elif mat == 1:
                part = dot_t(obuf[c, rowsl(d * orows, orows, orows), :], mbuf[c])
            elif mat == 2:
                part = dot_t(n2buf[c], ubuf[c, rowsl(d * fl, fl, fl), :])
            else:
                part = dot_t(zbuf[c, rowsl(d * fl, fl, fl), :], dybuf[c])
            acc = part if acc is None else acc + part
        return acc

    sizes = (qrows, orows, dm_)
    offs = (0, qrows, qrows + orows)

    def rows_of(mat):
        return pl.ds(offs[mat], sizes[mat])

    def half_of(mat, half):
        return pl.ds(offs[mat] + half * (sizes[mat] // 2), sizes[mat] // 2)

    def far_copy(mat, half):
        rows = pl.ds(offs[mat] // 2, sizes[mat] // 2)
        return ring_copy(stage_buf.at[0, half_of(mat, half)], (far_p, far_m)[half].at[rows],
                         rs_send.at[mat, half], rs_recv.at[mat, half], half)

    def near_copy(mat, side, half):
        way = 2 + 2 * side + half
        return ring_copy(stage_buf.at[1 + side, half_of(mat, half)], (near_l if side == half else near_e).at[half_of(mat, half)],
                         rs_send.at[mat, way], rs_recv.at[mat, way], side)

    mats = (2, 0, 1)

    @pl.loop(0, 3)
    def _(slot):
        who = lax.rem(me + jnp.where(slot == 0, far, jnp.where(slot == 1, plus, minus)), nm)
        for mat in mats:
            stage_buf[slot, rows_of(mat)] = wgrad(mat, who)

            @pl.when(slot == 0)
            def _():
                for half in range(2):
                    far_copy(mat, half).start()

            for side in range(2):
                @pl.when(slot == 1 + side)
                def _():
                    near_copy(mat, side, 1 - side).start()

    @pl.when(dy_inside)
    def _():
        dy_forward(0)

    @pl.when(jnp.logical_not(late | dy_inside))
    def _():
        for c in reversed(range(nc)):
            dy_forward(c)

    hd2 = dm_ // 2

    def gd_cols(half):
        return pl.ds(half * hd2, hd2) if isinstance(half, int) else pl.ds(pl.multiple_of(half * hd2, hd2), hd2)

    def gd_half(d, half):
        return functools.reduce(jnp.add, [
            dot_t(zbuf[c, rowsl(d * fl, fl, fl), :], dybuf[c, gd_cols(half), :]) for c in range(nc)])

    def gd_far_copy(half):
        return ring_copy(gdacc.at[:, gd_cols(half)], gd_far.at[half], gd_send.at[half], gd_recv.at[half], half)

    def gd_slot(side, half):
        return folded(n_st - 1, (2 * side + half) * fl, fl)

    def gd_near_copy(side, half):
        way = 2 + 2 * side + half
        return ring_copy(gd_slot(side, half), gd_near.at[1 if side == half else 0, half],
                         gd_send.at[way], gd_recv.at[way], side)

    @pl.when(late)
    def _():
        @pl.loop(0, 2)
        def _(half):
            gdacc[:, gd_cols(half)] = gd_half(peer(far), half)

        for half in range(2):
            gd_far_copy(half).start()

        @pl.loop(0, 4)
        def _(n):
            rows, cols = lax.rem(n, 2) * fl, (n // 2) * tc
            stage_buf[n_st - 1, pl.ds(pl.multiple_of(rows, fl), fl), pl.ds(pl.multiple_of(cols, tc), tc)] = gd_half(
                lax.rem(me + 1 + 2 * (n // 2), nm), lax.rem(n, 2))

        for side in range(2):
            gd_near_copy(side, 1 - side).start()

    def gd_add(src, ref):
        nr = min(fl, radd.shape[0])
        for r in range(0, fl, nr):
            copy = pltpu.make_async_copy(src.at[pl.ds(r, nr)], radd.at[pl.ds(0, nr), pl.ds(0, hd2)], ld_sem.at[0])
            copy.start()
            copy.wait()
            ref[pl.ds(r, nr), :] += radd[pl.ds(0, nr), pl.ds(0, hd2)]

    pieces = [(mat, half) for mat in mats for half in range(2)]
    cols = dvacc.shape[2]
    n_cols = dm_ // cols

    def piece_loads(n, kind):
        mat, half = pieces[n]
        nr = sizes[mat] // 2
        r0 = sum(sizes[m] // 2 for m, _ in pieces[:n])
        src = near_e.at[half_of(mat, half)] if kind else (far_p, far_m)[half].at[pl.ds(offs[mat] // 2, nr)]
        dst = dkacc if kind else dvacc
        return [pltpu.make_async_copy(src.at[:, pl.ds(k * cols, cols)], dst.at[k, pl.ds(r0, nr), :], pl_sem.at[kind, n])
                for k in range(n_cols)], dst, r0, nr

    def piece_start(n, kind):
        mat, half = pieces[n]
        if kind:
            near_copy(mat, 1 - half, half).wait_recv()
        else:
            far_copy(mat, half).wait_recv()
        for copy in piece_loads(n, kind)[0]:
            copy.start()

    def piece_add(n, kind, slot):
        mat, half = pieces[n]
        copies, src, r0, nr = piece_loads(n, kind)
        for copy in copies:
            copy.wait()
        rows = half_of(mat, half)
        for k in range(n_cols):
            stage_buf[slot, rows, pl.ds(k * cols, cols)] += src[k, pl.ds(r0, nr), :]

    piece_start(0, 0)
    for n, (mat, half) in enumerate(pieces):
        if n + 1 < len(pieces):
            piece_start(n + 1, 0)
        piece_add(n, 0, 1 + half)
        near_copy(mat, half, half).start()

    @pl.when(late)
    def _():
        for half in range(2):
            gd_far_copy(half).wait_recv()
            gd_add(gd_far.at[half], gd_slot(half, half))
            gd_near_copy(half, half).start()
            gd_far_copy(half).wait_send()

    for mat in mats:
        for half in range(2):
            far_copy(mat, half).wait_send()
        stage_buf[0, rows_of(mat)] = wgrad(mat, me)

    def zdy_load(n, buf):
        slot, c = n // nc, lax.rem(n, nc)
        return (pltpu.make_async_copy(z_recv.at[slot, c], dsbuf.at[2 * buf, pl.ds(0, fl)], ld_sem.at[1 + buf]),
                pltpu.make_async_copy(dy_recv.at[slot, c], dsbuf.at[2 * buf + 1, pl.ds(0, dm_)], ld_sem.at[3 + buf]))

    gdacc[...] = wgrad(3, me)

    @pl.when(jnp.logical_not(late))
    def _():
        for c in range(nc):
            for way in (0, 1, 4, 5):
                z_copy(c, way).wait_recv()
            for way in (2, 3):
                dy_copy(c, way).wait_recv()
        for cp in zdy_load(0, 0):
            cp.start()

        @pl.loop(0, 3 * nc)
        def _(n):
            buf = lax.rem(n, 2)

            @pl.when(n + 1 < 3 * nc)
            def _():
                for cp in zdy_load(n + 1, 1 - buf):
                    cp.start()

            for cp in zdy_load(n, buf):
                cp.wait()
            gdacc[...] += dot_t(dsbuf[2 * buf, pl.ds(0, fl), :], dsbuf[2 * buf + 1, pl.ds(0, dm_), :])

    def gd_arrivals(last_half):
        for half in range(2):
            side = half if last_half else 1 - half
            gd_near_copy(side, half).wait_recv()
            gd_add(gd_near.at[last_half, half], gdacc.at[:, gd_cols(half)])

    def out_copy(mat):
        if mat == 3:
            return pltpu.make_async_copy(gdacc, sum_out.at[pl.ds(qrows + orows + dm_, fl)], out_sem.at[3])
        return pltpu.make_async_copy(stage_buf.at[0, rows_of(mat)], sum_out.at[rows_of(mat)], out_sem.at[mat])

    piece_start(0, 1)
    for n, (mat, half) in enumerate(pieces):
        if n + 1 < len(pieces):
            piece_start(n + 1, 1)
        piece_add(n, 1, 0)
        if half:
            out_copy(mat).start()

    @pl.when(late)
    def _():
        gd_arrivals(0)
        gd_arrivals(1)

    out_copy(3).start()
    for mat in mats:
        for side in range(2):
            near_copy(mat, side, side).wait_recv()

    for mat in range(4):
        out_copy(mat).wait()

    @pl.when(jnp.logical_not(late))
    def _():
        for c in range(nc):
            for way in range(6):
                z_copy(c, way).wait_send()
            for way in range(4):
                dy_copy(c, way).wait_send()

    @pl.when(late)
    def _():
        for side in range(2):
            for half in range(2):
                gd_near_copy(side, half).wait_send()

    for idx in range(4):
        for way in range(4):
            w_copy(idx, way).wait_send()
    for mat in mats:
        for half in range(2):
            for side in range(2):
                near_copy(mat, side, half).wait_send()

    @pl.when(jnp.logical_not(first))
    def _():
        for c in range(nc):
            b_copy(c).wait_send()
        lf_copy().wait_send()

    @pl.when(last)
    def _():
        for k in range(1, nm):
            l_copy(k).wait_send()


def finish_kernel(sq, so, su, sd, lq, lo, lu, loss, gq, go, gu, gd, loss_out):
    gq[...] = sq[...] + lq[...]
    go[...] = so[...] + lo[...]
    gu[...] = su[...] + lu[...]
    gd[...] = sd[...]
    loss_out[0] = loss[0, 0]


def solution(mesh):
    ns = mesh.shape["stage"]
    nm = mesh.shape["model"]

    def per_device(tokens_in, targets, w_qkv, w_out, w_up, w_down):
        n_micro, seq_len, d_model = tokens_in.shape
        hl, hd, fl = w_qkv.shape[3], w_qkv.shape[5], w_up.shape[3]
        tc = min(CHUNK, seq_len // 2)
        nc = seq_len // tc
        qrows, orows = hl * 3 * hd, hl * hd
        assert n_micro == nm == 4 and w_qkv.shape[1] == 1 and hl == 2 and d_model == 2 * tc and qrows + orows + d_model == seq_len == 2 * fl and nc == 4
        wqT = jnp.transpose(w_qkv[0, 0], (1, 2, 3, 0)).reshape(qrows, d_model)
        wo = w_out[0, 0].reshape(orows, d_model)
        wu, wd = w_up[0, 0], w_down[0, 0]
        cfg = (ns, nm, nc, tc, d_model, hl, hd, fl)
        heads = nm * hl
        any_spec = pl.BlockSpec(memory_space=pl.ANY)
        f32 = lambda *shape: jax.ShapeDtypeStruct(shape, F32)
        rsum = qrows + orows + d_model
        seqb = nc * tc
        b16 = lambda *shape: jax.ShapeDtypeStruct(shape, BF16)
        out_shape = (f32(rsum + fl, d_model), f32(8, 128), f32(rsum // 2, d_model), f32(rsum // 2, d_model), f32(rsum, d_model),
                     f32(rsum, d_model), b16(3, nc, fl, tc), b16(2, nc, fl // 2, tc), b16(3, nc, d_model, tc),
                     f32(2, fl, d_model // 2), f32(2, 2, fl, d_model // 2))
        vb = lambda *shape: pltpu.VMEM(shape, BF16)
        vf = lambda *shape: pltpu.VMEM(shape, F32)
        dma = lambda *shape: pltpu.SemaphoreType.DMA(shape)
        scratch = [
            vb(nm * qrows, d_model), vb(d_model, nm * orows), vb(nm * fl, d_model), vb(d_model, nm * fl),
            vb(nm * fl, d_model), vb(d_model, nm * fl), vb(nm * orows, d_model), vb(d_model, nm * qrows),
            vb(nc, tc, d_model), vb(nc, d_model, tc), vb(nc, d_model, tc), vb(nc, nm * qrows, tc), vb(nm, seqb, orows), vb(nm, seqb, orows),
            vb(nc, nm * orows, tc), vb(nc, d_model, tc), vb(nc, d_model, tc), vb(nc, nm * fl, tc), vb(nc, nm * fl, tc),
            vb(nc * (nc + 1) // 2, heads, tc, tc), vb(nc, d_model, tc), vf(heads // 2, seqb, 2 * hd), vf(heads // 2, seqb, 2 * hd),
            vb(nc, d_model, tc), vb(nm * orows, tc), vf(nm + 2, 8, 128), vf(8, tc),
            vf(4, rsum, d_model), vf(256, d_model), vf(fl, d_model), vb(heads, max((nc - 1) * tc, fl), tc), vb(nm * orows, tc),
            dma(4, 4), dma(4, 4), dma(4), pltpu.SemaphoreType.REGULAR, dma(nc), dma(nc), dma(nc), dma(nc), dma(nc),
            dma(nm - 1), dma(nm - 1), pltpu.SemaphoreType.DMA, pltpu.SemaphoreType.DMA,
            dma(3, 6), dma(3, 6), dma(5), dma(4), dma(6, nc), dma(6, nc), dma(4, nc), dma(4, nc), dma(6), dma(6), dma(2, 6),
        ]
        res = pl.pallas_call(
            functools.partial(step_kernel, cfg),
            out_shape=out_shape,
            in_specs=[any_spec] * 6,
            out_specs=[any_spec, pl.BlockSpec(memory_space=pltpu.VMEM)] + [any_spec] * 9,
            scratch_shapes=scratch,
            compiler_params=pltpu.CompilerParams(collective_id=0, has_side_effects=True, vmem_limit_bytes=67043328),
            name="train_step",
        )(tokens_in, targets, wqT, wo, wu, wd)
        part, loss, late = res[0], res[1], res[5]
        steps = 2

        def spec(size, start):
            rows = size // steps
            return pl.BlockSpec((rows, d_model), lambda i: (start // rows + i, 0))

        q_s, o_s, u_s = spec(qrows, 0), spec(orows, qrows), spec(d_model, qrows + orows)
        g_qkv, g_out, g_up, g_down, loss = pl.pallas_call(
            finish_kernel,
            grid=(steps,),
            out_shape=(f32(qrows, d_model), f32(orows, d_model), f32(d_model, fl), f32(fl, d_model), f32(1)),
            in_specs=[q_s, o_s, u_s, spec(fl, rsum), q_s, o_s, u_s, pl.BlockSpec(memory_space=pltpu.SMEM)],
            out_specs=[spec(qrows, 0), spec(orows, 0), spec(d_model, 0), spec(fl, 0), pl.BlockSpec(memory_space=pltpu.SMEM)],
            name="finish",
        )(part, part, part, part, late, late, late, loss)
        g_qkv = jnp.transpose(g_qkv.reshape(hl, 3, hd, d_model), (3, 0, 1, 2))[None, None]
        return g_qkv, g_out.reshape(1, 1, hl, hd, d_model), g_up[None, None], g_down[None, None], loss

    tok_spec = P(None, "data", None)
    qkv_spec = P("stage", None, None, "model", None, None)
    out_spec = P("stage", None, "model", None, None)
    up_spec = P("stage", None, None, "model")
    down_spec = P("stage", None, "model", None)
    g_qkv_spec = P(("data", "stage"), None, None, "model", None, None)
    g_out_spec = P(("data", "stage"), None, "model", None, None)
    g_up_spec = P(("data", "stage"), None, None, "model")
    g_down_spec = P(("data", "stage"), None, "model", None)
    return jax.shard_map(per_device, mesh=mesh, in_specs=(tok_spec, tok_spec, qkv_spec, out_spec, up_spec, down_spec), out_specs=(g_qkv_spec, g_out_spec, g_up_spec, g_down_spec, P("data")), check_vma=False)
```

```python
import functools
import math

import jax
import jax.numpy as jnp
from jax import lax
from jax.experimental import pallas as pl
from jax.experimental.pallas import tpu as pltpu
from jax.sharding import PartitionSpec as P

F32 = jnp.float32
BF16 = jnp.bfloat16
MESH = pl.DeviceIdType.MESH
CHUNK = 256
NEG = -1e30
GELU_C = math.sqrt(2.0 / math.pi)
GELU_A = 0.044715

W_Q, W_O, W_U, W_D = range(4)


def dot(lhs, rhs):
    return jnp.dot(lhs, rhs, preferred_element_type=F32)


def dot_t(lhs, rhs):
    return lax.dot_general(lhs, rhs, (((1,), (1,)), ((), ())), preferred_element_type=F32)


def inv_rms(x32):
    return lax.rsqrt(jnp.mean(x32 * x32, axis=0, keepdims=True) + 1e-6)


def norm_pull(x32, inv, g32):
    mean_gx = jnp.mean(g32 * x32, axis=0, keepdims=True)
    return g32 * inv - x32 * (inv * inv * inv * mean_gx)


def gelu(u):
    tanh = jnp.tanh(u * (GELU_C + (GELU_C * GELU_A) * (u * u)))
    half = 0.5 * u
    return half + half * tanh


def gelu_grad(u):
    u2 = u * u
    sig = 0.5 + 0.5 * jnp.tanh(u * (GELU_C + (GELU_C * GELU_A) * u2))
    slope = u * (2.0 * GELU_C + (6.0 * GELU_C * GELU_A) * u2)
    return sig * (1.0 + slope * (1.0 - sig))


def step_kernel(cfg, x_hbm, t_hbm, wqT_in, wo_in, wu_in, wd_in,
                sum_out, loss_out, far_p, far_m, near_e, near_l, z_recv, z_fwd, dy_recv, gd_far, gd_near,
                wqT, woT, wuT, wdT, wd, wu, wo, wq,
                xin, hbuf, n1buf, qkv, kn, vn, obuf, mbuf, n2buf, ubuf, zbuf, pbuf, dybuf, dvacc, dkacc,
                ybuf, dobuf, losst, lossv, stage_buf, radd, gdacc, dsbuf, qsave,
                ag_send, ag_recv, ag_loc, go_sem, xsem, fsend, frecv, bsend, brecv, lsend, lrecv, lfsend, lfrecv,
                rs_send, rs_recv, ld_sem, out_sem, z_send, z_arr, dy_send, dy_arr, gd_send, gd_recv, pl_sem):
    ns, nm, nc, tc, dm_, hl, hd, fl = cfg
    heads = nm * hl
    qrows = hl * 3 * hd
    orows = hl * hd
    inv_d = 1.0 / (nm * nc * tc * dm_)
    scale = hd ** -0.5
    exp_c = scale * math.log2(math.e)
    me = lax.axis_index("model")
    st = lax.axis_index("stage")
    nxt = lax.rem(st + 1, ns)
    prv = lax.rem(st + ns - 1, ns)
    first = st == 0
    last = st == ns - 1

    def peer(k):
        return lax.rem(me + k, nm)

    bar = pltpu.get_barrier_semaphore()
    pl.semaphore_signal(bar, inc=1, device_id={"stage": nxt}, device_id_type=MESH)
    pl.semaphore_signal(bar, inc=1, device_id={"stage": prv}, device_id_type=MESH)
    for k in range(1, nm):
        pl.semaphore_signal(bar, inc=1, device_id={"model": peer(k)}, device_id_type=MESH)
    pl.semaphore_wait(bar, 2 + nm - 1)

    def rowsl(start, size, mult):
        return pl.ds(pl.multiple_of(start, mult), size)

    plus, minus, far = 1, nm - 1, 2

    def w_rows(idx, who, half=None):
        size = (qrows, orows, fl, fl)[idx]
        if idx in (W_Q, W_U):
            buf = wqT if idx == W_Q else wuT
            if half is None:
                return buf.at[rowsl(who * size, size, size), :]
            return buf.at[rowsl(who * size + half * (size // 2), size // 2, size // 2), :]
        view = (woT if idx == W_O else wdT).at[:, rowsl(who * size, size, size)]
        return view if half is None else view.at[pl.ds(half * (dm_ // 2), dm_ // 2), :]

    def w_copy(idx, way):
        to = plus if way in (0, 2) else minus
        if way < 2:
            src = wqT_in if idx == W_Q else w_rows(idx, me)
            dst = w_rows(idx, me)
        else:
            src = dst = w_rows(idx, peer(minus if way == 2 else plus), way - 2)
        return pltpu.make_async_remote_copy(
            src_ref=src, dst_ref=dst, send_sem=ag_send.at[idx, way], recv_sem=ag_recv.at[idx, way],
            device_id={"model": peer(to)}, device_id_type=MESH)

    def w_arrival(idx, way):
        who = peer((minus, plus, far, far)[way])
        ref = w_rows(idx, who) if way < 2 else w_rows(idx, who, way - 2)
        return pltpu.make_async_remote_copy(
            src_ref=ref, dst_ref=ref, send_sem=ag_send.at[idx, way], recv_sem=ag_recv.at[idx, way],
            device_id={"model": peer(plus)}, device_id_type=MESH)

    def w_local(idx):
        src = (wqT_in, wo_in, wu_in, wd_in)[idx]
        dst = (w_rows(W_Q, me), wo.at[rowsl(me * orows, orows, orows), :], wu.at[:, rowsl(me * fl, fl, fl)], wd.at[rowsl(me * fl, fl, fl), :])[idx]
        return pltpu.make_async_copy(src, dst, ag_loc.at[idx])

    def w_own(idx):
        for way in range(2):
            w_copy(idx, way).start()

    def w_forward(idx):
        for way in range(2):
            w_arrival(idx, way).wait_recv()
        for way in range(2, 4):
            w_copy(idx, way).start()

    def w_wait(idx):
        for way in range(2, 4):
            w_arrival(idx, way).wait_recv()

    def x_copy(c):
        return pltpu.make_async_copy(x_hbm.at[me, pl.ds(c * tc, tc), :], xin.at[c], xsem.at[c])

    def t_copy(c):
        return pltpu.make_async_copy(t_hbm.at[me, pl.ds(c * tc, tc), :], xin.at[c], xsem.at[c])

    @pl.when(first)
    def _():
        for c in range(nc):
            x_copy(c).start()

    @pl.when(last)
    def _():
        for c in range(nc):
            t_copy(c).start()

    for idx in range(4):
        w_local(idx).start()

    odd = lax.rem(st, 2) == 1
    early = st < 2

    @pl.when(odd)
    def _():
        pl.semaphore_wait(go_sem, 1)

    w_own(W_Q)
    w_local(W_O).wait()
    woT[:, rowsl(me * orows, orows, orows)] = jnp.transpose(wo[rowsl(me * orows, orows, orows), :])
    w_own(W_O)
    w_local(W_U).wait()
    wuT[rowsl(me * fl, fl, fl), :] = jnp.transpose(wu[:, rowsl(me * fl, fl, fl)])
    w_own(W_U)
    w_local(W_D).wait()
    wdT[:, rowsl(me * fl, fl, fl)] = jnp.transpose(wd[rowsl(me * fl, fl, fl), :])
    w_own(W_D)
    w_local(W_Q).wait()
    w_forward(W_Q)
    w_forward(W_O)

    @pl.when(jnp.logical_not(odd))
    def _():
        pl.semaphore_signal(go_sem, inc=1, device_id={"stage": nxt}, device_id_type=MESH)

    def natural_weights():
        @pl.loop(0, nm)
        def _(f):
            wu[:, rowsl(f * fl, fl, fl)] = jnp.transpose(wuT[rowsl(f * fl, fl, fl), :])
            wd[rowsl(f * fl, fl, fl), :] = jnp.transpose(wdT[:, rowsl(f * fl, fl, fl)])
            wo[rowsl(f * orows, orows, orows), :] = jnp.transpose(woT[:, rowsl(f * orows, orows, orows)])
            wq[:, rowsl(f * qrows, qrows, qrows)] = jnp.transpose(wqT[rowsl(f * qrows, qrows, qrows), :])

    late = st >= max(2, ns // 2)

    @pl.when(jnp.logical_not(early))
    def _():
        w_forward(W_U)
        w_forward(W_D)
        for idx in range(4):
            w_wait(idx)

    @pl.when(late)
    def _():
        natural_weights()

    def f_copy(c):
        return pltpu.make_async_remote_copy(
            src_ref=ybuf.at[c], dst_ref=hbuf.at[c], send_sem=fsend.at[c], recv_sem=frecv.at[c],
            device_id={"stage": nxt}, device_id_type=MESH)

    def b_copy(c):
        return pltpu.make_async_remote_copy(
            src_ref=ybuf.at[c], dst_ref=dybuf.at[c], send_sem=bsend.at[c], recv_sem=brecv.at[c],
            device_id={"stage": prv}, device_id_type=MESH)

    def ring_copy(src, dst, send, recv, way):
        return pltpu.make_async_remote_copy(
            src_ref=src, dst_ref=dst, send_sem=send, recv_sem=recv,
            device_id={"model": peer((plus, minus)[way % 2])}, device_id_type=MESH)

    hf = fl // 2

    def z_copy(c, way):
        if way < 2:
            src, dst = zbuf.at[c, rowsl(peer((plus, minus)[way]) * fl, fl, fl), :], z_recv.at[way, c]
        elif way < 4:
            src, dst = zbuf.at[c, rowsl(peer(far) * fl + (way - 2) * hf, hf, hf), :], z_fwd.at[way - 2, c]
        else:
            src, dst = z_fwd.at[way - 4, c], z_recv.at[2, c, pl.ds((way - 4) * hf, hf)]
        return ring_copy(src, dst, z_send.at[way, c], z_arr.at[way, c], way)

    def z_forward(c):
        for way in (2, 3):
            z_copy(c, way).wait_recv()
        for way in (4, 5):
            z_copy(c, way).start()

    def dy_copy(c, way):
        if way < 2:
            src, dst = dybuf.at[c], dy_recv.at[way, c]
        else:
            rows = pl.ds((way - 2) * (dm_ // 2), dm_ // 2)
            src, dst = dy_recv.at[way - 2, c, rows], dy_recv.at[2, c, rows]
        return ring_copy(src, dst, dy_send.at[way, c], dy_arr.at[way, c], way)

    def dy_forward(c):
        for way in (0, 1):
            dy_copy(c, way).wait_recv()
        for way in (2, 3):
            dy_copy(c, way).start()

    lossv[...] = jnp.zeros_like(lossv)

    def head_rows(p, h, part):
        return pl.ds(p * (2 * 3 * hd) + (h * 3 + part) * hd, hd)

    def pad_head(val, h):
        zero = jnp.zeros_like(val)
        return jnp.concatenate([val, zero] if h == 0 else [zero, val], axis=0)

    def causal(shape, row0):
        return lax.broadcasted_iota(jnp.int32, shape, 0) + row0 <= lax.broadcasted_iota(jnp.int32, shape, 1)

    n_st = stage_buf.shape[0]

    def folded(slot, row, n):
        fold = stage_buf.shape[1]
        return stage_buf.at[slot, pl.ds(row % fold, n), pl.ds((row // fold) * tc, tc)]

    def slope(c):
        blk = fl // 4
        per = stage_buf.shape[1] // blk

        @pl.loop(0, 4 * nm)
        def _(f):
            half = f // per
            rows = pl.ds(pl.multiple_of((f - half * per) * blk, blk), blk)
            cols = pl.ds(pl.multiple_of(half * tc, tc), tc)
            u = ubuf[c, pl.ds(pl.multiple_of(f * blk, blk), blk), :].astype(F32)
            stage_buf[nc - 1 - c, rows, cols] = gelu_grad(u)

    def attention(cc):
        nk = (cc + 1) * tc
        slots = min(heads, 2 * nc * tc // nk)
        ahead = min(4, slots - 1)
        sub = tc // 2

        def front(head):
            p, h = head // 2, head % 2
            base = (head % slots) * nk
            qz = pad_head(qkv[cc, head_rows(p, h, 0), :], h)
            tops, sums = [], []
            for j in range(cc + 1):
                s = dot(kn[p, pl.ds(j * tc, tc), :], qz)
                for r in range(0, tc, sub):
                    part = s[r:r + sub]
                    if j == cc:
                        part = jnp.where(causal(part.shape, r), part, NEG)
                    top = jnp.max(part, axis=0, keepdims=True)
                    e = jnp.exp2((part - top) * exp_c)
                    folded(n_st - 1, base + j * tc + r, sub)[...] = e
                    tops.append(top)
                    sums.append(jnp.sum(e, axis=0, keepdims=True))
            mx = functools.reduce(jnp.maximum, tops)
            scales = [jnp.exp2((top - mx) * exp_c) for top in tops]
            inv = 1.0 / functools.reduce(jnp.add, [a * b for a, b in zip(scales, sums)])
            return [a * inv for a in scales]

        def back(head, factors):
            p, h = head // 2, head % 2
            base = (head % slots) * nk
            o_t = None
            for j in range(cc + 1):
                parts = []
                for i in range(2):
                    pr = (folded(n_st - 1, base + j * tc + i * sub, sub)[...] * factors[2 * j + i]).astype(BF16)
                    pbuf[cc * (cc + 1) // 2 + j, head, pl.ds(i * sub, sub), :] = pr
                    parts.append(pr)
                part = dot(qkv[j, head_rows(p, h, 2), :], jnp.concatenate(parts, axis=0))
                o_t = part if o_t is None else o_t + part
            obuf[cc, pl.ds(head * hd, hd), :] = o_t.astype(BF16)

        factors = {}
        for head in range(ahead):
            factors[head] = front(head)
        for head in range(heads):
            if head + ahead < heads:
                factors[head + ahead] = front(head + ahead)
            back(head, factors.pop(head))

    def attention_grad(cc):
        units = [(p, j) for p in range(heads // 2) for j in range(cc + 1)]
        dqs = {}
        held = {}

        def of_head(p, h):
            if (p, h) not in held:
                rows = pl.ds((p * 2 + h) * hd, hd)
                do_t = dobuf[rows, :]
                dsum = jnp.sum(do_t.astype(F32) * obuf[cc, rows, :].astype(F32), axis=0, keepdims=True)
                held[p, h] = (pad_head(do_t, h), dsum)
            return held[p, h]

        def front(p, j):
            out = []
            for h in range(2):
                do_z, dsum = of_head(p, h)
                pr = pbuf[cc * (cc + 1) // 2 + j, p * 2 + h]
                dp = dot(vn[p, pl.ds(j * tc, tc), :], do_z).astype(BF16).astype(F32)
                ds = (pr.astype(F32) * (dp - dsum)).astype(BF16)
                if j < cc:
                    dsbuf[p * 2 + h, pl.ds(j * tc, tc), :] = ds
                out.append(ds)
            return out

        def back(p, j, ds):
            for h in range(2):
                dq_h = dot(qkv[j, head_rows(p, h, 1), :], ds[h])
                dqs[p, h] = dq_h if j == 0 else dqs[p, h] + dq_h
            if j < cc:
                return
            dv_new, dk_new = kv_grad(cc, p, j, [of_head(p, h)[0] for h in range(2)], ds,
                                     [qkv[cc, head_rows(p, h, 0), :] for h in range(2)])
            dv_t = jnp.transpose(dv_new).astype(BF16)
            dk_t = (jnp.transpose(dk_new) * scale).astype(BF16)
            for h in range(2):
                qsave[pl.ds((p * 2 + h) * hd, hd), :] = qkv[cc, head_rows(p, h, 0), :]
                qkv[cc, head_rows(p, h, 0), :] = (dqs[p, h] * scale).astype(BF16)
                qkv[cc, head_rows(p, h, 1), :] = dk_t[h * hd:(h + 1) * hd, :]
                qkv[cc, head_rows(p, h, 2), :] = dv_t[h * hd:(h + 1) * hd, :]

        ds = front(*units[0])
        for n, unit in enumerate(units):
            later = front(*units[n + 1]) if n + 1 < len(units) else None
            back(*unit, ds)
            ds = later

    def kv_grad(cc, p, j, do_z, ds, q_t):
        dv_new = dk_new = None
        for h in range(2):
            dv_h = dot_t(pbuf[cc * (cc + 1) // 2 + j, p * 2 + h], do_z[h])
            dk_h = dot_t(ds[h], pad_head(q_t[h], h))
            dv_new = dv_h if dv_new is None else dv_new + dv_h
            dk_new = dk_h if dk_new is None else dk_new + dk_h
        rows = pl.ds(j * tc, tc)
        if cc < nc - 1:
            dv_new = dv_new + dvacc[p, rows, :]
            dk_new = dk_new + dkacc[p, rows, :]
        return dv_new, dk_new

    def earlier_keys(cc):
        for p in range(heads // 2):
            heads_of = [pl.ds((p * 2 + h) * hd, hd) for h in range(2)]
            do_z = [pad_head(dobuf[heads_of[h], :], h) for h in range(2)]
            q_t = [qsave[heads_of[h], :] for h in range(2)]
            for j in range(cc):
                rows = pl.ds(j * tc, tc)
                dv_new, dk_new = kv_grad(cc, p, j, do_z, [dsbuf[p * 2 + h, rows, :] for h in range(2)], q_t)
                dvacc[p, rows, :] = dv_new
                dkacc[p, rows, :] = dk_new

    def attention_step(c):
        @pl.when(first)
        def _():
            x_copy(c).wait()
            hbuf[c] = jnp.transpose(xin[c])

        @pl.when(jnp.logical_not(first))
        def _():
            f_copy(c).wait_recv()

        @pl.when(early & (c == 0))
        def _():
            w_wait(W_Q)

        h32 = hbuf[c].astype(F32)
        n1 = (h32 * inv_rms(h32)).astype(BF16)
        n1buf[c] = n1
        for r in range(nm):
            rows = pl.ds(r * qrows, qrows)
            blk = dot(wqT[rows, :], n1).astype(BF16)
            qkv[c, rows, :] = blk
            for part, ref in ((1, kn), (2, vn)):
                both = jnp.concatenate([blk[(3 * h + part) * hd:(3 * h + part + 1) * hd] for h in range(2)], axis=0)
                ref[r, pl.ds(pl.multiple_of(c * tc, tc), tc), :] = jnp.transpose(both)

        for cc in range(nc):
            pl.when(c == cc)(functools.partial(attention, cc))

    def mlp_step(c):
        a = dot(woT[...], obuf[c]).astype(BF16)
        m32 = (hbuf[c].astype(F32) + a.astype(F32)).astype(BF16).astype(F32)
        mbuf[c] = m32.astype(BF16)
        n2 = (m32 * inv_rms(m32)).astype(BF16)
        n2buf[c] = n2

        blk = fl // 2
        for f in range(2 * nm):
            rows = pl.ds(f * blk, blk)
            u = dot(wuT[rows, :], n2buf[c]).astype(BF16)
            ubuf[c, rows, :] = u
            zbuf[c, rows, :] = gelu(u.astype(F32)).astype(BF16)
        acc = dot(wdT[...], zbuf[c])
        y32 = (mbuf[c].astype(F32) + acc.astype(BF16).astype(F32)).astype(BF16)
        ybuf[c] = y32

        @pl.when(jnp.logical_not(last))
        def _():
            f_copy(c).start()

        @pl.when(last)
        def _():
            t_copy(c).wait()
            err = ybuf[c].astype(F32) - jnp.transpose(xin[c]).astype(F32)
            lossv[...] += jnp.sum((err * err).reshape(dm_ // 8, 8, tc), axis=0)
            dybuf[c] = (err * inv_d).astype(BF16)


    @pl.loop(0, 2 * nc)
    def _(n):
        attn_turn = jnp.where(early, jnp.where(n < nc, 1, 0), 1 - lax.rem(n, 2))
        c = jnp.where(early, lax.rem(n, nc), n // 2)

        @pl.when(early & (n == 1))
        def _():
            w_forward(W_U)

        @pl.when(early & (n == 2))
        def _():
            w_forward(W_D)

        @pl.when(attn_turn == 1)
        def _():
            attention_step(c)

        @pl.when(early & (n == nc))
        def _():
            w_wait(W_O)
            w_wait(W_U)
            w_wait(W_D)

        @pl.when(attn_turn == 0)
        def _():
            mlp_step(c)

    def z_start():
        for c in range(nc):
            for way in range(4):
                z_copy(c, way).start()

    @pl.when(jnp.logical_not(late))
    def _():
        for c in range(nc):
            f_copy(c).wait_send()
        z_start()
        natural_weights()

    @pl.when(jnp.logical_not(last))
    def _():
        @pl.loop(0, nc)
        def _(c):
            slope(c)

    @pl.when(jnp.logical_not(late))
    def _():
        @pl.loop(0, nc)
        def _(c):
            z_forward(c)

    def l_copy(k):
        return pltpu.make_async_remote_copy(
            src_ref=losst.at[nm], dst_ref=losst.at[3 - k if nm == 4 else nm - 1 - k], send_sem=lsend.at[k - 1],
            recv_sem=lrecv.at[k - 1], device_id={"model": peer(k)}, device_id_type=MESH)

    def lf_copy():
        return pltpu.make_async_remote_copy(
            src_ref=losst.at[nm + 1], dst_ref=losst.at[nm + 1], send_sem=lfsend, recv_sem=lfrecv,
            device_id={"stage": prv}, device_id_type=MESH)

    @pl.when(last)
    def _():
        tot = jnp.sum(lossv[...]) * (0.5 * inv_d)
        losst[nm] = jnp.full(losst.shape[1:], tot, F32)
        for k in range(1, nm):
            l_copy(k).start()

    dy_inside = jnp.logical_not(late) & (first | odd)

    @pl.loop(0, nc)
    def _(i):
        c = nc - 1 - i

        @pl.when(jnp.logical_not(last))
        def _():
            b_copy(c).wait_recv()

        @pl.when(jnp.logical_not(late) & ((i == 0) | dy_inside))
        def _():
            for way in range(2):
                dy_copy(c, way).start()

        @pl.when(last)
        def _():
            slope(c)

        blk = fl // 4
        for f in range(4 * nm):
            rows = pl.ds(f * blk, blk)
            dz = dot(wd[rows, :], dybuf[c]).astype(BF16).astype(F32)
            ubuf[c, rows, :] = (dz * folded(i, f * blk, blk)[...]).astype(BF16)
        acc = dot(wu[...], ubuf[c])
        dn2 = acc.astype(BF16).astype(F32)
        m32 = mbuf[c].astype(F32)
        pull = norm_pull(m32, inv_rms(m32), dn2).astype(BF16)
        dmid = (dybuf[c].astype(F32) + pull.astype(F32)).astype(BF16)
        mbuf[c] = dmid
        dobuf[...] = dot(wo[...], dmid).astype(BF16)

        @pl.when(jnp.logical_not(late | dy_inside) & (i > 0))
        def _():
            for way in range(2):
                dy_copy(c, way).start()

        @pl.when(dy_inside & (i > 0))
        def _():
            dy_forward(c + 1)

        for cc in range(nc):
            pl.when(c == cc)(functools.partial(attention_grad, cc))

        dn1 = dot(wq[...], qkv[c]).astype(BF16).astype(F32)
        h32 = hbuf[c].astype(F32)
        pull1 = norm_pull(h32, inv_rms(h32), dn1).astype(BF16)

        @pl.when(late & jnp.logical_not(last))
        def _():
            f_copy(c).wait_send()

        ybuf[c] = (mbuf[c].astype(F32) + pull1.astype(F32)).astype(BF16)

        @pl.when(jnp.logical_not(first))
        def _():
            b_copy(c).start()

        for cc in range(1, nc):
            pl.when(c == cc)(functools.partial(earlier_keys, cc))

    @pl.when(last)
    def _():
        for k in range(1, nm):
            l_copy(k).wait_recv()
        vals = [losst[nm]] + [losst[k - 1] for k in range(1, nm)]
        tot = jnp.zeros_like(vals[0])
        for who in range(nm):
            pick = vals[0]
            for k in range(1, nm):
                pick = jnp.where(peer(k) == who, vals[k], pick)
            tot = tot + pick
        losst[nm + 1] = tot

    @pl.when(jnp.logical_not(last))
    def _():
        lf_copy().wait_recv()

    @pl.when(jnp.logical_not(first))
    def _():
        lf_copy().start()

    loss_out[...] = losst[nm + 1]

    def wgrad(mat, d):
        acc = None
        for c in range(nc):
            if mat == 0:
                part = dot_t(qkv[c, rowsl(d * qrows, qrows, qrows), :], n1buf[c])
            elif mat == 1:
                part = dot_t(obuf[c, rowsl(d * orows, orows, orows), :], mbuf[c])
            elif mat == 2:
                part = dot_t(n2buf[c], ubuf[c, rowsl(d * fl, fl, fl), :])
            else:
                part = dot_t(zbuf[c, rowsl(d * fl, fl, fl), :], dybuf[c])
            acc = part if acc is None else acc + part
        return acc

    sizes = (qrows, orows, dm_)
    offs = (0, qrows, qrows + orows)

    def rows_of(mat):
        return pl.ds(offs[mat], sizes[mat])

    def half_of(mat, half):
        return pl.ds(offs[mat] + half * (sizes[mat] // 2), sizes[mat] // 2)

    def far_copy(mat, half):
        rows = pl.ds(offs[mat] // 2, sizes[mat] // 2)
        return ring_copy(stage_buf.at[0, half_of(mat, half)], (far_p, far_m)[half].at[rows],
                         rs_send.at[mat, half], rs_recv.at[mat, half], half)

    def near_copy(mat, side, half):
        way = 2 + 2 * side + half
        return ring_copy(stage_buf.at[1 + side, half_of(mat, half)], (near_l if side == half else near_e).at[half_of(mat, half)],
                         rs_send.at[mat, way], rs_recv.at[mat, way], side)

    mats = (2, 0, 1)

    @pl.loop(0, 3)
    def _(slot):
        who = lax.rem(me + jnp.where(slot == 0, far, jnp.where(slot == 1, plus, minus)), nm)
        for mat in mats:
            stage_buf[slot, rows_of(mat)] = wgrad(mat, who)

            @pl.when(slot == 0)
            def _():
                for half in range(2):
                    far_copy(mat, half).start()

            for side in range(2):
                @pl.when(slot == 1 + side)
                def _():
                    near_copy(mat, side, 1 - side).start()

    @pl.when(dy_inside)
    def _():
        dy_forward(0)

    @pl.when(jnp.logical_not(late | dy_inside))
    def _():
        for c in reversed(range(nc)):
            dy_forward(c)

    hd2 = dm_ // 2

    def gd_cols(half):
        return pl.ds(half * hd2, hd2) if isinstance(half, int) else pl.ds(pl.multiple_of(half * hd2, hd2), hd2)

    def gd_half(d, half):
        return functools.reduce(jnp.add, [
            dot_t(zbuf[c, rowsl(d * fl, fl, fl), :], dybuf[c, gd_cols(half), :]) for c in range(nc)])

    def gd_far_copy(half):
        return ring_copy(gdacc.at[:, gd_cols(half)], gd_far.at[half], gd_send.at[half], gd_recv.at[half], half)

    def gd_slot(side, half):
        return folded(n_st - 1, (2 * side + half) * fl, fl)

    def gd_near_copy(side, half):
        way = 2 + 2 * side + half
        return ring_copy(gd_slot(side, half), gd_near.at[1 if side == half else 0, half],
                         gd_send.at[way], gd_recv.at[way], side)

    @pl.when(late)
    def _():
        @pl.loop(0, 2)
        def _(half):
            gdacc[:, gd_cols(half)] = gd_half(peer(far), half)

        for half in range(2):
            gd_far_copy(half).start()

        @pl.loop(0, 4)
        def _(n):
            rows, cols = lax.rem(n, 2) * fl, (n // 2) * tc
            stage_buf[n_st - 1, pl.ds(pl.multiple_of(rows, fl), fl), pl.ds(pl.multiple_of(cols, tc), tc)] = gd_half(
                lax.rem(me + 1 + 2 * (n // 2), nm), lax.rem(n, 2))

        for side in range(2):
            gd_near_copy(side, 1 - side).start()

    def gd_add(src, ref):
        nr = min(fl, radd.shape[0])
        for r in range(0, fl, nr):
            copy = pltpu.make_async_copy(src.at[pl.ds(r, nr)], radd.at[pl.ds(0, nr), pl.ds(0, hd2)], ld_sem.at[0])
            copy.start()
            copy.wait()
            ref[pl.ds(r, nr), :] += radd[pl.ds(0, nr), pl.ds(0, hd2)]

    pieces = [(mat, half) for mat in mats for half in range(2)]
    cols = dvacc.shape[2]
    n_cols = dm_ // cols

    def piece_loads(n, kind):
        mat, half = pieces[n]
        nr = sizes[mat] // 2
        r0 = sum(sizes[m] // 2 for m, _ in pieces[:n])
        src = near_e.at[half_of(mat, half)] if kind else (far_p, far_m)[half].at[pl.ds(offs[mat] // 2, nr)]
        dst = dkacc if kind else dvacc
        return [pltpu.make_async_copy(src.at[:, pl.ds(k * cols, cols)], dst.at[k, pl.ds(r0, nr), :], pl_sem.at[kind, n])
                for k in range(n_cols)], dst, r0, nr

    def piece_start(n, kind):
        mat, half = pieces[n]
        if kind:
            near_copy(mat, 1 - half, half).wait_recv()
        else:
            far_copy(mat, half).wait_recv()
        for copy in piece_loads(n, kind)[0]:
            copy.start()

    def piece_add(n, kind, slot):
        mat, half = pieces[n]
        copies, src, r0, nr = piece_loads(n, kind)
        for copy in copies:
            copy.wait()
        rows = half_of(mat, half)
        for k in range(n_cols):
            stage_buf[slot, rows, pl.ds(k * cols, cols)] += src[k, pl.ds(r0, nr), :]

    piece_start(0, 0)
    for n, (mat, half) in enumerate(pieces):
        if n + 1 < len(pieces):
            piece_start(n + 1, 0)
        piece_add(n, 0, 1 + half)
        near_copy(mat, half, half).start()

    @pl.when(late)
    def _():
        for half in range(2):
            gd_far_copy(half).wait_recv()
            gd_add(gd_far.at[half], gd_slot(half, half))
            gd_near_copy(half, half).start()
            gd_far_copy(half).wait_send()

    for mat in mats:
        for half in range(2):
            far_copy(mat, half).wait_send()
        stage_buf[0, rows_of(mat)] = wgrad(mat, me)

    def zdy_load(n, buf):
        slot, c = n // nc, lax.rem(n, nc)
        return (pltpu.make_async_copy(z_recv.at[slot, c], dsbuf.at[2 * buf, pl.ds(0, fl)], ld_sem.at[1 + buf]),
                pltpu.make_async_copy(dy_recv.at[slot, c], dsbuf.at[2 * buf + 1, pl.ds(0, dm_)], ld_sem.at[3 + buf]))

    gdacc[...] = wgrad(3, me)

    @pl.when(jnp.logical_not(late))
    def _():
        for c in range(nc):
            for way in (0, 1, 4, 5):
                z_copy(c, way).wait_recv()
            for way in (2, 3):
                dy_copy(c, way).wait_recv()
        for cp in zdy_load(0, 0):
            cp.start()

        @pl.loop(0, 3 * nc)
        def _(n):
            buf = lax.rem(n, 2)

            @pl.when(n + 1 < 3 * nc)
            def _():
                for cp in zdy_load(n + 1, 1 - buf):
                    cp.start()

            for cp in zdy_load(n, buf):
                cp.wait()
            gdacc[...] += dot_t(dsbuf[2 * buf, pl.ds(0, fl), :], dsbuf[2 * buf + 1, pl.ds(0, dm_), :])

    def gd_arrivals(last_half):
        for half in range(2):
            side = half if last_half else 1 - half
            gd_near_copy(side, half).wait_recv()
            gd_add(gd_near.at[last_half, half], gdacc.at[:, gd_cols(half)])

    def out_copy(mat):
        if mat == 3:
            return pltpu.make_async_copy(gdacc, sum_out.at[pl.ds(qrows + orows + dm_, fl)], out_sem.at[3])
        return pltpu.make_async_copy(stage_buf.at[0, rows_of(mat)], sum_out.at[rows_of(mat)], out_sem.at[mat])

    piece_start(0, 1)
    for n, (mat, half) in enumerate(pieces):
        if n + 1 < len(pieces):
            piece_start(n + 1, 1)
        piece_add(n, 1, 0)
        if half:
            out_copy(mat).start()

    @pl.when(late)
    def _():
        gd_arrivals(0)
        gd_arrivals(1)

    out_copy(3).start()
    for mat in mats:
        for side in range(2):
            near_copy(mat, side, side).wait_recv()

    for mat in range(4):
        out_copy(mat).wait()

    @pl.when(jnp.logical_not(late))
    def _():
        for c in range(nc):
            for way in range(6):
                z_copy(c, way).wait_send()
            for way in range(4):
                dy_copy(c, way).wait_send()

    @pl.when(late)
    def _():
        for side in range(2):
            for half in range(2):
                gd_near_copy(side, half).wait_send()

    for idx in range(4):
        for way in range(4):
            w_copy(idx, way).wait_send()
    for mat in mats:
        for half in range(2):
            for side in range(2):
                near_copy(mat, side, half).wait_send()

    @pl.when(jnp.logical_not(first))
    def _():
        for c in range(nc):
            b_copy(c).wait_send()
        lf_copy().wait_send()

    @pl.when(last)
    def _():
        for k in range(1, nm):
            l_copy(k).wait_send()


def finish_kernel(sq, so, su, sd, lq, lo, lu, loss, gq, go, gu, gd, loss_out):
    gq[...] = sq[...] + lq[...]
    go[...] = so[...] + lo[...]
    gu[...] = su[...] + lu[...]
    gd[...] = sd[...]
    loss_out[0] = loss[0, 0]


def solution(mesh):
    ns = mesh.shape["stage"]
    nm = mesh.shape["model"]

    def per_device(tokens_in, targets, w_qkv, w_out, w_up, w_down):
        n_micro, seq_len, d_model = tokens_in.shape
        hl, hd, fl = w_qkv.shape[3], w_qkv.shape[5], w_up.shape[3]
        tc = min(CHUNK, seq_len // 2)
        nc = seq_len // tc
        qrows, orows = hl * 3 * hd, hl * hd
        assert n_micro == nm == 4 and w_qkv.shape[1] == 1 and hl == 2 and d_model == 2 * tc and qrows + orows + d_model == seq_len == 2 * fl and nc == 4
        wqT = jnp.transpose(w_qkv[0, 0], (1, 2, 3, 0)).reshape(qrows, d_model)
        wo = w_out[0, 0].reshape(orows, d_model)
        wu, wd = w_up[0, 0], w_down[0, 0]
        cfg = (ns, nm, nc, tc, d_model, hl, hd, fl)
        heads = nm * hl
        any_spec = pl.BlockSpec(memory_space=pl.ANY)
        f32 = lambda *shape: jax.ShapeDtypeStruct(shape, F32)
        rsum = qrows + orows + d_model
        seqb = nc * tc
        b16 = lambda *shape: jax.ShapeDtypeStruct(shape, BF16)
        out_shape = (f32(rsum + fl, d_model), f32(8, 128), f32(rsum // 2, d_model), f32(rsum // 2, d_model), f32(rsum, d_model),
                     f32(rsum, d_model), b16(3, nc, fl, tc), b16(2, nc, fl // 2, tc), b16(3, nc, d_model, tc),
                     f32(2, fl, d_model // 2), f32(2, 2, fl, d_model // 2))
        vb = lambda *shape: pltpu.VMEM(shape, BF16)
        vf = lambda *shape: pltpu.VMEM(shape, F32)
        dma = lambda *shape: pltpu.SemaphoreType.DMA(shape)
        scratch = [
            vb(nm * qrows, d_model), vb(d_model, nm * orows), vb(nm * fl, d_model), vb(d_model, nm * fl),
            vb(nm * fl, d_model), vb(d_model, nm * fl), vb(nm * orows, d_model), vb(d_model, nm * qrows),
            vb(nc, tc, d_model), vb(nc, d_model, tc), vb(nc, d_model, tc), vb(nc, nm * qrows, tc), vb(nm, seqb, orows), vb(nm, seqb, orows),
            vb(nc, nm * orows, tc), vb(nc, d_model, tc), vb(nc, d_model, tc), vb(nc, nm * fl, tc), vb(nc, nm * fl, tc),
            vb(nc * (nc + 1) // 2, heads, tc, tc), vb(nc, d_model, tc), vf(heads // 2, seqb, 2 * hd), vf(heads // 2, seqb, 2 * hd),
            vb(nc, d_model, tc), vb(nm * orows, tc), vf(nm + 2, 8, 128), vf(8, tc),
            vf(4, rsum, d_model), vf(256, d_model), vf(fl, d_model), vb(heads, max((nc - 1) * tc, fl), tc), vb(nm * orows, tc),
            dma(4, 4), dma(4, 4), dma(4), pltpu.SemaphoreType.REGULAR, dma(nc), dma(nc), dma(nc), dma(nc), dma(nc),
            dma(nm - 1), dma(nm - 1), pltpu.SemaphoreType.DMA, pltpu.SemaphoreType.DMA,
            dma(3, 6), dma(3, 6), dma(5), dma(4), dma(6, nc), dma(6, nc), dma(4, nc), dma(4, nc), dma(6), dma(6), dma(2, 6),
        ]
        res = pl.pallas_call(
            functools.partial(step_kernel, cfg),
            out_shape=out_shape,
            in_specs=[any_spec] * 6,
            out_specs=[any_spec, pl.BlockSpec(memory_space=pltpu.VMEM)] + [any_spec] * 9,
            scratch_shapes=scratch,
            compiler_params=pltpu.CompilerParams(collective_id=0, has_side_effects=True, vmem_limit_bytes=67043328),
            name="train_step",
        )(tokens_in, targets, wqT, wo, wu, wd)
        part, loss, late = res[0], res[1], res[5]
        steps = 2

        def spec(size, start):
            rows = size // steps
            return pl.BlockSpec((rows, d_model), lambda i: (start // rows + i, 0))

        q_s, o_s, u_s = spec(qrows, 0), spec(orows, qrows), spec(d_model, qrows + orows)
        g_qkv, g_out, g_up, g_down, loss = pl.pallas_call(
            finish_kernel,
            grid=(steps,),
            out_shape=(f32(qrows, d_model), f32(orows, d_model), f32(d_model, fl), f32(fl, d_model), f32(1)),
            in_specs=[q_s, o_s, u_s, spec(fl, rsum), q_s, o_s, u_s, pl.BlockSpec(memory_space=pltpu.SMEM)],
            out_specs=[spec(qrows, 0), spec(orows, 0), spec(d_model, 0), spec(fl, 0), pl.BlockSpec(memory_space=pltpu.SMEM)],
            name="finish",
        )(part, part, part, part, late, late, late, loss)
        g_qkv = jnp.transpose(g_qkv.reshape(hl, 3, hd, d_model), (3, 0, 1, 2))[None, None]
        return g_qkv, g_out.reshape(1, 1, hl, hd, d_model), g_up[None, None], g_down[None, None], loss

    tok_spec = P(None, "data", None)
    qkv_spec = P("stage", None, None, "model", None, None)
    out_spec = P("stage", None, "model", None, None)
    up_spec = P("stage", None, None, "model")
    down_spec = P("stage", None, "model", None)
    g_qkv_spec = P(("data", "stage"), None, None, "model", None, None)
    g_out_spec = P(("data", "stage"), None, "model", None, None)
    g_up_spec = P(("data", "stage"), None, None, "model")
    g_down_spec = P(("data", "stage"), None, "model", None)
    return jax.shard_map(per_device, mesh=mesh, in_specs=(tok_spec, tok_spec, qkv_spec, out_spec, up_spec, down_spec), out_specs=(g_qkv_spec, g_out_spec, g_up_spec, g_down_spec, P("data")), check_vma=False)
```
